32 devices in a mesh: dp: 1 (over z), tp: 4 (over y), pp: 8 (over x, core).
Axes of the slice: x: 4, y: 4, z: 1, core: 2. Of those that a mesh axis runs over, the one named last changes fastest.
The devices are a block of a 4x4x8 slice.
Arguments:
- x_in: bfloat16 [4, 1, 1024, 1024], P('dp')
- seq_lens: int32 [4, 1], P('dp')
- ln1_gain: bfloat16 [8, 1024], P('pp')
- ln1_shift: bfloat16 [8, 1024], P('pp')
- w_qkv: bfloat16 [8, 1024, 3, 1024], P('pp', None, None, 'tp')
- b_qkv: bfloat16 [8, 3, 16, 64], P('pp', None, 'tp')
- w_out: bfloat16 [8, 1024, 1024], P('pp', 'tp')
- b_out: bfloat16 [8, 1024], P('pp')
- ln2_gain: bfloat16 [8, 1024], P('pp')
- ln2_shift: bfloat16 [8, 1024], P('pp')
- w_up: bfloat16 [8, 1024, 4096], P('pp', None, 'tp')
- b_up: bfloat16 [8, 4096], P('pp', 'tp')
- w_down: bfloat16 [8, 4096, 1024], P('pp', 'tp')
- b_down: bfloat16 [8, 1024], P('pp')
Outputs:
- output: bfloat16 [8, 4, 1, 1024, 1024], P('pp', 'dp')
All inputs are finite; a program needn't handle non-finite values.
Results may differ from the reference program's by a relative error of at most 0.02.
Values are sent between devices in bfloat16 or wider.
A program may use at most 768 MiB of HBM per device.

```python
import jax
import jax.numpy as jnp
from jax import lax
import math

LAYERS = 8
MICRO_COUNT = 4
BATCH_SIZE = 1
SEQ_LEN = 1024
MODEL_DIM = 1024
NUM_HEADS = 16
HIDDEN_DIM = 4096
HEAD_DIM = MODEL_DIM // NUM_HEADS


def alibi_slopes(heads_n):
    closest = 2 ** int(math.floor(math.log2(heads_n)))
    base_rate = 2.0 ** (-8.0 / closest)
    slope_list = [base_rate ** (head_idx + 1) for head_idx in range(closest)]
    extra_rate = 2.0 ** (-4.0 / closest)
    slope_list = slope_list + [extra_rate ** (2 * head_idx + 1) for head_idx in range(min(closest, heads_n - closest))]
    return jnp.array(slope_list, dtype=jnp.float32)


def layer_norm(values, gain_vec, shift_vec):
    val_f = values.astype(jnp.float32)
    mean_val = jnp.mean(val_f, axis=-1, keepdims=True)
    centered = val_f - mean_val
    var_val = jnp.mean(centered * centered, axis=-1, keepdims=True)
    normed = centered * lax.rsqrt(var_val + 1e-5)
    return (normed * gain_vec.astype(jnp.float32) + shift_vec.astype(jnp.float32)).astype(jnp.bfloat16)


def attention(query_all, key_all, val_all, slopes, lens_row):
    batch_n, seq_n, heads_n, head_dim = query_all.shape
    blk_len = min(seq_n, 128)
    key_pos = jnp.arange(seq_n)
    key_ok = key_pos[None, :] < lens_row[:, None]
    key_f = key_all.astype(jnp.float32)
    val_f = val_all.astype(jnp.float32)

    def one_block(blk_idx):
        query_blk = lax.dynamic_slice_in_dim(query_all, blk_idx * blk_len, blk_len, 1).astype(jnp.float32)
        scores = jnp.einsum('bqhe,bkhe->bhqk', query_blk, key_f) * (head_dim ** -0.5)
        query_pos = blk_idx * blk_len + jnp.arange(blk_len)
        distance = (query_pos[:, None] - key_pos[None, :]).astype(jnp.float32)
        scores = scores - slopes[None, :, None, None] * distance[None, None]
        allowed = (key_pos[None, :] <= query_pos[:, None])[None, None] & key_ok[:, None, None, :]
        scores = jnp.where(allowed, scores, -1e30)
        prob_bf = jax.nn.softmax(scores, axis=-1).astype(jnp.bfloat16)
        return jnp.einsum('bhqk,bkhe->bqhe', prob_bf.astype(jnp.float32), val_f).astype(jnp.bfloat16)

    blocks = lax.map(one_block, jnp.arange(seq_n // blk_len))
    return jnp.moveaxis(blocks, 0, 1).reshape(batch_n, seq_n, heads_n * head_dim)


def bloom_layer(act_in, lens_row, layer_w, slopes):
    ln1_gain, ln1_shift, w_qkv, b_qkv, w_out, b_out, ln2_gain, ln2_shift, w_up, b_up, w_down, b_down = layer_w
    batch_n, seq_n, model_n = act_in.shape
    tokens_n = batch_n * seq_n
    heads_n, head_dim = b_qkv.shape[1], b_qkv.shape[2]
    flat_in = act_in.reshape(tokens_n, model_n)
    normed = layer_norm(flat_in, ln1_gain, ln1_shift)
    qkv_all = (jnp.dot(normed, w_qkv.reshape(model_n, 3 * model_n), preferred_element_type=jnp.float32) + b_qkv.reshape(3 * model_n).astype(jnp.float32)).astype(jnp.bfloat16)
    qkv_all = qkv_all.reshape(batch_n, seq_n, 3, heads_n, head_dim)
    context = attention(qkv_all[:, :, 0], qkv_all[:, :, 1], qkv_all[:, :, 2], slopes, lens_row)
    attn_out = jnp.dot(context.reshape(tokens_n, model_n), w_out, preferred_element_type=jnp.float32)
    resid_act = (flat_in.astype(jnp.float32) + attn_out + b_out.astype(jnp.float32)).astype(jnp.bfloat16)
    normed_mlp = layer_norm(resid_act, ln2_gain, ln2_shift)
    hidden_act = jax.nn.gelu(jnp.dot(normed_mlp, w_up, preferred_element_type=jnp.float32) + b_up.astype(jnp.float32), approximate=True).astype(jnp.bfloat16)
    mlp_out = jnp.dot(hidden_act, w_down, preferred_element_type=jnp.float32)
    result = (resid_act.astype(jnp.float32) + mlp_out + b_down.astype(jnp.float32)).astype(jnp.bfloat16)
    return result.reshape(batch_n, seq_n, model_n)


def setup_inputs(seed: int = 0, part: int = 0) -> dict:
    w_keys = jax.random.split(jax.random.key(seed), 12)
    part_keys = jax.random.split(jax.random.fold_in(jax.random.key(seed + 1), part), 2)

    def normal_draw(rng_key, arr_shape, std_dev, offset):
        return (offset + std_dev * jax.random.normal(rng_key, arr_shape, jnp.float32)).astype(jnp.bfloat16)

    width_scale = MODEL_DIM ** -0.5
    lens_draw = jax.random.randint(part_keys[1], (MICRO_COUNT, BATCH_SIZE), 1, SEQ_LEN + 1, dtype=jnp.int32)
    return dict(
        x_in=normal_draw(part_keys[0], (MICRO_COUNT, BATCH_SIZE, SEQ_LEN, MODEL_DIM), 1.0, 0.0),
        seq_lens=lens_draw.at[0, 0].set(SEQ_LEN),
        ln1_gain=normal_draw(w_keys[0], (LAYERS, MODEL_DIM), 0.3, 1.0),
        ln1_shift=normal_draw(w_keys[1], (LAYERS, MODEL_DIM), 0.3, 0.0),
        w_qkv=normal_draw(w_keys[2], (LAYERS, MODEL_DIM, 3, MODEL_DIM), width_scale, 0.0),
        b_qkv=normal_draw(w_keys[3], (LAYERS, 3, NUM_HEADS, HEAD_DIM), 0.3, 0.0),
        w_out=normal_draw(w_keys[4], (LAYERS, MODEL_DIM, MODEL_DIM), width_scale, 0.0),
        b_out=normal_draw(w_keys[5], (LAYERS, MODEL_DIM), 0.3, 0.0),
        ln2_gain=normal_draw(w_keys[6], (LAYERS, MODEL_DIM), 0.3, 1.0),
        ln2_shift=normal_draw(w_keys[7], (LAYERS, MODEL_DIM), 0.3, 0.0),
        w_up=normal_draw(w_keys[8], (LAYERS, MODEL_DIM, HIDDEN_DIM), width_scale, 0.0),
        b_up=normal_draw(w_keys[9], (LAYERS, HIDDEN_DIM), 0.3, 0.0),
        w_down=normal_draw(w_keys[10], (LAYERS, HIDDEN_DIM, MODEL_DIM), HIDDEN_DIM ** -0.5, 0.0),
        b_down=normal_draw(w_keys[11], (LAYERS, MODEL_DIM), 0.3, 0.0),
    )


def reference(x_in, seq_lens, ln1_gain, ln1_shift, w_qkv, b_qkv, w_out, b_out, ln2_gain, ln2_shift, w_up, b_up, w_down, b_down):
    slopes = alibi_slopes(NUM_HEADS)

    def layer_step(current, layer_w):
        new_act = lax.map(lambda micro_pair: bloom_layer(micro_pair[0], micro_pair[1], layer_w, slopes), (current, seq_lens))
        return new_act, new_act

    final_act, hidden = lax.scan(layer_step, x_in, (ln1_gain, ln1_shift, w_qkv, b_qkv, w_out, b_out, ln2_gain, ln2_shift, w_up, b_up, w_down, b_down))
    return hidden
```

```python
import functools
import math

import jax
import jax.numpy as jnp
import numpy as np
from jax import lax
from jax.experimental import pallas as pl
from jax.experimental.pallas import tpu as pltpu
from jax.sharding import PartitionSpec as P

MESH = pl.DeviceIdType.MESH
UNIT = 128
KBLK = 256
LAG = 3
NEG = -1e30


def alibi_slopes(heads_n):
    closest = 2 ** int(math.floor(math.log2(heads_n)))
    base_rate = 2.0 ** (-8.0 / closest)
    slope_list = [base_rate ** (head_idx + 1) for head_idx in range(closest)]
    extra_rate = 2.0 ** (-4.0 / closest)
    slope_list = slope_list + [extra_rate ** (2 * head_idx + 1) for head_idx in range(min(closest, heads_n - closest))]
    return np.array(slope_list, dtype=np.float32)


def split_bf16(value):
    parts = []
    rest = np.float32(value)
    for _ in range(3):
        part = rest.astype(jnp.bfloat16).astype(np.float32)
        parts.append(float(part))
        rest = np.float32(rest - part)
    return parts


def layer_norm(x, gain, shift):
    mean = jnp.mean(x, axis=-1, keepdims=True)
    cent = x - mean
    var = jnp.mean(cent * cent, axis=-1, keepdims=True)
    return (cent * lax.rsqrt(var + 1e-5) * gain + shift).astype(jnp.bfloat16)


def gelu(x):
    inner = math.sqrt(2.0 / math.pi) * (x + 0.044715 * (x * x * x))
    return 0.5 * x * (1.0 + jnp.tanh(inner))


def kernel(heads_n, x_hbm, lens, wqkv_in, wout_in, wup_in, wdn_in, pack_in, out,
           wqkv, wout, wup, wdn, packs, rl_qkv, rl_out, rl_up, rl_dn,
           xbuf, ybuf, kc, vt, kx, qaug, cmask, sbuf, abuf, ctx, hbuf, ubuf,
           loc_sem, w_recv, fwd_send, rl_send, rl_recv, dir_send, pk_send,
           x0_sem, x_recv, s_send, od_send, da_send, db_send, fa_send, fb_send,
           rr_recv, rr_send, o_recv):
    tp_n = 4
    units = xbuf.shape[0]
    model = xbuf.shape[2]
    seq = units * UNIT
    quarter = wqkv.shape[3]
    hid_q = wup.shape[2]
    pairs = model // 128

    r = lax.axis_index("tp")
    p = lax.axis_index("pp")
    x = p // 2
    c = p % 2
    odd = (r + x) % 2
    layer = 2 * x + odd
    home = odd == c
    rp, rm, ro = (r + 1) % tp_n, (r + 3) % tp_n, (r + 2) % tp_n
    partner = 2 * x + (1 - c)
    sig = 1 - 2 * c
    r_fwd = (r + sig + tp_n) % tp_n
    r_bwd = (r - sig + tp_n) % tp_n
    stage0, stage1 = 2 * x, 2 * x + 1
    x_n = 4

    def micro_of(row, core, lay):
        hops = (lay + 1) // 2
        return 2 * (((row + 8 - (1 - 2 * core) * hops) % tp_n) // 2) + core

    m = micro_of(r, c, layer)

    def rcopy(src, dst, ssem, rsem, **dev):
        return pltpu.make_async_remote_copy(src_ref=src, dst_ref=dst, send_sem=ssem, recv_sem=rsem,
                                            device_id=dev, device_id_type=MESH)

    barrier = pltpu.get_barrier_semaphore()
    for dr in range(tp_n):
        for dc in range(2):
            if dr or dc:
                pl.semaphore_signal(barrier, inc=1, device_id={"tp": (r + dr) % tp_n, "pp": 2 * x + (c + dc) % 2}, device_id_type=MESH)
    for dx in (1, x_n - 1):
        pl.semaphore_signal(barrier, inc=1, device_id={"pp": 2 * ((x + dx) % x_n) + c}, device_id_type=MESH)
    pl.semaphore_wait(barrier, 9)

    def wsrc(k, h=None):
        if k == 0:
            return wqkv_in if h is None else wqkv_in.at[:, pl.ds(h * (model // 2), model // 2), :]
        ref = (None, wout_in, wup_in, wdn_in, pack_in)[k]
        if h is None:
            return ref
        half = ref.shape[0] // 2
        return ref.at[pl.ds(h * half, half)]

    def wdst(k, q, h=None):
        if k == 0:
            return wqkv.at[q] if h is None else wqkv.at[q, :, pl.ds(h * (model // 2), model // 2), :]
        if k == 2:
            return wup.at[q] if h is None else wup.at[q, pl.ds(h * (model // 2), model // 2)]
        if k == 4:
            return packs.at[q]
        ref, rows = (wout, quarter) if k == 1 else (wdn, hid_q)
        if h is None:
            return ref.at[pl.ds(pl.multiple_of(q * rows, rows), rows)]
        half = rows // 2
        return ref.at[pl.ds(pl.multiple_of(q * rows + h * half, half), half)]

    def rl(k, h):
        return (rl_qkv, rl_out, rl_up, rl_dn)[k].at[h]

    def wwait(view, sem):
        rcopy(view, view, sem, sem, pp=partner).wait_recv()

    @pl.when(home)
    def _():
        rcopy(wsrc(4), wdst(4, r), pk_send.at[0], w_recv.at[2, 4, 0], tp=ro).start()
        for k in range(4):
            rcopy(wsrc(k, 0), rl(k, 0), rl_send.at[0, k], rl_recv.at[0, k], tp=rp).start()
            rcopy(wsrc(k, 1), rl(k, 1), rl_send.at[1, k], rl_recv.at[1, k], tp=rm).start()
        for k in range(5):
            pltpu.make_async_copy(wsrc(k), wdst(k, r), loc_sem.at[k]).start()
            rcopy(wsrc(k), wdst(k, r), fwd_send.at[k], w_recv.at[0, k, 0], pp=partner).start()

    @pl.when(jnp.logical_not(home))
    def _():
        for k in (4, 0, 1, 2, 3):
            rcopy(wsrc(k), wdst(k, r), dir_send.at[0, k], w_recv.at[3, k, 0], tp=rp).start()
            rcopy(wsrc(k), wdst(k, r), dir_send.at[1, k], w_recv.at[1, k, 0], tp=rm).start()

    @pl.when(layer == 0)
    def _():
        for u in range(units):
            pltpu.make_async_copy(x_hbm.at[m, pl.ds(u * UNIT, UNIT)], xbuf.at[u], x0_sem.at[u]).start()

    kc[...] = jnp.zeros_like(kc)
    vt[...] = jnp.zeros_like(vt)
    length = lens[m]
    key = lax.broadcasted_iota(jnp.int32, (seq, 128), 0)
    lane = lax.broadcasted_iota(jnp.int32, (seq, 128), 1)
    high = (key // 256) * 256
    part = jnp.where(lane % 2 == 0, high, key - high).astype(jnp.float32)
    dead = jnp.where(key >= length, NEG, 0.0)
    kx[...] = jnp.where(lane < 6, part, jnp.where(lane == 6, dead, 0.0)).astype(jnp.bfloat16)
    slopes = alibi_slopes(heads_n)
    row = lax.broadcasted_iota(jnp.int32, (128, 256), 0)
    second = lax.broadcasted_iota(jnp.int32, (128, 256), 1) >= 128
    for pair in range(pairs):
        (h0, m0, l0), (h1, m1, l1) = split_bf16(slopes[2 * pair]), split_bf16(slopes[2 * pair + 1])
        hi, mid, low = jnp.where(second, h1, h0), jnp.where(second, m1, m0), jnp.where(second, l1, l0)
        val = jnp.where(row < 2, hi, jnp.where(row < 4, mid, jnp.where(row < 6, low, jnp.where(row == 6, 1.0, 0.0))))
        qaug[pair, 128:, :] = val.astype(jnp.bfloat16)
    kpos = lax.broadcasted_iota(jnp.int32, (KBLK, 256), 0)
    qpos = lax.broadcasted_iota(jnp.int32, (KBLK, 256), 1) % 128
    cmask[0] = jnp.where(kpos <= qpos, 0.0, NEG)
    cmask[1] = jnp.where(kpos <= qpos + 128, 0.0, NEG)

    @pl.when(home)
    def _():
        idx = 5
        for k in (4, 0, 1, 2, 3):
            for d, q in ((1, rp), (3, rm)):
                wwait(wdst(k, q), w_recv.at[d, k, 0])
                rcopy(wdst(k, q), wdst(k, q), fwd_send.at[idx], w_recv.at[d, k, 0], pp=partner).start()
                idx += 1
        wwait(wdst(4, ro), w_recv.at[2, 4, 0])
        rcopy(wdst(4, ro), wdst(4, ro), fwd_send.at[idx], w_recv.at[2, 4, 0], pp=partner).start()
        idx += 1
        for k in range(4):
            for h in range(2):
                wwait(wdst(k, ro, h), w_recv.at[2, k, h])
                rcopy(wdst(k, ro, h), wdst(k, ro, h), fwd_send.at[idx], w_recv.at[2, k, h], pp=partner).start()
                idx += 1
        for k in range(5):
            pltpu.make_async_copy(wsrc(k), wdst(k, r), loc_sem.at[k]).wait()

    @pl.when(jnp.logical_not(home))
    def _():
        for k in range(4):
            wwait(rl(k, 0), rl_recv.at[0, k])
            rcopy(rl(k, 0), wdst(k, rm, 0), rl_send.at[0, k], w_recv.at[2, k, 0], tp=rp).start()
            wwait(rl(k, 1), rl_recv.at[1, k])
            rcopy(rl(k, 1), wdst(k, rp, 1), rl_send.at[1, k], w_recv.at[2, k, 1], tp=rm).start()
        for k in range(5):
            for d, q in ((0, r), (1, rp), (3, rm)):
                wwait(wdst(k, q), w_recv.at[d, k, 0])
        wwait(wdst(4, ro), w_recv.at[2, 4, 0])
        for k in range(4):
            for h in range(2):
                wwait(wdst(k, ro, h), w_recv.at[2, k, h])

    def out_at(mm, u):
        return out.at[mm, pl.ds(pl.multiple_of(u * UNIT, UNIT), UNIT)]

    m_a = micro_of(rm, 0, stage1)
    m_b = micro_of(rp, 1, stage1)
    relay = jnp.logical_and(odd == 0, c == 1)

    def relay_unit(v):
        wwait(out_at(m_a, v), rr_recv.at[0, v])
        rcopy(out_at(m_a, v), out_at(m_a, v), rr_send.at[0, v], o_recv, tp=rp).start()
        wwait(out_at(m_b, v), rr_recv.at[1, v])
        rcopy(out_at(m_b, v), out_at(m_b, v), rr_send.at[1, v], o_recv, tp=rm).start()

    def attention(nb, diag):
        def one_pair(pair, carry):
            col = pl.ds(pl.multiple_of(pair * 128, 128), 128)
            q_rhs = qaug[pair]
            top = None
            for b in range(nb):
                keys = jnp.concatenate([kc[b * KBLK:(b + 1) * KBLK, col], kx[b * KBLK:(b + 1) * KBLK, :]], axis=1)
                s = jnp.dot(keys, q_rhs, preferred_element_type=jnp.float32)
                if b == nb - 1:
                    s = s + diag
                sbuf[b] = s
                peak = jnp.max(s, axis=0, keepdims=True)
                top = peak if top is None else jnp.maximum(top, peak)
            total = None
            acc = None
            for b in range(nb):
                e = jnp.exp(sbuf[b] - top)
                part_sum = jnp.sum(e, axis=0, keepdims=True)
                total = part_sum if total is None else total + part_sum
                pv = jnp.dot(vt[col, b * KBLK:(b + 1) * KBLK], e.astype(jnp.bfloat16), preferred_element_type=jnp.float32)
                acc = pv if acc is None else acc + pv
            acc = acc * (1.0 / total)
            both = jnp.concatenate([acc[:64, :128], acc[64:, 128:]], axis=0)
            ctx[:, col] = both.T.astype(jnp.bfloat16)
            return carry

        lax.fori_loop(0, pairs, one_pair, 0, unroll=2)

    def unit_step(u, carry):
        tok = pl.ds(pl.multiple_of(u * UNIT, UNIT), UNIT)

        @pl.when(layer == 0)
        def _():
            pltpu.make_async_copy(x_hbm.at[m, tok], xbuf.at[u], x0_sem.at[u]).wait()

        @pl.when(layer > 0)
        def _():
            wwait(xbuf.at[u], x_recv.at[u])

        @pl.when(odd == 1)
        def _():
            @pl.when(c == 0)
            def _():
                pltpu.make_async_copy(xbuf.at[u], out_at(m, u), o_recv).start()

            @pl.when(c == 1)
            def _():
                rcopy(xbuf.at[u], out_at(m, u), fa_send.at[u], o_recv, pp=stage0).start()

            rcopy(xbuf.at[u], out_at(m, u), fb_send.at[u], o_recv, tp=r_fwd, pp=stage0).start()

        xin = xbuf[u].astype(jnp.float32)
        abuf[...] = layer_norm(xin, packs[0, 0:1, :], packs[0, 1:2, :])
        head_row = lax.broadcasted_iota(jnp.int32, (128, 128), 0) < 64
        for q in range(tp_n):
            for j in range(3):
                o = jnp.dot(abuf[...], wqkv[q, j], preferred_element_type=jnp.float32)
                o = (o + packs[q, 7:8, j * quarter:(j + 1) * quarter]).astype(jnp.bfloat16)
                if j == 0:
                    o = o.astype(jnp.float32) * 0.125
                    for half in range(quarter // 128):
                        q_t = o[:, half * 128:(half + 1) * 128].T
                        pair = q * (quarter // 128) + half
                        qaug[pair, :128, :128] = jnp.where(head_row, q_t, 0.0).astype(jnp.bfloat16)
                        qaug[pair, :128, 128:] = jnp.where(head_row, 0.0, q_t).astype(jnp.bfloat16)
                elif j == 1:
                    kc[tok, q * quarter:(q + 1) * quarter] = o
                else:
                    vt[q * quarter:(q + 1) * quarter, tok] = o.astype(jnp.float32).T.astype(jnp.bfloat16)

        for nb in range(1, seq // KBLK + 1):
            @pl.when(u // 2 + 1 == nb)
            def _():
                attention(nb, cmask[u % 2])

        for n in range(model // quarter):
            cols = slice(n * quarter, (n + 1) * quarter)
            attn = jnp.dot(ctx[...], wout[:, cols], preferred_element_type=jnp.float32)
            hbuf[:, cols] = (xbuf[u, :, cols].astype(jnp.float32) + attn + packs[0, 2:3, cols]).astype(jnp.bfloat16)
        abuf[...] = layer_norm(hbuf[...].astype(jnp.float32), packs[0, 3:4, :], packs[0, 4:5, :])
        for q in range(tp_n):
            for n in range(hid_q // quarter):
                cols = slice(n * quarter, (n + 1) * quarter)
                up = jnp.dot(abuf[...], wup[q, :, cols], preferred_element_type=jnp.float32)
                up = up + packs[q, 6:7, cols]
                ubuf[:, q * hid_q + n * quarter:q * hid_q + (n + 1) * quarter] = gelu(up).astype(jnp.bfloat16)
        for n in range(model // quarter):
            cols = slice(n * quarter, (n + 1) * quarter)
            down = jnp.dot(ubuf[...], wdn[:, cols], preferred_element_type=jnp.float32)
            ybuf[u, :, cols] = (hbuf[:, cols].astype(jnp.float32) + down + packs[0, 5:6, cols]).astype(jnp.bfloat16)

        @pl.when(odd == 0)
        def _():
            rcopy(ybuf.at[u], xbuf.at[u], s_send.at[u], x_recv.at[u], tp=r_fwd).start()
            rcopy(ybuf.at[u], out_at(m, u), da_send.at[u], o_recv, tp=r_bwd, pp=stage0).start()

            @pl.when(c == 0)
            def _():
                pltpu.make_async_copy(ybuf.at[u], out_at(m, u), o_recv).start()

            @pl.when(c == 1)
            def _():
                rcopy(ybuf.at[u], out_at(m, u), od_send.at[u], o_recv, pp=stage0).start()

        @pl.when(odd == 1)
        def _():
            @pl.when(x < x_n - 1)
            def _():
                rcopy(ybuf.at[u], xbuf.at[u], s_send.at[u], x_recv.at[u], pp=(p + 2) % (2 * x_n)).start()

            rcopy(ybuf.at[u], out_at(m, u), da_send.at[u], rr_recv.at[c, u], tp=r_fwd, pp=stage1).start()
            rcopy(ybuf.at[u], out_at(m, u), db_send.at[u], o_recv, tp=r_bwd, pp=stage1).start()

            @pl.when(c == 1)
            def _():
                pltpu.make_async_copy(ybuf.at[u], out_at(m, u), o_recv).start()

            @pl.when(c == 0)
            def _():
                rcopy(ybuf.at[u], out_at(m, u), od_send.at[u], o_recv, pp=stage1).start()

        @pl.when(jnp.logical_and(relay, u >= LAG))
        def _():
            relay_unit(u - LAG)

        return carry

    lax.fori_loop(0, units, unit_step, 0)

    @pl.when(relay)
    def _():
        for v in range(max(0, units - LAG), units):
            relay_unit(v)

    def sent(view, sem):
        rcopy(view, view, sem, sem, pp=partner).wait_send()

    @pl.when(home)
    def _():
        sent(wsrc(4), pk_send.at[0])
        for k in range(4):
            sent(rl(k, 0), rl_send.at[0, k])
            sent(rl(k, 1), rl_send.at[1, k])
        for k in range(5):
            sent(wsrc(k), fwd_send.at[k])
        idx = 5
        for k in (4, 0, 1, 2, 3):
            for d in range(2):
                sent(wsrc(k), fwd_send.at[idx])
                idx += 1
        sent(wsrc(4), fwd_send.at[idx])
        idx += 1
        for k in range(4):
            for h in range(2):
                sent(wsrc(k, h), fwd_send.at[idx])
                idx += 1

    @pl.when(jnp.logical_not(home))
    def _():
        for k in range(5):
            for d in range(2):
                sent(wsrc(k), dir_send.at[d, k])
        for k in range(4):
            for d in range(2):
                sent(rl(k, d), rl_send.at[d, k])

    def drain(u, carry):
        @pl.when(odd == 0)
        def _():
            sent(ybuf.at[u], s_send.at[u])
            sent(ybuf.at[u], da_send.at[u])

            @pl.when(c == 1)
            def _():
                sent(ybuf.at[u], od_send.at[u])
                sent(ybuf.at[u], rr_send.at[0, u])
                sent(ybuf.at[u], rr_send.at[1, u])

        @pl.when(odd == 1)
        def _():
            @pl.when(x < x_n - 1)
            def _():
                sent(ybuf.at[u], s_send.at[u])

            sent(ybuf.at[u], da_send.at[u])
            sent(ybuf.at[u], db_send.at[u])
            sent(ybuf.at[u], fb_send.at[u])

            @pl.when(c == 0)
            def _():
                sent(ybuf.at[u], od_send.at[u])

            @pl.when(c == 1)
            def _():
                sent(ybuf.at[u], fa_send.at[u])

        return carry

    lax.fori_loop(0, units, drain, 0)

    @pl.when(relay)
    def _():
        wwait(out.at[pl.ds(0, out.shape[0] // 2)], o_recv)

    @pl.when(jnp.logical_not(relay))
    def _():
        wwait(out, o_recv)


def solution(mesh):
    tp_size = mesh.shape['tp']
    in_specs = (P('dp'), P('dp'), P('pp'), P('pp'), P('pp', None, None, 'tp'), P('pp', None, 'tp', None), P('pp', 'tp', None), P('pp'), P('pp'), P('pp'), P('pp', None, 'tp'), P('pp', 'tp'), P('pp', 'tp', None), P('pp'))

    def per_device(x_in, seq_lens, ln1_gain, ln1_shift, w_qkv, b_qkv, w_out, b_out, ln2_gain, ln2_shift, w_up, b_up, w_down, b_down):
        micro_n, batch_n, seq_n, model_n = x_in.shape
        heads_n = b_qkv.shape[2] * tp_size
        quarter = w_qkv.shape[3]
        hid_q = w_up.shape[2]
        bf16, f32 = jnp.bfloat16, jnp.float32
        wqkv_t = jnp.transpose(w_qkv[0], (1, 0, 2))
        b_qkv_row = jnp.pad(b_qkv.reshape(1, 3 * quarter), ((0, 0), (0, model_n - 3 * quarter)))
        pack = jnp.concatenate([ln1_gain, ln1_shift, b_out, ln2_gain, ln2_shift, b_down, b_up, b_qkv_row], axis=0).astype(f32)
        units = seq_n // UNIT
        pairs = model_n // 128
        dma = pltpu.SemaphoreType.DMA
        anywhere = pl.BlockSpec(memory_space=pl.ANY)
        tokens = batch_n * seq_n
        out = pl.pallas_call(
            functools.partial(kernel, heads_n),
            out_shape=jax.ShapeDtypeStruct((micro_n, tokens, model_n), bf16),
            in_specs=[anywhere, pl.BlockSpec(memory_space=pltpu.SMEM)] + [anywhere] * 5,
            out_specs=anywhere,
            scratch_shapes=[
                pltpu.VMEM((tp_size, 3, model_n, quarter), bf16),
                pltpu.VMEM((tp_size * quarter, model_n), bf16),
                pltpu.VMEM((tp_size, model_n, hid_q), bf16),
                pltpu.VMEM((tp_size * hid_q, model_n), bf16),
                pltpu.VMEM((tp_size,) + pack.shape, f32),
                pltpu.VMEM((2, 3, model_n // 2, quarter), bf16),
                pltpu.VMEM((2, quarter // 2, model_n), bf16),
                pltpu.VMEM((2, model_n // 2, hid_q), bf16),
                pltpu.VMEM((2, hid_q // 2, model_n), bf16),
                pltpu.VMEM((units, UNIT, model_n), bf16),
                pltpu.VMEM((units, UNIT, model_n), bf16),
                pltpu.VMEM((seq_n, model_n), bf16),
                pltpu.VMEM((model_n, seq_n), bf16),
                pltpu.VMEM((seq_n, 128), bf16),
                pltpu.VMEM((pairs, 256, 256), bf16),
                pltpu.VMEM((2, KBLK, 256), f32),
                pltpu.VMEM((seq_n // KBLK, KBLK, 256), f32),
                pltpu.VMEM((UNIT, model_n), bf16),
                pltpu.VMEM((UNIT, model_n), bf16),
                pltpu.VMEM((UNIT, model_n), bf16),
                pltpu.VMEM((UNIT, tp_size * hid_q), bf16),
                dma((5,)), dma((4, 5, 2)), dma((24,)), dma((2, 4)), dma((2, 4)), dma((2, 5)), dma((1,)),
                dma((units,)), dma((units,)), dma((units,)), dma((units,)), dma((units,)), dma((units,)), dma((units,)), dma((units,)),
                dma((2, units)), dma((2, units)), dma,
            ],
            compiler_params=pltpu.CompilerParams(collective_id=0, has_side_effects=True, vmem_limit_bytes=63 * 1024 * 1024),
            cost_estimate=pl.CostEstimate(flops=30 * 10 ** 9, bytes_accessed=40 * 10 ** 6, transcendentals=10 ** 7),
        )(x_in.reshape(micro_n, tokens, model_n), seq_lens.reshape(micro_n * batch_n), wqkv_t, w_out[0], w_up[0], w_down[0], pack)
        return out.reshape((1,) + x_in.shape)

    return jax.shard_map(per_device, mesh=mesh, in_specs=in_specs, out_specs=P('pp', 'dp'), check_vma=False)
```

```python
import functools
import math

import jax
import jax.numpy as jnp
import numpy as np
from jax import lax
from jax.experimental import pallas as pl
from jax.experimental.pallas import tpu as pltpu
from jax.sharding import PartitionSpec as P

MESH = pl.DeviceIdType.MESH
UNIT = 128
KBLK = 256
LAG = 4
NEG = -1e30


def alibi_slopes(heads_n):
    closest = 2 ** int(math.floor(math.log2(heads_n)))
    base_rate = 2.0 ** (-8.0 / closest)
    slope_list = [base_rate ** (head_idx + 1) for head_idx in range(closest)]
    extra_rate = 2.0 ** (-4.0 / closest)
    slope_list = slope_list + [extra_rate ** (2 * head_idx + 1) for head_idx in range(min(closest, heads_n - closest))]
    return np.array(slope_list, dtype=np.float32)


def split_bf16(value):
    parts = []
    rest = np.float32(value)
    for _ in range(3):
        part = rest.astype(jnp.bfloat16).astype(np.float32)
        parts.append(float(part))
        rest = np.float32(rest - part)
    return parts


def layer_norm(x, gain, shift):
    mean = jnp.mean(x, axis=-1, keepdims=True)
    cent = x - mean
    var = jnp.mean(cent * cent, axis=-1, keepdims=True)
    return (cent * lax.rsqrt(var + 1e-5) * gain + shift).astype(jnp.bfloat16)


def gelu(x):
    inner = math.sqrt(2.0 / math.pi) * (x + 0.044715 * (x * x * x))
    return 0.5 * x * (1.0 + jnp.tanh(inner))


def kernel(heads_n, x_hbm, lens, wqkv_in, wout_in, wup_in, wdn_in, pack_in, out,
           wqkv, wout, wup, wdn, packs, rl_qkv, rl_out, rl_up, rl_dn,
           xbuf, ybuf, kc, vt, kx, qaug, cmask, sbuf, abuf, ctx, hbuf, ubuf,
           loc_sem, w_recv, fwd_send, rl_send, rl_recv, dir_send, pk_send,
           x0_sem, x_recv, s_send, od_send, da_send, db_send, fa_send, fb_send,
           rr_recv, rr_send, o_recv):
    tp_n = 4
    units = xbuf.shape[0]
    model = xbuf.shape[2]
    seq = units * UNIT
    quarter = wqkv.shape[3]
    hid_q = wup.shape[2]
    pairs = model // 128

    r = lax.axis_index("tp")
    p = lax.axis_index("pp")
    x = p // 2
    c = p % 2
    odd = (r + x) % 2
    layer = 2 * x + odd
    home = odd == c
    rp, rm, ro = (r + 1) % tp_n, (r + 3) % tp_n, (r + 2) % tp_n
    partner = 2 * x + (1 - c)
    sig = 1 - 2 * c
    r_fwd = (r + sig + tp_n) % tp_n
    r_bwd = (r - sig + tp_n) % tp_n
    stage0, stage1 = 2 * x, 2 * x + 1
    x_n = 4

    def micro_of(row, core, lay):
        hops = (lay + 1) // 2
        return 2 * (((row + 8 - (1 - 2 * core) * hops) % tp_n) // 2) + core

    m = micro_of(r, c, layer)

    def rcopy(src, dst, ssem, rsem, **dev):
        return pltpu.make_async_remote_copy(src_ref=src, dst_ref=dst, send_sem=ssem, recv_sem=rsem,
                                            device_id=dev, device_id_type=MESH)

    barrier = pltpu.get_barrier_semaphore()
    for dr in range(tp_n):
        for dc in range(2):
            if dr or dc:
                pl.semaphore_signal(barrier, inc=1, device_id={"tp": (r + dr) % tp_n, "pp": 2 * x + (c + dc) % 2}, device_id_type=MESH)
    for dx in (1, x_n - 1):
        pl.semaphore_signal(barrier, inc=1, device_id={"pp": 2 * ((x + dx) % x_n) + c}, device_id_type=MESH)
    pl.semaphore_wait(barrier, 9)

    def wsrc(k, h=None):
        if k == 0:
            return wqkv_in if h is None else wqkv_in.at[:, pl.ds(h * (model // 2), model // 2), :]
        ref = (None, wout_in, wup_in, wdn_in, pack_in)[k]
        if h is None:
            return ref
        half = ref.shape[0] // 2
        return ref.at[pl.ds(h * half, half)]

    def wdst(k, q, h=None):
        if k == 0:
            return wqkv.at[q] if h is None else wqkv.at[q, :, pl.ds(h * (model // 2), model // 2), :]
        if k == 2:
            return wup.at[q] if h is None else wup.at[q, pl.ds(h * (model // 2), model // 2)]
        if k == 4:
            return packs.at[q]
        ref, rows = (wout, quarter) if k == 1 else (wdn, hid_q)
        if h is None:
            return ref.at[pl.ds(pl.multiple_of(q * rows, rows), rows)]
        half = rows // 2
        return ref.at[pl.ds(pl.multiple_of(q * rows + h * half, half), half)]

    def rl(k, h):
        return (rl_qkv, rl_out, rl_up, rl_dn)[k].at[h]

    def wwait(view, sem):
        rcopy(view, view, sem, sem, pp=partner).wait_recv()

    @pl.when(home)
    def _():
        rcopy(wsrc(4), wdst(4, r), pk_send.at[0], w_recv.at[2, 4, 0], tp=ro).start()
        for k in range(4):
            rcopy(wsrc(k, 0), rl(k, 0), rl_send.at[0, k], rl_recv.at[0, k], tp=rp).start()
            rcopy(wsrc(k, 1), rl(k, 1), rl_send.at[1, k], rl_recv.at[1, k], tp=rm).start()
        for k in range(5):
            pltpu.make_async_copy(wsrc(k), wdst(k, r), loc_sem.at[k]).start()
            rcopy(wsrc(k), wdst(k, r), fwd_send.at[k], w_recv.at[0, k, 0], pp=partner).start()

    @pl.when(jnp.logical_not(home))
    def _():
        for k in (4, 0, 1, 2, 3):
            rcopy(wsrc(k), wdst(k, r), dir_send.at[0, k], w_recv.at[3, k, 0], tp=rp).start()
            rcopy(wsrc(k), wdst(k, r), dir_send.at[1, k], w_recv.at[1, k, 0], tp=rm).start()

    @pl.when(layer == 0)
    def _():
        for u in range(units):
            pltpu.make_async_copy(x_hbm.at[m, pl.ds(u * UNIT, UNIT)], xbuf.at[u], x0_sem.at[u]).start()

    kc[...] = jnp.zeros_like(kc)
    vt[...] = jnp.zeros_like(vt)
    length = lens[m]
    key = lax.broadcasted_iota(jnp.int32, (seq, 128), 0)
    lane = lax.broadcasted_iota(jnp.int32, (seq, 128), 1)
    high = (key // 256) * 256
    part = jnp.where(lane % 2 == 0, high, key - high).astype(jnp.float32)
    dead = jnp.where(key >= length, NEG, 0.0)
    kx[...] = jnp.where(lane < 6, part, jnp.where(lane == 6, dead, 0.0)).astype(jnp.bfloat16)
    slopes = alibi_slopes(heads_n)
    row = lax.broadcasted_iota(jnp.int32, (128, 256), 0)
    second = lax.broadcasted_iota(jnp.int32, (128, 256), 1) >= 128
    for pair in range(pairs):
        (h0, m0, l0), (h1, m1, l1) = split_bf16(slopes[2 * pair]), split_bf16(slopes[2 * pair + 1])
        hi, mid, low = jnp.where(second, h1, h0), jnp.where(second, m1, m0), jnp.where(second, l1, l0)
        val = jnp.where(row < 2, hi, jnp.where(row < 4, mid, jnp.where(row < 6, low, jnp.where(row == 6, 1.0, 0.0))))
        qaug[pair, 128:, :] = val.astype(jnp.bfloat16)
    kpos = lax.broadcasted_iota(jnp.int32, (KBLK, 256), 0)
    qpos = lax.broadcasted_iota(jnp.int32, (KBLK, 256), 1) % 128
    cmask[0] = jnp.where(kpos <= qpos, 0.0, NEG)
    cmask[1] = jnp.where(kpos <= qpos + 128, 0.0, NEG)

    @pl.when(home)
    def _():
        idx = 5
        for k in (4, 0, 1, 2, 3):
            for d, q in ((1, rp), (3, rm)):
                wwait(wdst(k, q), w_recv.at[d, k, 0])
                rcopy(wdst(k, q), wdst(k, q), fwd_send.at[idx], w_recv.at[d, k, 0], pp=partner).start()
                idx += 1
        wwait(wdst(4, ro), w_recv.at[2, 4, 0])
        rcopy(wdst(4, ro), wdst(4, ro), fwd_send.at[idx], w_recv.at[2, 4, 0], pp=partner).start()
        idx += 1
        for k in range(4):
            for h in range(2):
                wwait(wdst(k, ro, h), w_recv.at[2, k, h])
                rcopy(wdst(k, ro, h), wdst(k, ro, h), fwd_send.at[idx], w_recv.at[2, k, h], pp=partner).start()
                idx += 1
        for k in range(5):
            pltpu.make_async_copy(wsrc(k), wdst(k, r), loc_sem.at[k]).wait()

    @pl.when(jnp.logical_not(home))
    def _():
        for k in range(4):
            wwait(rl(k, 0), rl_recv.at[0, k])
            rcopy(rl(k, 0), wdst(k, rm, 0), rl_send.at[0, k], w_recv.at[2, k, 0], tp=rp).start()
            wwait(rl(k, 1), rl_recv.at[1, k])
            rcopy(rl(k, 1), wdst(k, rp, 1), rl_send.at[1, k], w_recv.at[2, k, 1], tp=rm).start()
        for k in range(5):
            for d, q in ((0, r), (1, rp), (3, rm)):
                wwait(wdst(k, q), w_recv.at[d, k, 0])
        wwait(wdst(4, ro), w_recv.at[2, 4, 0])
        for k in range(4):
            for h in range(2):
                wwait(wdst(k, ro, h), w_recv.at[2, k, h])

    def out_at(mm, u):
        return out.at[mm, pl.ds(pl.multiple_of(u * UNIT, UNIT), UNIT)]

    m_a = micro_of(rm, 0, stage1)
    m_b = micro_of(rp, 1, stage1)
    relay = jnp.logical_and(odd == 0, c == 1)

    def relay_unit(v):
        wwait(out_at(m_a, v), rr_recv.at[0, v])
        rcopy(out_at(m_a, v), out_at(m_a, v), rr_send.at[0, v], o_recv, tp=rp).start()
        wwait(out_at(m_b, v), rr_recv.at[1, v])
        rcopy(out_at(m_b, v), out_at(m_b, v), rr_send.at[1, v], o_recv, tp=rm).start()

    def attention(nb, diag):
        def scores(pair):
            col = slice(pair * 128, (pair + 1) * 128)
            top = None
            for b in range(nb):
                keys = jnp.concatenate([kc[b * KBLK:(b + 1) * KBLK, col], kx[b * KBLK:(b + 1) * KBLK, :]], axis=1)
                s = jnp.dot(keys, qaug[pair], preferred_element_type=jnp.float32)
                if b == nb - 1:
                    s = s + diag
                sbuf[pair % 2, b] = s
                peak = jnp.max(s, axis=0, keepdims=True)
                top = peak if top is None else jnp.maximum(top, peak)
            return top

        def weigh(pair, top):
            col = slice(pair * 128, (pair + 1) * 128)
            total = None
            acc = None
            for b in range(nb):
                e = jnp.exp(sbuf[pair % 2, b] - top)
                part_sum = jnp.sum(e, axis=0, keepdims=True)
                total = part_sum if total is None else total + part_sum
                pv = jnp.dot(vt[col, b * KBLK:(b + 1) * KBLK], e.astype(jnp.bfloat16), preferred_element_type=jnp.float32)
                acc = pv if acc is None else acc + pv
            acc = acc * (1.0 / total)
            both = jnp.concatenate([acc[:64, :128], acc[64:, 128:]], axis=0)
            ctx[:, col] = both.T.astype(jnp.bfloat16)

        top = scores(0)
        for pair in range(pairs):
            later = scores(pair + 1) if pair + 1 < pairs else None
            weigh(pair, top)
            top = later

    r_next = (r + (1 - odd) * sig + tp_n) % tp_n
    p_next = (p + 2 * odd) % (2 * x_n)

    def store_unit(v):
        @pl.when(home)
        def _():
            pltpu.make_async_copy(ybuf.at[v], out_at(m, v), o_recv).start()

        @pl.when(jnp.logical_not(home))
        def _():
            rcopy(ybuf.at[v], out_at(m, v), od_send.at[v], o_recv, pp=partner).start()

        rcopy(ybuf.at[v], out_at(m, v), da_send.at[v], o_recv, tp=r_bwd, pp=2 * x + odd).start()

        @pl.when(odd == 1)
        def _():
            rcopy(ybuf.at[v], out_at(m, v), db_send.at[v], rr_recv.at[c, v], tp=r_fwd, pp=stage1).start()

    def unit_step(u, carry):
        tok = pl.ds(pl.multiple_of(u * UNIT, UNIT), UNIT)

        @pl.when(layer == 0)
        def _():
            pltpu.make_async_copy(x_hbm.at[m, tok], xbuf.at[u], x0_sem.at[u]).wait()

        @pl.when(layer > 0)
        def _():
            wwait(xbuf.at[u], x_recv.at[u])

        @pl.when(odd == 1)
        def _():
            @pl.when(c == 0)
            def _():
                pltpu.make_async_copy(xbuf.at[u], out_at(m, u), o_recv).start()

            @pl.when(c == 1)
            def _():
                rcopy(xbuf.at[u], out_at(m, u), fa_send.at[u], o_recv, pp=partner).start()

            rcopy(xbuf.at[u], out_at(m, u), fb_send.at[u], o_recv, tp=r_fwd, pp=stage0).start()

        @pl.when(u > 0)
        def _():
            store_unit(u - 1)

        xin = xbuf[u].astype(jnp.float32)
        abuf[...] = layer_norm(xin, packs[0, 0:1, :], packs[0, 1:2, :])
        head_row = lax.broadcasted_iota(jnp.int32, (128, 128), 0) < 64
        for q in range(tp_n):
            for j in range(3):
                o = jnp.dot(abuf[...], wqkv[q, j], preferred_element_type=jnp.float32)
                o = (o + packs[q, 7:8, j * quarter:(j + 1) * quarter]).astype(jnp.bfloat16)
                if j == 0:
                    o = o.astype(jnp.float32) * 0.125
                    for half in range(quarter // 128):
                        q_t = o[:, half * 128:(half + 1) * 128].T
                        pair = q * (quarter // 128) + half
                        qaug[pair, :128, :128] = jnp.where(head_row, q_t, 0.0).astype(jnp.bfloat16)
                        qaug[pair, :128, 128:] = jnp.where(head_row, 0.0, q_t).astype(jnp.bfloat16)
                elif j == 1:
                    kc[tok, q * quarter:(q + 1) * quarter] = o
                else:
                    vt[q * quarter:(q + 1) * quarter, tok] = o.astype(jnp.float32).T.astype(jnp.bfloat16)

        for nb in range(1, seq // KBLK + 1):
            @pl.when(u // 2 + 1 == nb)
            def _():
                attention(nb, cmask[u % 2])

        for n in range(model // quarter):
            cols = slice(n * quarter, (n + 1) * quarter)
            attn = jnp.dot(ctx[...], wout[:, cols], preferred_element_type=jnp.float32)
            hbuf[:, cols] = (xbuf[u, :, cols].astype(jnp.float32) + attn + packs[0, 2:3, cols]).astype(jnp.bfloat16)
        abuf[...] = layer_norm(hbuf[...].astype(jnp.float32), packs[0, 3:4, :], packs[0, 4:5, :])
        for q in range(tp_n):
            for n in range(hid_q // quarter):
                cols = slice(n * quarter, (n + 1) * quarter)
                up = jnp.dot(abuf[...], wup[q, :, cols], preferred_element_type=jnp.float32)
                up = up + packs[q, 6:7, cols]
                ubuf[:, q * hid_q + n * quarter:q * hid_q + (n + 1) * quarter] = gelu(up).astype(jnp.bfloat16)
        half_model = model // 2
        for n in range(2):
            cols = slice(n * half_model, (n + 1) * half_model)
            down = jnp.dot(ubuf[...], wdn[:, cols], preferred_element_type=jnp.float32)
            ybuf[u, :, cols] = (hbuf[:, cols].astype(jnp.float32) + down + packs[0, 5:6, cols]).astype(jnp.bfloat16)
            rcopy(ybuf.at[u, :, cols], xbuf.at[u, :, cols], s_send.at[u], x_recv.at[u], tp=r_next, pp=p_next).start()

        @pl.when(jnp.logical_and(relay, u >= LAG))
        def _():
            relay_unit(u - LAG)

        return carry

    lax.fori_loop(0, units, unit_step, 0)
    store_unit(units - 1)

    @pl.when(relay)
    def _():
        for v in range(max(0, units - LAG), units):
            relay_unit(v)

    def sent(view, sem):
        rcopy(view, view, sem, sem, pp=partner).wait_send()

    @pl.when(home)
    def _():
        sent(wsrc(4), pk_send.at[0])
        for k in range(4):
            sent(rl(k, 0), rl_send.at[0, k])
            sent(rl(k, 1), rl_send.at[1, k])
        for k in range(5):
            sent(wsrc(k), fwd_send.at[k])
        idx = 5
        for k in (4, 0, 1, 2, 3):
            for d in range(2):
                sent(wsrc(k), fwd_send.at[idx])
                idx += 1
        sent(wsrc(4), fwd_send.at[idx])
        idx += 1
        for k in range(4):
            for h in range(2):
                sent(wsrc(k, h), fwd_send.at[idx])
                idx += 1

    @pl.when(jnp.logical_not(home))
    def _():
        for k in range(5):
            for d in range(2):
                sent(wsrc(k), dir_send.at[d, k])
        for k in range(4):
            for d in range(2):
                sent(rl(k, d), rl_send.at[d, k])

    def drain(u, carry):
        sent(ybuf.at[u], s_send.at[u])
        sent(ybuf.at[u], da_send.at[u])

        @pl.when(jnp.logical_not(home))
        def _():
            sent(ybuf.at[u], od_send.at[u])

        @pl.when(relay)
        def _():
            sent(ybuf.at[u], rr_send.at[0, u])
            sent(ybuf.at[u], rr_send.at[1, u])

        @pl.when(odd == 1)
        def _():
            sent(ybuf.at[u], db_send.at[u])
            sent(ybuf.at[u], fb_send.at[u])

            @pl.when(c == 1)
            def _():
                sent(ybuf.at[u], fa_send.at[u])

        @pl.when(layer == 0)
        def _():
            wwait(xbuf.at[u], x_recv.at[u])

        return carry

    lax.fori_loop(0, units, drain, 0)

    @pl.when(relay)
    def _():
        wwait(out.at[pl.ds(0, out.shape[0] // 2)], o_recv)

    @pl.when(jnp.logical_not(relay))
    def _():
        wwait(out, o_recv)


def solution(mesh):
    tp_size = mesh.shape['tp']
    in_specs = (P('dp'), P('dp'), P('pp'), P('pp'), P('pp', None, None, 'tp'), P('pp', None, 'tp', None), P('pp', 'tp', None), P('pp'), P('pp'), P('pp'), P('pp', None, 'tp'), P('pp', 'tp'), P('pp', 'tp', None), P('pp'))

    def per_device(x_in, seq_lens, ln1_gain, ln1_shift, w_qkv, b_qkv, w_out, b_out, ln2_gain, ln2_shift, w_up, b_up, w_down, b_down):
        micro_n, batch_n, seq_n, model_n = x_in.shape
        heads_n = b_qkv.shape[2] * tp_size
        quarter = w_qkv.shape[3]
        hid_q = w_up.shape[2]
        bf16, f32 = jnp.bfloat16, jnp.float32
        wqkv_t = jnp.transpose(w_qkv[0], (1, 0, 2))
        b_qkv_row = jnp.pad(b_qkv.reshape(1, 3 * quarter), ((0, 0), (0, model_n - 3 * quarter)))
        pack = jnp.concatenate([ln1_gain, ln1_shift, b_out, ln2_gain, ln2_shift, b_down, b_up, b_qkv_row], axis=0).astype(f32)
        units = seq_n // UNIT
        pairs = model_n // 128
        dma = pltpu.SemaphoreType.DMA
        anywhere = pl.BlockSpec(memory_space=pl.ANY)
        tokens = batch_n * seq_n
        out = pl.pallas_call(
            functools.partial(kernel, heads_n),
            out_shape=jax.ShapeDtypeStruct((micro_n, tokens, model_n), bf16),
            in_specs=[anywhere, pl.BlockSpec(memory_space=pltpu.SMEM)] + [anywhere] * 5,
            out_specs=anywhere,
            scratch_shapes=[
                pltpu.VMEM((tp_size, 3, model_n, quarter), bf16),
                pltpu.VMEM((tp_size * quarter, model_n), bf16),
                pltpu.VMEM((tp_size, model_n, hid_q), bf16),
                pltpu.VMEM((tp_size * hid_q, model_n), bf16),
                pltpu.VMEM((tp_size,) + pack.shape, f32),
                pltpu.VMEM((2, 3, model_n // 2, quarter), bf16),
                pltpu.VMEM((2, quarter // 2, model_n), bf16),
                pltpu.VMEM((2, model_n // 2, hid_q), bf16),
                pltpu.VMEM((2, hid_q // 2, model_n), bf16),
                pltpu.VMEM((units, UNIT, model_n), bf16),
                pltpu.VMEM((units, UNIT, model_n), bf16),
                pltpu.VMEM((seq_n, model_n), bf16),
                pltpu.VMEM((model_n, seq_n), bf16),
                pltpu.VMEM((seq_n, 128), bf16),
                pltpu.VMEM((pairs, 256, 256), bf16),
                pltpu.VMEM((2, KBLK, 256), f32),
                pltpu.VMEM((2, seq_n // KBLK, KBLK, 256), f32),
                pltpu.VMEM((UNIT, model_n), bf16),
                pltpu.VMEM((UNIT, model_n), bf16),
                pltpu.VMEM((UNIT, model_n), bf16),
                pltpu.VMEM((UNIT, tp_size * hid_q), bf16),
                dma((5,)), dma((4, 5, 2)), dma((24,)), dma((2, 4)), dma((2, 4)), dma((2, 5)), dma((1,)),
                dma((units,)), dma((units,)), dma((units,)), dma((units,)), dma((units,)), dma((units,)), dma((units,)), dma((units,)),
                dma((2, units)), dma((2, units)), dma,
            ],
            compiler_params=pltpu.CompilerParams(collective_id=0, has_side_effects=True, vmem_limit_bytes=63 * 1024 * 1024),
            cost_estimate=pl.CostEstimate(flops=30 * 10 ** 9, bytes_accessed=40 * 10 ** 6, transcendentals=10 ** 7),
        )(x_in.reshape(micro_n, tokens, model_n), seq_lens.reshape(micro_n * batch_n), wqkv_t, w_out[0], w_up[0], w_down[0], pack)
        return out.reshape((1,) + x_in.shape)

    return jax.shard_map(per_device, mesh=mesh, in_specs=in_specs, out_specs=P('pp', 'dp'), check_vma=False)
```

```python
import functools
import math

import jax
import jax.numpy as jnp
import numpy as np
from jax import lax
from jax.experimental import pallas as pl
from jax.experimental.pallas import tpu as pltpu
from jax.sharding import PartitionSpec as P

MESH = pl.DeviceIdType.MESH
UNIT = 128
KBLK = 256
NEG = -1e30


def alibi_slopes(heads_n):
    closest = 2 ** int(math.floor(math.log2(heads_n)))
    base_rate = 2.0 ** (-8.0 / closest)
    slope_list = [base_rate ** (head_idx + 1) for head_idx in range(closest)]
    extra_rate = 2.0 ** (-4.0 / closest)
    slope_list = slope_list + [extra_rate ** (2 * head_idx + 1) for head_idx in range(min(closest, heads_n - closest))]
    return np.array(slope_list, dtype=np.float32)


def split_bf16(value):
    parts = []
    rest = np.float32(value)
    for _ in range(3):
        part = rest.astype(jnp.bfloat16).astype(np.float32)
        parts.append(float(part))
        rest = np.float32(rest - part)
    return parts


def layer_norm(x, gain, shift):
    mean = jnp.mean(x, axis=-1, keepdims=True)
    cent = x - mean
    var = jnp.mean(cent * cent, axis=-1, keepdims=True)
    return (cent * lax.rsqrt(var + 1e-5) * gain + shift).astype(jnp.bfloat16)


def gelu(x):
    inner = math.sqrt(2.0 / math.pi) * (x + 0.044715 * (x * x * x))
    return 0.5 * x * (1.0 + jnp.tanh(inner))


def kernel(heads_n, x_hbm, lens, wqkv_in, wout_in, wup_in, wdn_in, pack_in, out,
           wqkv, wout, wup, wdn, packs, rl_qkv, rl_out, rl_up, rl_dn, sw_qkv, sw_out, sw_up, sw_dn, sw_pack,
           xbuf, ybuf, kc0, kc1, kc2, kc3, vt0, vt1, vt2, vt3, kx, qaug, cmask, sbuf, abuf, ctx, hbuf, ubuf,
           sw_send, sw_recv, w_recv, fwd_send, rl_send, rl_recv, dir_send, pk_send, go,
           x0_sem, x_recv, s_send, od_send, da_send, db_send, fa_send, fb_send, fc_send,
           rr_recv, rr_send, o_recv):
    tp_n = 4
    units = xbuf.shape[0]
    model = xbuf.shape[2]
    seq = units * UNIT
    quarter = wqkv.shape[3]
    hid_q = wup.shape[2]
    pairs = model // 128

    r = lax.axis_index("tp")
    p = lax.axis_index("pp")
    x = p // 2
    c = p % 2
    odd = (r + (x + 1) // 2 + 1) % 2
    even_col = x + (1 - x % 2) * (2 - 2 * x)
    layer = odd * (2 * x + 1) + (1 - odd) * 2 * even_col
    home = odd == c
    moved = jnp.logical_and(c == 0, x % 2 == 0)
    early_row = r % 2 == 0
    rp, rm, ro = (r + 1) % tp_n, (r + 3) % tp_n, (r + 2) % tp_n
    partner = 2 * x + (1 - c)
    sig = 1 - 2 * c
    r_fwd = (r + sig + tp_n) % tp_n
    r_bwd = (r - sig + tp_n) % tp_n
    stage0, stage1 = 2 * x, 2 * x + 1
    x_n = 4

    def micro_of(row, core, lay):
        hops = (lay + 1) // 4
        return 2 * (((row + 8 - (1 - 2 * core) * hops) % tp_n) // 2) + core

    m = micro_of(r, c, layer)

    def rcopy(src, dst, ssem, rsem, **dev):
        return pltpu.make_async_remote_copy(src_ref=src, dst_ref=dst, send_sem=ssem, recv_sem=rsem,
                                            device_id=dev, device_id_type=MESH)

    barrier = pltpu.get_barrier_semaphore()
    for dr in range(tp_n):
        for dc in range(2):
            if dr or dc:
                pl.semaphore_signal(barrier, inc=1, device_id={"tp": (r + dr) % tp_n, "pp": 2 * x + (c + dc) % 2}, device_id_type=MESH)
    for dx in range(1, x_n):
        pl.semaphore_signal(barrier, inc=1, device_id={"pp": 2 * ((x + dx) % x_n) + c}, device_id_type=MESH)
    pl.semaphore_wait(barrier, 10)

    def wsrc(k, h=None):
        if k == 4:
            return pack_in
        if k == 0:
            return wqkv_in if h is None else wqkv_in.at[:, pl.ds(h * (model // 2), model // 2), :]
        ref = (None, wout_in, wup_in, wdn_in)[k]
        if h is None:
            return ref
        half = ref.shape[0] // 2
        return ref.at[pl.ds(h * half, half)]

    def wdst(k, q, h=None):
        if k == 0:
            return wqkv.at[q] if h is None else wqkv.at[q, :, pl.ds(h * (model // 2), model // 2), :]
        if k == 2:
            return wup.at[q] if h is None else wup.at[q, pl.ds(h * (model // 2), model // 2)]
        if k == 4:
            return packs.at[q]
        ref, rows = (wout, quarter) if k == 1 else (wdn, hid_q)
        if h is None:
            return ref.at[pl.ds(pl.multiple_of(q * rows, rows), rows)]
        half = rows // 2
        return ref.at[pl.ds(pl.multiple_of(q * rows + h * half, half), half)]

    def rl(k, h):
        return (rl_qkv, rl_out, rl_up, rl_dn)[k].at[h]

    def sw(k, h):
        if k == 4:
            return sw_pack
        if k == 0:
            return sw_qkv.at[:, pl.ds(h * (model // 2), model // 2), :]
        ref = (None, sw_out, sw_up, sw_dn)[k]
        half = ref.shape[0] // 2
        return ref.at[pl.ds(h * half, half)]

    def wwait(view, sem):
        rcopy(view, view, sem, sem, pp=partner).wait_recv()

    pieces = [(4, 0), (1, 0), (1, 1), (0, 0), (0, 1), (2, 0), (2, 1), (3, 0), (3, 1)]
    mats = pieces[1:]

    @pl.when(jnp.logical_and(moved, odd == 1))
    def _():
        for k, h in pieces:
            rcopy(wsrc(k, h), wdst(k, r, h), sw_send.at[k, h], sw_recv.at[k, h], pp=2 * (2 - x)).start()

    @pl.when(jnp.logical_and(moved, odd == 0))
    def _():
        for k, h in pieces:
            rcopy(wsrc(k, h), sw(k, h), sw_send.at[k, h], sw_recv.at[k, h], pp=2 * (2 - x)).start()

    @pl.when(jnp.logical_and(jnp.logical_not(moved), home))
    def _():
        for k, h in pieces:
            pltpu.make_async_copy(wsrc(k, h), wdst(k, r, h), sw_recv.at[k, h]).start()

    @pl.when(jnp.logical_not(jnp.logical_or(moved, home)))
    def _():
        for k, h in pieces:
            pltpu.make_async_copy(wsrc(k, h), sw(k, h), sw_recv.at[k, h]).start()

    @pl.when(layer == 0)
    def _():
        for u in range(units):
            pltpu.make_async_copy(x_hbm.at[m, pl.ds(u * UNIT, UNIT)], xbuf.at[u], x0_sem.at[u]).start()

    kc, vt = (kc0, kc1, kc2, kc3), (vt0, vt1, vt2, vt3)
    for ref in kc + vt:
        ref[...] = jnp.zeros_like(ref)
    length = lens[m]
    key = lax.broadcasted_iota(jnp.int32, (seq, 128), 0)
    lane = lax.broadcasted_iota(jnp.int32, (seq, 128), 1)
    high = (key // 256) * 256
    part = jnp.where(lane % 2 == 0, high, key - high).astype(jnp.float32)
    dead = jnp.where(key >= length, NEG, 0.0)
    kx[...] = jnp.where(lane < 6, part, jnp.where(lane == 6, dead, 0.0)).astype(jnp.bfloat16)
    slopes = alibi_slopes(heads_n)
    row = lax.broadcasted_iota(jnp.int32, (128, 256), 0)
    second = lax.broadcasted_iota(jnp.int32, (128, 256), 1) >= 128
    for pair in range(pairs):
        (h0, m0, l0), (h1, m1, l1) = split_bf16(slopes[2 * pair]), split_bf16(slopes[2 * pair + 1])
        hi, mid, low = jnp.where(second, h1, h0), jnp.where(second, m1, m0), jnp.where(second, l1, l0)
        val = jnp.where(row < 2, hi, jnp.where(row < 4, mid, jnp.where(row < 6, low, jnp.where(row == 6, 1.0, 0.0))))
        qaug[pair, 128:, :] = val.astype(jnp.bfloat16)
    kpos = lax.broadcasted_iota(jnp.int32, (KBLK, 256), 0)
    qpos = lax.broadcasted_iota(jnp.int32, (KBLK, 256), 1) % 128
    cmask[0] = jnp.where(kpos <= qpos, 0.0, NEG)
    cmask[1] = jnp.where(kpos <= qpos + 128, 0.0, NEG)

    def to_relay(k, h):
        rcopy(wdst(k, r, h), rl(k, h), rl_send.at[h, k], rl_recv.at[h, k], tp=(rp, rm)[h]).start()

    def to_partner(k, q, d, h):
        rcopy(wdst(k, q, h), wdst(k, q, h), fwd_send.at[d, k, h], w_recv.at[d, k, h], pp=partner).start()

    def hand_out():
        for k, h in pieces:
            wwait(sw(k, h), sw_recv.at[k, h])
            rcopy(sw(k, h), wdst(k, r, h), dir_send.at[0, k, h], w_recv.at[3, k, h], tp=rp).start()
            rcopy(sw(k, h), wdst(k, r, h), dir_send.at[1, k, h], w_recv.at[1, k, h], tp=rm).start()

    def relay_weights(k, h):
        wwait(rl(k, h), rl_recv.at[h, k])
        rcopy(rl(k, h), wdst(k, (rm, rp)[h], h), rl_send.at[h, k], w_recv.at[2, k, h], tp=(rp, rm)[h]).start()

    def from_partner():
        for d, q in ((0, r), (1, rp), (3, rm), (2, ro)):
            for k, h in pieces:
                wwait(wdst(k, q, h), w_recv.at[d, k, h])

    def sent(view, sem):
        rcopy(view, view, sem, sem, pp=partner).wait_send()

    def handed_out():
        for k, h in pieces:
            for d in range(2):
                sent(sw(k, h), dir_send.at[d, k, h])
        for k, h in mats:
            sent(rl(k, h), rl_send.at[h, k])

    @pl.when(home)
    def _():
        for k, h in pieces:
            wwait(wdst(k, r, h), sw_recv.at[k, h])
            if k == 4:
                rcopy(wdst(k, r), wdst(k, r), pk_send.at[0], w_recv.at[2, k, h], tp=ro).start()
            else:
                @pl.when(early_row)
                def _():
                    to_relay(k, h)
            to_partner(k, r, 0, h)

        @pl.when(jnp.logical_not(early_row))
        def _():
            pl.semaphore_wait(go, 1)
            for k, h in mats:
                to_relay(k, h)

        for k, h in pieces:
            for d, q in ((1, rp), (3, rm)):
                wwait(wdst(k, q, h), w_recv.at[d, k, h])
                to_partner(k, q, d, h)
        for k, h in pieces:
            wwait(wdst(k, ro, h), w_recv.at[2, k, h])
            to_partner(k, ro, 2, h)

    late_source = jnp.logical_and(early_row, jnp.logical_not(home))

    @pl.when(jnp.logical_not(jnp.logical_or(home, early_row)))
    def _():
        hand_out()
        for k, h in mats:
            relay_weights(k, h)
        handed_out()
        pl.semaphore_signal(go, inc=1, device_id={"pp": partner}, device_id_type=MESH)
        from_partner()

    @pl.when(late_source)
    def _():
        from_partner()
        hand_out()

    def out_at(mm, u):
        return out.at[mm, pl.ds(pl.multiple_of(u * UNIT, UNIT), UNIT)]

    m_a = micro_of(rm, 0, stage1)
    m_b = micro_of(rp, 1, stage1)
    relay = jnp.logical_and(odd == 0, jnp.logical_or(c == 1, x % 2 == 0))
    lag = min(5, units) * (x % 2) + units * ((x // 2) * (1 - x % 2))

    def relay_unit(v):
        wwait(out_at(m_a, v), rr_recv.at[0, v])
        rcopy(out_at(m_a, v), out_at(m_a, v), rr_send.at[0, v], o_recv, tp=rp).start()
        wwait(out_at(m_b, v), rr_recv.at[1, v])
        rcopy(out_at(m_b, v), out_at(m_b, v), rr_send.at[1, v], o_recv, tp=rm).start()

    def attention(nb, diag, tok):
        per_q = quarter // 128
        head_row = lax.broadcasted_iota(jnp.int32, (128, 128), 0) < 64

        def project(q):
            for j in range(3):
                o = jnp.dot(abuf[...], wqkv[q, j], preferred_element_type=jnp.float32)
                o = (o + packs[q, 7:8, j * quarter:(j + 1) * quarter]).astype(jnp.bfloat16)
                if j == 0:
                    o = o.astype(jnp.float32) * 0.125
                    for half in range(per_q):
                        q_t = o[:, half * 128:(half + 1) * 128].T
                        qaug[q * per_q + half, :128, :128] = jnp.where(head_row, q_t, 0.0).astype(jnp.bfloat16)
                        qaug[q * per_q + half, :128, 128:] = jnp.where(head_row, 0.0, q_t).astype(jnp.bfloat16)
                elif j == 1:
                    kc[q][tok, :] = o
                else:
                    vt[q][:, tok] = o.astype(jnp.float32).T.astype(jnp.bfloat16)

        def scores(pair):
            col = slice(pair % per_q * 128, (pair % per_q + 1) * 128)
            kq = kc[pair // per_q]
            top = None
            for b in range(nb):
                keys = jnp.concatenate([kq[b * KBLK:(b + 1) * KBLK, col], kx[b * KBLK:(b + 1) * KBLK, :]], axis=1)
                s = jnp.dot(keys, qaug[pair], preferred_element_type=jnp.float32)
                if b == nb - 1:
                    s = s + diag
                sbuf[pair % 2, b] = s
                peak = jnp.max(s, axis=0, keepdims=True)
                top = peak if top is None else jnp.maximum(top, peak)
            return top

        def weigh(pair, top):
            col = slice(pair % per_q * 128, (pair % per_q + 1) * 128)
            vq = vt[pair // per_q]
            total = None
            acc = None
            for b in range(nb):
                e = jnp.exp(sbuf[pair % 2, b] - top)
                part_sum = jnp.sum(e, axis=0, keepdims=True)
                total = part_sum if total is None else total + part_sum
                pv = jnp.dot(vq[col, b * KBLK:(b + 1) * KBLK], e.astype(jnp.bfloat16), preferred_element_type=jnp.float32)
                acc = pv if acc is None else acc + pv
            acc = acc * (1.0 / total)
            both = jnp.concatenate([acc[:64, :128], acc[64:, 128:]], axis=0)
            ctx[:, pair * 128:(pair + 1) * 128] = both.T.astype(jnp.bfloat16)

        project(0)
        top = None
        for pair in range(pairs + 1):
            if pair % per_q == 0 and pair // per_q + 1 < tp_n:
                project(pair // per_q + 1)
            later = scores(pair) if pair < pairs else None
            if pair > 0:
                weigh(pair - 1, top)
            top = later

    more = layer < 2 * x_n - 1
    nxt = (layer + 1) % (2 * x_n)
    half_n = nxt // 2
    x_next = half_n + (1 - nxt % 2) * (1 - half_n % 2) * (2 - 2 * half_n)
    p_next = 2 * x_next + c
    r_next = (r + (1 - odd) * (x % 2) * sig + tp_n) % tp_n

    def store_unit(v):
        @pl.when(home)
        def _():
            pltpu.make_async_copy(ybuf.at[v], out_at(m, v), o_recv).start()

        @pl.when(jnp.logical_not(home))
        def _():
            rcopy(ybuf.at[v], out_at(m, v), od_send.at[v], o_recv, pp=partner).start()

        rcopy(ybuf.at[v], out_at(m, v), da_send.at[v], o_recv, tp=r_bwd, pp=2 * x + odd).start()

        @pl.when(odd == 1)
        def _():
            rcopy(ybuf.at[v], out_at(m, v), db_send.at[v], rr_recv.at[c, v], tp=r_fwd, pp=stage1).start()

    stores = jnp.logical_or(odd == 1, x % 2 == 1)

    def unit_step(u, carry):
        tok = pl.ds(pl.multiple_of(u * UNIT, UNIT), UNIT)

        for group, (step0, step1) in (((0, 1), (1, 0)), ((2,), (3, 1)), ((3,), (5, 3))):
            now = jnp.logical_or(jnp.logical_and(layer == 0, u == min(step0, units - 1)),
                                 jnp.logical_or(jnp.logical_and(layer == 1, u == min(step1, units - 1)), jnp.logical_and(layer > 1, u == 0)))

            @pl.when(jnp.logical_and(late_source, now))
            def _():
                for k in group:
                    for h in range(2):
                        relay_weights(k, h)

        @pl.when(jnp.logical_and(relay, u >= lag))
        def _():
            relay_unit(u - lag)

        @pl.when(layer == 0)
        def _():
            pltpu.make_async_copy(x_hbm.at[m, tok], xbuf.at[u], x0_sem.at[u]).wait()

        @pl.when(layer > 0)
        def _():
            wwait(xbuf.at[u], x_recv.at[u])

        @pl.when(odd == 1)
        def _():
            @pl.when(c == 0)
            def _():
                pltpu.make_async_copy(xbuf.at[u], out_at(m, u), o_recv).start()

            @pl.when(c == 1)
            def _():
                rcopy(xbuf.at[u], out_at(m, u), fa_send.at[u], o_recv, pp=partner).start()

            @pl.when(x % 2 == 1)
            def _():
                rcopy(xbuf.at[u], out_at(m, u), fb_send.at[u], o_recv, tp=r_fwd, pp=stage0).start()

            @pl.when(x % 2 == 0)
            def _():
                rcopy(xbuf.at[u], out_at(m, u), fb_send.at[u], rr_recv.at[c, u], tp=r_fwd, pp=stage0).start()
                rcopy(xbuf.at[u], out_at(m, u), fc_send.at[u], o_recv, tp=r_bwd, pp=stage0).start()

        @pl.when(jnp.logical_and(stores, u > 0))
        def _():
            store_unit(u - 1)

        xin = xbuf[u].astype(jnp.float32)
        abuf[...] = layer_norm(xin, packs[0, 0:1, :], packs[0, 1:2, :])
        for nb in range(1, seq // KBLK + 1):
            @pl.when(u // 2 + 1 == nb)
            def _():
                attention(nb, cmask[u % 2], tok)

        for n in range(model // quarter):
            cols = slice(n * quarter, (n + 1) * quarter)
            attn = jnp.dot(ctx[...], wout[:, cols], preferred_element_type=jnp.float32)
            hbuf[:, cols] = (xbuf[u, :, cols].astype(jnp.float32) + attn + packs[0, 2:3, cols]).astype(jnp.bfloat16)
        abuf[...] = layer_norm(hbuf[...].astype(jnp.float32), packs[0, 3:4, :], packs[0, 4:5, :])
        for q in range(tp_n):
            for n in range(hid_q // quarter):
                cols = slice(n * quarter, (n + 1) * quarter)
                up = jnp.dot(abuf[...], wup[q, :, cols], preferred_element_type=jnp.float32)
                up = up + packs[q, 6:7, cols]
                ubuf[:, q * hid_q + n * quarter:q * hid_q + (n + 1) * quarter] = gelu(up).astype(jnp.bfloat16)
        half_model = model // 2
        for n in range(2):
            cols = slice(n * half_model, (n + 1) * half_model)
            down = jnp.dot(ubuf[...], wdn[:, cols], preferred_element_type=jnp.float32)
            ybuf[u, :, cols] = (hbuf[:, cols].astype(jnp.float32) + down + packs[0, 5:6, cols]).astype(jnp.bfloat16)

            @pl.when(more)
            def _():
                rcopy(ybuf.at[u, :, cols], xbuf.at[u, :, cols], s_send.at[u], x_recv.at[u], tp=r_next, pp=p_next).start()

        return carry

    lax.fori_loop(0, units, unit_step, 0)

    @pl.when(stores)
    def _():
        store_unit(units - 1)

    @pl.when(relay)
    def _():
        def rest(v, carry):
            relay_unit(v)
            return carry

        lax.fori_loop(units - lag, units, rest, 0)

    @pl.when(moved)
    def _():
        for k, h in pieces:
            sent(sw(k, h), sw_send.at[k, h])

    @pl.when(home)
    def _():
        sent(sw_pack, pk_send.at[0])
        for k, h in mats:
            sent(rl(k, h), rl_send.at[h, k])
        for d in range(4):
            for k, h in pieces:
                sent(sw(k, h), fwd_send.at[d, k, h])

    @pl.when(late_source)
    def _():
        handed_out()

    def drain(u, carry):
        @pl.when(more)
        def _():
            sent(ybuf.at[u], s_send.at[u])

        @pl.when(stores)
        def _():
            sent(ybuf.at[u], da_send.at[u])

            @pl.when(jnp.logical_not(home))
            def _():
                sent(ybuf.at[u], od_send.at[u])

        @pl.when(relay)
        def _():
            sent(ybuf.at[u], rr_send.at[0, u])
            sent(ybuf.at[u], rr_send.at[1, u])

        @pl.when(odd == 1)
        def _():
            sent(ybuf.at[u], db_send.at[u])
            sent(ybuf.at[u], fb_send.at[u])

            @pl.when(x % 2 == 0)
            def _():
                sent(ybuf.at[u], fc_send.at[u])

            @pl.when(c == 1)
            def _():
                sent(ybuf.at[u], fa_send.at[u])

        return carry

    lax.fori_loop(0, units, drain, 0)

    @pl.when(relay)
    def _():
        wwait(out.at[pl.ds(0, out.shape[0] // 2)], o_recv)

    @pl.when(jnp.logical_not(relay))
    def _():
        wwait(out, o_recv)


def solution(mesh):
    tp_size = mesh.shape['tp']
    in_specs = (P('dp'), P('dp'), P('pp'), P('pp'), P('pp', None, None, 'tp'), P('pp', None, 'tp', None), P('pp', 'tp', None), P('pp'), P('pp'), P('pp'), P('pp', None, 'tp'), P('pp', 'tp'), P('pp', 'tp', None), P('pp'))

    def per_device(x_in, seq_lens, ln1_gain, ln1_shift, w_qkv, b_qkv, w_out, b_out, ln2_gain, ln2_shift, w_up, b_up, w_down, b_down):
        micro_n, batch_n, seq_n, model_n = x_in.shape
        heads_n = b_qkv.shape[2] * tp_size
        quarter = w_qkv.shape[3]
        hid_q = w_up.shape[2]
        bf16, f32 = jnp.bfloat16, jnp.float32
        wqkv_t = jnp.transpose(w_qkv[0], (1, 0, 2))
        b_qkv_row = jnp.pad(b_qkv.reshape(1, 3 * quarter), ((0, 0), (0, model_n - 3 * quarter)))
        pack = jnp.concatenate([ln1_gain, ln1_shift, b_out, ln2_gain, ln2_shift, b_down, b_up, b_qkv_row], axis=0).astype(f32)
        units = seq_n // UNIT
        pairs = model_n // 128
        dma = pltpu.SemaphoreType.DMA
        anywhere = pl.BlockSpec(memory_space=pl.ANY)
        tokens = batch_n * seq_n
        out = pl.pallas_call(
            functools.partial(kernel, heads_n),
            out_shape=jax.ShapeDtypeStruct((micro_n, tokens, model_n), bf16),
            in_specs=[anywhere, pl.BlockSpec(memory_space=pltpu.SMEM)] + [anywhere] * 5,
            out_specs=anywhere,
            scratch_shapes=[
                pltpu.VMEM((tp_size, 3, model_n, quarter), bf16),
                pltpu.VMEM((tp_size * quarter, model_n), bf16),
                pltpu.VMEM((tp_size, model_n, hid_q), bf16),
                pltpu.VMEM((tp_size * hid_q, model_n), bf16),
                pltpu.VMEM((tp_size,) + pack.shape, f32),
                pltpu.VMEM((2, 3, model_n // 2, quarter), bf16),
                pltpu.VMEM((2, quarter // 2, model_n), bf16),
                pltpu.VMEM((2, model_n // 2, hid_q), bf16),
                pltpu.VMEM((2, hid_q // 2, model_n), bf16),
                pltpu.VMEM((3, model_n, quarter), bf16),
                pltpu.VMEM((quarter, model_n), bf16),
                pltpu.VMEM((model_n, hid_q), bf16),
                pltpu.VMEM((hid_q, model_n), bf16),
                pltpu.VMEM(pack.shape, f32),
                pltpu.VMEM((units, UNIT, model_n), bf16),
                pltpu.VMEM((units, UNIT, model_n), bf16),
                *[pltpu.VMEM((seq_n, quarter), bf16)] * tp_size,
                *[pltpu.VMEM((quarter, seq_n), bf16)] * tp_size,
                pltpu.VMEM((seq_n, 128), bf16),
                pltpu.VMEM((pairs, 256, 256), bf16),
                pltpu.VMEM((2, KBLK, 256), f32),
                pltpu.VMEM((2, seq_n // KBLK, KBLK, 256), f32),
                pltpu.VMEM((UNIT, model_n), bf16),
                pltpu.VMEM((UNIT, model_n), bf16),
                pltpu.VMEM((UNIT, model_n), bf16),
                pltpu.VMEM((UNIT, tp_size * hid_q), bf16),
                dma((5, 2)), dma((5, 2)), dma((4, 5, 2)), dma((4, 5, 2)), dma((2, 4)), dma((2, 4)), dma((2, 5, 2)), dma((1,)), pltpu.SemaphoreType.REGULAR,
                *[dma((units,))] * 9,
                dma((2, units)), dma((2, units)), dma,
            ],
            compiler_params=pltpu.CompilerParams(collective_id=0, has_side_effects=True, vmem_limit_bytes=63 * 1024 * 1024),
            cost_estimate=pl.CostEstimate(flops=30 * 10 ** 9, bytes_accessed=40 * 10 ** 6, transcendentals=10 ** 7),
        )(x_in.reshape(micro_n, tokens, model_n), seq_lens.reshape(micro_n * batch_n), wqkv_t, w_out[0], w_up[0], w_down[0], pack)
        return out.reshape((1,) + x_in.shape)

    return jax.shard_map(per_device, mesh=mesh, in_specs=in_specs, out_specs=P('pp', 'dp'), check_vma=False)
```

```python
import functools
import math

import jax
import jax.numpy as jnp
import numpy as np
from jax import lax
from jax.experimental import pallas as pl
from jax.experimental.pallas import tpu as pltpu
from jax.sharding import PartitionSpec as P

MESH = pl.DeviceIdType.MESH
UNIT = 128
KBLK = 256
NEG = -1e30


def alibi_slopes(heads_n):
    closest = 2 ** int(math.floor(math.log2(heads_n)))
    base_rate = 2.0 ** (-8.0 / closest)
    slope_list = [base_rate ** (head_idx + 1) for head_idx in range(closest)]
    extra_rate = 2.0 ** (-4.0 / closest)
    slope_list = slope_list + [extra_rate ** (2 * head_idx + 1) for head_idx in range(min(closest, heads_n - closest))]
    return np.array(slope_list, dtype=np.float32)


def split_bf16(value):
    parts = []
    rest = np.float32(value)
    for _ in range(3):
        part = rest.astype(jnp.bfloat16).astype(np.float32)
        parts.append(float(part))
        rest = np.float32(rest - part)
    return parts


def layer_norm(x, gain, shift):
    mean = jnp.mean(x, axis=-1, keepdims=True)
    cent = x - mean
    var = jnp.mean(cent * cent, axis=-1, keepdims=True)
    return (cent * lax.rsqrt(var + 1e-5) * gain + shift).astype(jnp.bfloat16)


def gelu(x):
    inner = math.sqrt(2.0 / math.pi) * (x + 0.044715 * (x * x * x))
    return 0.5 * x * (1.0 + jnp.tanh(inner))


def kernel(heads_n, x_hbm, lens, wqkv_in, wout_in, wup_in, wdn_in, pack_in, out,
           wqkv, wout, wup, wdn, packs, rl_qkv, rl_out, rl_up, rl_dn, sw_qkv, sw_out, sw_up, sw_dn, sw_pack,
           xbuf, ybuf, kc0, kc1, kc2, kc3, vt0, vt1, vt2, vt3, kx, qaug, cmask, sbuf, abuf, ctx, hbuf, ubuf,
           sw_send, sw_recv, w_recv, fwd_send, rl_send, rl_recv, dir_send, pk_send, go,
           x0_sem, x_recv, s_send, od_send, da_send, db_send, fa_send, fb_send, fc_send,
           rr_recv, rr_send, o_recv):
    tp_n = 4
    units = xbuf.shape[0]
    model = xbuf.shape[2]
    seq = units * UNIT
    quarter = wqkv.shape[3]
    hid_q = wup.shape[2]
    pairs = model // 128

    r = lax.axis_index("tp")
    p = lax.axis_index("pp")
    x = p // 2
    c = p % 2
    odd = (r + (x + 1) // 2 + 1) % 2
    even_col = x + (1 - x % 2) * (2 - 2 * x)
    layer = odd * (2 * x + 1) + (1 - odd) * 2 * even_col
    home = odd == c
    moved = jnp.logical_and(c == 0, x % 2 == 0)
    early_row = r % 2 == 0
    rp, rm, ro = (r + 1) % tp_n, (r + 3) % tp_n, (r + 2) % tp_n
    partner = 2 * x + (1 - c)
    sig = 1 - 2 * c
    r_fwd = (r + sig + tp_n) % tp_n
    r_bwd = (r - sig + tp_n) % tp_n
    stage0, stage1 = 2 * x, 2 * x + 1
    x_n = 4

    def micro_of(row, core, lay):
        hops = (lay + 1) // 4
        return 2 * (((row + 8 - (1 - 2 * core) * hops) % tp_n) // 2) + core

    m = micro_of(r, c, layer)

    def rcopy(src, dst, ssem, rsem, **dev):
        return pltpu.make_async_remote_copy(src_ref=src, dst_ref=dst, send_sem=ssem, recv_sem=rsem,
                                            device_id=dev, device_id_type=MESH)

    barrier = pltpu.get_barrier_semaphore()
    for dr in range(tp_n):
        for dc in range(2):
            if dr or dc:
                pl.semaphore_signal(barrier, inc=1, device_id={"tp": (r + dr) % tp_n, "pp": 2 * x + (c + dc) % 2}, device_id_type=MESH)
    for dx in range(1, x_n):
        pl.semaphore_signal(barrier, inc=1, device_id={"pp": 2 * ((x + dx) % x_n) + c}, device_id_type=MESH)
    pl.semaphore_wait(barrier, 10)

    def wsrc(k, h=None):
        if k == 4:
            return pack_in
        if k == 0:
            return wqkv_in if h is None else wqkv_in.at[:, pl.ds(h * (model // 2), model // 2), :]
        ref = (None, wout_in, wup_in, wdn_in)[k]
        if h is None:
            return ref
        half = ref.shape[0] // 2
        return ref.at[pl.ds(h * half, half)]

    def wdst(k, q, h=None):
        if k == 0:
            return wqkv.at[q] if h is None else wqkv.at[q, :, pl.ds(h * (model // 2), model // 2), :]
        if k == 2:
            return wup.at[q] if h is None else wup.at[q, pl.ds(h * (model // 2), model // 2)]
        if k == 4:
            return packs.at[q]
        ref, rows = (wout, quarter) if k == 1 else (wdn, hid_q)
        if h is None:
            return ref.at[pl.ds(pl.multiple_of(q * rows, rows), rows)]
        half = rows // 2
        return ref.at[pl.ds(pl.multiple_of(q * rows + h * half, half), half)]

    def rl(k, h):
        return (rl_qkv, rl_out, rl_up, rl_dn)[k].at[h]

    def sw(k, h):
        if k == 4:
            return sw_pack
        if k == 0:
            return sw_qkv.at[:, pl.ds(h * (model // 2), model // 2), :]
        ref = (None, sw_out, sw_up, sw_dn)[k]
        half = ref.shape[0] // 2
        return ref.at[pl.ds(h * half, half)]

    def wwait(view, sem):
        rcopy(view, view, sem, sem, pp=partner).wait_recv()

    pieces = [(4, 0), (1, 0), (1, 1), (0, 0), (0, 1), (2, 0), (2, 1), (3, 0), (3, 1)]
    mats = pieces[1:]

    @pl.when(jnp.logical_and(moved, odd == 1))
    def _():
        for k, h in pieces:
            rcopy(wsrc(k, h), wdst(k, r, h), sw_send.at[k, h], sw_recv.at[k, h], pp=2 * (2 - x)).start()

    @pl.when(jnp.logical_and(moved, odd == 0))
    def _():
        for k, h in pieces:
            rcopy(wsrc(k, h), sw(k, h), sw_send.at[k, h], sw_recv.at[k, h], pp=2 * (2 - x)).start()

    @pl.when(jnp.logical_and(jnp.logical_not(moved), home))
    def _():
        for k, h in pieces:
            pltpu.make_async_copy(wsrc(k, h), wdst(k, r, h), sw_recv.at[k, h]).start()

    @pl.when(jnp.logical_not(jnp.logical_or(moved, home)))
    def _():
        for k, h in pieces:
            pltpu.make_async_copy(wsrc(k, h), sw(k, h), sw_recv.at[k, h]).start()

    @pl.when(layer == 0)
    def _():
        for u in range(units):
            pltpu.make_async_copy(x_hbm.at[m, pl.ds(u * UNIT, UNIT)], xbuf.at[u], x0_sem.at[u]).start()

    kc, vt = (kc0, kc1, kc2, kc3), (vt0, vt1, vt2, vt3)
    for ref in kc + vt:
        ref[...] = jnp.zeros_like(ref)
    length = lens[m]
    key = lax.broadcasted_iota(jnp.int32, (seq, 128), 0)
    lane = lax.broadcasted_iota(jnp.int32, (seq, 128), 1)
    high = (key // 256) * 256
    part = jnp.where(lane % 2 == 0, high, key - high).astype(jnp.float32)
    dead = jnp.where(key >= length, NEG, 0.0)
    kx[...] = jnp.where(lane < 6, part, jnp.where(lane == 6, dead, 0.0)).astype(jnp.bfloat16)
    slopes = alibi_slopes(heads_n)
    row = lax.broadcasted_iota(jnp.int32, (128, 256), 0)
    second = lax.broadcasted_iota(jnp.int32, (128, 256), 1) >= 128
    for pair in range(pairs):
        (h0, m0, l0), (h1, m1, l1) = split_bf16(slopes[2 * pair]), split_bf16(slopes[2 * pair + 1])
        hi, mid, low = jnp.where(second, h1, h0), jnp.where(second, m1, m0), jnp.where(second, l1, l0)
        val = jnp.where(row < 2, hi, jnp.where(row < 4, mid, jnp.where(row < 6, low, jnp.where(row == 6, 1.0, 0.0))))
        qaug[pair, 128:, :] = val.astype(jnp.bfloat16)
    kpos = lax.broadcasted_iota(jnp.int32, (KBLK, 256), 0)
    qpos = lax.broadcasted_iota(jnp.int32, (KBLK, 256), 1) % 128
    cmask[0] = jnp.where(kpos <= qpos, 0.0, NEG)
    cmask[1] = jnp.where(kpos <= qpos + 128, 0.0, NEG)

    def to_relay(k, h):
        rcopy(wdst(k, r, h), rl(k, h), rl_send.at[h, k], rl_recv.at[h, k], tp=(rp, rm)[h]).start()

    def to_partner(k, q, d, h):
        rcopy(wdst(k, q, h), wdst(k, q, h), fwd_send.at[d, k, h], w_recv.at[d, k, h], pp=partner).start()

    def hand_out():
        for k, h in pieces:
            wwait(sw(k, h), sw_recv.at[k, h])
            rcopy(sw(k, h), wdst(k, r, h), dir_send.at[0, k, h], w_recv.at[3, k, h], tp=rp).start()
            rcopy(sw(k, h), wdst(k, r, h), dir_send.at[1, k, h], w_recv.at[1, k, h], tp=rm).start()

    def relay_weights(k, h):
        wwait(rl(k, h), rl_recv.at[h, k])
        rcopy(rl(k, h), wdst(k, (rm, rp)[h], h), rl_send.at[h, k], w_recv.at[2, k, h], tp=(rp, rm)[h]).start()

    def from_partner():
        for d, q in ((0, r), (1, rp), (3, rm), (2, ro)):
            for k, h in pieces:
                wwait(wdst(k, q, h), w_recv.at[d, k, h])

    def sent(view, sem):
        rcopy(view, view, sem, sem, pp=partner).wait_send()

    def handed_out():
        for k, h in pieces:
            for d in range(2):
                sent(sw(k, h), dir_send.at[d, k, h])
        for k, h in mats:
            sent(rl(k, h), rl_send.at[h, k])

    @pl.when(home)
    def _():
        for k, h in pieces:
            wwait(wdst(k, r, h), sw_recv.at[k, h])
            if k == 4:
                rcopy(wdst(k, r), wdst(k, r), pk_send.at[0], w_recv.at[2, k, h], tp=ro).start()
            else:
                @pl.when(early_row)
                def _():
                    to_relay(k, h)
            to_partner(k, r, 0, h)

        @pl.when(jnp.logical_not(early_row))
        def _():
            pl.semaphore_wait(go, 1)
            for k, h in mats:
                to_relay(k, h)

        for k, h in pieces:
            for d, q in ((1, rp), (3, rm)):
                wwait(wdst(k, q, h), w_recv.at[d, k, h])
                to_partner(k, q, d, h)
        for k, h in pieces:
            wwait(wdst(k, ro, h), w_recv.at[2, k, h])
            to_partner(k, ro, 2, h)

    late_source = jnp.logical_and(early_row, jnp.logical_not(home))

    @pl.when(jnp.logical_not(jnp.logical_or(home, early_row)))
    def _():
        hand_out()
        for k, h in mats:
            relay_weights(k, h)
        handed_out()
        pl.semaphore_signal(go, inc=1, device_id={"pp": partner}, device_id_type=MESH)
        from_partner()

    @pl.when(late_source)
    def _():
        hand_out()
        from_partner()

    def out_at(mm, u):
        return out.at[mm, pl.ds(pl.multiple_of(u * UNIT, UNIT), UNIT)]

    m_a = micro_of(rm, 0, stage1)
    m_b = micro_of(rp, 1, stage1)
    relay = jnp.logical_and(odd == 0, jnp.logical_or(c == 1, x % 2 == 0))
    lag = min(5, units) * (x % 2) + units * ((x // 2) * (1 - x % 2))

    def relay_unit(v):
        wwait(out_at(m_a, v), rr_recv.at[0, v])
        rcopy(out_at(m_a, v), out_at(m_a, v), rr_send.at[0, v], o_recv, tp=rp).start()
        wwait(out_at(m_b, v), rr_recv.at[1, v])
        rcopy(out_at(m_b, v), out_at(m_b, v), rr_send.at[1, v], o_recv, tp=rm).start()

    def attention(nb, diag, tok):
        per_q = quarter // 128
        head_row = lax.broadcasted_iota(jnp.int32, (128, 128), 0) < 64

        def project(q):
            for j in range(3):
                o = jnp.dot(abuf[...], wqkv[q, j], preferred_element_type=jnp.float32)
                o = (o + packs[q, 7:8, j * quarter:(j + 1) * quarter]).astype(jnp.bfloat16)
                if j == 0:
                    o = o.astype(jnp.float32) * 0.125
                    for half in range(per_q):
                        q_t = o[:, half * 128:(half + 1) * 128].T
                        qaug[q * per_q + half, :128, :128] = jnp.where(head_row, q_t, 0.0).astype(jnp.bfloat16)
                        qaug[q * per_q + half, :128, 128:] = jnp.where(head_row, 0.0, q_t).astype(jnp.bfloat16)
                elif j == 1:
                    kc[q][tok, :] = o
                else:
                    vt[q][:, tok] = o.astype(jnp.float32).T.astype(jnp.bfloat16)

        def scores(pair):
            col = slice(pair % per_q * 128, (pair % per_q + 1) * 128)
            kq = kc[pair // per_q]
            top = None
            for b in range(nb):
                keys = jnp.concatenate([kq[b * KBLK:(b + 1) * KBLK, col], kx[b * KBLK:(b + 1) * KBLK, :]], axis=1)
                s = jnp.dot(keys, qaug[pair], preferred_element_type=jnp.float32)
                if b == nb - 1:
                    s = s + diag
                sbuf[pair % 2, b] = s
                peak = jnp.max(s, axis=0, keepdims=True)
                top = peak if top is None else jnp.maximum(top, peak)
            return top

        def weigh(pair, top):
            col = slice(pair % per_q * 128, (pair % per_q + 1) * 128)
            vq = vt[pair // per_q]
            total = None
            acc = None
            for b in range(nb):
                e = jnp.exp(sbuf[pair % 2, b] - top)
                part_sum = jnp.sum(e, axis=0, keepdims=True)
                total = part_sum if total is None else total + part_sum
                pv = jnp.dot(vq[col, b * KBLK:(b + 1) * KBLK], e.astype(jnp.bfloat16), preferred_element_type=jnp.float32)
                acc = pv if acc is None else acc + pv
            acc = acc * (1.0 / total)
            both = jnp.concatenate([acc[:64, :128], acc[64:, 128:]], axis=0)
            ctx[:, pair * 128:(pair + 1) * 128] = both.T.astype(jnp.bfloat16)

        project(0)
        top = None
        for pair in range(pairs + 1):
            if pair % per_q == 0 and pair // per_q + 1 < tp_n:
                project(pair // per_q + 1)
            later = scores(pair) if pair < pairs else None
            if pair > 0:
                weigh(pair - 1, top)
            top = later

    more = layer < 2 * x_n - 1
    nxt = (layer + 1) % (2 * x_n)
    half_n = nxt // 2
    x_next = half_n + (1 - nxt % 2) * (1 - half_n % 2) * (2 - 2 * half_n)
    p_next = 2 * x_next + c
    r_next = (r + (1 - odd) * (x % 2) * sig + tp_n) % tp_n

    def store_unit(v):
        @pl.when(home)
        def _():
            pltpu.make_async_copy(ybuf.at[v], out_at(m, v), o_recv).start()

        @pl.when(jnp.logical_not(home))
        def _():
            rcopy(ybuf.at[v], out_at(m, v), od_send.at[v], o_recv, pp=partner).start()

        rcopy(ybuf.at[v], out_at(m, v), da_send.at[v], o_recv, tp=r_bwd, pp=2 * x + odd).start()

        @pl.when(odd == 1)
        def _():
            rcopy(ybuf.at[v], out_at(m, v), db_send.at[v], rr_recv.at[c, v], tp=r_fwd, pp=stage1).start()

    stores = jnp.logical_or(odd == 1, x % 2 == 1)

    def unit_step(u, carry):
        tok = pl.ds(pl.multiple_of(u * UNIT, UNIT), UNIT)

        for group, (step0, step1) in (((0, 1), (1, 0)), ((2,), (3, 1)), ((3,), (5, 3))):
            now = jnp.logical_or(jnp.logical_and(layer == 0, u == min(step0, units - 1)),
                                 jnp.logical_or(jnp.logical_and(layer == 1, u == min(step1, units - 1)), jnp.logical_and(layer > 1, u == 0)))

            @pl.when(jnp.logical_and(late_source, now))
            def _():
                for k in group:
                    for h in range(2):
                        relay_weights(k, h)

        @pl.when(jnp.logical_and(relay, u >= lag))
        def _():
            relay_unit(u - lag)

        @pl.when(layer == 0)
        def _():
            pltpu.make_async_copy(x_hbm.at[m, tok], xbuf.at[u], x0_sem.at[u]).wait()

        @pl.when(layer > 0)
        def _():
            wwait(xbuf.at[u], x_recv.at[u])

        @pl.when(odd == 1)
        def _():
            @pl.when(c == 0)
            def _():
                pltpu.make_async_copy(xbuf.at[u], out_at(m, u), o_recv).start()

            @pl.when(c == 1)
            def _():
                rcopy(xbuf.at[u], out_at(m, u), fa_send.at[u], o_recv, pp=partner).start()

            @pl.when(x % 2 == 1)
            def _():
                rcopy(xbuf.at[u], out_at(m, u), fb_send.at[u], o_recv, tp=r_fwd, pp=stage0).start()

            @pl.when(x % 2 == 0)
            def _():
                rcopy(xbuf.at[u], out_at(m, u), fb_send.at[u], rr_recv.at[c, u], tp=r_fwd, pp=stage0).start()
                rcopy(xbuf.at[u], out_at(m, u), fc_send.at[u], o_recv, tp=r_bwd, pp=stage0).start()

        @pl.when(jnp.logical_and(stores, u > 0))
        def _():
            store_unit(u - 1)

        xin = xbuf[u].astype(jnp.float32)
        abuf[...] = layer_norm(xin, packs[0, 0:1, :], packs[0, 1:2, :])
        for nb in range(1, seq // KBLK + 1):
            @pl.when(u // 2 + 1 == nb)
            def _():
                attention(nb, cmask[u % 2], tok)

        for n in range(model // quarter):
            cols = slice(n * quarter, (n + 1) * quarter)
            attn = jnp.dot(ctx[...], wout[:, cols], preferred_element_type=jnp.float32)
            hbuf[:, cols] = (xbuf[u, :, cols].astype(jnp.float32) + attn + packs[0, 2:3, cols]).astype(jnp.bfloat16)
        abuf[...] = layer_norm(hbuf[...].astype(jnp.float32), packs[0, 3:4, :], packs[0, 4:5, :])
        for q in range(tp_n):
            for n in range(hid_q // quarter):
                cols = slice(n * quarter, (n + 1) * quarter)
                up = jnp.dot(abuf[...], wup[q, :, cols], preferred_element_type=jnp.float32)
                up = up + packs[q, 6:7, cols]
                ubuf[:, q * hid_q + n * quarter:q * hid_q + (n + 1) * quarter] = gelu(up).astype(jnp.bfloat16)
        half_model = model // 2
        for n in range(2):
            cols = slice(n * half_model, (n + 1) * half_model)
            down = jnp.dot(ubuf[...], wdn[:, cols], preferred_element_type=jnp.float32)
            ybuf[u, :, cols] = (hbuf[:, cols].astype(jnp.float32) + down + packs[0, 5:6, cols]).astype(jnp.bfloat16)

            @pl.when(more)
            def _():
                rcopy(ybuf.at[u, :, cols], xbuf.at[u, :, cols], s_send.at[u], x_recv.at[u], tp=r_next, pp=p_next).start()

        return carry

    lax.fori_loop(0, units, unit_step, 0)

    @pl.when(stores)
    def _():
        store_unit(units - 1)

    @pl.when(relay)
    def _():
        def rest(v, carry):
            relay_unit(v)
            return carry

        lax.fori_loop(units - lag, units, rest, 0)

    @pl.when(moved)
    def _():
        for k, h in pieces:
            sent(sw(k, h), sw_send.at[k, h])

    @pl.when(home)
    def _():
        sent(sw_pack, pk_send.at[0])
        for k, h in mats:
            sent(rl(k, h), rl_send.at[h, k])
        for d in range(4):
            for k, h in pieces:
                sent(sw(k, h), fwd_send.at[d, k, h])

    @pl.when(late_source)
    def _():
        handed_out()

    def drain(u, carry):
        @pl.when(more)
        def _():
            sent(ybuf.at[u], s_send.at[u])

        @pl.when(stores)
        def _():
            sent(ybuf.at[u], da_send.at[u])

            @pl.when(jnp.logical_not(home))
            def _():
                sent(ybuf.at[u], od_send.at[u])

        @pl.when(relay)
        def _():
            sent(ybuf.at[u], rr_send.at[0, u])
            sent(ybuf.at[u], rr_send.at[1, u])

        @pl.when(odd == 1)
        def _():
            sent(ybuf.at[u], db_send.at[u])
            sent(ybuf.at[u], fb_send.at[u])

            @pl.when(x % 2 == 0)
            def _():
                sent(ybuf.at[u], fc_send.at[u])

            @pl.when(c == 1)
            def _():
                sent(ybuf.at[u], fa_send.at[u])

        return carry

    lax.fori_loop(0, units, drain, 0)

    @pl.when(relay)
    def _():
        wwait(out.at[pl.ds(0, out.shape[0] // 2)], o_recv)

    @pl.when(jnp.logical_not(relay))
    def _():
        wwait(out, o_recv)


def solution(mesh):
    tp_size = mesh.shape['tp']
    in_specs = (P('dp'), P('dp'), P('pp'), P('pp'), P('pp', None, None, 'tp'), P('pp', None, 'tp', None), P('pp', 'tp', None), P('pp'), P('pp'), P('pp'), P('pp', None, 'tp'), P('pp', 'tp'), P('pp', 'tp', None), P('pp'))

    def per_device(x_in, seq_lens, ln1_gain, ln1_shift, w_qkv, b_qkv, w_out, b_out, ln2_gain, ln2_shift, w_up, b_up, w_down, b_down):
        micro_n, batch_n, seq_n, model_n = x_in.shape
        heads_n = b_qkv.shape[2] * tp_size
        quarter = w_qkv.shape[3]
        hid_q = w_up.shape[2]
        bf16, f32 = jnp.bfloat16, jnp.float32
        wqkv_t = jnp.transpose(w_qkv[0], (1, 0, 2))
        b_qkv_row = jnp.pad(b_qkv.reshape(1, 3 * quarter), ((0, 0), (0, model_n - 3 * quarter)))
        pack = jnp.concatenate([ln1_gain, ln1_shift, b_out, ln2_gain, ln2_shift, b_down, b_up, b_qkv_row], axis=0).astype(f32)
        units = seq_n // UNIT
        pairs = model_n // 128
        dma = pltpu.SemaphoreType.DMA
        anywhere = pl.BlockSpec(memory_space=pl.ANY)
        tokens = batch_n * seq_n
        out = pl.pallas_call(
            functools.partial(kernel, heads_n),
            out_shape=jax.ShapeDtypeStruct((micro_n, tokens, model_n), bf16),
            in_specs=[anywhere, pl.BlockSpec(memory_space=pltpu.SMEM)] + [anywhere] * 5,
            out_specs=anywhere,
            scratch_shapes=[
                pltpu.VMEM((tp_size, 3, model_n, quarter), bf16),
                pltpu.VMEM((tp_size * quarter, model_n), bf16),
                pltpu.VMEM((tp_size, model_n, hid_q), bf16),
                pltpu.VMEM((tp_size * hid_q, model_n), bf16),
                pltpu.VMEM((tp_size,) + pack.shape, f32),
                pltpu.VMEM((2, 3, model_n // 2, quarter), bf16),
                pltpu.VMEM((2, quarter // 2, model_n), bf16),
                pltpu.VMEM((2, model_n // 2, hid_q), bf16),
                pltpu.VMEM((2, hid_q // 2, model_n), bf16),
                pltpu.VMEM((3, model_n, quarter), bf16),
                pltpu.VMEM((quarter, model_n), bf16),
                pltpu.VMEM((model_n, hid_q), bf16),
                pltpu.VMEM((hid_q, model_n), bf16),
                pltpu.VMEM(pack.shape, f32),
                pltpu.VMEM((units, UNIT, model_n), bf16),
                pltpu.VMEM((units, UNIT, model_n), bf16),
                *[pltpu.VMEM((seq_n, quarter), bf16)] * tp_size,
                *[pltpu.VMEM((quarter, seq_n), bf16)] * tp_size,
                pltpu.VMEM((seq_n, 128), bf16),
                pltpu.VMEM((pairs, 256, 256), bf16),
                pltpu.VMEM((2, KBLK, 256), f32),
                pltpu.VMEM((2, seq_n // KBLK, KBLK, 256), f32),
                pltpu.VMEM((UNIT, model_n), bf16),
                pltpu.VMEM((UNIT, model_n), bf16),
                pltpu.VMEM((UNIT, model_n), bf16),
                pltpu.VMEM((UNIT, tp_size * hid_q), bf16),
                dma((5, 2)), dma((5, 2)), dma((4, 5, 2)), dma((4, 5, 2)), dma((2, 4)), dma((2, 4)), dma((2, 5, 2)), dma((1,)), pltpu.SemaphoreType.REGULAR,
                *[dma((units,))] * 9,
                dma((2, units)), dma((2, units)), dma,
            ],
            compiler_params=pltpu.CompilerParams(collective_id=0, has_side_effects=True, vmem_limit_bytes=63 * 1024 * 1024),
            cost_estimate=pl.CostEstimate(flops=30 * 10 ** 9, bytes_accessed=40 * 10 ** 6, transcendentals=10 ** 7),
        )(x_in.reshape(micro_n, tokens, model_n), seq_lens.reshape(micro_n * batch_n), wqkv_t, w_out[0], w_up[0], w_down[0], pack)
        return out.reshape((1,) + x_in.shape)

    return jax.shard_map(per_device, mesh=mesh, in_specs=in_specs, out_specs=P('pp', 'dp'), check_vma=False)
```

```python
import functools
import math

import jax
import jax.numpy as jnp
import numpy as np
from jax import lax
from jax.experimental import pallas as pl
from jax.experimental.pallas import tpu as pltpu
from jax.sharding import PartitionSpec as P

MESH = pl.DeviceIdType.MESH
UNIT = 128
KBLK = 256
NEG = -1e30


def alibi_slopes(heads_n):
    closest = 2 ** int(math.floor(math.log2(heads_n)))
    base_rate = 2.0 ** (-8.0 / closest)
    slope_list = [base_rate ** (head_idx + 1) for head_idx in range(closest)]
    extra_rate = 2.0 ** (-4.0 / closest)
    slope_list = slope_list + [extra_rate ** (2 * head_idx + 1) for head_idx in range(min(closest, heads_n - closest))]
    return np.array(slope_list, dtype=np.float32)


def split_bf16(value):
    parts = []
    rest = np.float32(value)
    for _ in range(3):
        part = rest.astype(jnp.bfloat16).astype(np.float32)
        parts.append(float(part))
        rest = np.float32(rest - part)
    return parts


def layer_norm(x, gain, shift):
    mean = jnp.mean(x, axis=-1, keepdims=True)
    cent = x - mean
    var = jnp.mean(cent * cent, axis=-1, keepdims=True)
    return (cent * lax.rsqrt(var + 1e-5) * gain + shift).astype(jnp.bfloat16)


def gelu(x):
    inner = math.sqrt(2.0 / math.pi) * (x + 0.044715 * (x * x * x))
    return 0.5 * x * (1.0 + jnp.tanh(inner))


def kernel(heads_n, x_hbm, lens, wqkv_in, wout_in, wup_in, wdn_in, pack_in, out,
           wqkv, wout, wup, wdn, packs, rl_qkv, rl_out, rl_up, rl_dn, sw_qkv, sw_out, sw_up, sw_dn, sw_pack,
           xbuf, ybuf, kc0, kc1, kc2, kc3, vt0, vt1, vt2, vt3, kx, qaug, cmask, sbuf, abuf, ctx, hbuf, ubuf,
           sw_send, sw_recv, w_recv, fwd_send, rl_send, rl_recv, dir_send, pk_send, go,
           x0_sem, x_recv, s_send, od_send, da_send, db_send, fa_send, fb_send, fc_send,
           rr_recv, rr_send, o_recv):
    tp_n = 4
    units = xbuf.shape[0]
    model = xbuf.shape[2]
    seq = units * UNIT
    quarter = wqkv.shape[3]
    hid_q = wup.shape[2]
    pairs = model // 128

    r = lax.axis_index("tp")
    p = lax.axis_index("pp")
    x = p // 2
    c = p % 2
    odd = (r + (x + 1) // 2 + 1) % 2
    even_col = x + (1 - x % 2) * (2 - 2 * x)
    layer = odd * (2 * x + 1) + (1 - odd) * 2 * even_col
    home = odd == c
    moved = jnp.logical_and(c == 0, x % 2 == 0)
    early_row = r % 2 == 0
    rp, rm, ro = (r + 1) % tp_n, (r + 3) % tp_n, (r + 2) % tp_n
    partner = 2 * x + (1 - c)
    sig = 1 - 2 * c
    r_fwd = (r + sig + tp_n) % tp_n
    r_bwd = (r - sig + tp_n) % tp_n
    stage0, stage1 = 2 * x, 2 * x + 1
    x_n = 4

    def micro_of(row, core, lay):
        hops = (lay + 1) // 4
        return 2 * (((row + 8 - (1 - 2 * core) * hops) % tp_n) // 2) + core

    m = micro_of(r, c, layer)

    def rcopy(src, dst, ssem, rsem, **dev):
        return pltpu.make_async_remote_copy(src_ref=src, dst_ref=dst, send_sem=ssem, recv_sem=rsem,
                                            device_id=dev, device_id_type=MESH)

    barrier = pltpu.get_barrier_semaphore()
    for dr in range(tp_n):
        for dc in range(2):
            if dr or dc:
                pl.semaphore_signal(barrier, inc=1, device_id={"tp": (r + dr) % tp_n, "pp": 2 * x + (c + dc) % 2}, device_id_type=MESH)
    for dx in range(1, x_n):
        pl.semaphore_signal(barrier, inc=1, device_id={"pp": 2 * ((x + dx) % x_n) + c}, device_id_type=MESH)
    pl.semaphore_wait(barrier, 10)

    def wsrc(k, h=None):
        if k == 4:
            return pack_in
        if k == 0:
            return wqkv_in if h is None else wqkv_in.at[:, pl.ds(h * (model // 2), model // 2), :]
        ref = (None, wout_in, wup_in, wdn_in)[k]
        if h is None:
            return ref
        half = ref.shape[0] // 2
        return ref.at[pl.ds(h * half, half)]

    def wdst(k, q, h=None):
        if k == 0:
            return wqkv.at[q] if h is None else wqkv.at[q, :, pl.ds(h * (model // 2), model // 2), :]
        if k == 2:
            return wup.at[q] if h is None else wup.at[q, pl.ds(h * (model // 2), model // 2)]
        if k == 4:
            return packs.at[q]
        ref, rows = (wout, quarter) if k == 1 else (wdn, hid_q)
        if h is None:
            return ref.at[pl.ds(pl.multiple_of(q * rows, rows), rows)]
        half = rows // 2
        return ref.at[pl.ds(pl.multiple_of(q * rows + h * half, half), half)]

    def rl(k, h):
        return (rl_qkv, rl_out, rl_up, rl_dn)[k].at[h]

    def sw(k, h):
        if k == 4:
            return sw_pack
        if k == 0:
            return sw_qkv.at[:, pl.ds(h * (model // 2), model // 2), :]
        ref = (None, sw_out, sw_up, sw_dn)[k]
        half = ref.shape[0] // 2
        return ref.at[pl.ds(h * half, half)]

    def wwait(view, sem):
        rcopy(view, view, sem, sem, pp=partner).wait_recv()

    pieces = [(4, 0), (1, 0), (1, 1), (0, 0), (0, 1), (2, 0), (2, 1), (3, 0), (3, 1)]
    mats = pieces[1:]

    @pl.when(jnp.logical_and(moved, odd == 1))
    def _():
        for k, h in pieces:
            rcopy(wsrc(k, h), wdst(k, r, h), sw_send.at[k, h], sw_recv.at[k, h], pp=2 * (2 - x)).start()

    @pl.when(jnp.logical_and(moved, odd == 0))
    def _():
        for k, h in pieces:
            rcopy(wsrc(k, h), sw(k, h), sw_send.at[k, h], sw_recv.at[k, h], pp=2 * (2 - x)).start()

    @pl.when(jnp.logical_and(jnp.logical_not(moved), home))
    def _():
        for k, h in pieces:
            pltpu.make_async_copy(wsrc(k, h), wdst(k, r, h), sw_recv.at[k, h]).start()

    @pl.when(jnp.logical_not(jnp.logical_or(moved, home)))
    def _():
        for k, h in pieces:
            pltpu.make_async_copy(wsrc(k, h), sw(k, h), sw_recv.at[k, h]).start()

    @pl.when(layer == 0)
    def _():
        for u in range(units):
            pltpu.make_async_copy(x_hbm.at[m, pl.ds(u * UNIT, UNIT)], xbuf.at[u], x0_sem.at[u]).start()

    kc, vt = (kc0, kc1, kc2, kc3), (vt0, vt1, vt2, vt3)
    for ref in kc + vt:
        ref[...] = jnp.zeros_like(ref)
    length = lens[m]
    key = lax.broadcasted_iota(jnp.int32, (seq, 128), 0)
    lane = lax.broadcasted_iota(jnp.int32, (seq, 128), 1)
    high = (key // 256) * 256
    part = jnp.where(lane % 2 == 0, high, key - high).astype(jnp.float32)
    dead = jnp.where(key >= length, NEG, 0.0)
    kx[...] = jnp.where(lane < 6, part, jnp.where(lane == 6, dead, 0.0)).astype(jnp.bfloat16)
    slopes = alibi_slopes(heads_n)
    row = lax.broadcasted_iota(jnp.int32, (128, 256), 0)
    second = lax.broadcasted_iota(jnp.int32, (128, 256), 1) >= 128
    for pair in range(pairs):
        (h0, m0, l0), (h1, m1, l1) = split_bf16(slopes[2 * pair]), split_bf16(slopes[2 * pair + 1])
        hi, mid, low = jnp.where(second, h1, h0), jnp.where(second, m1, m0), jnp.where(second, l1, l0)
        val = jnp.where(row < 2, hi, jnp.where(row < 4, mid, jnp.where(row < 6, low, jnp.where(row == 6, 1.0, 0.0))))
        qaug[pair, 128:, :] = val.astype(jnp.bfloat16)
    kpos = lax.broadcasted_iota(jnp.int32, (KBLK, 256), 0)
    qpos = lax.broadcasted_iota(jnp.int32, (KBLK, 256), 1) % 128
    cmask[0] = jnp.where(kpos <= qpos, 0.0, NEG)
    cmask[1] = jnp.where(kpos <= qpos + 128, 0.0, NEG)

    def to_relay(k, h):
        rcopy(wdst(k, r, h), rl(k, h), rl_send.at[h, k], rl_recv.at[h, k], tp=(rp, rm)[h]).start()

    def to_partner(k, q, d, h):
        rcopy(wdst(k, q, h), wdst(k, q, h), fwd_send.at[d, k, h], w_recv.at[d, k, h], pp=partner).start()

    def hand_out():
        for k, h in pieces:
            wwait(sw(k, h), sw_recv.at[k, h])
            rcopy(sw(k, h), wdst(k, r, h), dir_send.at[0, k, h], w_recv.at[3, k, h], tp=rp).start()
            rcopy(sw(k, h), wdst(k, r, h), dir_send.at[1, k, h], w_recv.at[1, k, h], tp=rm).start()

    def relay_weights(k, h):
        wwait(rl(k, h), rl_recv.at[h, k])
        rcopy(rl(k, h), wdst(k, (rm, rp)[h], h), rl_send.at[h, k], w_recv.at[2, k, h], tp=(rp, rm)[h]).start()

    def from_partner():
        for d, q in ((0, r), (1, rp), (3, rm), (2, ro)):
            for k, h in pieces:
                wwait(wdst(k, q, h), w_recv.at[d, k, h])

    def sent(view, sem):
        rcopy(view, view, sem, sem, pp=partner).wait_send()

    def handed_out():
        for k, h in pieces:
            for d in range(2):
                sent(sw(k, h), dir_send.at[d, k, h])
        for k, h in mats:
            sent(rl(k, h), rl_send.at[h, k])

    @pl.when(home)
    def _():
        for k, h in pieces:
            wwait(wdst(k, r, h), sw_recv.at[k, h])
            if k == 4:
                rcopy(wdst(k, r), wdst(k, r), pk_send.at[0], w_recv.at[2, k, h], tp=ro).start()
            else:
                @pl.when(early_row)
                def _():
                    to_relay(k, h)
            to_partner(k, r, 0, h)

        @pl.when(jnp.logical_not(early_row))
        def _():
            pl.semaphore_wait(go, 1)
            for k, h in mats:
                to_relay(k, h)

        for k, h in pieces:
            for d, q in ((1, rp), (3, rm)):
                wwait(wdst(k, q, h), w_recv.at[d, k, h])
                to_partner(k, q, d, h)
        for k, h in pieces:
            wwait(wdst(k, ro, h), w_recv.at[2, k, h])
            to_partner(k, ro, 2, h)

    late_source = jnp.logical_and(early_row, jnp.logical_not(home))

    @pl.when(jnp.logical_not(jnp.logical_or(home, early_row)))
    def _():
        hand_out()
        for k, h in mats:
            relay_weights(k, h)
        handed_out()
        pl.semaphore_signal(go, inc=1, device_id={"pp": partner}, device_id_type=MESH)
        from_partner()

    @pl.when(late_source)
    def _():
        hand_out()
        from_partner()

    def out_at(mm, u):
        return out.at[mm, pl.ds(pl.multiple_of(u * UNIT, UNIT), UNIT)]

    m_a = micro_of(rm, 0, stage1)
    m_b = micro_of(rp, 1, stage1)
    relay = jnp.logical_and(odd == 0, jnp.logical_or(c == 1, x % 2 == 0))
    lag = min(5, units) * (x % 2) + (1 - x % 2) * (min(5, units) + (units - min(5, units)) * (x // 2))
    hold = min(4, units) * (1 - (x + 2) // 3) + (x + 2) // 3

    def relay_unit(v):
        wwait(out_at(m_a, v), rr_recv.at[0, v])
        rcopy(out_at(m_a, v), out_at(m_a, v), rr_send.at[0, v], o_recv, tp=rp).start()
        wwait(out_at(m_b, v), rr_recv.at[1, v])
        rcopy(out_at(m_b, v), out_at(m_b, v), rr_send.at[1, v], o_recv, tp=rm).start()

    def attention(nb, diag, tok):
        per_q = quarter // 128
        head_row = lax.broadcasted_iota(jnp.int32, (128, 128), 0) < 64

        def project(q):
            for j in range(3):
                o = jnp.dot(abuf[...], wqkv[q, j], preferred_element_type=jnp.float32)
                o = (o + packs[q, 7:8, j * quarter:(j + 1) * quarter]).astype(jnp.bfloat16)
                if j == 0:
                    o = o.astype(jnp.float32) * 0.125
                    for half in range(per_q):
                        q_t = o[:, half * 128:(half + 1) * 128].T
                        qaug[q * per_q + half, :128, :128] = jnp.where(head_row, q_t, 0.0).astype(jnp.bfloat16)
                        qaug[q * per_q + half, :128, 128:] = jnp.where(head_row, 0.0, q_t).astype(jnp.bfloat16)
                elif j == 1:
                    kc[q][tok, :] = o
                else:
                    vt[q][:, tok] = o.astype(jnp.float32).T.astype(jnp.bfloat16)

        def scores(pair):
            col = slice(pair % per_q * 128, (pair % per_q + 1) * 128)
            kq = kc[pair // per_q]
            top = None
            for b in range(nb):
                keys = jnp.concatenate([kq[b * KBLK:(b + 1) * KBLK, col], kx[b * KBLK:(b + 1) * KBLK, :]], axis=1)
                s = jnp.dot(keys, qaug[pair], preferred_element_type=jnp.float32)
                if b == nb - 1:
                    s = s + diag
                sbuf[pair % 2, b] = s
                peak = jnp.max(s, axis=0, keepdims=True)
                top = peak if top is None else jnp.maximum(top, peak)
            return top

        def weigh(pair, top):
            col = slice(pair % per_q * 128, (pair % per_q + 1) * 128)
            vq = vt[pair // per_q]
            total = None
            acc = None
            for b in range(nb):
                e = jnp.exp(sbuf[pair % 2, b] - top)
                part_sum = jnp.sum(e, axis=0, keepdims=True)
                total = part_sum if total is None else total + part_sum
                pv = jnp.dot(vq[col, b * KBLK:(b + 1) * KBLK], e.astype(jnp.bfloat16), preferred_element_type=jnp.float32)
                acc = pv if acc is None else acc + pv
            acc = acc * (1.0 / total)
            both = jnp.concatenate([acc[:64, :128], acc[64:, 128:]], axis=0)
            ctx[:, pair * 128:(pair + 1) * 128] = both.T.astype(jnp.bfloat16)

        project(0)
        top = None
        for pair in range(pairs + 1):
            if pair % per_q == 0 and pair // per_q + 1 < tp_n:
                project(pair // per_q + 1)
            later = scores(pair) if pair < pairs else None
            if pair > 0:
                weigh(pair - 1, top)
            top = later

    more = layer < 2 * x_n - 1
    nxt = (layer + 1) % (2 * x_n)
    half_n = nxt // 2
    x_next = half_n + (1 - nxt % 2) * (1 - half_n % 2) * (2 - 2 * half_n)
    p_next = 2 * x_next + c
    r_next = (r + (1 - odd) * (x % 2) * sig + tp_n) % tp_n

    def store_unit(v):
        @pl.when(odd == 1)
        def _():
            @pl.when(c == 0)
            def _():
                pltpu.make_async_copy(xbuf.at[v], out_at(m, v), o_recv).start()

            @pl.when(c == 1)
            def _():
                rcopy(xbuf.at[v], out_at(m, v), fa_send.at[v], o_recv, pp=partner).start()

            @pl.when(x % 2 == 1)
            def _():
                rcopy(xbuf.at[v], out_at(m, v), fb_send.at[v], o_recv, tp=r_fwd, pp=stage0).start()

            @pl.when(x % 2 == 0)
            def _():
                rcopy(xbuf.at[v], out_at(m, v), fb_send.at[v], rr_recv.at[c, v], tp=r_fwd, pp=stage0).start()
                rcopy(xbuf.at[v], out_at(m, v), fc_send.at[v], o_recv, tp=r_bwd, pp=stage0).start()

        @pl.when(home)
        def _():
            pltpu.make_async_copy(ybuf.at[v], out_at(m, v), o_recv).start()

        @pl.when(jnp.logical_not(home))
        def _():
            rcopy(ybuf.at[v], out_at(m, v), od_send.at[v], o_recv, pp=partner).start()

        rcopy(ybuf.at[v], out_at(m, v), da_send.at[v], o_recv, tp=r_bwd, pp=2 * x + odd).start()

        @pl.when(odd == 1)
        def _():
            rcopy(ybuf.at[v], out_at(m, v), db_send.at[v], rr_recv.at[c, v], tp=r_fwd, pp=stage1).start()

    stores = jnp.logical_or(odd == 1, x % 2 == 1)

    def unit_step(u, carry):
        tok = pl.ds(pl.multiple_of(u * UNIT, UNIT), UNIT)

        for group, (step0, step1) in (((0, 1), (1, 0)), ((2,), (3, 1)), ((3,), (5, 3))):
            now = jnp.logical_or(jnp.logical_and(layer == 0, u == min(step0, units - 1)),
                                 jnp.logical_or(jnp.logical_and(layer == 1, u == min(step1, units - 1)), jnp.logical_and(layer > 1, u == 0)))

            @pl.when(jnp.logical_and(late_source, now))
            def _():
                for k in group:
                    for h in range(2):
                        relay_weights(k, h)

        @pl.when(jnp.logical_and(relay, u >= lag))
        def _():
            relay_unit(u - lag)

        @pl.when(layer == 0)
        def _():
            pltpu.make_async_copy(x_hbm.at[m, tok], xbuf.at[u], x0_sem.at[u]).wait()

        @pl.when(layer > 0)
        def _():
            wwait(xbuf.at[u], x_recv.at[u])

        @pl.when(jnp.logical_and(stores, u >= hold))
        def _():
            store_unit(u - hold)

        xin = xbuf[u].astype(jnp.float32)
        abuf[...] = layer_norm(xin, packs[0, 0:1, :], packs[0, 1:2, :])
        for nb in range(1, seq // KBLK + 1):
            @pl.when(u // 2 + 1 == nb)
            def _():
                attention(nb, cmask[u % 2], tok)

        for n in range(model // quarter):
            cols = slice(n * quarter, (n + 1) * quarter)
            attn = jnp.dot(ctx[...], wout[:, cols], preferred_element_type=jnp.float32)
            hbuf[:, cols] = (xbuf[u, :, cols].astype(jnp.float32) + attn + packs[0, 2:3, cols]).astype(jnp.bfloat16)
        abuf[...] = layer_norm(hbuf[...].astype(jnp.float32), packs[0, 3:4, :], packs[0, 4:5, :])
        for q in range(tp_n):
            for n in range(hid_q // quarter):
                cols = slice(n * quarter, (n + 1) * quarter)
                up = jnp.dot(abuf[...], wup[q, :, cols], preferred_element_type=jnp.float32)
                up = up + packs[q, 6:7, cols]
                ubuf[:, q * hid_q + n * quarter:q * hid_q + (n + 1) * quarter] = gelu(up).astype(jnp.bfloat16)
        half_model = model // 2
        for n in range(2):
            cols = slice(n * half_model, (n + 1) * half_model)
            down = jnp.dot(ubuf[...], wdn[:, cols], preferred_element_type=jnp.float32)
            ybuf[u, :, cols] = (hbuf[:, cols].astype(jnp.float32) + down + packs[0, 5:6, cols]).astype(jnp.bfloat16)

            @pl.when(more)
            def _():
                rcopy(ybuf.at[u, :, cols], xbuf.at[u, :, cols], s_send.at[u], x_recv.at[u], tp=r_next, pp=p_next).start()

        return carry

    lax.fori_loop(0, units, unit_step, 0)

    @pl.when(stores)
    def _():
        def last(v, carry):
            store_unit(v)
            return carry

        lax.fori_loop(units - hold, units, last, 0)

    @pl.when(relay)
    def _():
        def rest(v, carry):
            relay_unit(v)
            return carry

        lax.fori_loop(units - lag, units, rest, 0)

    @pl.when(moved)
    def _():
        for k, h in pieces:
            sent(sw(k, h), sw_send.at[k, h])

    @pl.when(home)
    def _():
        sent(sw_pack, pk_send.at[0])
        for k, h in mats:
            sent(rl(k, h), rl_send.at[h, k])
        for d in range(4):
            for k, h in pieces:
                sent(sw(k, h), fwd_send.at[d, k, h])

    @pl.when(late_source)
    def _():
        handed_out()

    def drain(u, carry):
        @pl.when(more)
        def _():
            sent(ybuf.at[u], s_send.at[u])

        @pl.when(stores)
        def _():
            sent(ybuf.at[u], da_send.at[u])

            @pl.when(jnp.logical_not(home))
            def _():
                sent(ybuf.at[u], od_send.at[u])

        @pl.when(relay)
        def _():
            sent(ybuf.at[u], rr_send.at[0, u])
            sent(ybuf.at[u], rr_send.at[1, u])

        @pl.when(odd == 1)
        def _():
            sent(ybuf.at[u], db_send.at[u])
            sent(ybuf.at[u], fb_send.at[u])

            @pl.when(x % 2 == 0)
            def _():
                sent(ybuf.at[u], fc_send.at[u])

            @pl.when(c == 1)
            def _():
                sent(ybuf.at[u], fa_send.at[u])

        return carry

    lax.fori_loop(0, units, drain, 0)

    @pl.when(relay)
    def _():
        wwait(out.at[pl.ds(0, out.shape[0] // 2)], o_recv)

    @pl.when(jnp.logical_not(relay))
    def _():
        wwait(out, o_recv)


def solution(mesh):
    tp_size = mesh.shape['tp']
    in_specs = (P('dp'), P('dp'), P('pp'), P('pp'), P('pp', None, None, 'tp'), P('pp', None, 'tp', None), P('pp', 'tp', None), P('pp'), P('pp'), P('pp'), P('pp', None, 'tp'), P('pp', 'tp'), P('pp', 'tp', None), P('pp'))

    def per_device(x_in, seq_lens, ln1_gain, ln1_shift, w_qkv, b_qkv, w_out, b_out, ln2_gain, ln2_shift, w_up, b_up, w_down, b_down):
        micro_n, batch_n, seq_n, model_n = x_in.shape
        heads_n = b_qkv.shape[2] * tp_size
        quarter = w_qkv.shape[3]
        hid_q = w_up.shape[2]
        bf16, f32 = jnp.bfloat16, jnp.float32
        wqkv_t = jnp.transpose(w_qkv[0], (1, 0, 2))
        b_qkv_row = jnp.pad(b_qkv.reshape(1, 3 * quarter), ((0, 0), (0, model_n - 3 * quarter)))
        pack = jnp.concatenate([ln1_gain, ln1_shift, b_out, ln2_gain, ln2_shift, b_down, b_up, b_qkv_row], axis=0).astype(f32)
        units = seq_n // UNIT
        pairs = model_n // 128
        dma = pltpu.SemaphoreType.DMA
        anywhere = pl.BlockSpec(memory_space=pl.ANY)
        tokens = batch_n * seq_n
        out = pl.pallas_call(
            functools.partial(kernel, heads_n),
            out_shape=jax.ShapeDtypeStruct((micro_n, tokens, model_n), bf16),
            in_specs=[anywhere, pl.BlockSpec(memory_space=pltpu.SMEM)] + [anywhere] * 5,
            out_specs=anywhere,
            scratch_shapes=[
                pltpu.VMEM((tp_size, 3, model_n, quarter), bf16),
                pltpu.VMEM((tp_size * quarter, model_n), bf16),
                pltpu.VMEM((tp_size, model_n, hid_q), bf16),
                pltpu.VMEM((tp_size * hid_q, model_n), bf16),
                pltpu.VMEM((tp_size,) + pack.shape, f32),
                pltpu.VMEM((2, 3, model_n // 2, quarter), bf16),
                pltpu.VMEM((2, quarter // 2, model_n), bf16),
                pltpu.VMEM((2, model_n // 2, hid_q), bf16),
                pltpu.VMEM((2, hid_q // 2, model_n), bf16),
                pltpu.VMEM((3, model_n, quarter), bf16),
                pltpu.VMEM((quarter, model_n), bf16),
                pltpu.VMEM((model_n, hid_q), bf16),
                pltpu.VMEM((hid_q, model_n), bf16),
                pltpu.VMEM(pack.shape, f32),
                pltpu.VMEM((units, UNIT, model_n), bf16),
                pltpu.VMEM((units, UNIT, model_n), bf16),
                *[pltpu.VMEM((seq_n, quarter), bf16)] * tp_size,
                *[pltpu.VMEM((quarter, seq_n), bf16)] * tp_size,
                pltpu.VMEM((seq_n, 128), bf16),
                pltpu.VMEM((pairs, 256, 256), bf16),
                pltpu.VMEM((2, KBLK, 256), f32),
                pltpu.VMEM((2, seq_n // KBLK, KBLK, 256), f32),
                pltpu.VMEM((UNIT, model_n), bf16),
                pltpu.VMEM((UNIT, model_n), bf16),
                pltpu.VMEM((UNIT, model_n), bf16),
                pltpu.VMEM((UNIT, tp_size * hid_q), bf16),
                dma((5, 2)), dma((5, 2)), dma((4, 5, 2)), dma((4, 5, 2)), dma((2, 4)), dma((2, 4)), dma((2, 5, 2)), dma((1,)), pltpu.SemaphoreType.REGULAR,
                *[dma((units,))] * 9,
                dma((2, units)), dma((2, units)), dma,
            ],
            compiler_params=pltpu.CompilerParams(collective_id=0, has_side_effects=True, vmem_limit_bytes=63 * 1024 * 1024),
            cost_estimate=pl.CostEstimate(flops=30 * 10 ** 9, bytes_accessed=40 * 10 ** 6, transcendentals=10 ** 7),
        )(x_in.reshape(micro_n, tokens, model_n), seq_lens.reshape(micro_n * batch_n), wqkv_t, w_out[0], w_up[0], w_down[0], pack)
        return out.reshape((1,) + x_in.shape)

    return jax.shard_map(per_device, mesh=mesh, in_specs=in_specs, out_specs=P('pp', 'dp'), check_vma=False)
```

```python
import functools
import math

import jax
import jax.numpy as jnp
import numpy as np
from jax import lax
from jax.experimental import pallas as pl
from jax.experimental.pallas import tpu as pltpu
from jax.sharding import PartitionSpec as P

MESH = pl.DeviceIdType.MESH
UNIT = 128
KBLK = 256
NEG = -1e30


def alibi_slopes(heads_n):
    closest = 2 ** int(math.floor(math.log2(heads_n)))
    base_rate = 2.0 ** (-8.0 / closest)
    slope_list = [base_rate ** (head_idx + 1) for head_idx in range(closest)]
    extra_rate = 2.0 ** (-4.0 / closest)
    slope_list = slope_list + [extra_rate ** (2 * head_idx + 1) for head_idx in range(min(closest, heads_n - closest))]
    return np.array(slope_list, dtype=np.float32)


def split_bf16(value):
    parts = []
    rest = np.float32(value)
    for _ in range(3):
        part = rest.astype(jnp.bfloat16).astype(np.float32)
        parts.append(float(part))
        rest = np.float32(rest - part)
    return parts


def layer_norm(x, gain, shift):
    mean = jnp.mean(x, axis=-1, keepdims=True)
    cent = x - mean
    var = jnp.mean(cent * cent, axis=-1, keepdims=True)
    return (cent * lax.rsqrt(var + 1e-5) * gain + shift).astype(jnp.bfloat16)


def gelu(x):
    inner = math.sqrt(2.0 / math.pi) * (x + 0.044715 * (x * x * x))
    return 0.5 * x * (1.0 + jnp.tanh(inner))


def kernel(heads_n, x_hbm, lens, wqkv_in, wout_in, wup_in, wdn_in, pack_in, out,
           wqkv, wout, wup, wdn, packs, rl_qkv, rl_out, rl_up, rl_dn, sw_qkv, sw_out, sw_up, sw_dn, sw_pack,
           xbuf, ybuf, kc0, kc1, kc2, kc3, vt0, vt1, vt2, vt3, kx, qaug, cmask, sbuf, abuf, ctx, hbuf, ubuf,
           sw_send, sw_recv, w_recv, fwd_send, rl_send, rl_recv, dir_send, pk_send, go,
           x0_sem, x_recv, s_send, od_send, da_send, db_send, fa_send, fb_send, fc_send,
           rr_recv, rr_send, o_recv):
    tp_n = 4
    units = xbuf.shape[0]
    model = xbuf.shape[2]
    seq = units * UNIT
    quarter = wqkv.shape[3]
    hid_q = wup.shape[2]
    pairs = model // 128

    r = lax.axis_index("tp")
    p = lax.axis_index("pp")
    x = p // 2
    c = p % 2
    odd = (r + (x + 1) // 2 + 1) % 2
    even_col = x + (1 - x % 2) * (2 - 2 * x)
    layer = odd * (2 * x + 1) + (1 - odd) * 2 * even_col
    home = odd == c
    moved = jnp.logical_and(c == 0, x % 2 == 0)
    early_row = r % 2 == 0
    rp, rm, ro = (r + 1) % tp_n, (r + 3) % tp_n, (r + 2) % tp_n
    partner = 2 * x + (1 - c)
    sig = 1 - 2 * c
    r_fwd = (r + sig + tp_n) % tp_n
    r_bwd = (r - sig + tp_n) % tp_n
    stage0, stage1 = 2 * x, 2 * x + 1
    x_n = 4

    def micro_of(row, core, lay):
        hops = (lay + 1) // 4
        return 2 * (((row + 8 - (1 - 2 * core) * hops) % tp_n) // 2) + core

    m = micro_of(r, c, layer)

    def rcopy(src, dst, ssem, rsem, **dev):
        return pltpu.make_async_remote_copy(src_ref=src, dst_ref=dst, send_sem=ssem, recv_sem=rsem,
                                            device_id=dev, device_id_type=MESH)

    barrier = pltpu.get_barrier_semaphore()
    for dr in range(tp_n):
        for dc in range(2):
            if dr or dc:
                pl.semaphore_signal(barrier, inc=1, device_id={"tp": (r + dr) % tp_n, "pp": 2 * x + (c + dc) % 2}, device_id_type=MESH)
    for dx in range(1, x_n):
        pl.semaphore_signal(barrier, inc=1, device_id={"pp": 2 * ((x + dx) % x_n) + c}, device_id_type=MESH)
    pl.semaphore_wait(barrier, 10)

    def wsrc(k, h=None):
        if k == 4:
            return pack_in
        if k == 0:
            return wqkv_in if h is None else wqkv_in.at[:, pl.ds(h * (model // 2), model // 2), :]
        ref = (None, wout_in, wup_in, wdn_in)[k]
        if h is None:
            return ref
        half = ref.shape[0] // 2
        return ref.at[pl.ds(h * half, half)]

    def wdst(k, q, h=None):
        if k == 0:
            return wqkv.at[q] if h is None else wqkv.at[q, :, pl.ds(h * (model // 2), model // 2), :]
        if k == 2:
            return wup.at[q] if h is None else wup.at[q, pl.ds(h * (model // 2), model // 2)]
        if k == 4:
            return packs.at[q]
        ref, rows = (wout, quarter) if k == 1 else (wdn, hid_q)
        if h is None:
            return ref.at[pl.ds(pl.multiple_of(q * rows, rows), rows)]
        half = rows // 2
        return ref.at[pl.ds(pl.multiple_of(q * rows + h * half, half), half)]

    def rl(k, h):
        return (rl_qkv, rl_out, rl_up, rl_dn)[k].at[h]

    def sw(k, h):
        if k == 4:
            return sw_pack
        if k == 0:
            return sw_qkv.at[:, pl.ds(h * (model // 2), model // 2), :]
        ref = (None, sw_out, sw_up, sw_dn)[k]
        half = ref.shape[0] // 2
        return ref.at[pl.ds(h * half, half)]

    def wwait(view, sem):
        rcopy(view, view, sem, sem, pp=partner).wait_recv()

    pieces = [(4, 0), (1, 0), (1, 1), (0, 0), (0, 1), (2, 0), (2, 1), (3, 0), (3, 1)]
    mats = pieces[1:]

    @pl.when(jnp.logical_and(moved, odd == 1))
    def _():
        for k, h in pieces:
            rcopy(wsrc(k, h), wdst(k, r, h), sw_send.at[k, h], sw_recv.at[k, h], pp=2 * (2 - x)).start()

    @pl.when(jnp.logical_and(moved, odd == 0))
    def _():
        for k, h in pieces:
            rcopy(wsrc(k, h), sw(k, h), sw_send.at[k, h], sw_recv.at[k, h], pp=2 * (2 - x)).start()

    @pl.when(jnp.logical_and(jnp.logical_not(moved), home))
    def _():
        for k, h in pieces:
            pltpu.make_async_copy(wsrc(k, h), wdst(k, r, h), sw_recv.at[k, h]).start()

    @pl.when(jnp.logical_not(jnp.logical_or(moved, home)))
    def _():
        for k, h in pieces:
            pltpu.make_async_copy(wsrc(k, h), sw(k, h), sw_recv.at[k, h]).start()

    @pl.when(layer == 0)
    def _():
        for u in range(units):
            pltpu.make_async_copy(x_hbm.at[m, pl.ds(u * UNIT, UNIT)], xbuf.at[u], x0_sem.at[u]).start()

    kc, vt = (kc0, kc1, kc2, kc3), (vt0, vt1, vt2, vt3)
    for ref in kc + vt:
        ref[...] = jnp.zeros_like(ref)
    length = lens[m]
    key = lax.broadcasted_iota(jnp.int32, (seq, 128), 0)
    lane = lax.broadcasted_iota(jnp.int32, (seq, 128), 1)
    high = (key // 256) * 256
    part = jnp.where(lane % 2 == 0, high, key - high).astype(jnp.float32)
    dead = jnp.where(key >= length, NEG, 0.0)
    kx[...] = jnp.where(lane < 6, part, jnp.where(lane == 6, dead, 0.0)).astype(jnp.bfloat16)
    slopes = alibi_slopes(heads_n)
    row = lax.broadcasted_iota(jnp.int32, (128, 256), 0)
    second = lax.broadcasted_iota(jnp.int32, (128, 256), 1) >= 128
    for pair in range(pairs):
        (h0, m0, l0), (h1, m1, l1) = split_bf16(slopes[2 * pair]), split_bf16(slopes[2 * pair + 1])
        hi, mid, low = jnp.where(second, h1, h0), jnp.where(second, m1, m0), jnp.where(second, l1, l0)
        val = jnp.where(row < 2, hi, jnp.where(row < 4, mid, jnp.where(row < 6, low, jnp.where(row == 6, 1.0, 0.0))))
        qaug[pair, 128:, :] = val.astype(jnp.bfloat16)
    kpos = lax.broadcasted_iota(jnp.int32, (KBLK, 256), 0)
    qpos = lax.broadcasted_iota(jnp.int32, (KBLK, 256), 1) % 128
    cmask[0] = jnp.where(kpos <= qpos, 0.0, NEG)
    cmask[1] = jnp.where(kpos <= qpos + 128, 0.0, NEG)

    def to_relay(k, h):
        rcopy(wdst(k, r, h), rl(k, h), rl_send.at[h, k], rl_recv.at[h, k], tp=(rp, rm)[h]).start()

    def to_partner(k, q, d, h):
        rcopy(wdst(k, q, h), wdst(k, q, h), fwd_send.at[d, k, h], w_recv.at[d, k, h], pp=partner).start()

    def hand_out(behind=()):
        for i, (k, h) in enumerate(pieces):
            wwait(sw(k, h), sw_recv.at[k, h])
            rcopy(sw(k, h), wdst(k, r, h), dir_send.at[0, k, h], w_recv.at[3, k, h], tp=rp).start()
            rcopy(sw(k, h), wdst(k, r, h), dir_send.at[1, k, h], w_recv.at[1, k, h], tp=rm).start()
            if 3 <= i < len(behind) + 3:
                relay_weights(*behind[i - 3])

    def relay_weights(k, h):
        wwait(rl(k, h), rl_recv.at[h, k])
        rcopy(rl(k, h), wdst(k, (rm, rp)[h], h), rl_send.at[h, k], w_recv.at[2, k, h], tp=(rp, rm)[h]).start()

    def from_partner():
        for d, q in ((0, r), (1, rp), (3, rm), (2, ro)):
            for k, h in pieces:
                wwait(wdst(k, q, h), w_recv.at[d, k, h])

    def sent(view, sem):
        rcopy(view, view, sem, sem, pp=partner).wait_send()

    def handed_out():
        for k, h in pieces:
            for d in range(2):
                sent(sw(k, h), dir_send.at[d, k, h])
        for k, h in mats:
            sent(rl(k, h), rl_send.at[h, k])

    @pl.when(home)
    def _():
        for k, h in pieces:
            wwait(wdst(k, r, h), sw_recv.at[k, h])
            if k == 4:
                rcopy(wdst(k, r), wdst(k, r), pk_send.at[0], w_recv.at[2, k, h], tp=ro).start()
            else:
                @pl.when(early_row)
                def _():
                    to_relay(k, h)
            to_partner(k, r, 0, h)

        @pl.when(jnp.logical_not(early_row))
        def _():
            pl.semaphore_wait(go, 1)
            for k, h in mats:
                to_relay(k, h)

        for k, h in pieces:
            for d, q in ((1, rp), (3, rm)):
                wwait(wdst(k, q, h), w_recv.at[d, k, h])
                to_partner(k, q, d, h)
        for k, h in pieces:
            wwait(wdst(k, ro, h), w_recv.at[2, k, h])
            to_partner(k, ro, 2, h)

    late_source = jnp.logical_and(early_row, jnp.logical_not(home))

    @pl.when(jnp.logical_not(jnp.logical_or(home, early_row)))
    def _():
        hand_out(mats)
        for k, h in mats[len(pieces) - 3:]:
            relay_weights(k, h)
        handed_out()
        pl.semaphore_signal(go, inc=1, device_id={"pp": partner}, device_id_type=MESH)
        from_partner()

    @pl.when(late_source)
    def _():
        hand_out()
        from_partner()

    def out_at(mm, u):
        return out.at[mm, pl.ds(pl.multiple_of(u * UNIT, UNIT), UNIT)]

    m_a = micro_of(rm, 0, stage1)
    m_b = micro_of(rp, 1, stage1)
    relay = jnp.logical_and(odd == 0, jnp.logical_or(c == 1, x % 2 == 0))
    lag = min(5, units) * (x % 2) + (1 - x % 2) * (min(5, units) + (units - min(5, units)) * (x // 2))
    hold = min(4, units) * (1 - (x + 2) // 3) + (x + 2) // 3

    def relay_unit(v):
        wwait(out_at(m_a, v), rr_recv.at[0, v])
        rcopy(out_at(m_a, v), out_at(m_a, v), rr_send.at[0, v], o_recv, tp=rp).start()
        wwait(out_at(m_b, v), rr_recv.at[1, v])
        rcopy(out_at(m_b, v), out_at(m_b, v), rr_send.at[1, v], o_recv, tp=rm).start()

    def attention(nb, diag, tok):
        per_q = quarter // 128
        head_row = lax.broadcasted_iota(jnp.int32, (128, 128), 0) < 64

        def project(q):
            for j in range(3):
                o = jnp.dot(abuf[...], wqkv[q, j], preferred_element_type=jnp.float32)
                o = (o + packs[q, 7:8, j * quarter:(j + 1) * quarter]).astype(jnp.bfloat16)
                if j == 0:
                    o = o.astype(jnp.float32) * 0.125
                    for half in range(per_q):
                        q_t = o[:, half * 128:(half + 1) * 128].T
                        qaug[q * per_q + half, :128, :128] = jnp.where(head_row, q_t, 0.0).astype(jnp.bfloat16)
                        qaug[q * per_q + half, :128, 128:] = jnp.where(head_row, 0.0, q_t).astype(jnp.bfloat16)
                elif j == 1:
                    kc[q][tok, :] = o
                else:
                    vt[q][:, tok] = o.astype(jnp.float32).T.astype(jnp.bfloat16)

        def scores(pair):
            col = slice(pair % per_q * 128, (pair % per_q + 1) * 128)
            kq = kc[pair // per_q]
            top = None
            for b in range(nb):
                keys = jnp.concatenate([kq[b * KBLK:(b + 1) * KBLK, col], kx[b * KBLK:(b + 1) * KBLK, :]], axis=1)
                s = jnp.dot(keys, qaug[pair], preferred_element_type=jnp.float32)
                if b == nb - 1:
                    s = s + diag
                sbuf[pair % 2, b] = s
                peak = jnp.max(s, axis=0, keepdims=True)
                top = peak if top is None else jnp.maximum(top, peak)
            return top

        def weigh(pair, top):
            col = slice(pair % per_q * 128, (pair % per_q + 1) * 128)
            vq = vt[pair // per_q]
            total = None
            acc = None
            for b in range(nb):
                e = jnp.exp(sbuf[pair % 2, b] - top)
                part_sum = jnp.sum(e, axis=0, keepdims=True)
                total = part_sum if total is None else total + part_sum
                pv = jnp.dot(vq[col, b * KBLK:(b + 1) * KBLK], e.astype(jnp.bfloat16), preferred_element_type=jnp.float32)
                acc = pv if acc is None else acc + pv
            acc = acc * (1.0 / total)
            both = jnp.concatenate([acc[:64, :128], acc[64:, 128:]], axis=0)
            ctx[:, pair * 128:(pair + 1) * 128] = both.T.astype(jnp.bfloat16)

        project(0)
        top = None
        for pair in range(pairs + 1):
            if pair % per_q == 0 and pair // per_q + 1 < tp_n:
                project(pair // per_q + 1)
            later = scores(pair) if pair < pairs else None
            if pair > 0:
                weigh(pair - 1, top)
            top = later

    more = layer < 2 * x_n - 1
    nxt = (layer + 1) % (2 * x_n)
    half_n = nxt // 2
    x_next = half_n + (1 - nxt % 2) * (1 - half_n % 2) * (2 - 2 * half_n)
    p_next = 2 * x_next + c
    r_next = (r + (1 - odd) * (x % 2) * sig + tp_n) % tp_n

    def store_input(v):
        @pl.when(odd == 1)
        def _():
            @pl.when(c == 0)
            def _():
                pltpu.make_async_copy(xbuf.at[v], out_at(m, v), o_recv).start()

            @pl.when(c == 1)
            def _():
                rcopy(xbuf.at[v], out_at(m, v), fa_send.at[v], o_recv, pp=partner).start()

            @pl.when(x % 2 == 1)
            def _():
                rcopy(xbuf.at[v], out_at(m, v), fb_send.at[v], o_recv, tp=r_fwd, pp=stage0).start()

            @pl.when(x % 2 == 0)
            def _():
                rcopy(xbuf.at[v], out_at(m, v), fb_send.at[v], rr_recv.at[c, v], tp=r_fwd, pp=stage0).start()
                rcopy(xbuf.at[v], out_at(m, v), fc_send.at[v], o_recv, tp=r_bwd, pp=stage0).start()

    def store_unit(v):
        @pl.when(home)
        def _():
            pltpu.make_async_copy(ybuf.at[v], out_at(m, v), o_recv).start()

        @pl.when(jnp.logical_not(home))
        def _():
            rcopy(ybuf.at[v], out_at(m, v), od_send.at[v], o_recv, pp=partner).start()

        rcopy(ybuf.at[v], out_at(m, v), da_send.at[v], o_recv, tp=r_bwd, pp=2 * x + odd).start()

        @pl.when(odd == 1)
        def _():
            rcopy(ybuf.at[v], out_at(m, v), db_send.at[v], rr_recv.at[c, v], tp=r_fwd, pp=stage1).start()

    stores = jnp.logical_or(odd == 1, x % 2 == 1)

    def unit_step(u, carry):
        tok = pl.ds(pl.multiple_of(u * UNIT, UNIT), UNIT)

        for group, (step0, step1) in (((0, 1), (2, 0)), ((2,), (4, 1)), ((3,), (6, 3))):
            now = jnp.logical_or(jnp.logical_and(layer == 0, u == min(step0, units - 1)),
                                 jnp.logical_or(jnp.logical_and(layer == 1, u == min(step1, units - 1)), jnp.logical_and(layer > 1, u == 0)))

            @pl.when(jnp.logical_and(late_source, now))
            def _():
                for k in group:
                    for h in range(2):
                        relay_weights(k, h)

        @pl.when(jnp.logical_and(relay, u >= lag))
        def _():
            relay_unit(u - lag)

        @pl.when(layer == 0)
        def _():
            pltpu.make_async_copy(x_hbm.at[m, tok], xbuf.at[u], x0_sem.at[u]).wait()

        @pl.when(layer > 0)
        def _():
            wwait(xbuf.at[u], x_recv.at[u])

        @pl.when(jnp.logical_and(stores, u >= hold - 1))
        def _():
            store_input(u - hold + 1)

        @pl.when(jnp.logical_and(stores, u >= hold))
        def _():
            store_unit(u - hold)

        xin = xbuf[u].astype(jnp.float32)
        abuf[...] = layer_norm(xin, packs[0, 0:1, :], packs[0, 1:2, :])
        for nb in range(1, seq // KBLK + 1):
            @pl.when(u // 2 + 1 == nb)
            def _():
                attention(nb, cmask[u % 2], tok)

        for n in range(model // quarter):
            cols = slice(n * quarter, (n + 1) * quarter)
            attn = jnp.dot(ctx[...], wout[:, cols], preferred_element_type=jnp.float32)
            hbuf[:, cols] = (xbuf[u, :, cols].astype(jnp.float32) + attn + packs[0, 2:3, cols]).astype(jnp.bfloat16)
        abuf[...] = layer_norm(hbuf[...].astype(jnp.float32), packs[0, 3:4, :], packs[0, 4:5, :])
        for q in range(tp_n):
            for n in range(hid_q // quarter):
                cols = slice(n * quarter, (n + 1) * quarter)
                up = jnp.dot(abuf[...], wup[q, :, cols], preferred_element_type=jnp.float32)
                up = up + packs[q, 6:7, cols]
                ubuf[:, q * hid_q + n * quarter:q * hid_q + (n + 1) * quarter] = gelu(up).astype(jnp.bfloat16)
        half_model = model // 2
        for n in range(2):
            cols = slice(n * half_model, (n + 1) * half_model)
            down = jnp.dot(ubuf[...], wdn[:, cols], preferred_element_type=jnp.float32)
            ybuf[u, :, cols] = (hbuf[:, cols].astype(jnp.float32) + down + packs[0, 5:6, cols]).astype(jnp.bfloat16)

            @pl.when(more)
            def _():
                rcopy(ybuf.at[u, :, cols], xbuf.at[u, :, cols], s_send.at[u], x_recv.at[u], tp=r_next, pp=p_next).start()

        return carry

    lax.fori_loop(0, units, unit_step, 0)

    @pl.when(stores)
    def _():
        def last(v, carry):
            store_unit(v)
            return carry

        lax.fori_loop(units - hold, units, last, 0)

        def last_input(v, carry):
            store_input(v)
            return carry

        lax.fori_loop(units - hold + 1, units, last_input, 0)

    @pl.when(relay)
    def _():
        def rest(v, carry):
            relay_unit(v)
            return carry

        lax.fori_loop(units - lag, units, rest, 0)

    @pl.when(moved)
    def _():
        for k, h in pieces:
            sent(sw(k, h), sw_send.at[k, h])

    @pl.when(home)
    def _():
        sent(sw_pack, pk_send.at[0])
        for k, h in mats:
            sent(rl(k, h), rl_send.at[h, k])
        for d in range(4):
            for k, h in pieces:
                sent(sw(k, h), fwd_send.at[d, k, h])

    @pl.when(late_source)
    def _():
        handed_out()

    def drain(u, carry):
        @pl.when(more)
        def _():
            sent(ybuf.at[u], s_send.at[u])

        @pl.when(stores)
        def _():
            sent(ybuf.at[u], da_send.at[u])

            @pl.when(jnp.logical_not(home))
            def _():
                sent(ybuf.at[u], od_send.at[u])

        @pl.when(relay)
        def _():
            sent(ybuf.at[u], rr_send.at[0, u])
            sent(ybuf.at[u], rr_send.at[1, u])

        @pl.when(odd == 1)
        def _():
            sent(ybuf.at[u], db_send.at[u])
            sent(ybuf.at[u], fb_send.at[u])

            @pl.when(x % 2 == 0)
            def _():
                sent(ybuf.at[u], fc_send.at[u])

            @pl.when(c == 1)
            def _():
                sent(ybuf.at[u], fa_send.at[u])

        return carry

    lax.fori_loop(0, units, drain, 0)

    @pl.when(relay)
    def _():
        wwait(out.at[pl.ds(0, out.shape[0] // 2)], o_recv)

    @pl.when(jnp.logical_not(relay))
    def _():
        wwait(out, o_recv)


def solution(mesh):
    tp_size = mesh.shape['tp']
    in_specs = (P('dp'), P('dp'), P('pp'), P('pp'), P('pp', None, None, 'tp'), P('pp', None, 'tp', None), P('pp', 'tp', None), P('pp'), P('pp'), P('pp'), P('pp', None, 'tp'), P('pp', 'tp'), P('pp', 'tp', None), P('pp'))

    def per_device(x_in, seq_lens, ln1_gain, ln1_shift, w_qkv, b_qkv, w_out, b_out, ln2_gain, ln2_shift, w_up, b_up, w_down, b_down):
        micro_n, batch_n, seq_n, model_n = x_in.shape
        heads_n = b_qkv.shape[2] * tp_size
        quarter = w_qkv.shape[3]
        hid_q = w_up.shape[2]
        bf16, f32 = jnp.bfloat16, jnp.float32
        wqkv_t = jnp.transpose(w_qkv[0], (1, 0, 2))
        b_qkv_row = jnp.pad(b_qkv.reshape(1, 3 * quarter), ((0, 0), (0, model_n - 3 * quarter)))
        pack = jnp.concatenate([ln1_gain, ln1_shift, b_out, ln2_gain, ln2_shift, b_down, b_up, b_qkv_row], axis=0).astype(f32)
        units = seq_n // UNIT
        pairs = model_n // 128
        dma = pltpu.SemaphoreType.DMA
        anywhere = pl.BlockSpec(memory_space=pl.ANY)
        tokens = batch_n * seq_n
        out = pl.pallas_call(
            functools.partial(kernel, heads_n),
            out_shape=jax.ShapeDtypeStruct((micro_n, tokens, model_n), bf16),
            in_specs=[anywhere, pl.BlockSpec(memory_space=pltpu.SMEM)] + [anywhere] * 5,
            out_specs=anywhere,
            scratch_shapes=[
                pltpu.VMEM((tp_size, 3, model_n, quarter), bf16),
                pltpu.VMEM((tp_size * quarter, model_n), bf16),
                pltpu.VMEM((tp_size, model_n, hid_q), bf16),
                pltpu.VMEM((tp_size * hid_q, model_n), bf16),
                pltpu.VMEM((tp_size,) + pack.shape, f32),
                pltpu.VMEM((2, 3, model_n // 2, quarter), bf16),
                pltpu.VMEM((2, quarter // 2, model_n), bf16),
                pltpu.VMEM((2, model_n // 2, hid_q), bf16),
                pltpu.VMEM((2, hid_q // 2, model_n), bf16),
                pltpu.VMEM((3, model_n, quarter), bf16),
                pltpu.VMEM((quarter, model_n), bf16),
                pltpu.VMEM((model_n, hid_q), bf16),
                pltpu.VMEM((hid_q, model_n), bf16),
                pltpu.VMEM(pack.shape, f32),
                pltpu.VMEM((units, UNIT, model_n), bf16),
                pltpu.VMEM((units, UNIT, model_n), bf16),
                *[pltpu.VMEM((seq_n, quarter), bf16)] * tp_size,
                *[pltpu.VMEM((quarter, seq_n), bf16)] * tp_size,
                pltpu.VMEM((seq_n, 128), bf16),
                pltpu.VMEM((pairs, 256, 256), bf16),
                pltpu.VMEM((2, KBLK, 256), f32),
                pltpu.VMEM((2, seq_n // KBLK, KBLK, 256), f32),
                pltpu.VMEM((UNIT, model_n), bf16),
                pltpu.VMEM((UNIT, model_n), bf16),
                pltpu.VMEM((UNIT, model_n), bf16),
                pltpu.VMEM((UNIT, tp_size * hid_q), bf16),
                dma((5, 2)), dma((5, 2)), dma((4, 5, 2)), dma((4, 5, 2)), dma((2, 4)), dma((2, 4)), dma((2, 5, 2)), dma((1,)), pltpu.SemaphoreType.REGULAR,
                *[dma((units,))] * 9,
                dma((2, units)), dma((2, units)), dma,
            ],
            compiler_params=pltpu.CompilerParams(collective_id=0, has_side_effects=True, vmem_limit_bytes=63 * 1024 * 1024),
            cost_estimate=pl.CostEstimate(flops=30 * 10 ** 9, bytes_accessed=40 * 10 ** 6, transcendentals=10 ** 7),
        )(x_in.reshape(micro_n, tokens, model_n), seq_lens.reshape(micro_n * batch_n), wqkv_t, w_out[0], w_up[0], w_down[0], pack)
        return out.reshape((1,) + x_in.shape)

    return jax.shard_map(per_device, mesh=mesh, in_specs=in_specs, out_specs=P('pp', 'dp'), check_vma=False)
```

```python
import functools
import math

import jax
import jax.numpy as jnp
import numpy as np
from jax import lax
from jax.experimental import pallas as pl
from jax.experimental.pallas import tpu as pltpu
from jax.sharding import PartitionSpec as P

MESH = pl.DeviceIdType.MESH
UNIT = 128
KBLK = 256
NEG = -1e30


def alibi_slopes(heads_n):
    closest = 2 ** int(math.floor(math.log2(heads_n)))
    base_rate = 2.0 ** (-8.0 / closest)
    slope_list = [base_rate ** (head_idx + 1) for head_idx in range(closest)]
    extra_rate = 2.0 ** (-4.0 / closest)
    slope_list = slope_list + [extra_rate ** (2 * head_idx + 1) for head_idx in range(min(closest, heads_n - closest))]
    return np.array(slope_list, dtype=np.float32)


def split_bf16(value):
    parts = []
    rest = np.float32(value)
    for _ in range(3):
        part = rest.astype(jnp.bfloat16).astype(np.float32)
        parts.append(float(part))
        rest = np.float32(rest - part)
    return parts


def layer_norm(x, gain, shift):
    mean = jnp.mean(x, axis=-1, keepdims=True)
    cent = x - mean
    var = jnp.mean(cent * cent, axis=-1, keepdims=True)
    return (cent * lax.rsqrt(var + 1e-5) * gain + shift).astype(jnp.bfloat16)


def gelu(x):
    inner = math.sqrt(2.0 / math.pi) * (x + 0.044715 * (x * x * x))
    return 0.5 * x * (1.0 + jnp.tanh(inner))


def kernel(heads_n, x_hbm, lens, wqkv_in, wout_in, wup_in, wdn_in, pack_in, out,
           wqkv, wout, wup, wdn, packs, rl_qkv, rl_out, rl_up, rl_dn, sw_qkv, sw_out, sw_up, sw_dn, sw_pack,
           xbuf, ybuf, kc0, kc1, kc2, kc3, vt0, vt1, vt2, vt3, kx, qaug, cmask, sbuf, abuf, ctx, hbuf, ubuf,
           sw_send, sw_recv, w_recv, fwd_send, rl_send, rl_recv, dir_send, pk_send, go,
           x0_sem, x_recv, s_send, od_send, da_send, db_send, fa_send, fb_send, fc_send,
           rr_recv, rr_send, o_recv):
    tp_n = 4
    units = xbuf.shape[0]
    model = xbuf.shape[2]
    seq = units * UNIT
    quarter = wqkv.shape[3]
    hid_q = wup.shape[2]
    pairs = model // 128

    r = lax.axis_index("tp")
    p = lax.axis_index("pp")
    x = p // 2
    c = p % 2
    odd = (r + (x + 1) // 2 + 1) % 2
    even_col = x + (1 - x % 2) * (2 - 2 * x)
    layer = odd * (2 * x + 1) + (1 - odd) * 2 * even_col
    home = odd == c
    moved = jnp.logical_and(c == 0, x % 2 == 0)
    level = x == 1
    ahead = jnp.logical_or(r % 2 == 0, level)
    rp, rm, ro = (r + 1) % tp_n, (r + 3) % tp_n, (r + 2) % tp_n
    partner = 2 * x + (1 - c)
    sig = 1 - 2 * c
    r_fwd = (r + sig + tp_n) % tp_n
    r_bwd = (r - sig + tp_n) % tp_n
    stage0, stage1 = 2 * x, 2 * x + 1
    x_n = 4

    def micro_of(row, core, lay):
        hops = (lay + 1) // 4
        return 2 * (((row + 8 - (1 - 2 * core) * hops) % tp_n) // 2) + core

    m = micro_of(r, c, layer)

    def rcopy(src, dst, ssem, rsem, **dev):
        return pltpu.make_async_remote_copy(src_ref=src, dst_ref=dst, send_sem=ssem, recv_sem=rsem,
                                            device_id=dev, device_id_type=MESH)

    barrier = pltpu.get_barrier_semaphore()
    for dr in range(tp_n):
        for dc in range(2):
            if dr or dc:
                pl.semaphore_signal(barrier, inc=1, device_id={"tp": (r + dr) % tp_n, "pp": 2 * x + (c + dc) % 2}, device_id_type=MESH)
    for dx in range(1, x_n):
        pl.semaphore_signal(barrier, inc=1, device_id={"pp": 2 * ((x + dx) % x_n) + c}, device_id_type=MESH)
    pl.semaphore_wait(barrier, 10)

    def wsrc(k, h=None):
        if k == 4:
            return pack_in
        if k == 0:
            return wqkv_in if h is None else wqkv_in.at[:, pl.ds(h * (model // 2), model // 2), :]
        ref = (None, wout_in, wup_in, wdn_in)[k]
        if h is None:
            return ref
        half = ref.shape[0] // 2
        return ref.at[pl.ds(h * half, half)]

    def wdst(k, q, h=None):
        if k == 0:
            return wqkv.at[q] if h is None else wqkv.at[q, :, pl.ds(h * (model // 2), model // 2), :]
        if k == 2:
            return wup.at[q] if h is None else wup.at[q, pl.ds(h * (model // 2), model // 2)]
        if k == 4:
            return packs.at[q]
        ref, rows = (wout, quarter) if k == 1 else (wdn, hid_q)
        if h is None:
            return ref.at[pl.ds(pl.multiple_of(q * rows, rows), rows)]
        half = rows // 2
        return ref.at[pl.ds(pl.multiple_of(q * rows + h * half, half), half)]

    def rl(k, h):
        return (rl_qkv, rl_out, rl_up, rl_dn)[k].at[h]

    def sw(k, h):
        if k == 4:
            return sw_pack
        if k == 0:
            return sw_qkv.at[:, pl.ds(h * (model // 2), model // 2), :]
        ref = (None, sw_out, sw_up, sw_dn)[k]
        half = ref.shape[0] // 2
        return ref.at[pl.ds(h * half, half)]

    def wwait(view, sem):
        rcopy(view, view, sem, sem, pp=partner).wait_recv()

    pieces = [(4, 0), (1, 0), (1, 1), (0, 0), (0, 1), (2, 0), (2, 1), (3, 0), (3, 1)]
    mats = pieces[1:]

    @pl.when(jnp.logical_and(moved, odd == 1))
    def _():
        for k, h in pieces:
            rcopy(wsrc(k, h), wdst(k, r, h), sw_send.at[k, h], sw_recv.at[k, h], pp=2 * (2 - x)).start()

    @pl.when(jnp.logical_and(moved, odd == 0))
    def _():
        for k, h in pieces:
            rcopy(wsrc(k, h), sw(k, h), sw_send.at[k, h], sw_recv.at[k, h], pp=2 * (2 - x)).start()

    @pl.when(jnp.logical_and(jnp.logical_not(moved), home))
    def _():
        for k, h in pieces:
            pltpu.make_async_copy(wsrc(k, h), wdst(k, r, h), sw_recv.at[k, h]).start()

    @pl.when(jnp.logical_not(jnp.logical_or(moved, home)))
    def _():
        for k, h in pieces:
            pltpu.make_async_copy(wsrc(k, h), sw(k, h), sw_recv.at[k, h]).start()

    @pl.when(layer == 0)
    def _():
        for u in range(units):
            pltpu.make_async_copy(x_hbm.at[m, pl.ds(u * UNIT, UNIT)], xbuf.at[u], x0_sem.at[u]).start()

    kc, vt = (kc0, kc1, kc2, kc3), (vt0, vt1, vt2, vt3)
    for ref in kc + vt:
        ref[...] = jnp.zeros_like(ref)
    length = lens[m]
    key = lax.broadcasted_iota(jnp.int32, (seq, 128), 0)
    lane = lax.broadcasted_iota(jnp.int32, (seq, 128), 1)
    high = (key // 256) * 256
    part = jnp.where(lane % 2 == 0, high, key - high).astype(jnp.float32)
    dead = jnp.where(key >= length, NEG, 0.0)
    kx[...] = jnp.where(lane < 6, part, jnp.where(lane == 6, dead, 0.0)).astype(jnp.bfloat16)
    slopes = alibi_slopes(heads_n)
    row = lax.broadcasted_iota(jnp.int32, (128, 256), 0)
    second = lax.broadcasted_iota(jnp.int32, (128, 256), 1) >= 128
    for pair in range(pairs):
        (h0, m0, l0), (h1, m1, l1) = split_bf16(slopes[2 * pair]), split_bf16(slopes[2 * pair + 1])
        hi, mid, low = jnp.where(second, h1, h0), jnp.where(second, m1, m0), jnp.where(second, l1, l0)
        val = jnp.where(row < 2, hi, jnp.where(row < 4, mid, jnp.where(row < 6, low, jnp.where(row == 6, 1.0, 0.0))))
        qaug[pair, 128:, :] = val.astype(jnp.bfloat16)
    kpos = lax.broadcasted_iota(jnp.int32, (KBLK, 256), 0)
    qpos = lax.broadcasted_iota(jnp.int32, (KBLK, 256), 1) % 128
    cmask[0] = jnp.where(kpos <= qpos, 0.0, NEG)
    cmask[1] = jnp.where(kpos <= qpos + 128, 0.0, NEG)

    def to_relay(k, h):
        rcopy(wdst(k, r, h), rl(k, h), rl_send.at[h, k], rl_recv.at[h, k], tp=(rp, rm)[h]).start()

    def to_partner(k, q, d, h):
        rcopy(wdst(k, q, h), wdst(k, q, h), fwd_send.at[d, k, h], w_recv.at[d, k, h], pp=partner).start()

    def hand_out(behind=()):
        for i, (k, h) in enumerate(pieces):
            wwait(sw(k, h), sw_recv.at[k, h])
            rcopy(sw(k, h), wdst(k, r, h), dir_send.at[0, k, h], w_recv.at[3, k, h], tp=rp).start()
            rcopy(sw(k, h), wdst(k, r, h), dir_send.at[1, k, h], w_recv.at[1, k, h], tp=rm).start()
            if 3 <= i < len(behind) + 3:
                relay_weights(*behind[i - 3])

    def relay_weights(k, h):
        wwait(rl(k, h), rl_recv.at[h, k])
        rcopy(rl(k, h), wdst(k, (rm, rp)[h], h), rl_send.at[h, k], w_recv.at[2, k, h], tp=(rp, rm)[h]).start()

    def from_partner():
        for d, q in ((0, r), (1, rp), (3, rm), (2, ro)):
            for k, h in pieces:
                wwait(wdst(k, q, h), w_recv.at[d, k, h])

    def sent(view, sem):
        rcopy(view, view, sem, sem, pp=partner).wait_send()

    def handed_out():
        for k, h in pieces:
            for d in range(2):
                sent(sw(k, h), dir_send.at[d, k, h])
        for k, h in mats:
            sent(rl(k, h), rl_send.at[h, k])

    @pl.when(home)
    def _():
        for k, h in pieces:
            wwait(wdst(k, r, h), sw_recv.at[k, h])
            if k == 4:
                rcopy(wdst(k, r), wdst(k, r), pk_send.at[0], w_recv.at[2, k, h], tp=ro).start()
            else:
                @pl.when(ahead)
                def _():
                    to_relay(k, h)
            to_partner(k, r, 0, h)

        @pl.when(jnp.logical_not(ahead))
        def _():
            pl.semaphore_wait(go, 1)
            for k, h in mats:
                to_relay(k, h)

        for k, h in pieces:
            for d, q in ((1, rp), (3, rm)):
                wwait(wdst(k, q, h), w_recv.at[d, k, h])
                to_partner(k, q, d, h)
        for k, h in pieces:
            wwait(wdst(k, ro, h), w_recv.at[2, k, h])
            to_partner(k, ro, 2, h)

    late_source = jnp.logical_not(jnp.logical_or(home, jnp.logical_or(r % 2 == 1, level)))

    @pl.when(jnp.logical_not(jnp.logical_or(home, late_source)))
    def _():
        hand_out(mats)
        for k, h in mats[len(pieces) - 3:]:
            relay_weights(k, h)
        handed_out()

        @pl.when(jnp.logical_not(level))
        def _():
            pl.semaphore_signal(go, inc=1, device_id={"pp": partner}, device_id_type=MESH)

        from_partner()

    @pl.when(late_source)
    def _():
        hand_out()
        from_partner()

    def out_at(mm, u):
        return out.at[mm, pl.ds(pl.multiple_of(u * UNIT, UNIT), UNIT)]

    m_a = micro_of(rm, 0, stage1)
    m_b = micro_of(rp, 1, stage1)
    relay = jnp.logical_and(odd == 0, jnp.logical_or(c == 1, x % 2 == 0))
    lag = min(5, units) * (x % 2) + (1 - x % 2) * (min(5, units) + (units - min(5, units)) * (x // 2))
    hold = min(4, units) * (1 - (x + 2) // 3) + (x + 2) // 3

    def relay_unit(v):
        wwait(out_at(m_a, v), rr_recv.at[0, v])
        rcopy(out_at(m_a, v), out_at(m_a, v), rr_send.at[0, v], o_recv, tp=rp).start()
        wwait(out_at(m_b, v), rr_recv.at[1, v])
        rcopy(out_at(m_b, v), out_at(m_b, v), rr_send.at[1, v], o_recv, tp=rm).start()

    def attention(nb, diag, tok):
        per_q = quarter // 128
        head_row = lax.broadcasted_iota(jnp.int32, (128, 128), 0) < 64

        def project(q):
            for j in range(3):
                o = jnp.dot(abuf[...], wqkv[q, j], preferred_element_type=jnp.float32)
                o = (o + packs[q, 7:8, j * quarter:(j + 1) * quarter]).astype(jnp.bfloat16)
                if j == 0:
                    o = o.astype(jnp.float32) * 0.125
                    for half in range(per_q):
                        q_t = o[:, half * 128:(half + 1) * 128].T
                        qaug[q * per_q + half, :128, :128] = jnp.where(head_row, q_t, 0.0).astype(jnp.bfloat16)
                        qaug[q * per_q + half, :128, 128:] = jnp.where(head_row, 0.0, q_t).astype(jnp.bfloat16)
                elif j == 1:
                    kc[q][tok, :] = o
                else:
                    vt[q][:, tok] = o.astype(jnp.float32).T.astype(jnp.bfloat16)

        def scores(pair):
            col = slice(pair % per_q * 128, (pair % per_q + 1) * 128)
            kq = kc[pair // per_q]
            top = None
            for b in range(nb):
                keys = jnp.concatenate([kq[b * KBLK:(b + 1) * KBLK, col], kx[b * KBLK:(b + 1) * KBLK, :]], axis=1)
                s = jnp.dot(keys, qaug[pair], preferred_element_type=jnp.float32)
                if b == nb - 1:
                    s = s + diag
                sbuf[pair % 2, b] = s
                peak = jnp.max(s, axis=0, keepdims=True)
                top = peak if top is None else jnp.maximum(top, peak)
            return top

        def weigh(pair, top):
            col = slice(pair % per_q * 128, (pair % per_q + 1) * 128)
            vq = vt[pair // per_q]
            total = None
            acc = None
            for b in range(nb):
                e = jnp.exp(sbuf[pair % 2, b] - top)
                part_sum = jnp.sum(e, axis=0, keepdims=True)
                total = part_sum if total is None else total + part_sum
                pv = jnp.dot(vq[col, b * KBLK:(b + 1) * KBLK], e.astype(jnp.bfloat16), preferred_element_type=jnp.float32)
                acc = pv if acc is None else acc + pv
            acc = acc * (1.0 / total)
            both = jnp.concatenate([acc[:64, :128], acc[64:, 128:]], axis=0)
            ctx[:, pair * 128:(pair + 1) * 128] = both.T.astype(jnp.bfloat16)

        project(0)
        top = None
        for pair in range(pairs + 1):
            if pair % per_q == 0 and pair // per_q + 1 < tp_n:
                project(pair // per_q + 1)
            later = scores(pair) if pair < pairs else None
            if pair > 0:
                weigh(pair - 1, top)
            top = later

    more = layer < 2 * x_n - 1
    nxt = (layer + 1) % (2 * x_n)
    half_n = nxt // 2
    x_next = half_n + (1 - nxt % 2) * (1 - half_n % 2) * (2 - 2 * half_n)
    p_next = 2 * x_next + c
    r_next = (r + (1 - odd) * (x % 2) * sig + tp_n) % tp_n

    def store_input(v):
        @pl.when(odd == 1)
        def _():
            @pl.when(c == 0)
            def _():
                pltpu.make_async_copy(xbuf.at[v], out_at(m, v), o_recv).start()

            @pl.when(c == 1)
            def _():
                rcopy(xbuf.at[v], out_at(m, v), fa_send.at[v], o_recv, pp=partner).start()

            @pl.when(x % 2 == 1)
            def _():
                rcopy(xbuf.at[v], out_at(m, v), fb_send.at[v], o_recv, tp=r_fwd, pp=stage0).start()

            @pl.when(x % 2 == 0)
            def _():
                rcopy(xbuf.at[v], out_at(m, v), fb_send.at[v], rr_recv.at[c, v], tp=r_fwd, pp=stage0).start()
                rcopy(xbuf.at[v], out_at(m, v), fc_send.at[v], o_recv, tp=r_bwd, pp=stage0).start()

    def store_unit(v):
        @pl.when(home)
        def _():
            pltpu.make_async_copy(ybuf.at[v], out_at(m, v), o_recv).start()

        @pl.when(jnp.logical_not(home))
        def _():
            rcopy(ybuf.at[v], out_at(m, v), od_send.at[v], o_recv, pp=partner).start()

        rcopy(ybuf.at[v], out_at(m, v), da_send.at[v], o_recv, tp=r_bwd, pp=2 * x + odd).start()

        @pl.when(odd == 1)
        def _():
            rcopy(ybuf.at[v], out_at(m, v), db_send.at[v], rr_recv.at[c, v], tp=r_fwd, pp=stage1).start()

    stores = jnp.logical_or(odd == 1, x % 2 == 1)

    def unit_step(u, carry):
        tok = pl.ds(pl.multiple_of(u * UNIT, UNIT), UNIT)

        for group, (step0, step1) in (((0, 1), (3, 1)), ((2,), (5, 3)), ((3,), (7, 4))):
            now = jnp.logical_or(jnp.logical_and(layer == 0, u == min(step0, units - 1)),
                                 jnp.logical_or(jnp.logical_and(layer == 1, u == min(step1, units - 1)), jnp.logical_and(layer > 1, u == 0)))

            @pl.when(jnp.logical_and(late_source, now))
            def _():
                for k in group:
                    for h in range(2):
                        relay_weights(k, h)

        @pl.when(jnp.logical_and(relay, u >= lag))
        def _():
            relay_unit(u - lag)

        @pl.when(layer == 0)
        def _():
            pltpu.make_async_copy(x_hbm.at[m, tok], xbuf.at[u], x0_sem.at[u]).wait()

        @pl.when(layer > 0)
        def _():
            wwait(xbuf.at[u], x_recv.at[u])

        @pl.when(jnp.logical_and(stores, u >= hold - 1))
        def _():
            store_input(u - hold + 1)

        @pl.when(jnp.logical_and(stores, u >= hold))
        def _():
            store_unit(u - hold)

        xin = xbuf[u].astype(jnp.float32)
        abuf[...] = layer_norm(xin, packs[0, 0:1, :], packs[0, 1:2, :])
        for nb in range(1, seq // KBLK + 1):
            @pl.when(u // 2 + 1 == nb)
            def _():
                attention(nb, cmask[u % 2], tok)

        for n in range(model // quarter):
            cols = slice(n * quarter, (n + 1) * quarter)
            attn = jnp.dot(ctx[...], wout[:, cols], preferred_element_type=jnp.float32)
            hbuf[:, cols] = (xbuf[u, :, cols].astype(jnp.float32) + attn + packs[0, 2:3, cols]).astype(jnp.bfloat16)
        abuf[...] = layer_norm(hbuf[...].astype(jnp.float32), packs[0, 3:4, :], packs[0, 4:5, :])
        for q in range(tp_n):
            for n in range(hid_q // quarter):
                cols = slice(n * quarter, (n + 1) * quarter)
                up = jnp.dot(abuf[...], wup[q, :, cols], preferred_element_type=jnp.float32)
                up = up + packs[q, 6:7, cols]
                ubuf[:, q * hid_q + n * quarter:q * hid_q + (n + 1) * quarter] = gelu(up).astype(jnp.bfloat16)
        half_model = model // 2
        for n in range(2):
            cols = slice(n * half_model, (n + 1) * half_model)
            down = jnp.dot(ubuf[...], wdn[:, cols], preferred_element_type=jnp.float32)
            ybuf[u, :, cols] = (hbuf[:, cols].astype(jnp.float32) + down + packs[0, 5:6, cols]).astype(jnp.bfloat16)

            @pl.when(more)
            def _():
                rcopy(ybuf.at[u, :, cols], xbuf.at[u, :, cols], s_send.at[u], x_recv.at[u], tp=r_next, pp=p_next).start()

        return carry

    lax.fori_loop(0, units, unit_step, 0)

    @pl.when(stores)
    def _():
        def last(v, carry):
            store_unit(v)
            return carry

        lax.fori_loop(units - hold, units, last, 0)

        def last_input(v, carry):
            store_input(v)
            return carry

        lax.fori_loop(units - hold + 1, units, last_input, 0)

    @pl.when(relay)
    def _():
        def rest(v, carry):
            relay_unit(v)
            return carry

        lax.fori_loop(units - lag, units, rest, 0)

    @pl.when(moved)
    def _():
        for k, h in pieces:
            sent(sw(k, h), sw_send.at[k, h])

    @pl.when(home)
    def _():
        sent(sw_pack, pk_send.at[0])
        for k, h in mats:
            sent(rl(k, h), rl_send.at[h, k])
        for d in range(4):
            for k, h in pieces:
                sent(sw(k, h), fwd_send.at[d, k, h])

    @pl.when(late_source)
    def _():
        handed_out()

    def drain(u, carry):
        @pl.when(more)
        def _():
            sent(ybuf.at[u], s_send.at[u])

        @pl.when(stores)
        def _():
            sent(ybuf.at[u], da_send.at[u])

            @pl.when(jnp.logical_not(home))
            def _():
                sent(ybuf.at[u], od_send.at[u])

        @pl.when(relay)
        def _():
            sent(ybuf.at[u], rr_send.at[0, u])
            sent(ybuf.at[u], rr_send.at[1, u])

        @pl.when(odd == 1)
        def _():
            sent(ybuf.at[u], db_send.at[u])
            sent(ybuf.at[u], fb_send.at[u])

            @pl.when(x % 2 == 0)
            def _():
                sent(ybuf.at[u], fc_send.at[u])

            @pl.when(c == 1)
            def _():
                sent(ybuf.at[u], fa_send.at[u])

        return carry

    lax.fori_loop(0, units, drain, 0)

    @pl.when(relay)
    def _():
        wwait(out.at[pl.ds(0, out.shape[0] // 2)], o_recv)

    @pl.when(jnp.logical_not(relay))
    def _():
        wwait(out, o_recv)


def solution(mesh):
    tp_size = mesh.shape['tp']
    in_specs = (P('dp'), P('dp'), P('pp'), P('pp'), P('pp', None, None, 'tp'), P('pp', None, 'tp', None), P('pp', 'tp', None), P('pp'), P('pp'), P('pp'), P('pp', None, 'tp'), P('pp', 'tp'), P('pp', 'tp', None), P('pp'))

    def per_device(x_in, seq_lens, ln1_gain, ln1_shift, w_qkv, b_qkv, w_out, b_out, ln2_gain, ln2_shift, w_up, b_up, w_down, b_down):
        micro_n, batch_n, seq_n, model_n = x_in.shape
        heads_n = b_qkv.shape[2] * tp_size
        quarter = w_qkv.shape[3]
        hid_q = w_up.shape[2]
        bf16, f32 = jnp.bfloat16, jnp.float32
        wqkv_t = jnp.transpose(w_qkv[0], (1, 0, 2))
        b_qkv_row = jnp.pad(b_qkv.reshape(1, 3 * quarter), ((0, 0), (0, model_n - 3 * quarter)))
        pack = jnp.concatenate([ln1_gain, ln1_shift, b_out, ln2_gain, ln2_shift, b_down, b_up, b_qkv_row], axis=0).astype(f32)
        units = seq_n // UNIT
        pairs = model_n // 128
        dma = pltpu.SemaphoreType.DMA
        anywhere = pl.BlockSpec(memory_space=pl.ANY)
        tokens = batch_n * seq_n
        out = pl.pallas_call(
            functools.partial(kernel, heads_n),
            out_shape=jax.ShapeDtypeStruct((micro_n, tokens, model_n), bf16),
            in_specs=[anywhere, pl.BlockSpec(memory_space=pltpu.SMEM)] + [anywhere] * 5,
            out_specs=anywhere,
            scratch_shapes=[
                pltpu.VMEM((tp_size, 3, model_n, quarter), bf16),
                pltpu.VMEM((tp_size * quarter, model_n), bf16),
                pltpu.VMEM((tp_size, model_n, hid_q), bf16),
                pltpu.VMEM((tp_size * hid_q, model_n), bf16),
                pltpu.VMEM((tp_size,) + pack.shape, f32),
                pltpu.VMEM((2, 3, model_n // 2, quarter), bf16),
                pltpu.VMEM((2, quarter // 2, model_n), bf16),
                pltpu.VMEM((2, model_n // 2, hid_q), bf16),
                pltpu.VMEM((2, hid_q // 2, model_n), bf16),
                pltpu.VMEM((3, model_n, quarter), bf16),
                pltpu.VMEM((quarter, model_n), bf16),
                pltpu.VMEM((model_n, hid_q), bf16),
                pltpu.VMEM((hid_q, model_n), bf16),
                pltpu.VMEM(pack.shape, f32),
                pltpu.VMEM((units, UNIT, model_n), bf16),
                pltpu.VMEM((units, UNIT, model_n), bf16),
                *[pltpu.VMEM((seq_n, quarter), bf16)] * tp_size,
                *[pltpu.VMEM((quarter, seq_n), bf16)] * tp_size,
                pltpu.VMEM((seq_n, 128), bf16),
                pltpu.VMEM((pairs, 256, 256), bf16),
                pltpu.VMEM((2, KBLK, 256), f32),
                pltpu.VMEM((2, seq_n // KBLK, KBLK, 256), f32),
                pltpu.VMEM((UNIT, model_n), bf16),
                pltpu.VMEM((UNIT, model_n), bf16),
                pltpu.VMEM((UNIT, model_n), bf16),
                pltpu.VMEM((UNIT, tp_size * hid_q), bf16),
                dma((5, 2)), dma((5, 2)), dma((4, 5, 2)), dma((4, 5, 2)), dma((2, 4)), dma((2, 4)), dma((2, 5, 2)), dma((1,)), pltpu.SemaphoreType.REGULAR,
                *[dma((units,))] * 9,
                dma((2, units)), dma((2, units)), dma,
            ],
            compiler_params=pltpu.CompilerParams(collective_id=0, has_side_effects=True, vmem_limit_bytes=63 * 1024 * 1024),
            cost_estimate=pl.CostEstimate(flops=30 * 10 ** 9, bytes_accessed=40 * 10 ** 6, transcendentals=10 ** 7),
        )(x_in.reshape(micro_n, tokens, model_n), seq_lens.reshape(micro_n * batch_n), wqkv_t, w_out[0], w_up[0], w_down[0], pack)
        return out.reshape((1,) + x_in.shape)

    return jax.shard_map(per_device, mesh=mesh, in_specs=in_specs, out_specs=P('pp', 'dp'), check_vma=False)
```

```python
import functools
import math

import jax
import jax.numpy as jnp
import numpy as np
from jax import lax
from jax.experimental import pallas as pl
from jax.experimental.pallas import tpu as pltpu
from jax.sharding import PartitionSpec as P

MESH = pl.DeviceIdType.MESH
UNIT = 128
KBLK = 256
NEG = -1e30


def alibi_slopes(heads_n):
    closest = 2 ** int(math.floor(math.log2(heads_n)))
    base_rate = 2.0 ** (-8.0 / closest)
    slope_list = [base_rate ** (head_idx + 1) for head_idx in range(closest)]
    extra_rate = 2.0 ** (-4.0 / closest)
    slope_list = slope_list + [extra_rate ** (2 * head_idx + 1) for head_idx in range(min(closest, heads_n - closest))]
    return np.array(slope_list, dtype=np.float32)


def split_bf16(value):
    parts = []
    rest = np.float32(value)
    for _ in range(3):
        part = rest.astype(jnp.bfloat16).astype(np.float32)
        parts.append(float(part))
        rest = np.float32(rest - part)
    return parts


def layer_norm(x, gain, shift):
    mean = jnp.mean(x, axis=-1, keepdims=True)
    cent = x - mean
    var = jnp.mean(cent * cent, axis=-1, keepdims=True)
    return (cent * lax.rsqrt(var + 1e-5) * gain + shift).astype(jnp.bfloat16)


def gelu(x):
    inner = math.sqrt(2.0 / math.pi) * (x + 0.044715 * (x * x * x))
    return 0.5 * x * (1.0 + jnp.tanh(inner))


def kernel(heads_n, x_hbm, lens, wqkv_in, wout_in, wup_in, wdn_in, pack_in, out,
           wqkv, wout, wup, wdn, packs, rl_qkv, rl_out, rl_up, rl_dn, sw_qkv, sw_out, sw_up, sw_dn, sw_pack,
           xbuf, ybuf, kc0, kc1, kc2, kc3, vt0, vt1, vt2, vt3, kx, qaug, cmask, sbuf, abuf, ctx, hbuf, ubuf,
           sw_send, sw_recv, w_recv, fwd_send, rl_send, rl_recv, dir_send, pk_send, go,
           x0_sem, x_recv, s_send, od_send, da_send, db_send, fa_send, fb_send, fc_send,
           rr_recv, rr_send, o_recv):
    tp_n = 4
    units = xbuf.shape[0]
    model = xbuf.shape[2]
    seq = units * UNIT
    quarter = wqkv.shape[3]
    hid_q = wup.shape[2]
    pairs = model // 128

    r = lax.axis_index("tp")
    p = lax.axis_index("pp")
    x = p // 2
    c = p % 2
    odd = (r + (x + 1) // 2 + 1) % 2
    even_col = x + (1 - x % 2) * (2 - 2 * x)
    layer = odd * (2 * x + 1) + (1 - odd) * 2 * even_col
    home = odd == c
    moved = jnp.logical_and(c == 0, x % 2 == 0)
    level = x == 1
    ahead = jnp.logical_or(r % 2 == 0, level)
    rp, rm, ro = (r + 1) % tp_n, (r + 3) % tp_n, (r + 2) % tp_n
    partner = 2 * x + (1 - c)
    sig = 1 - 2 * c
    r_fwd = (r + sig + tp_n) % tp_n
    r_bwd = (r - sig + tp_n) % tp_n
    stage0, stage1 = 2 * x, 2 * x + 1
    x_n = 4

    def micro_of(row, core, lay):
        hops = (lay + 1) // 4
        return 2 * (((row + 8 - (1 - 2 * core) * hops) % tp_n) // 2) + core

    m = micro_of(r, c, layer)

    def rcopy(src, dst, ssem, rsem, **dev):
        return pltpu.make_async_remote_copy(src_ref=src, dst_ref=dst, send_sem=ssem, recv_sem=rsem,
                                            device_id=dev, device_id_type=MESH)

    barrier = pltpu.get_barrier_semaphore()
    for dr in range(tp_n):
        for dc in range(2):
            if dr or dc:
                pl.semaphore_signal(barrier, inc=1, device_id={"tp": (r + dr) % tp_n, "pp": 2 * x + (c + dc) % 2}, device_id_type=MESH)
    for dx in range(1, x_n):
        pl.semaphore_signal(barrier, inc=1, device_id={"pp": 2 * ((x + dx) % x_n) + c}, device_id_type=MESH)
    pl.semaphore_wait(barrier, 10)

    def wsrc(k, h=None):
        if k == 4:
            return pack_in
        if k == 0:
            return wqkv_in if h is None else wqkv_in.at[:, pl.ds(h * (model // 2), model // 2), :]
        ref = (None, wout_in, wup_in, wdn_in)[k]
        if h is None:
            return ref
        half = ref.shape[0] // 2
        return ref.at[pl.ds(h * half, half)]

    def wdst(k, q, h=None):
        if k == 0:
            return wqkv.at[q] if h is None else wqkv.at[q, :, pl.ds(h * (model // 2), model // 2), :]
        if k == 2:
            return wup.at[q] if h is None else wup.at[q, pl.ds(h * (model // 2), model // 2)]
        if k == 4:
            return packs.at[q]
        ref, rows = (wout, quarter) if k == 1 else (wdn, hid_q)
        if h is None:
            return ref.at[pl.ds(pl.multiple_of(q * rows, rows), rows)]
        half = rows // 2
        return ref.at[pl.ds(pl.multiple_of(q * rows + h * half, half), half)]

    def rl(k, h):
        return (rl_qkv, rl_out, rl_up, rl_dn)[k].at[h]

    def sw(k, h):
        if k == 4:
            return sw_pack
        if k == 0:
            return sw_qkv.at[:, pl.ds(h * (model // 2), model // 2), :]
        ref = (None, sw_out, sw_up, sw_dn)[k]
        half = ref.shape[0] // 2
        return ref.at[pl.ds(h * half, half)]

    def wwait(view, sem):
        rcopy(view, view, sem, sem, pp=partner).wait_recv()

    pieces = [(4, 0), (1, 0), (1, 1), (0, 0), (0, 1), (2, 0), (2, 1), (3, 0), (3, 1)]
    mats = pieces[1:]

    @pl.when(jnp.logical_and(moved, odd == 1))
    def _():
        for k, h in pieces:
            rcopy(wsrc(k, h), wdst(k, r, h), sw_send.at[k, h], sw_recv.at[k, h], pp=2 * (2 - x)).start()

    @pl.when(jnp.logical_and(moved, odd == 0))
    def _():
        for k, h in pieces:
            rcopy(wsrc(k, h), sw(k, h), sw_send.at[k, h], sw_recv.at[k, h], pp=2 * (2 - x)).start()

    @pl.when(jnp.logical_and(jnp.logical_not(moved), home))
    def _():
        for k, h in pieces:
            pltpu.make_async_copy(wsrc(k, h), wdst(k, r, h), sw_recv.at[k, h]).start()

    @pl.when(jnp.logical_not(jnp.logical_or(moved, home)))
    def _():
        for k, h in pieces:
            pltpu.make_async_copy(wsrc(k, h), sw(k, h), sw_recv.at[k, h]).start()

    @pl.when(layer == 0)
    def _():
        for u in range(units):
            pltpu.make_async_copy(x_hbm.at[m, pl.ds(u * UNIT, UNIT)], xbuf.at[u], x0_sem.at[u]).start()

    kc, vt = (kc0, kc1, kc2, kc3), (vt0, vt1, vt2, vt3)
    for ref in kc + vt:
        ref[...] = jnp.zeros_like(ref)
    length = lens[m]
    key = lax.broadcasted_iota(jnp.int32, (seq, 128), 0)
    lane = lax.broadcasted_iota(jnp.int32, (seq, 128), 1)
    high = (key // 256) * 256
    part = jnp.where(lane % 2 == 0, high, key - high).astype(jnp.float32)
    dead = jnp.where(key >= length, NEG, 0.0)
    kx[...] = jnp.where(lane < 6, part, jnp.where(lane == 6, dead, 0.0)).astype(jnp.bfloat16)
    slopes = alibi_slopes(heads_n)
    row = lax.broadcasted_iota(jnp.int32, (128, 256), 0)
    second = lax.broadcasted_iota(jnp.int32, (128, 256), 1) >= 128
    for pair in range(pairs):
        (h0, m0, l0), (h1, m1, l1) = split_bf16(slopes[2 * pair]), split_bf16(slopes[2 * pair + 1])
        hi, mid, low = jnp.where(second, h1, h0), jnp.where(second, m1, m0), jnp.where(second, l1, l0)
        val = jnp.where(row < 2, hi, jnp.where(row < 4, mid, jnp.where(row < 6, low, jnp.where(row == 6, 1.0, 0.0))))
        qaug[pair, 128:, :] = val.astype(jnp.bfloat16)
    kpos = lax.broadcasted_iota(jnp.int32, (KBLK, 256), 0)
    qpos = lax.broadcasted_iota(jnp.int32, (KBLK, 256), 1) % 128
    cmask[0] = jnp.where(kpos <= qpos, 0.0, NEG)
    cmask[1] = jnp.where(kpos <= qpos + 128, 0.0, NEG)

    def to_relay(k, h):
        rcopy(wdst(k, r, h), rl(k, h), rl_send.at[h, k], rl_recv.at[h, k], tp=(rp, rm)[h]).start()

    def to_partner(k, q, d, h):
        rcopy(wdst(k, q, h), wdst(k, q, h), fwd_send.at[d, k, h], w_recv.at[d, k, h], pp=partner).start()

    def hand_out(behind=()):
        for i, (k, h) in enumerate(pieces):
            wwait(sw(k, h), sw_recv.at[k, h])
            rcopy(sw(k, h), wdst(k, r, h), dir_send.at[0, k, h], w_recv.at[3, k, h], tp=rp).start()
            rcopy(sw(k, h), wdst(k, r, h), dir_send.at[1, k, h], w_recv.at[1, k, h], tp=rm).start()
            if 3 <= i < len(behind) + 3:
                relay_weights(*behind[i - 3])

    def relay_weights(k, h):
        wwait(rl(k, h), rl_recv.at[h, k])
        rcopy(rl(k, h), wdst(k, (rm, rp)[h], h), rl_send.at[h, k], w_recv.at[2, k, h], tp=(rp, rm)[h]).start()

    def from_partner():
        for d, q in ((0, r), (1, rp), (3, rm), (2, ro)):
            for k, h in pieces:
                wwait(wdst(k, q, h), w_recv.at[d, k, h])

    def sent(view, sem):
        rcopy(view, view, sem, sem, pp=partner).wait_send()

    def handed_out():
        for k, h in pieces:
            for d in range(2):
                sent(sw(k, h), dir_send.at[d, k, h])
        for k, h in mats:
            sent(rl(k, h), rl_send.at[h, k])

    @pl.when(home)
    def _():
        for k, h in pieces:
            wwait(wdst(k, r, h), sw_recv.at[k, h])
            if k == 4:
                rcopy(wdst(k, r), wdst(k, r), pk_send.at[0], w_recv.at[2, k, h], tp=ro).start()
            else:
                @pl.when(ahead)
                def _():
                    to_relay(k, h)
            to_partner(k, r, 0, h)

        @pl.when(jnp.logical_not(ahead))
        def _():
            pl.semaphore_wait(go, 1)
            for k, h in mats:
                to_relay(k, h)

        for k, h in pieces:
            for d, q in ((1, rp), (3, rm)):
                wwait(wdst(k, q, h), w_recv.at[d, k, h])
                to_partner(k, q, d, h)
        for k, h in pieces:
            wwait(wdst(k, ro, h), w_recv.at[2, k, h])
            to_partner(k, ro, 2, h)

    late_source = jnp.logical_not(jnp.logical_or(home, jnp.logical_or(r % 2 == 1, level)))

    @pl.when(jnp.logical_not(jnp.logical_or(home, late_source)))
    def _():
        hand_out(mats)
        for k, h in mats[len(pieces) - 3:]:
            relay_weights(k, h)
        handed_out()

        @pl.when(jnp.logical_not(level))
        def _():
            pl.semaphore_signal(go, inc=1, device_id={"pp": partner}, device_id_type=MESH)

        from_partner()

    @pl.when(late_source)
    def _():
        hand_out()
        from_partner()

    def out_at(mm, u):
        return out.at[mm, pl.ds(pl.multiple_of(u * UNIT, UNIT), UNIT)]

    m_a = micro_of(rm, 0, stage1)
    m_b = micro_of(rp, 1, stage1)
    relay = jnp.logical_and(odd == 0, jnp.logical_or(c == 1, x % 2 == 0))
    lag = min(5, units) * (x % 2) + (1 - x % 2) * (min(5, units) + (units - min(5, units)) * (x // 2))
    hold = min(5, units) * (1 - (x + 2) // 3) + (x + 2) // 3

    def relay_unit(v):
        wwait(out_at(m_a, v), rr_recv.at[0, v])
        rcopy(out_at(m_a, v), out_at(m_a, v), rr_send.at[0, v], o_recv, tp=rp).start()
        wwait(out_at(m_b, v), rr_recv.at[1, v])
        rcopy(out_at(m_b, v), out_at(m_b, v), rr_send.at[1, v], o_recv, tp=rm).start()

    def attention(nb, diag, tok):
        per_q = quarter // 128
        head_row = lax.broadcasted_iota(jnp.int32, (128, 128), 0) < 64

        def project(q):
            for j in range(3):
                o = jnp.dot(abuf[...], wqkv[q, j], preferred_element_type=jnp.float32)
                o = (o + packs[q, 7:8, j * quarter:(j + 1) * quarter]).astype(jnp.bfloat16)
                if j == 0:
                    o = o.astype(jnp.float32) * 0.125
                    for half in range(per_q):
                        q_t = o[:, half * 128:(half + 1) * 128].T
                        qaug[q * per_q + half, :128, :128] = jnp.where(head_row, q_t, 0.0).astype(jnp.bfloat16)
                        qaug[q * per_q + half, :128, 128:] = jnp.where(head_row, 0.0, q_t).astype(jnp.bfloat16)
                elif j == 1:
                    kc[q][tok, :] = o
                else:
                    vt[q][:, tok] = o.astype(jnp.float32).T.astype(jnp.bfloat16)

        def scores(pair):
            col = slice(pair % per_q * 128, (pair % per_q + 1) * 128)
            kq = kc[pair // per_q]
            top = None
            for b in range(nb):
                keys = jnp.concatenate([kq[b * KBLK:(b + 1) * KBLK, col], kx[b * KBLK:(b + 1) * KBLK, :]], axis=1)
                s = jnp.dot(keys, qaug[pair], preferred_element_type=jnp.float32)
                if b == nb - 1:
                    s = s + diag
                sbuf[pair % 2, b] = s
                peak = jnp.max(s, axis=0, keepdims=True)
                top = peak if top is None else jnp.maximum(top, peak)
            return top

        def weigh(pair, top):
            col = slice(pair % per_q * 128, (pair % per_q + 1) * 128)
            vq = vt[pair // per_q]
            total = None
            acc = None
            for b in range(nb):
                e = jnp.exp(sbuf[pair % 2, b] - top)
                part_sum = jnp.sum(e, axis=0, keepdims=True)
                total = part_sum if total is None else total + part_sum
                pv = jnp.dot(vq[col, b * KBLK:(b + 1) * KBLK], e.astype(jnp.bfloat16), preferred_element_type=jnp.float32)
                acc = pv if acc is None else acc + pv
            acc = acc * (1.0 / total)
            both = jnp.concatenate([acc[:64, :128], acc[64:, 128:]], axis=0)
            ctx[:, pair * 128:(pair + 1) * 128] = both.T.astype(jnp.bfloat16)

        project(0)
        top = None
        for pair in range(pairs + 1):
            if pair % per_q == 0 and pair // per_q + 1 < tp_n:
                project(pair // per_q + 1)
            later = scores(pair) if pair < pairs else None
            if pair > 0:
                weigh(pair - 1, top)
            top = later

    more = layer < 2 * x_n - 1
    nxt = (layer + 1) % (2 * x_n)
    half_n = nxt // 2
    x_next = half_n + (1 - nxt % 2) * (1 - half_n % 2) * (2 - 2 * half_n)
    p_next = 2 * x_next + c
    r_next = (r + (1 - odd) * (x % 2) * sig + tp_n) % tp_n

    def store_input(v):
        @pl.when(odd == 1)
        def _():
            @pl.when(c == 0)
            def _():
                pltpu.make_async_copy(xbuf.at[v], out_at(m, v), o_recv).start()

            @pl.when(c == 1)
            def _():
                rcopy(xbuf.at[v], out_at(m, v), fa_send.at[v], o_recv, pp=partner).start()

            @pl.when(x % 2 == 1)
            def _():
                rcopy(xbuf.at[v], out_at(m, v), fb_send.at[v], o_recv, tp=r_fwd, pp=stage0).start()

            @pl.when(x % 2 == 0)
            def _():
                rcopy(xbuf.at[v], out_at(m, v), fb_send.at[v], rr_recv.at[c, v], tp=r_fwd, pp=stage0).start()
                rcopy(xbuf.at[v], out_at(m, v), fc_send.at[v], o_recv, tp=r_bwd, pp=stage0).start()

    def store_unit(v):
        @pl.when(home)
        def _():
            pltpu.make_async_copy(ybuf.at[v], out_at(m, v), o_recv).start()

        @pl.when(jnp.logical_not(home))
        def _():
            rcopy(ybuf.at[v], out_at(m, v), od_send.at[v], o_recv, pp=partner).start()

        rcopy(ybuf.at[v], out_at(m, v), da_send.at[v], o_recv, tp=r_bwd, pp=2 * x + odd).start()

        @pl.when(odd == 1)
        def _():
            rcopy(ybuf.at[v], out_at(m, v), db_send.at[v], rr_recv.at[c, v], tp=r_fwd, pp=stage1).start()

    stores = jnp.logical_or(odd == 1, x % 2 == 1)

    def unit_step(u, carry):
        tok = pl.ds(pl.multiple_of(u * UNIT, UNIT), UNIT)

        for group, (step0, step1) in (((0, 1), (2, 0)), ((2,), (4, 1)), ((3,), (6, 2))):
            now = jnp.logical_or(jnp.logical_and(layer == 0, u == min(step0, units - 1)),
                                 jnp.logical_or(jnp.logical_and(layer == 1, u == min(step1, units - 1)), jnp.logical_and(layer > 1, u == 0)))

            @pl.when(jnp.logical_and(late_source, now))
            def _():
                for k in group:
                    for h in range(2):
                        relay_weights(k, h)

        @pl.when(jnp.logical_and(relay, u >= lag))
        def _():
            relay_unit(u - lag)

        @pl.when(layer == 0)
        def _():
            pltpu.make_async_copy(x_hbm.at[m, tok], xbuf.at[u], x0_sem.at[u]).wait()

        @pl.when(layer > 0)
        def _():
            wwait(xbuf.at[u], x_recv.at[u])

        @pl.when(jnp.logical_and(stores, u >= hold - 1))
        def _():
            store_input(u - hold + 1)

        @pl.when(jnp.logical_and(stores, u >= hold))
        def _():
            store_unit(u - hold)

        xin = xbuf[u].astype(jnp.float32)
        abuf[...] = layer_norm(xin, packs[0, 0:1, :], packs[0, 1:2, :])
        for nb in range(1, seq // KBLK + 1):
            @pl.when(u // 2 + 1 == nb)
            def _():
                attention(nb, cmask[u % 2], tok)

        for n in range(model // quarter):
            cols = slice(n * quarter, (n + 1) * quarter)
            attn = jnp.dot(ctx[...], wout[:, cols], preferred_element_type=jnp.float32)
            hbuf[:, cols] = (xbuf[u, :, cols].astype(jnp.float32) + attn + packs[0, 2:3, cols]).astype(jnp.bfloat16)
        abuf[...] = layer_norm(hbuf[...].astype(jnp.float32), packs[0, 3:4, :], packs[0, 4:5, :])
        for q in range(tp_n):
            for n in range(hid_q // quarter):
                cols = slice(n * quarter, (n + 1) * quarter)
                up = jnp.dot(abuf[...], wup[q, :, cols], preferred_element_type=jnp.float32)
                up = up + packs[q, 6:7, cols]
                ubuf[:, q * hid_q + n * quarter:q * hid_q + (n + 1) * quarter] = gelu(up).astype(jnp.bfloat16)
        half_model = model // 2
        for n in range(2):
            cols = slice(n * half_model, (n + 1) * half_model)
            down = jnp.dot(ubuf[...], wdn[:, cols], preferred_element_type=jnp.float32)
            ybuf[u, :, cols] = (hbuf[:, cols].astype(jnp.float32) + down + packs[0, 5:6, cols]).astype(jnp.bfloat16)

            @pl.when(more)
            def _():
                rcopy(ybuf.at[u, :, cols], xbuf.at[u, :, cols], s_send.at[u], x_recv.at[u], tp=r_next, pp=p_next).start()

        return carry

    lax.fori_loop(0, units, unit_step, 0)

    @pl.when(stores)
    def _():
        def last(v, carry):
            store_unit(v)
            return carry

        lax.fori_loop(units - hold, units, last, 0)

        def last_input(v, carry):
            store_input(v)
            return carry

        lax.fori_loop(units - hold + 1, units, last_input, 0)

    @pl.when(relay)
    def _():
        def rest(v, carry):
            relay_unit(v)
            return carry

        lax.fori_loop(units - lag, units, rest, 0)

    @pl.when(moved)
    def _():
        for k, h in pieces:
            sent(sw(k, h), sw_send.at[k, h])

    @pl.when(home)
    def _():
        sent(sw_pack, pk_send.at[0])
        for k, h in mats:
            sent(rl(k, h), rl_send.at[h, k])
        for d in range(4):
            for k, h in pieces:
                sent(sw(k, h), fwd_send.at[d, k, h])

    @pl.when(late_source)
    def _():
        handed_out()

    def drain(u, carry):
        @pl.when(more)
        def _():
            sent(ybuf.at[u], s_send.at[u])

        @pl.when(stores)
        def _():
            sent(ybuf.at[u], da_send.at[u])

            @pl.when(jnp.logical_not(home))
            def _():
                sent(ybuf.at[u], od_send.at[u])

        @pl.when(relay)
        def _():
            sent(ybuf.at[u], rr_send.at[0, u])
            sent(ybuf.at[u], rr_send.at[1, u])

        @pl.when(odd == 1)
        def _():
            sent(ybuf.at[u], db_send.at[u])
            sent(ybuf.at[u], fb_send.at[u])

            @pl.when(x % 2 == 0)
            def _():
                sent(ybuf.at[u], fc_send.at[u])

            @pl.when(c == 1)
            def _():
                sent(ybuf.at[u], fa_send.at[u])

        return carry

    lax.fori_loop(0, units, drain, 0)

    @pl.when(relay)
    def _():
        wwait(out.at[pl.ds(0, out.shape[0] // 2)], o_recv)

    @pl.when(jnp.logical_not(relay))
    def _():
        wwait(out, o_recv)


def solution(mesh):
    tp_size = mesh.shape['tp']
    in_specs = (P('dp'), P('dp'), P('pp'), P('pp'), P('pp', None, None, 'tp'), P('pp', None, 'tp', None), P('pp', 'tp', None), P('pp'), P('pp'), P('pp'), P('pp', None, 'tp'), P('pp', 'tp'), P('pp', 'tp', None), P('pp'))

    def per_device(x_in, seq_lens, ln1_gain, ln1_shift, w_qkv, b_qkv, w_out, b_out, ln2_gain, ln2_shift, w_up, b_up, w_down, b_down):
        micro_n, batch_n, seq_n, model_n = x_in.shape
        heads_n = b_qkv.shape[2] * tp_size
        quarter = w_qkv.shape[3]
        hid_q = w_up.shape[2]
        bf16, f32 = jnp.bfloat16, jnp.float32
        wqkv_t = jnp.transpose(w_qkv[0], (1, 0, 2))
        b_qkv_row = jnp.pad(b_qkv.reshape(1, 3 * quarter), ((0, 0), (0, model_n - 3 * quarter)))
        pack = jnp.concatenate([ln1_gain, ln1_shift, b_out, ln2_gain, ln2_shift, b_down, b_up, b_qkv_row], axis=0).astype(f32)
        units = seq_n // UNIT
        pairs = model_n // 128
        dma = pltpu.SemaphoreType.DMA
        anywhere = pl.BlockSpec(memory_space=pl.ANY)
        tokens = batch_n * seq_n
        out = pl.pallas_call(
            functools.partial(kernel, heads_n),
            out_shape=jax.ShapeDtypeStruct((micro_n, tokens, model_n), bf16),
            in_specs=[anywhere, pl.BlockSpec(memory_space=pltpu.SMEM)] + [anywhere] * 5,
            out_specs=anywhere,
            scratch_shapes=[
                pltpu.VMEM((tp_size, 3, model_n, quarter), bf16),
                pltpu.VMEM((tp_size * quarter, model_n), bf16),
                pltpu.VMEM((tp_size, model_n, hid_q), bf16),
                pltpu.VMEM((tp_size * hid_q, model_n), bf16),
                pltpu.VMEM((tp_size,) + pack.shape, f32),
                pltpu.VMEM((2, 3, model_n // 2, quarter), bf16),
                pltpu.VMEM((2, quarter // 2, model_n), bf16),
                pltpu.VMEM((2, model_n // 2, hid_q), bf16),
                pltpu.VMEM((2, hid_q // 2, model_n), bf16),
                pltpu.VMEM((3, model_n, quarter), bf16),
                pltpu.VMEM((quarter, model_n), bf16),
                pltpu.VMEM((model_n, hid_q), bf16),
                pltpu.VMEM((hid_q, model_n), bf16),
                pltpu.VMEM(pack.shape, f32),
                pltpu.VMEM((units, UNIT, model_n), bf16),
                pltpu.VMEM((units, UNIT, model_n), bf16),
                *[pltpu.VMEM((seq_n, quarter), bf16)] * tp_size,
                *[pltpu.VMEM((quarter, seq_n), bf16)] * tp_size,
                pltpu.VMEM((seq_n, 128), bf16),
                pltpu.VMEM((pairs, 256, 256), bf16),
                pltpu.VMEM((2, KBLK, 256), f32),
                pltpu.VMEM((2, seq_n // KBLK, KBLK, 256), f32),
                pltpu.VMEM((UNIT, model_n), bf16),
                pltpu.VMEM((UNIT, model_n), bf16),
                pltpu.VMEM((UNIT, model_n), bf16),
                pltpu.VMEM((UNIT, tp_size * hid_q), bf16),
                dma((5, 2)), dma((5, 2)), dma((4, 5, 2)), dma((4, 5, 2)), dma((2, 4)), dma((2, 4)), dma((2, 5, 2)), dma((1,)), pltpu.SemaphoreType.REGULAR,
                *[dma((units,))] * 9,
                dma((2, units)), dma((2, units)), dma,
            ],
            compiler_params=pltpu.CompilerParams(collective_id=0, has_side_effects=True, vmem_limit_bytes=63 * 1024 * 1024),
            cost_estimate=pl.CostEstimate(flops=30 * 10 ** 9, bytes_accessed=40 * 10 ** 6, transcendentals=10 ** 7),
        )(x_in.reshape(micro_n, tokens, model_n), seq_lens.reshape(micro_n * batch_n), wqkv_t, w_out[0], w_up[0], w_down[0], pack)
        return out.reshape((1,) + x_in.shape)

    return jax.shard_map(per_device, mesh=mesh, in_specs=in_specs, out_specs=P('pp', 'dp'), check_vma=False)
```

```python
import functools
import math

import jax
import jax.numpy as jnp
import numpy as np
from jax import lax
from jax.experimental import pallas as pl
from jax.experimental.pallas import tpu as pltpu
from jax.sharding import PartitionSpec as P

MESH = pl.DeviceIdType.MESH
UNIT = 128
KBLK = 256
NEG = -1e30


def alibi_slopes(heads_n):
    closest = 2 ** int(math.floor(math.log2(heads_n)))
    base_rate = 2.0 ** (-8.0 / closest)
    slope_list = [base_rate ** (head_idx + 1) for head_idx in range(closest)]
    extra_rate = 2.0 ** (-4.0 / closest)
    slope_list = slope_list + [extra_rate ** (2 * head_idx + 1) for head_idx in range(min(closest, heads_n - closest))]
    return np.array(slope_list, dtype=np.float32)


def split_bf16(value):
    parts = []
    rest = np.float32(value)
    for _ in range(3):
        part = rest.astype(jnp.bfloat16).astype(np.float32)
        parts.append(float(part))
        rest = np.float32(rest - part)
    return parts


def layer_norm(x, gain, shift):
    mean = jnp.mean(x, axis=-1, keepdims=True)
    cent = x - mean
    var = jnp.mean(cent * cent, axis=-1, keepdims=True)
    return (cent * lax.rsqrt(var + 1e-5) * gain + shift).astype(jnp.bfloat16)


def gelu(x):
    inner = math.sqrt(2.0 / math.pi) * (x + 0.044715 * (x * x * x))
    return 0.5 * x * (1.0 + jnp.tanh(inner))


def kernel(heads_n, x_hbm, lens, wqkv_in, wout_in, wup_in, wdn_in, pack_in, out,
           wqkv, wout, wup, wdn, packs, rl_qkv, rl_out, rl_up, rl_dn, sw_qkv, sw_out, sw_up, sw_dn, sw_pack,
           xbuf, ybuf, kc0, kc1, kc2, kc3, vt0, vt1, vt2, vt3, kx, qaug, cmask, sbuf, abuf, ctx, hbuf, ubuf,
           sw_send, sw_recv, w_recv, fwd_send, rl_send, rl_recv, dir_send, pk_send, go,
           x0_sem, x_recv, s_send, od_send, da_send, db_send, fa_send, fb_send, fc_send,
           rr_recv, rr_send, o_recv):
    tp_n = 4
    units = xbuf.shape[0]
    model = xbuf.shape[2]
    seq = units * UNIT
    quarter = wqkv.shape[1] // 3 * 128
    hid_q = wup.shape[1] * 128
    pairs = model // 128
    per_q = quarter // 128

    r = lax.axis_index("tp")
    p = lax.axis_index("pp")
    x = p // 2
    c = p % 2
    odd = (r + (x + 1) // 2 + 1) % 2
    even_col = x + (1 - x % 2) * (2 - 2 * x)
    layer = odd * (2 * x + 1) + (1 - odd) * 2 * even_col
    home = odd == c
    moved = jnp.logical_and(c == 0, x % 2 == 0)
    level = x == 1
    ahead = jnp.logical_or(r % 2 == 0, level)
    rp, rm, ro = (r + 1) % tp_n, (r + 3) % tp_n, (r + 2) % tp_n
    partner = 2 * x + (1 - c)
    sig = 1 - 2 * c
    r_fwd = (r + sig + tp_n) % tp_n
    r_bwd = (r - sig + tp_n) % tp_n
    stage0, stage1 = 2 * x, 2 * x + 1
    x_n = 4

    def micro_of(row, core, lay):
        hops = (lay + 1) // 4
        return 2 * (((row + 8 - (1 - 2 * core) * hops) % tp_n) // 2) + core

    m = micro_of(r, c, layer)

    def rcopy(src, dst, ssem, rsem, **dev):
        return pltpu.make_async_remote_copy(src_ref=src, dst_ref=dst, send_sem=ssem, recv_sem=rsem,
                                            device_id=dev, device_id_type=MESH)

    barrier = pltpu.get_barrier_semaphore()
    for dr in range(tp_n):
        for dc in range(2):
            if dr or dc:
                pl.semaphore_signal(barrier, inc=1, device_id={"tp": (r + dr) % tp_n, "pp": 2 * x + (c + dc) % 2}, device_id_type=MESH)
    for dx in range(1, x_n):
        pl.semaphore_signal(barrier, inc=1, device_id={"pp": 2 * ((x + dx) % x_n) + c}, device_id_type=MESH)
    pl.semaphore_wait(barrier, 10)

    def wsrc(k, h, n):
        if k == 0:
            return wqkv_in.at[n // per_q, pl.ds(h * (model // 2), model // 2), pl.ds(n % per_q * 128, 128)]
        ref = (None, wout_in, wup_in, wdn_in)[k]
        half = ref.shape[0] // 2
        return ref.at[pl.ds(h * half, half), pl.ds(n * 128, 128)]

    def wdst(k, q, h=0):
        if k == 4:
            return packs.at[q]
        if k == 0 or k == 2:
            return (wqkv, None, wup)[k].at[q, :, pl.ds(h * (model // 2), model // 2), :]
        ref, half = (wout, quarter // 2) if k == 1 else (wdn, hid_q // 2)
        return ref.at[:, pl.ds(pl.multiple_of((2 * q + h) * half, half), half), :]

    def rl(k, h):
        return (rl_qkv, rl_out, rl_up, rl_dn)[k].at[h]

    def sw(k, h):
        if k == 4:
            return sw_pack
        ref = (sw_qkv, sw_out, sw_up, sw_dn)[k]
        half = ref.shape[1] // 2
        return ref.at[:, pl.ds(h * half, half), :]

    def fetch(k, h, dst, move):
        if k == 4:
            todo = [(pack_in, dst)]
        else:
            todo = [(wsrc(k, h, n), dst.at[n]) for n in range(dst.shape[0])]
        for src, to in todo:
            if move:
                rcopy(src, to, sw_send.at[k, h], sw_recv.at[k, h], pp=2 * (2 - x)).start()
            else:
                pltpu.make_async_copy(src, to, sw_recv.at[k, h]).start()

    def wwait(view, sem):
        rcopy(view, view, sem, sem, pp=partner).wait_recv()

    pieces = [(4, 0), (1, 0), (1, 1), (0, 0), (0, 1), (2, 0), (2, 1), (3, 0), (3, 1)]
    mats = pieces[1:]

    @pl.when(jnp.logical_and(moved, odd == 1))
    def _():
        for k, h in pieces:
            fetch(k, h, wdst(k, r, h), True)

    @pl.when(jnp.logical_and(moved, odd == 0))
    def _():
        for k, h in pieces:
            fetch(k, h, sw(k, h), True)

    @pl.when(jnp.logical_and(jnp.logical_not(moved), home))
    def _():
        for k, h in pieces:
            fetch(k, h, wdst(k, r, h), False)

    @pl.when(jnp.logical_not(jnp.logical_or(moved, home)))
    def _():
        for k, h in pieces:
            fetch(k, h, sw(k, h), False)

    @pl.when(layer == 0)
    def _():
        for u in range(units):
            pltpu.make_async_copy(x_hbm.at[m, pl.ds(u * UNIT, UNIT)], xbuf.at[u], x0_sem.at[u]).start()

    kc, vt = (kc0, kc1, kc2, kc3), (vt0, vt1, vt2, vt3)
    for ref in kc + vt:
        ref[...] = jnp.zeros_like(ref)
    length = lens[m]
    key = lax.broadcasted_iota(jnp.int32, (seq, 128), 0)
    lane = lax.broadcasted_iota(jnp.int32, (seq, 128), 1)
    high = (key // 256) * 256
    part = jnp.where(lane % 2 == 0, high, key - high).astype(jnp.float32)
    dead = jnp.where(key >= length, NEG, 0.0)
    kx[...] = jnp.where(lane < 6, part, jnp.where(lane == 6, dead, 0.0)).astype(jnp.bfloat16)
    slopes = alibi_slopes(heads_n)
    row = lax.broadcasted_iota(jnp.int32, (128, 256), 0)
    second = lax.broadcasted_iota(jnp.int32, (128, 256), 1) >= 128
    for pair in range(pairs):
        (h0, m0, l0), (h1, m1, l1) = split_bf16(slopes[2 * pair]), split_bf16(slopes[2 * pair + 1])
        hi, mid, low = jnp.where(second, h1, h0), jnp.where(second, m1, m0), jnp.where(second, l1, l0)
        val = jnp.where(row < 2, hi, jnp.where(row < 4, mid, jnp.where(row < 6, low, jnp.where(row == 6, 1.0, 0.0))))
        for side in range(2):
            qaug[pair, side, 128:, :] = val[:, side * 128:(side + 1) * 128].astype(jnp.bfloat16)
    kpos = lax.broadcasted_iota(jnp.int32, (KBLK, 256), 0)
    qpos = lax.broadcasted_iota(jnp.int32, (KBLK, 256), 1) % 128
    cmask[0] = jnp.where(kpos <= qpos, 0.0, NEG)
    cmask[1] = jnp.where(kpos <= qpos + 128, 0.0, NEG)

    def to_relay(k, h):
        rcopy(wdst(k, r, h), rl(k, h), rl_send.at[h, k], rl_recv.at[h, k], tp=(rp, rm)[h]).start()

    def to_partner(k, q, d, h):
        rcopy(wdst(k, q, h), wdst(k, q, h), fwd_send.at[d, k, h], w_recv.at[d, k, h], pp=partner).start()

    def hand_out(behind=()):
        for i, (k, h) in enumerate(pieces):
            wwait(sw(k, h), sw_recv.at[k, h])
            rcopy(sw(k, h), wdst(k, r, h), dir_send.at[0, k, h], w_recv.at[3, k, h], tp=rp).start()
            rcopy(sw(k, h), wdst(k, r, h), dir_send.at[1, k, h], w_recv.at[1, k, h], tp=rm).start()
            if 3 <= i < len(behind) + 3:
                relay_weights(*behind[i - 3])

    def relay_weights(k, h):
        wwait(rl(k, h), rl_recv.at[h, k])
        rcopy(rl(k, h), wdst(k, (rm, rp)[h], h), rl_send.at[h, k], w_recv.at[2, k, h], tp=(rp, rm)[h]).start()

    def from_partner():
        for d, q in ((0, r), (1, rp), (3, rm), (2, ro)):
            for k, h in pieces:
                wwait(wdst(k, q, h), w_recv.at[d, k, h])

    def sent(view, sem):
        rcopy(view, view, sem, sem, pp=partner).wait_send()

    def handed_out():
        for k, h in pieces:
            for d in range(2):
                sent(sw(k, h), dir_send.at[d, k, h])
        for k, h in mats:
            sent(rl(k, h), rl_send.at[h, k])

    @pl.when(home)
    def _():
        for k, h in pieces:
            wwait(wdst(k, r, h), sw_recv.at[k, h])
            if k == 4:
                rcopy(wdst(k, r), wdst(k, r), pk_send.at[0], w_recv.at[2, k, h], tp=ro).start()
            else:
                @pl.when(ahead)
                def _():
                    to_relay(k, h)
            to_partner(k, r, 0, h)

        @pl.when(jnp.logical_not(ahead))
        def _():
            pl.semaphore_wait(go, 1)
            for k, h in mats:
                to_relay(k, h)

        for k, h in pieces:
            for d, q in ((1, rp), (3, rm)):
                wwait(wdst(k, q, h), w_recv.at[d, k, h])
                to_partner(k, q, d, h)
        for k, h in pieces:
            wwait(wdst(k, ro, h), w_recv.at[2, k, h])
            to_partner(k, ro, 2, h)

    late_source = jnp.logical_not(jnp.logical_or(home, jnp.logical_or(r % 2 == 1, level)))

    @pl.when(jnp.logical_not(jnp.logical_or(home, late_source)))
    def _():
        hand_out(mats)
        for k, h in mats[len(pieces) - 3:]:
            relay_weights(k, h)
        handed_out()

        @pl.when(jnp.logical_not(level))
        def _():
            pl.semaphore_signal(go, inc=1, device_id={"pp": partner}, device_id_type=MESH)

        from_partner()

    @pl.when(late_source)
    def _():
        hand_out()
        from_partner()

    def out_at(mm, u):
        return out.at[mm, pl.ds(pl.multiple_of(u * UNIT, UNIT), UNIT)]

    m_a = micro_of(rm, 0, stage1)
    m_b = micro_of(rp, 1, stage1)
    relay = jnp.logical_and(odd == 0, jnp.logical_or(c == 1, x % 2 == 0))
    lag = min(5, units) * (x % 2) + (1 - x % 2) * (min(5, units) + (units - min(5, units)) * (x // 2))
    hold = min(5, units) * (1 - (x + 2) // 3) + (x + 2) // 3

    def relay_unit(v):
        wwait(out_at(m_a, v), rr_recv.at[0, v])
        rcopy(out_at(m_a, v), out_at(m_a, v), rr_send.at[0, v], o_recv, tp=rp).start()
        wwait(out_at(m_b, v), rr_recv.at[1, v])
        rcopy(out_at(m_b, v), out_at(m_b, v), rr_send.at[1, v], o_recv, tp=rm).start()

    def wide(parts):
        return jnp.concatenate(parts, axis=1)

    def blocks(ref, first, count):
        return wide([ref[first + i] for i in range(count)])

    def put_blocks(ref, first, val):
        for i in range(val.shape[1] // 128):
            ref[first + i] = val[:, i * 128:(i + 1) * 128]

    def attention(nb, diag, tok, u):
        head_row = lax.broadcasted_iota(jnp.int32, (128, 128), 0) < 64

        def project(q):
            for j in range(3):
                weights = wide([wqkv[q, j * per_q + i] for i in range(per_q)])
                o = jnp.dot(blocks(abuf, 0, pairs), weights, preferred_element_type=jnp.float32)
                o = (o + packs[q, 7:8, j * quarter:(j + 1) * quarter]).astype(jnp.bfloat16)
                for i in range(per_q):
                    part = o[:, i * 128:(i + 1) * 128]
                    if j == 0:
                        q_t = (part.astype(jnp.float32) * 0.125).T
                        qaug[q * per_q + i, 0, :128, :] = jnp.where(head_row, q_t, 0.0).astype(jnp.bfloat16)
                        qaug[q * per_q + i, 1, :128, :] = jnp.where(head_row, 0.0, q_t).astype(jnp.bfloat16)
                    elif j == 1:
                        kc[q][i, tok, :] = part
                    else:
                        vt[q][i, u] = part.astype(jnp.float32).T.astype(jnp.bfloat16)

        def scores(pair):
            kq = kc[pair // per_q]
            q_rhs = blocks(qaug.at[pair], 0, 2)
            top = None
            for b in range(nb):
                keys = wide([kq[pair % per_q, b * KBLK:(b + 1) * KBLK, :], kx[b * KBLK:(b + 1) * KBLK, :]])
                s = jnp.dot(keys, q_rhs, preferred_element_type=jnp.float32)
                if b == nb - 1:
                    s = s + diag
                sbuf[pair % 2, b] = s
                peak = jnp.max(s, axis=0, keepdims=True)
                top = peak if top is None else jnp.maximum(top, peak)
            return top

        def weigh(pair, top):
            vq = vt[pair // per_q].at[pair % per_q]
            total = None
            acc = None
            for b in range(nb):
                e = jnp.exp(sbuf[pair % 2, b] - top)
                part_sum = jnp.sum(e, axis=0, keepdims=True)
                total = part_sum if total is None else total + part_sum
                pv = jnp.dot(blocks(vq, b * KBLK // UNIT, KBLK // UNIT), e.astype(jnp.bfloat16), preferred_element_type=jnp.float32)
                acc = pv if acc is None else acc + pv
            acc = acc * (1.0 / total)
            both = jnp.concatenate([acc[:64, :128], acc[64:, 128:]], axis=0)
            ctx[pair] = both.T.astype(jnp.bfloat16)

        project(0)
        top = None
        for pair in range(pairs + 1):
            if pair % per_q == 0 and pair // per_q + 1 < tp_n:
                project(pair // per_q + 1)
            later = scores(pair) if pair < pairs else None
            if pair > 0:
                weigh(pair - 1, top)
            top = later

    more = layer < 2 * x_n - 1
    nxt = (layer + 1) % (2 * x_n)
    half_n = nxt // 2
    x_next = half_n + (1 - nxt % 2) * (1 - half_n % 2) * (2 - 2 * half_n)
    p_next = 2 * x_next + c
    r_next = (r + (1 - odd) * (x % 2) * sig + tp_n) % tp_n

    def store_input(v):
        @pl.when(odd == 1)
        def _():
            @pl.when(c == 0)
            def _():
                pltpu.make_async_copy(xbuf.at[v], out_at(m, v), o_recv).start()

            @pl.when(c == 1)
            def _():
                rcopy(xbuf.at[v], out_at(m, v), fa_send.at[v], o_recv, pp=partner).start()

            @pl.when(x % 2 == 1)
            def _():
                rcopy(xbuf.at[v], out_at(m, v), fb_send.at[v], o_recv, tp=r_fwd, pp=stage0).start()

            @pl.when(x % 2 == 0)
            def _():
                rcopy(xbuf.at[v], out_at(m, v), fb_send.at[v], rr_recv.at[c, v], tp=r_fwd, pp=stage0).start()
                rcopy(xbuf.at[v], out_at(m, v), fc_send.at[v], o_recv, tp=r_bwd, pp=stage0).start()

    def store_unit(v):
        @pl.when(home)
        def _():
            pltpu.make_async_copy(ybuf.at[v], out_at(m, v), o_recv).start()

        @pl.when(jnp.logical_not(home))
        def _():
            rcopy(ybuf.at[v], out_at(m, v), od_send.at[v], o_recv, pp=partner).start()

        rcopy(ybuf.at[v], out_at(m, v), da_send.at[v], o_recv, tp=r_bwd, pp=2 * x + odd).start()

        @pl.when(odd == 1)
        def _():
            rcopy(ybuf.at[v], out_at(m, v), db_send.at[v], rr_recv.at[c, v], tp=r_fwd, pp=stage1).start()

    stores = jnp.logical_or(odd == 1, x % 2 == 1)

    def unit_step(u, carry):
        tok = pl.ds(pl.multiple_of(u * UNIT, UNIT), UNIT)

        for group, (step0, step1) in (((0, 1), (2, 0)), ((2,), (4, 1)), ((3,), (6, 2))):
            now = jnp.logical_or(jnp.logical_and(layer == 0, u == min(step0, units - 1)),
                                 jnp.logical_or(jnp.logical_and(layer == 1, u == min(step1, units - 1)), jnp.logical_and(layer > 1, u == 0)))

            @pl.when(jnp.logical_and(late_source, now))
            def _():
                for k in group:
                    for h in range(2):
                        relay_weights(k, h)

        @pl.when(jnp.logical_and(relay, u >= lag))
        def _():
            relay_unit(u - lag)

        @pl.when(layer == 0)
        def _():
            pltpu.make_async_copy(x_hbm.at[m, tok], xbuf.at[u], x0_sem.at[u]).wait()

        @pl.when(layer > 0)
        def _():
            wwait(xbuf.at[u], x_recv.at[u])

        @pl.when(jnp.logical_and(stores, u >= hold - 1))
        def _():
            store_input(u - hold + 1)

        @pl.when(jnp.logical_and(stores, u >= hold))
        def _():
            store_unit(u - hold)

        xin = xbuf[u].astype(jnp.float32)
        put_blocks(abuf, 0, layer_norm(xin, packs[0, 0:1, :], packs[0, 1:2, :]))
        for nb in range(1, seq // KBLK + 1):
            @pl.when(u // 2 + 1 == nb)
            def _():
                attention(nb, cmask[u % 2], tok, u)

        for n in range(model // 256):
            cols = slice(n * 256, (n + 1) * 256)
            attn = jnp.dot(blocks(ctx, 0, pairs), blocks(wout, 2 * n, 2), preferred_element_type=jnp.float32)
            hbuf[:, cols] = (xbuf[u, :, cols].astype(jnp.float32) + attn + packs[0, 2:3, cols]).astype(jnp.bfloat16)
        put_blocks(abuf, 0, layer_norm(hbuf[...].astype(jnp.float32), packs[0, 3:4, :], packs[0, 4:5, :]))
        for q in range(tp_n):
            for n in range(hid_q // 256):
                up = jnp.dot(blocks(abuf, 0, pairs), blocks(wup.at[q], 2 * n, 2), preferred_element_type=jnp.float32)
                up = up + packs[q, 6:7, n * 256:(n + 1) * 256]
                put_blocks(ubuf, q * (hid_q // 128) + 2 * n, gelu(up).astype(jnp.bfloat16))
        half_model = model // 2
        for n in range(2):
            cols = slice(n * half_model, (n + 1) * half_model)
            down = jnp.dot(blocks(ubuf, 0, ubuf.shape[0]), blocks(wdn, n * (half_model // 128), half_model // 128), preferred_element_type=jnp.float32)
            ybuf[u, :, cols] = (hbuf[:, cols].astype(jnp.float32) + down + packs[0, 5:6, cols]).astype(jnp.bfloat16)

            @pl.when(more)
            def _():
                rcopy(ybuf.at[u, :, cols], xbuf.at[u, :, cols], s_send.at[u], x_recv.at[u], tp=r_next, pp=p_next).start()

        return carry

    lax.fori_loop(0, units, unit_step, 0)

    @pl.when(stores)
    def _():
        def last(v, carry):
            store_unit(v)
            return carry

        lax.fori_loop(units - hold, units, last, 0)

        def last_input(v, carry):
            store_input(v)
            return carry

        lax.fori_loop(units - hold + 1, units, last_input, 0)

    @pl.when(relay)
    def _():
        def rest(v, carry):
            relay_unit(v)
            return carry

        lax.fori_loop(units - lag, units, rest, 0)

    @pl.when(moved)
    def _():
        for k, h in pieces:
            sent(sw(k, h), sw_send.at[k, h])

    @pl.when(home)
    def _():
        sent(sw_pack, pk_send.at[0])
        for k, h in mats:
            sent(rl(k, h), rl_send.at[h, k])
        for d in range(4):
            for k, h in pieces:
                sent(sw(k, h), fwd_send.at[d, k, h])

    @pl.when(late_source)
    def _():
        handed_out()

    def drain(u, carry):
        @pl.when(more)
        def _():
            sent(ybuf.at[u], s_send.at[u])

        @pl.when(stores)
        def _():
            sent(ybuf.at[u], da_send.at[u])

            @pl.when(jnp.logical_not(home))
            def _():
                sent(ybuf.at[u], od_send.at[u])

        @pl.when(relay)
        def _():
            sent(ybuf.at[u], rr_send.at[0, u])
            sent(ybuf.at[u], rr_send.at[1, u])

        @pl.when(odd == 1)
        def _():
            sent(ybuf.at[u], db_send.at[u])
            sent(ybuf.at[u], fb_send.at[u])

            @pl.when(x % 2 == 0)
            def _():
                sent(ybuf.at[u], fc_send.at[u])

            @pl.when(c == 1)
            def _():
                sent(ybuf.at[u], fa_send.at[u])

        return carry

    lax.fori_loop(0, units, drain, 0)

    @pl.when(relay)
    def _():
        wwait(out.at[pl.ds(0, out.shape[0] // 2)], o_recv)

    @pl.when(jnp.logical_not(relay))
    def _():
        wwait(out, o_recv)


def solution(mesh):
    tp_size = mesh.shape['tp']
    in_specs = (P('dp'), P('dp'), P('pp'), P('pp'), P('pp', None, None, 'tp'), P('pp', None, 'tp', None), P('pp', 'tp', None), P('pp'), P('pp'), P('pp'), P('pp', None, 'tp'), P('pp', 'tp'), P('pp', 'tp', None), P('pp'))

    def per_device(x_in, seq_lens, ln1_gain, ln1_shift, w_qkv, b_qkv, w_out, b_out, ln2_gain, ln2_shift, w_up, b_up, w_down, b_down):
        micro_n, batch_n, seq_n, model_n = x_in.shape
        heads_n = b_qkv.shape[2] * tp_size
        quarter = w_qkv.shape[3]
        hid_q = w_up.shape[2]
        bf16, f32 = jnp.bfloat16, jnp.float32
        wqkv_t = jnp.transpose(w_qkv[0], (1, 0, 2))
        b_qkv_row = jnp.pad(b_qkv.reshape(1, 3 * quarter), ((0, 0), (0, model_n - 3 * quarter)))
        pack = jnp.concatenate([ln1_gain, ln1_shift, b_out, ln2_gain, ln2_shift, b_down, b_up, b_qkv_row], axis=0).astype(f32)
        units = seq_n // UNIT
        pairs = model_n // 128
        dma = pltpu.SemaphoreType.DMA
        anywhere = pl.BlockSpec(memory_space=pl.ANY)
        tokens = batch_n * seq_n
        out = pl.pallas_call(
            functools.partial(kernel, heads_n),
            out_shape=jax.ShapeDtypeStruct((micro_n, tokens, model_n), bf16),
            in_specs=[anywhere, pl.BlockSpec(memory_space=pltpu.SMEM)] + [anywhere] * 5,
            out_specs=anywhere,
            scratch_shapes=[
                pltpu.VMEM((tp_size, 3 * quarter // 128, model_n, 128), bf16),
                pltpu.VMEM((model_n // 128, tp_size * quarter, 128), bf16),
                pltpu.VMEM((tp_size, hid_q // 128, model_n, 128), bf16),
                pltpu.VMEM((model_n // 128, tp_size * hid_q, 128), bf16),
                pltpu.VMEM((tp_size,) + pack.shape, f32),
                pltpu.VMEM((2, 3 * quarter // 128, model_n // 2, 128), bf16),
                pltpu.VMEM((2, model_n // 128, quarter // 2, 128), bf16),
                pltpu.VMEM((2, hid_q // 128, model_n // 2, 128), bf16),
                pltpu.VMEM((2, model_n // 128, hid_q // 2, 128), bf16),
                pltpu.VMEM((3 * quarter // 128, model_n, 128), bf16),
                pltpu.VMEM((model_n // 128, quarter, 128), bf16),
                pltpu.VMEM((hid_q // 128, model_n, 128), bf16),
                pltpu.VMEM((model_n // 128, hid_q, 128), bf16),
                pltpu.VMEM(pack.shape, f32),
                pltpu.VMEM((units, UNIT, model_n), bf16),
                pltpu.VMEM((units, UNIT, model_n), bf16),
                *[pltpu.VMEM((quarter // 128, seq_n, 128), bf16)] * tp_size,
                *[pltpu.VMEM((quarter // 128, units, 128, UNIT), bf16)] * tp_size,
                pltpu.VMEM((seq_n, 128), bf16),
                pltpu.VMEM((pairs, 2, 256, 128), bf16),
                pltpu.VMEM((2, KBLK, 256), f32),
                pltpu.VMEM((2, seq_n // KBLK, KBLK, 256), f32),
                pltpu.VMEM((model_n // 128, UNIT, 128), bf16),
                pltpu.VMEM((model_n // 128, UNIT, 128), bf16),
                pltpu.VMEM((UNIT, model_n), bf16),
                pltpu.VMEM((tp_size * hid_q // 128, UNIT, 128), bf16),
                dma((5, 2)), dma((5, 2)), dma((4, 5, 2)), dma((4, 5, 2)), dma((2, 4)), dma((2, 4)), dma((2, 5, 2)), dma((1,)), pltpu.SemaphoreType.REGULAR,
                *[dma((units,))] * 9,
                dma((2, units)), dma((2, units)), dma,
            ],
            compiler_params=pltpu.CompilerParams(collective_id=0, has_side_effects=True, vmem_limit_bytes=63 * 1024 * 1024),
            cost_estimate=pl.CostEstimate(flops=30 * 10 ** 9, bytes_accessed=40 * 10 ** 6, transcendentals=10 ** 7),
        )(x_in.reshape(micro_n, tokens, model_n), seq_lens.reshape(micro_n * batch_n), wqkv_t, w_out[0], w_up[0], w_down[0], pack)
        return out.reshape((1,) + x_in.shape)

    return jax.shard_map(per_device, mesh=mesh, in_specs=in_specs, out_specs=P('pp', 'dp'), check_vma=False)
```

```python
import functools
import math

import jax
import jax.numpy as jnp
import numpy as np
from jax import lax
from jax.experimental import pallas as pl
from jax.experimental.pallas import tpu as pltpu
from jax.sharding import PartitionSpec as P

MESH = pl.DeviceIdType.MESH
UNIT = 128
LANE = 128
KBLK = 256
NEG = -1e30


def alibi_slopes(heads_n):
    closest = 2 ** int(math.floor(math.log2(heads_n)))
    base_rate = 2.0 ** (-8.0 / closest)
    slope_list = [base_rate ** (head_idx + 1) for head_idx in range(closest)]
    extra_rate = 2.0 ** (-4.0 / closest)
    slope_list = slope_list + [extra_rate ** (2 * head_idx + 1) for head_idx in range(min(closest, heads_n - closest))]
    return np.array(slope_list, dtype=np.float32)


def split_bf16(value):
    parts = []
    rest = np.float32(value)
    for _ in range(3):
        part = rest.astype(jnp.bfloat16).astype(np.float32)
        parts.append(float(part))
        rest = np.float32(rest - part)
    return parts


def layer_norm(x, gain, shift):
    mean = jnp.mean(x, axis=-1, keepdims=True)
    cent = x - mean
    var = jnp.mean(cent * cent, axis=-1, keepdims=True)
    return (cent * lax.rsqrt(var + 1e-5) * gain + shift).astype(jnp.bfloat16)


def gelu(x):
    inner = math.sqrt(2.0 / math.pi) * (x + 0.044715 * (x * x * x))
    return 0.5 * x * (1.0 + jnp.tanh(inner))


def kernel(heads_n, x_hbm, lens, wqkv_in, wout_in, wup_in, wdn_in, pack_in, out,
           wqkv, wout, wup, wdn, packs, rl_qkv, rl_out, rl_up, rl_dn, sw_qkv, sw_out, sw_up, sw_dn, sw_pack,
           xbuf, ybuf, kc0, kc1, kc2, kc3, vt0, vt1, vt2, vt3, kx, qaug, cmask, sbuf, abuf, ctx, hbuf, ubuf,
           sw_send, sw_recv, w_recv, fwd_send, rl_send, rl_recv, dir_send, pk_send, go,
           x0_sem, x_recv, s_send, od_send, da_send, db_send, fa_send, fb_send, fc_send,
           rr_recv, rr_send, o_recv):
    tp_n = 4
    units = xbuf.shape[0]
    model = xbuf.shape[2]
    seq = units * UNIT
    quarter = wqkv.shape[1] // 3 * LANE
    hid_q = wup.shape[1] * LANE
    pairs = model // LANE
    per_q = quarter // LANE

    r = lax.axis_index("tp")
    p = lax.axis_index("pp")
    x = p // 2
    c = p % 2
    odd = (r + (x + 1) // 2 + 1) % 2
    even_col = x + (1 - x % 2) * (2 - 2 * x)
    layer = odd * (2 * x + 1) + (1 - odd) * 2 * even_col
    home = odd == c
    moved = jnp.logical_and(c == 0, x % 2 == 0)
    level = x == 1
    ahead = jnp.logical_or(r % 2 == 0, level)
    rp, rm, ro = (r + 1) % tp_n, (r + 3) % tp_n, (r + 2) % tp_n
    partner = 2 * x + (1 - c)
    sig = 1 - 2 * c
    r_fwd = (r + sig + tp_n) % tp_n
    r_bwd = (r - sig + tp_n) % tp_n
    stage0, stage1 = 2 * x, 2 * x + 1
    x_n = 4

    def micro_of(row, core, lay):
        hops = (lay + 1) // 4
        return 2 * (((row + 8 - (1 - 2 * core) * hops) % tp_n) // 2) + core

    m = micro_of(r, c, layer)

    def rcopy(src, dst, ssem, rsem, **dev):
        return pltpu.make_async_remote_copy(src_ref=src, dst_ref=dst, send_sem=ssem, recv_sem=rsem,
                                            device_id=dev, device_id_type=MESH)

    barrier = pltpu.get_barrier_semaphore()
    for dr in range(tp_n):
        for dc in range(2):
            if dr or dc:
                pl.semaphore_signal(barrier, inc=1, device_id={"tp": (r + dr) % tp_n, "pp": 2 * x + (c + dc) % 2}, device_id_type=MESH)
    for dx in range(1, x_n):
        pl.semaphore_signal(barrier, inc=1, device_id={"pp": 2 * ((x + dx) % x_n) + c}, device_id_type=MESH)
    pl.semaphore_wait(barrier, 10)

    def wsrc(k, h, n):
        if k == 0:
            return wqkv_in.at[n // per_q, pl.ds(h * (model // 2), model // 2), pl.ds(n % per_q * LANE, LANE)]
        ref = (None, wout_in, wup_in, wdn_in)[k]
        half = ref.shape[0] // 2
        return ref.at[pl.ds(h * half, half), pl.ds(n * LANE, LANE)]

    def wdst(k, q, h=0):
        if k == 4:
            return packs.at[q]
        if k == 0 or k == 2:
            return (wqkv, None, wup)[k].at[q, :, pl.ds(h * (model // 2), model // 2), :]
        ref, half = (wout, quarter // 2) if k == 1 else (wdn, hid_q // 2)
        return ref.at[:, pl.ds(pl.multiple_of((2 * q + h) * half, half), half), :]

    def rl(k, h):
        return (rl_qkv, rl_out, rl_up, rl_dn)[k].at[h]

    def sw(k, h):
        if k == 4:
            return sw_pack
        ref = (sw_qkv, sw_out, sw_up, sw_dn)[k]
        half = ref.shape[1] // 2
        return ref.at[:, pl.ds(h * half, half), :]

    def fetch(k, h, dst, move):
        if k == 4:
            todo = [(pack_in, dst)]
        else:
            todo = [(wsrc(k, h, n), dst.at[n]) for n in range(dst.shape[0])]
        for src, to in todo:
            if move:
                rcopy(src, to, sw_send.at[k, h], sw_recv.at[k, h], pp=2 * (2 - x)).start()
            else:
                pltpu.make_async_copy(src, to, sw_recv.at[k, h]).start()

    def wwait(view, sem):
        rcopy(view, view, sem, sem, pp=partner).wait_recv()

    pieces = [(4, 0), (1, 0), (1, 1), (0, 0), (0, 1), (2, 0), (2, 1), (3, 0), (3, 1)]
    mats = pieces[1:]

    @pl.when(jnp.logical_and(moved, odd == 1))
    def _():
        for k, h in pieces:
            fetch(k, h, wdst(k, r, h), True)

    @pl.when(jnp.logical_and(moved, odd == 0))
    def _():
        for k, h in pieces:
            fetch(k, h, sw(k, h), True)

    @pl.when(jnp.logical_and(jnp.logical_not(moved), home))
    def _():
        for k, h in pieces:
            fetch(k, h, wdst(k, r, h), False)

    @pl.when(jnp.logical_not(jnp.logical_or(moved, home)))
    def _():
        for k, h in pieces:
            fetch(k, h, sw(k, h), False)

    @pl.when(layer == 0)
    def _():
        for u in range(units):
            pltpu.make_async_copy(x_hbm.at[m, pl.ds(u * UNIT, UNIT)], xbuf.at[u], x0_sem.at[u]).start()

    kc, vt = (kc0, kc1, kc2, kc3), (vt0, vt1, vt2, vt3)
    for ref in kc + vt:
        ref[...] = jnp.zeros_like(ref)
    length = lens[m]
    key = lax.broadcasted_iota(jnp.int32, (seq, LANE), 0)
    lane = lax.broadcasted_iota(jnp.int32, (seq, LANE), 1)
    high = (key // KBLK) * KBLK
    part = jnp.where(lane % 2 == 0, high, key - high).astype(jnp.float32)
    dead = jnp.where(key >= length, NEG, 0.0)
    kx[...] = jnp.where(lane < 6, part, jnp.where(lane == 6, dead, 0.0)).astype(jnp.bfloat16)
    slopes = alibi_slopes(heads_n)
    row = lax.broadcasted_iota(jnp.int32, (LANE, KBLK), 0)
    second = lax.broadcasted_iota(jnp.int32, (LANE, KBLK), 1) >= LANE
    for pair in range(pairs):
        (h0, m0, l0), (h1, m1, l1) = split_bf16(slopes[2 * pair]), split_bf16(slopes[2 * pair + 1])
        hi, mid, low = jnp.where(second, h1, h0), jnp.where(second, m1, m0), jnp.where(second, l1, l0)
        val = jnp.where(row < 2, hi, jnp.where(row < 4, mid, jnp.where(row < 6, low, jnp.where(row == 6, 1.0, 0.0))))
        for side in range(2):
            qaug[pair, side, LANE:, :] = val[:, side * LANE:(side + 1) * LANE].astype(jnp.bfloat16)
    kpos = lax.broadcasted_iota(jnp.int32, (KBLK, KBLK), 0)
    qpos = lax.broadcasted_iota(jnp.int32, (KBLK, KBLK), 1) % LANE
    cmask[0] = jnp.where(kpos <= qpos, 0.0, NEG)
    cmask[1] = jnp.where(kpos <= qpos + LANE, 0.0, NEG)

    def to_relay(k, h):
        rcopy(wdst(k, r, h), rl(k, h), rl_send.at[h, k], rl_recv.at[h, k], tp=(rp, rm)[h]).start()

    def to_partner(k, q, d, h):
        rcopy(wdst(k, q, h), wdst(k, q, h), fwd_send.at[d, k, h], w_recv.at[d, k, h], pp=partner).start()

    def hand_out(behind=()):
        for i, (k, h) in enumerate(pieces):
            wwait(sw(k, h), sw_recv.at[k, h])
            rcopy(sw(k, h), wdst(k, r, h), dir_send.at[0, k, h], w_recv.at[3, k, h], tp=rp).start()
            rcopy(sw(k, h), wdst(k, r, h), dir_send.at[1, k, h], w_recv.at[1, k, h], tp=rm).start()
            if 3 <= i < len(behind) + 3:
                relay_weights(*behind[i - 3])

    def relay_weights(k, h):
        wwait(rl(k, h), rl_recv.at[h, k])
        rcopy(rl(k, h), wdst(k, (rm, rp)[h], h), rl_send.at[h, k], w_recv.at[2, k, h], tp=(rp, rm)[h]).start()

    def from_partner():
        for d, q in ((0, r), (1, rp), (3, rm), (2, ro)):
            for k, h in pieces:
                wwait(wdst(k, q, h), w_recv.at[d, k, h])

    def sent(view, sem):
        rcopy(view, view, sem, sem, pp=partner).wait_send()

    def handed_out():
        for k, h in pieces:
            for d in range(2):
                sent(sw(k, h), dir_send.at[d, k, h])
        for k, h in mats:
            sent(rl(k, h), rl_send.at[h, k])

    @pl.when(home)
    def _():
        for k, h in pieces:
            wwait(wdst(k, r, h), sw_recv.at[k, h])
            if k == 4:
                rcopy(wdst(k, r), wdst(k, r), pk_send.at[0], w_recv.at[2, k, h], tp=ro).start()
            else:
                @pl.when(ahead)
                def _():
                    to_relay(k, h)
            to_partner(k, r, 0, h)

        @pl.when(jnp.logical_not(ahead))
        def _():
            pl.semaphore_wait(go, 1)
            for k, h in mats:
                to_relay(k, h)

        for k, h in pieces:
            for d, q in ((1, rp), (3, rm)):
                wwait(wdst(k, q, h), w_recv.at[d, k, h])
                to_partner(k, q, d, h)
        for k, h in pieces:
            wwait(wdst(k, ro, h), w_recv.at[2, k, h])
            to_partner(k, ro, 2, h)

    late_source = jnp.logical_not(jnp.logical_or(home, jnp.logical_or(r % 2 == 1, level)))

    @pl.when(jnp.logical_not(jnp.logical_or(home, late_source)))
    def _():
        hand_out(mats)
        for k, h in mats[len(pieces) - 3:]:
            relay_weights(k, h)
        handed_out()

        @pl.when(jnp.logical_not(level))
        def _():
            pl.semaphore_signal(go, inc=1, device_id={"pp": partner}, device_id_type=MESH)

        from_partner()

    @pl.when(late_source)
    def _():
        hand_out()
        from_partner()

    def out_at(mm, u):
        return out.at[mm, pl.ds(pl.multiple_of(u * UNIT, UNIT), UNIT)]

    m_a = micro_of(rm, 0, stage1)
    m_b = micro_of(rp, 1, stage1)
    relay = jnp.logical_and(odd == 0, jnp.logical_or(c == 1, x % 2 == 0))
    lag = min(5, units) * (x % 2) + (1 - x % 2) * (min(5, units) + (units - min(5, units)) * (x // 2))
    hold = min(5, units) * (1 - (x + 2) // 3) + (x + 2) // 3

    def relay_unit(v):
        wwait(out_at(m_a, v), rr_recv.at[0, v])
        rcopy(out_at(m_a, v), out_at(m_a, v), rr_send.at[0, v], o_recv, tp=rp).start()
        wwait(out_at(m_b, v), rr_recv.at[1, v])
        rcopy(out_at(m_b, v), out_at(m_b, v), rr_send.at[1, v], o_recv, tp=rm).start()

    def wide(parts):
        return jnp.concatenate(parts, axis=1)

    def blocks(ref, first, count):
        return wide([ref[first + i] for i in range(count)])

    def put_blocks(ref, first, val):
        for i in range(val.shape[1] // LANE):
            ref[first + i] = val[:, i * LANE:(i + 1) * LANE]

    def attention(nb, diag, tok, u):
        head_row = lax.broadcasted_iota(jnp.int32, (LANE, LANE), 0) < 64

        def project(q):
            for j in range(3):
                weights = wide([wqkv[q, j * per_q + i] for i in range(per_q)])
                o = jnp.dot(blocks(abuf, 0, pairs), weights, preferred_element_type=jnp.float32)
                o = (o + packs[q, 7:8, j * quarter:(j + 1) * quarter]).astype(jnp.bfloat16)
                for i in range(per_q):
                    part = o[:, i * LANE:(i + 1) * LANE]
                    if j == 0:
                        q_t = (part.astype(jnp.float32) * 0.125).T
                        qaug[q * per_q + i, 0, :LANE, :] = jnp.where(head_row, q_t, 0.0).astype(jnp.bfloat16)
                        qaug[q * per_q + i, 1, :LANE, :] = jnp.where(head_row, 0.0, q_t).astype(jnp.bfloat16)
                    elif j == 1:
                        kc[q][i, tok, :] = part
                    else:
                        vt[q][i, u] = part.astype(jnp.float32).T.astype(jnp.bfloat16)

        def scores(pair):
            kq = kc[pair // per_q]
            q_rhs = blocks(qaug.at[pair], 0, 2)
            top = None
            for b in range(nb):
                keys = wide([kq[pair % per_q, b * KBLK:(b + 1) * KBLK, :], kx[b * KBLK:(b + 1) * KBLK, :]])
                s = jnp.dot(keys, q_rhs, preferred_element_type=jnp.float32)
                if b == nb - 1:
                    s = s + diag
                sbuf[pair % 2, b] = s
                peak = jnp.max(s, axis=0, keepdims=True)
                top = peak if top is None else jnp.maximum(top, peak)
            return top

        def weigh(pair, top):
            vq = vt[pair // per_q].at[pair % per_q]
            total = None
            acc = None
            for b in range(nb):
                e = jnp.exp(sbuf[pair % 2, b] - top)
                part_sum = jnp.sum(e, axis=0, keepdims=True)
                total = part_sum if total is None else total + part_sum
                pv = jnp.dot(blocks(vq, b * KBLK // UNIT, KBLK // UNIT), e.astype(jnp.bfloat16), preferred_element_type=jnp.float32)
                acc = pv if acc is None else acc + pv
            acc = acc * (1.0 / total)
            both = jnp.concatenate([acc[:64, :LANE], acc[64:, LANE:]], axis=0)
            ctx[pair] = both.T.astype(jnp.bfloat16)

        project(0)
        top = None
        for pair in range(pairs + 1):
            if pair % per_q == 0 and pair // per_q + 1 < tp_n:
                project(pair // per_q + 1)
            later = scores(pair) if pair < pairs else None
            if pair > 0:
                weigh(pair - 1, top)
            top = later

    more = layer < 2 * x_n - 1
    nxt = (layer + 1) % (2 * x_n)
    half_n = nxt // 2
    x_next = half_n + (1 - nxt % 2) * (1 - half_n % 2) * (2 - 2 * half_n)
    p_next = 2 * x_next + c
    r_next = (r + (1 - odd) * (x % 2) * sig + tp_n) % tp_n

    def store_input(v):
        @pl.when(odd == 1)
        def _():
            @pl.when(c == 0)
            def _():
                pltpu.make_async_copy(xbuf.at[v], out_at(m, v), o_recv).start()

            @pl.when(c == 1)
            def _():
                rcopy(xbuf.at[v], out_at(m, v), fa_send.at[v], o_recv, pp=partner).start()

            @pl.when(x % 2 == 1)
            def _():
                rcopy(xbuf.at[v], out_at(m, v), fb_send.at[v], o_recv, tp=r_fwd, pp=stage0).start()

            @pl.when(x % 2 == 0)
            def _():
                rcopy(xbuf.at[v], out_at(m, v), fb_send.at[v], rr_recv.at[c, v], tp=r_fwd, pp=stage0).start()
                rcopy(xbuf.at[v], out_at(m, v), fc_send.at[v], o_recv, tp=r_bwd, pp=stage0).start()

    def store_unit(v):
        @pl.when(home)
        def _():
            pltpu.make_async_copy(ybuf.at[v], out_at(m, v), o_recv).start()

        @pl.when(jnp.logical_not(home))
        def _():
            rcopy(ybuf.at[v], out_at(m, v), od_send.at[v], o_recv, pp=partner).start()

        rcopy(ybuf.at[v], out_at(m, v), da_send.at[v], o_recv, tp=r_bwd, pp=2 * x + odd).start()

        @pl.when(odd == 1)
        def _():
            rcopy(ybuf.at[v], out_at(m, v), db_send.at[v], rr_recv.at[c, v], tp=r_fwd, pp=stage1).start()

    stores = jnp.logical_or(odd == 1, x % 2 == 1)

    def unit_step(u, carry):
        tok = pl.ds(pl.multiple_of(u * UNIT, UNIT), UNIT)

        for group, (step0, step1) in (((0, 1), (2, 0)), ((2,), (4, 1)), ((3,), (6, 2))):
            now = jnp.logical_or(jnp.logical_and(layer == 0, u == min(step0, units - 1)),
                                 jnp.logical_or(jnp.logical_and(layer == 1, u == min(step1, units - 1)), jnp.logical_and(layer > 1, u == 0)))

            @pl.when(jnp.logical_and(late_source, now))
            def _():
                for k in group:
                    for h in range(2):
                        relay_weights(k, h)

        @pl.when(layer == 0)
        def _():
            pltpu.make_async_copy(x_hbm.at[m, tok], xbuf.at[u], x0_sem.at[u]).wait()

        @pl.when(layer > 0)
        def _():
            wwait(xbuf.at[u], x_recv.at[u])

        xin = xbuf[u].astype(jnp.float32)
        put_blocks(abuf, 0, layer_norm(xin, packs[0, 0:1, :], packs[0, 1:2, :]))
        for nb in range(1, seq // KBLK + 1):
            @pl.when(u // 2 + 1 == nb)
            def _():
                attention(nb, cmask[u % 2], tok, u)

        @pl.when(jnp.logical_and(stores, u >= hold - 1))
        def _():
            store_input(u - hold + 1)

        @pl.when(jnp.logical_and(stores, u >= hold))
        def _():
            store_unit(u - hold)

        @pl.when(jnp.logical_and(relay, u >= lag))
        def _():
            relay_unit(u - lag)

        for n in range(model // KBLK):
            cols = slice(n * KBLK, (n + 1) * KBLK)
            attn = jnp.dot(blocks(ctx, 0, pairs), blocks(wout, 2 * n, 2), preferred_element_type=jnp.float32)
            hbuf[:, cols] = (xbuf[u, :, cols].astype(jnp.float32) + attn + packs[0, 2:3, cols]).astype(jnp.bfloat16)
        put_blocks(abuf, 0, layer_norm(hbuf[...].astype(jnp.float32), packs[0, 3:4, :], packs[0, 4:5, :]))
        for q in range(tp_n):
            for n in range(hid_q // KBLK):
                up = jnp.dot(blocks(abuf, 0, pairs), blocks(wup.at[q], 2 * n, 2), preferred_element_type=jnp.float32)
                up = up + packs[q, 6:7, n * KBLK:(n + 1) * KBLK]
                put_blocks(ubuf, q * (hid_q // LANE) + 2 * n, gelu(up).astype(jnp.bfloat16))
        half_model = model // 2
        for n in range(2):
            cols = slice(n * half_model, (n + 1) * half_model)
            down = jnp.dot(blocks(ubuf, 0, ubuf.shape[0]), blocks(wdn, n * (half_model // LANE), half_model // LANE), preferred_element_type=jnp.float32)
            ybuf[u, :, cols] = (hbuf[:, cols].astype(jnp.float32) + down + packs[0, 5:6, cols]).astype(jnp.bfloat16)

            @pl.when(more)
            def _():
                rcopy(ybuf.at[u, :, cols], xbuf.at[u, :, cols], s_send.at[u], x_recv.at[u], tp=r_next, pp=p_next).start()

        return carry

    lax.fori_loop(0, units, unit_step, 0)

    @pl.when(stores)
    def _():
        def last(v, carry):
            store_unit(v)
            return carry

        lax.fori_loop(units - hold, units, last, 0)

        def last_input(v, carry):
            store_input(v)
            return carry

        lax.fori_loop(units - hold + 1, units, last_input, 0)

    @pl.when(relay)
    def _():
        def rest(v, carry):
            relay_unit(v)
            return carry

        lax.fori_loop(units - lag, units, rest, 0)

    @pl.when(moved)
    def _():
        for k, h in pieces:
            sent(sw(k, h), sw_send.at[k, h])

    @pl.when(home)
    def _():
        sent(sw_pack, pk_send.at[0])
        for k, h in mats:
            sent(rl(k, h), rl_send.at[h, k])
        for d in range(4):
            for k, h in pieces:
                sent(sw(k, h), fwd_send.at[d, k, h])

    @pl.when(late_source)
    def _():
        handed_out()

    def drain(u, carry):
        @pl.when(more)
        def _():
            sent(ybuf.at[u], s_send.at[u])

        @pl.when(stores)
        def _():
            sent(ybuf.at[u], da_send.at[u])

            @pl.when(jnp.logical_not(home))
            def _():
                sent(ybuf.at[u], od_send.at[u])

        @pl.when(relay)
        def _():
            sent(ybuf.at[u], rr_send.at[0, u])
            sent(ybuf.at[u], rr_send.at[1, u])

        @pl.when(odd == 1)
        def _():
            sent(ybuf.at[u], db_send.at[u])
            sent(ybuf.at[u], fb_send.at[u])

            @pl.when(x % 2 == 0)
            def _():
                sent(ybuf.at[u], fc_send.at[u])

            @pl.when(c == 1)
            def _():
                sent(ybuf.at[u], fa_send.at[u])

        return carry

    lax.fori_loop(0, units, drain, 0)

    @pl.when(relay)
    def _():
        wwait(out.at[pl.ds(0, out.shape[0] // 2)], o_recv)

    @pl.when(jnp.logical_not(relay))
    def _():
        wwait(out, o_recv)


def copy_kernel(src, dst):
    dst[...] = src[...]


def copy_out(val):
    rows, cols = val.shape
    spec = pl.BlockSpec((rows // 8, cols), lambda i: (i, 0))
    return pl.pallas_call(copy_kernel, out_shape=jax.ShapeDtypeStruct(val.shape, val.dtype), grid=(8,), in_specs=[spec], out_specs=spec,
                          cost_estimate=pl.CostEstimate(flops=rows * cols, bytes_accessed=4 * rows * cols, transcendentals=0))(val)


def solution(mesh):
    tp_size = mesh.shape['tp']
    in_specs = (P('dp'), P('dp'), P('pp'), P('pp'), P('pp', None, None, 'tp'), P('pp', None, 'tp', None), P('pp', 'tp', None), P('pp'), P('pp'), P('pp'), P('pp', None, 'tp'), P('pp', 'tp'), P('pp', 'tp', None), P('pp'))

    def per_device(x_in, seq_lens, ln1_gain, ln1_shift, w_qkv, b_qkv, w_out, b_out, ln2_gain, ln2_shift, w_up, b_up, w_down, b_down):
        micro_n, batch_n, seq_n, model_n = x_in.shape
        heads_n = b_qkv.shape[2] * tp_size
        quarter = w_qkv.shape[3]
        hid_q = w_up.shape[2]
        bf16, f32 = jnp.bfloat16, jnp.float32
        wqkv_t = jnp.transpose(w_qkv[0], (1, 0, 2))
        b_qkv_row = jnp.pad(b_qkv.reshape(1, 3 * quarter), ((0, 0), (0, model_n - 3 * quarter)))
        pack = jnp.concatenate([ln1_gain, ln1_shift, b_out, ln2_gain, ln2_shift, b_down, b_up, b_qkv_row], axis=0).astype(f32)
        units = seq_n // UNIT
        pairs = model_n // LANE
        dma = pltpu.SemaphoreType.DMA
        anywhere = pl.BlockSpec(memory_space=pl.ANY)
        tokens = batch_n * seq_n
        out = pl.pallas_call(
            functools.partial(kernel, heads_n),
            out_shape=jax.ShapeDtypeStruct((micro_n, tokens, model_n), bf16),
            in_specs=[anywhere, pl.BlockSpec(memory_space=pltpu.SMEM)] + [anywhere] * 5,
            out_specs=anywhere,
            scratch_shapes=[
                pltpu.VMEM((tp_size, 3 * quarter // LANE, model_n, LANE), bf16),
                pltpu.VMEM((model_n // LANE, tp_size * quarter, LANE), bf16),
                pltpu.VMEM((tp_size, hid_q // LANE, model_n, LANE), bf16),
                pltpu.VMEM((model_n // LANE, tp_size * hid_q, LANE), bf16),
                pltpu.VMEM((tp_size,) + pack.shape, f32),
                pltpu.VMEM((2, 3 * quarter // LANE, model_n // 2, LANE), bf16),
                pltpu.VMEM((2, model_n // LANE, quarter // 2, LANE), bf16),
                pltpu.VMEM((2, hid_q // LANE, model_n // 2, LANE), bf16),
                pltpu.VMEM((2, model_n // LANE, hid_q // 2, LANE), bf16),
                pltpu.VMEM((3 * quarter // LANE, model_n, LANE), bf16),
                pltpu.VMEM((model_n // LANE, quarter, LANE), bf16),
                pltpu.VMEM((hid_q // LANE, model_n, LANE), bf16),
                pltpu.VMEM((model_n // LANE, hid_q, LANE), bf16),
                pltpu.VMEM(pack.shape, f32),
                pltpu.VMEM((units, UNIT, model_n), bf16),
                pltpu.VMEM((units, UNIT, model_n), bf16),
                *[pltpu.VMEM((quarter // LANE, seq_n, LANE), bf16)] * tp_size,
                *[pltpu.VMEM((quarter // LANE, units, LANE, UNIT), bf16)] * tp_size,
                pltpu.VMEM((seq_n, LANE), bf16),
                pltpu.VMEM((pairs, 2, KBLK, LANE), bf16),
                pltpu.VMEM((2, KBLK, KBLK), f32),
                pltpu.VMEM((2, seq_n // KBLK, KBLK, KBLK), f32),
                pltpu.VMEM((model_n // LANE, UNIT, LANE), bf16),
                pltpu.VMEM((model_n // LANE, UNIT, LANE), bf16),
                pltpu.VMEM((UNIT, model_n), bf16),
                pltpu.VMEM((tp_size * hid_q // LANE, UNIT, LANE), bf16),
                dma((5, 2)), dma((5, 2)), dma((4, 5, 2)), dma((4, 5, 2)), dma((2, 4)), dma((2, 4)), dma((2, 5, 2)), dma((1,)), pltpu.SemaphoreType.REGULAR,
                *[dma((units,))] * 9,
                dma((2, units)), dma((2, units)), dma,
            ],
            compiler_params=pltpu.CompilerParams(collective_id=0, has_side_effects=True, vmem_limit_bytes=63 * 1024 * 1024),
            cost_estimate=pl.CostEstimate(flops=30 * 10 ** 9, bytes_accessed=40 * 10 ** 6, transcendentals=10 ** 7),
        )(x_in.reshape(micro_n, tokens, model_n), seq_lens.reshape(micro_n * batch_n), wqkv_t, w_out[0], w_up[0], w_down[0], pack)
        return copy_out(out.reshape(micro_n * tokens, model_n)).reshape((1,) + x_in.shape)

    return jax.shard_map(per_device, mesh=mesh, in_specs=in_specs, out_specs=P('pp', 'dp'), check_vma=False)
```

```python
import functools
import math

import jax
import jax.numpy as jnp
import numpy as np
from jax import lax
from jax.experimental import pallas as pl
from jax.experimental.pallas import tpu as pltpu
from jax.sharding import PartitionSpec as P

MESH = pl.DeviceIdType.MESH
UNIT = 128
LANE = 128
KBLK = 256
NEG = -1e30


def alibi_slopes(heads_n):
    closest = 2 ** int(math.floor(math.log2(heads_n)))
    base_rate = 2.0 ** (-8.0 / closest)
    slope_list = [base_rate ** (head_idx + 1) for head_idx in range(closest)]
    extra_rate = 2.0 ** (-4.0 / closest)
    slope_list = slope_list + [extra_rate ** (2 * head_idx + 1) for head_idx in range(min(closest, heads_n - closest))]
    return np.array(slope_list, dtype=np.float32)


def split_bf16(value):
    parts = []
    rest = np.float32(value)
    for _ in range(3):
        part = rest.astype(jnp.bfloat16).astype(np.float32)
        parts.append(float(part))
        rest = np.float32(rest - part)
    return parts


def layer_norm(x, gain, shift):
    mean = jnp.mean(x, axis=-1, keepdims=True)
    cent = x - mean
    var = jnp.mean(cent * cent, axis=-1, keepdims=True)
    return (cent * lax.rsqrt(var + 1e-5) * gain + shift).astype(jnp.bfloat16)


def gelu(x):
    inner = math.sqrt(2.0 / math.pi) * (x + 0.044715 * (x * x * x))
    return 0.5 * x * (1.0 + jnp.tanh(inner))


def kernel(heads_n, x_hbm, lens, wqkv_in, wout_in, wup_in, wdn_in,
           ln1_gain, ln1_shift, b_out, ln2_gain, ln2_shift, b_down, b_up, b_qkv, out,
           wqkv, wout, wup, wdn, packs, pack_in, rl_qkv, rl_out, rl_up, rl_dn, sw_qkv, sw_out, sw_up, sw_dn, sw_pack,
           xbuf, ybuf, kc0, kc1, kc2, kc3, vt0, vt1, vt2, vt3, kx, qaug, cmask, sbuf, abuf, ctx, hbuf, ubuf,
           sw_send, sw_recv, w_recv, fwd_send, rl_send, rl_recv, dir_send, pk_send, go,
           x0_sem, x_recv, s_send, od_send, da_send, db_send, fa_send, fb_send, fc_send,
           rr_recv, rr_send, o_recv):
    tp_n = 4
    units = xbuf.shape[0]
    model = xbuf.shape[2]
    seq = units * UNIT
    quarter = wqkv.shape[1] // 3 * LANE
    hid_q = wup.shape[1] * LANE
    pairs = model // LANE
    per_q = quarter // LANE

    r = lax.axis_index("tp")
    p = lax.axis_index("pp")
    x = p // 2
    c = p % 2
    odd = (r + (x + 1) // 2 + 1) % 2
    even_col = x + (1 - x % 2) * (2 - 2 * x)
    layer = odd * (2 * x + 1) + (1 - odd) * 2 * even_col
    home = odd == c
    moved = jnp.logical_and(c == 0, x % 2 == 0)
    level = x == 1
    ahead = jnp.logical_or(r % 2 == 0, level)
    rp, rm, ro = (r + 1) % tp_n, (r + 3) % tp_n, (r + 2) % tp_n
    partner = 2 * x + (1 - c)
    sig = 1 - 2 * c
    r_fwd = (r + sig + tp_n) % tp_n
    r_bwd = (r - sig + tp_n) % tp_n
    stage0, stage1 = 2 * x, 2 * x + 1
    x_n = 4

    def micro_of(row, core, lay):
        hops = (lay + 1) // 4
        return 2 * (((row + 8 - (1 - 2 * core) * hops) % tp_n) // 2) + core

    m = micro_of(r, c, layer)

    def rcopy(src, dst, ssem, rsem, **dev):
        return pltpu.make_async_remote_copy(src_ref=src, dst_ref=dst, send_sem=ssem, recv_sem=rsem,
                                            device_id=dev, device_id_type=MESH)

    barrier = pltpu.get_barrier_semaphore()
    for dr in range(tp_n):
        for dc in range(2):
            if dr or dc:
                pl.semaphore_signal(barrier, inc=1, device_id={"tp": (r + dr) % tp_n, "pp": 2 * x + (c + dc) % 2}, device_id_type=MESH)
    for dx in range(1, x_n):
        pl.semaphore_signal(barrier, inc=1, device_id={"pp": 2 * ((x + dx) % x_n) + c}, device_id_type=MESH)

    for i, vec in enumerate((ln1_gain, ln1_shift, b_out, ln2_gain, ln2_shift, b_down, b_up)):
        pack_in[i:i + 1, :] = vec[...].astype(jnp.float32)
    width = b_qkv.shape[3]
    for j in range(3):
        for head in range(quarter // width):
            at = j * quarter + head * width
            pack_in[7:8, at:at + width] = b_qkv[0, j, head:head + 1, :].astype(jnp.float32)
    pl.semaphore_wait(barrier, 10)

    def wsrc(k, h, n):
        if k == 0:
            return wqkv_in.at[n // per_q, pl.ds(h * (model // 2), model // 2), pl.ds(n % per_q * LANE, LANE)]
        ref = (None, wout_in, wup_in, wdn_in)[k]
        half = ref.shape[0] // 2
        return ref.at[pl.ds(h * half, half), pl.ds(n * LANE, LANE)]

    def wdst(k, q, h=0):
        if k == 4:
            return packs.at[q]
        if k == 0 or k == 2:
            return (wqkv, None, wup)[k].at[q, :, pl.ds(h * (model // 2), model // 2), :]
        ref, half = (wout, quarter // 2) if k == 1 else (wdn, hid_q // 2)
        return ref.at[:, pl.ds(pl.multiple_of((2 * q + h) * half, half), half), :]

    def rl(k, h):
        return (rl_qkv, rl_out, rl_up, rl_dn)[k].at[h]

    def sw(k, h):
        if k == 4:
            return sw_pack
        ref = (sw_qkv, sw_out, sw_up, sw_dn)[k]
        half = ref.shape[1] // 2
        return ref.at[:, pl.ds(h * half, half), :]

    def fetch(k, h, dst, move):
        if k == 4:
            todo = [(pack_in, dst)]
        else:
            todo = [(wsrc(k, h, n), dst.at[n]) for n in range(dst.shape[0])]
        for src, to in todo:
            if move:
                rcopy(src, to, sw_send.at[k, h], sw_recv.at[k, h], pp=2 * (2 - x)).start()
            else:
                pltpu.make_async_copy(src, to, sw_recv.at[k, h]).start()

    def wwait(view, sem):
        rcopy(view, view, sem, sem, pp=partner).wait_recv()

    pieces = [(4, 0), (1, 0), (1, 1), (0, 0), (0, 1), (2, 0), (2, 1), (3, 0), (3, 1)]
    mats = pieces[1:]

    @pl.when(jnp.logical_and(moved, odd == 1))
    def _():
        for k, h in pieces:
            fetch(k, h, wdst(k, r, h), True)

    @pl.when(jnp.logical_and(moved, odd == 0))
    def _():
        for k, h in pieces:
            fetch(k, h, sw(k, h), True)

    @pl.when(jnp.logical_and(jnp.logical_not(moved), home))
    def _():
        for k, h in pieces:
            fetch(k, h, wdst(k, r, h), False)

    @pl.when(jnp.logical_not(jnp.logical_or(moved, home)))
    def _():
        for k, h in pieces:
            fetch(k, h, sw(k, h), False)

    @pl.when(layer == 0)
    def _():
        for u in range(units):
            pltpu.make_async_copy(x_hbm.at[m, pl.ds(u * UNIT, UNIT)], xbuf.at[u], x0_sem.at[u]).start()

    kc, vt = (kc0, kc1, kc2, kc3), (vt0, vt1, vt2, vt3)
    for ref in kc + vt:
        ref[...] = jnp.zeros_like(ref)
    length = lens[m]
    key = lax.broadcasted_iota(jnp.int32, (seq, LANE), 0)
    lane = lax.broadcasted_iota(jnp.int32, (seq, LANE), 1)
    high = (key // KBLK) * KBLK
    part = jnp.where(lane % 2 == 0, high, key - high).astype(jnp.float32)
    dead = jnp.where(key >= length, NEG, 0.0)
    kx[...] = jnp.where(lane < 6, part, jnp.where(lane == 6, dead, 0.0)).astype(jnp.bfloat16)
    slopes = alibi_slopes(heads_n)
    row = lax.broadcasted_iota(jnp.int32, (LANE, KBLK), 0)
    second = lax.broadcasted_iota(jnp.int32, (LANE, KBLK), 1) >= LANE
    for pair in range(pairs):
        (h0, m0, l0), (h1, m1, l1) = split_bf16(slopes[2 * pair]), split_bf16(slopes[2 * pair + 1])
        hi, mid, low = jnp.where(second, h1, h0), jnp.where(second, m1, m0), jnp.where(second, l1, l0)
        val = jnp.where(row < 2, hi, jnp.where(row < 4, mid, jnp.where(row < 6, low, jnp.where(row == 6, 1.0, 0.0))))
        for side in range(2):
            qaug[pair, side, LANE:, :] = val[:, side * LANE:(side + 1) * LANE].astype(jnp.bfloat16)
    kpos = lax.broadcasted_iota(jnp.int32, (KBLK, KBLK), 0)
    qpos = lax.broadcasted_iota(jnp.int32, (KBLK, KBLK), 1) % LANE
    cmask[0] = jnp.where(kpos <= qpos, 0.0, NEG)
    cmask[1] = jnp.where(kpos <= qpos + LANE, 0.0, NEG)

    def to_relay(k, h):
        rcopy(wdst(k, r, h), rl(k, h), rl_send.at[h, k], rl_recv.at[h, k], tp=(rp, rm)[h]).start()

    def to_partner(k, q, d, h):
        rcopy(wdst(k, q, h), wdst(k, q, h), fwd_send.at[d, k, h], w_recv.at[d, k, h], pp=partner).start()

    def hand_out(behind=()):
        for i, (k, h) in enumerate(pieces):
            wwait(sw(k, h), sw_recv.at[k, h])
            rcopy(sw(k, h), wdst(k, r, h), dir_send.at[0, k, h], w_recv.at[3, k, h], tp=rp).start()
            rcopy(sw(k, h), wdst(k, r, h), dir_send.at[1, k, h], w_recv.at[1, k, h], tp=rm).start()
            if 3 <= i < len(behind) + 3:
                relay_weights(*behind[i - 3])

    def relay_weights(k, h):
        wwait(rl(k, h), rl_recv.at[h, k])
        rcopy(rl(k, h), wdst(k, (rm, rp)[h], h), rl_send.at[h, k], w_recv.at[2, k, h], tp=(rp, rm)[h]).start()

    def from_partner():
        for d, q in ((0, r), (1, rp), (3, rm), (2, ro)):
            for k, h in pieces:
                wwait(wdst(k, q, h), w_recv.at[d, k, h])

    def sent(view, sem):
        rcopy(view, view, sem, sem, pp=partner).wait_send()

    def handed_out():
        for k, h in pieces:
            for d in range(2):
                sent(sw(k, h), dir_send.at[d, k, h])
        for k, h in mats:
            sent(rl(k, h), rl_send.at[h, k])

    @pl.when(home)
    def _():
        for k, h in pieces:
            wwait(wdst(k, r, h), sw_recv.at[k, h])
            if k == 4:
                rcopy(wdst(k, r), wdst(k, r), pk_send.at[0], w_recv.at[2, k, h], tp=ro).start()
            else:
                @pl.when(ahead)
                def _():
                    to_relay(k, h)
            to_partner(k, r, 0, h)

        @pl.when(jnp.logical_not(ahead))
        def _():
            pl.semaphore_wait(go, 1)
            for k, h in mats:
                to_relay(k, h)

        for k, h in pieces:
            for d, q in ((1, rp), (3, rm)):
                wwait(wdst(k, q, h), w_recv.at[d, k, h])
                to_partner(k, q, d, h)
        for k, h in pieces:
            wwait(wdst(k, ro, h), w_recv.at[2, k, h])
            to_partner(k, ro, 2, h)

    late_source = jnp.logical_not(jnp.logical_or(home, jnp.logical_or(r % 2 == 1, level)))

    @pl.when(jnp.logical_not(jnp.logical_or(home, late_source)))
    def _():
        hand_out(mats)
        for k, h in mats[len(pieces) - 3:]:
            relay_weights(k, h)
        handed_out()

        @pl.when(jnp.logical_not(level))
        def _():
            pl.semaphore_signal(go, inc=1, device_id={"pp": partner}, device_id_type=MESH)

        from_partner()

    @pl.when(late_source)
    def _():
        hand_out()
        from_partner()

    def out_at(mm, u):
        return out.at[mm, pl.ds(pl.multiple_of(u * UNIT, UNIT), UNIT)]

    m_a = micro_of(rm, 0, stage1)
    m_b = micro_of(rp, 1, stage1)
    relay = jnp.logical_and(odd == 0, jnp.logical_or(c == 1, x % 2 == 0))
    lag = min(5, units) * (x % 2) + (1 - x % 2) * (min(5, units) + (units - min(5, units)) * (x // 2))
    hold = min(5, units) * (1 - (x + 2) // 3) + (x + 2) // 3

    def relay_unit(v):
        wwait(out_at(m_a, v), rr_recv.at[0, v])
        rcopy(out_at(m_a, v), out_at(m_a, v), rr_send.at[0, v], o_recv, tp=rp).start()
        wwait(out_at(m_b, v), rr_recv.at[1, v])
        rcopy(out_at(m_b, v), out_at(m_b, v), rr_send.at[1, v], o_recv, tp=rm).start()

    def wide(parts):
        return jnp.concatenate(parts, axis=1)

    def blocks(ref, first, count):
        return wide([ref[first + i] for i in range(count)])

    def put_blocks(ref, first, val):
        for i in range(val.shape[1] // LANE):
            ref[first + i] = val[:, i * LANE:(i + 1) * LANE]

    def attention(nb, diag, tok, u):
        head_row = lax.broadcasted_iota(jnp.int32, (LANE, LANE), 0) < 64

        def project(q):
            for j in range(3):
                weights = wide([wqkv[q, j * per_q + i] for i in range(per_q)])
                o = jnp.dot(blocks(abuf, 0, pairs), weights, preferred_element_type=jnp.float32)
                o = (o + packs[q, 7:8, j * quarter:(j + 1) * quarter]).astype(jnp.bfloat16)
                for i in range(per_q):
                    part = o[:, i * LANE:(i + 1) * LANE]
                    if j == 0:
                        q_t = (part.astype(jnp.float32) * 0.125).T
                        qaug[q * per_q + i, 0, :LANE, :] = jnp.where(head_row, q_t, 0.0).astype(jnp.bfloat16)
                        qaug[q * per_q + i, 1, :LANE, :] = jnp.where(head_row, 0.0, q_t).astype(jnp.bfloat16)
                    elif j == 1:
                        kc[q][i, tok, :] = part
                    else:
                        vt[q][i, u] = part.astype(jnp.float32).T.astype(jnp.bfloat16)

        def scores(pair):
            kq = kc[pair // per_q]
            q_rhs = blocks(qaug.at[pair], 0, 2)
            top = None
            for b in range(nb):
                keys = wide([kq[pair % per_q, b * KBLK:(b + 1) * KBLK, :], kx[b * KBLK:(b + 1) * KBLK, :]])
                s = jnp.dot(keys, q_rhs, preferred_element_type=jnp.float32)
                if b == nb - 1:
                    s = s + diag
                sbuf[pair % 2, b] = s
                peak = jnp.max(s, axis=0, keepdims=True)
                top = peak if top is None else jnp.maximum(top, peak)
            return top

        def weigh(pair, top):
            vq = vt[pair // per_q].at[pair % per_q]
            total = None
            acc = None
            for b in range(nb):
                e = jnp.exp(sbuf[pair % 2, b] - top)
                part_sum = jnp.sum(e, axis=0, keepdims=True)
                total = part_sum if total is None else total + part_sum
                pv = jnp.dot(blocks(vq, b * KBLK // UNIT, KBLK // UNIT), e.astype(jnp.bfloat16), preferred_element_type=jnp.float32)
                acc = pv if acc is None else acc + pv
            acc = acc * (1.0 / total)
            both = jnp.concatenate([acc[:64, :LANE], acc[64:, LANE:]], axis=0)
            ctx[pair] = both.T.astype(jnp.bfloat16)

        project(0)
        top = None
        for pair in range(pairs + 1):
            if pair % per_q == 0 and pair // per_q + 1 < tp_n:
                project(pair // per_q + 1)
            later = scores(pair) if pair < pairs else None
            if pair > 0:
                weigh(pair - 1, top)
            top = later

    more = layer < 2 * x_n - 1
    nxt = (layer + 1) % (2 * x_n)
    half_n = nxt // 2
    x_next = half_n + (1 - nxt % 2) * (1 - half_n % 2) * (2 - 2 * half_n)
    p_next = 2 * x_next + c
    r_next = (r + (1 - odd) * (x % 2) * sig + tp_n) % tp_n

    def store_input(v):
        @pl.when(odd == 1)
        def _():
            @pl.when(c == 0)
            def _():
                pltpu.make_async_copy(xbuf.at[v], out_at(m, v), o_recv).start()

            @pl.when(c == 1)
            def _():
                rcopy(xbuf.at[v], out_at(m, v), fa_send.at[v], o_recv, pp=partner).start()

            @pl.when(x % 2 == 1)
            def _():
                rcopy(xbuf.at[v], out_at(m, v), fb_send.at[v], o_recv, tp=r_fwd, pp=stage0).start()

            @pl.when(x % 2 == 0)
            def _():
                rcopy(xbuf.at[v], out_at(m, v), fb_send.at[v], rr_recv.at[c, v], tp=r_fwd, pp=stage0).start()
                rcopy(xbuf.at[v], out_at(m, v), fc_send.at[v], o_recv, tp=r_bwd, pp=stage0).start()

    def store_unit(v, cols=slice(None)):
        src, dst = ybuf.at[v, :, cols], out.at[m, pl.ds(pl.multiple_of(v * UNIT, UNIT), UNIT), cols]

        @pl.when(odd == 1)
        def _():
            rcopy(src, dst, db_send.at[v], rr_recv.at[c, v], tp=r_fwd, pp=stage1).start()

        rcopy(src, dst, da_send.at[v], o_recv, tp=r_bwd, pp=2 * x + odd).start()

        @pl.when(home)
        def _():
            pltpu.make_async_copy(src, dst, o_recv).start()

        @pl.when(jnp.logical_not(home))
        def _():
            rcopy(src, dst, od_send.at[v], o_recv, pp=partner).start()

    stores = jnp.logical_or(odd == 1, x % 2 == 1)
    stores_later = jnp.logical_and(stores, more)

    def unit_step(u, carry):
        tok = pl.ds(pl.multiple_of(u * UNIT, UNIT), UNIT)

        for group, (step0, step1) in (((0, 1), (2, 0)), ((2,), (4, 1)), ((3,), (6, 2))):
            now = jnp.logical_or(jnp.logical_and(layer == 0, u == min(step0, units - 1)),
                                 jnp.logical_or(jnp.logical_and(layer == 1, u == min(step1, units - 1)), jnp.logical_and(layer > 1, u == 0)))

            @pl.when(jnp.logical_and(late_source, now))
            def _():
                for k in group:
                    for h in range(2):
                        relay_weights(k, h)

        @pl.when(jnp.logical_and(relay, u >= lag))
        def _():
            relay_unit(u - lag)

        @pl.when(layer == 0)
        def _():
            pltpu.make_async_copy(x_hbm.at[m, tok], xbuf.at[u], x0_sem.at[u]).wait()

        @pl.when(layer > 0)
        def _():
            wwait(xbuf.at[u], x_recv.at[u])

        @pl.when(jnp.logical_and(stores, u >= hold - 1))
        def _():
            store_input(u - hold + 1)

        @pl.when(jnp.logical_and(stores_later, u >= hold))
        def _():
            store_unit(u - hold)

        xin = xbuf[u].astype(jnp.float32)
        put_blocks(abuf, 0, layer_norm(xin, packs[0, 0:1, :], packs[0, 1:2, :]))
        for nb in range(1, seq // KBLK + 1):
            @pl.when(u // 2 + 1 == nb)
            def _():
                attention(nb, cmask[u % 2], tok, u)

        for n in range(model // KBLK):
            cols = slice(n * KBLK, (n + 1) * KBLK)
            attn = jnp.dot(blocks(ctx, 0, pairs), blocks(wout, 2 * n, 2), preferred_element_type=jnp.float32)
            hbuf[:, cols] = (xbuf[u, :, cols].astype(jnp.float32) + attn + packs[0, 2:3, cols]).astype(jnp.bfloat16)
        put_blocks(abuf, 0, layer_norm(hbuf[...].astype(jnp.float32), packs[0, 3:4, :], packs[0, 4:5, :]))
        for q in range(tp_n):
            for n in range(hid_q // KBLK):
                up = jnp.dot(blocks(abuf, 0, pairs), blocks(wup.at[q], 2 * n, 2), preferred_element_type=jnp.float32)
                up = up + packs[q, 6:7, n * KBLK:(n + 1) * KBLK]
                put_blocks(ubuf, q * (hid_q // LANE) + 2 * n, gelu(up).astype(jnp.bfloat16))
        half_model = model // 2
        for n in range(2):
            cols = slice(n * half_model, (n + 1) * half_model)
            down = jnp.dot(blocks(ubuf, 0, ubuf.shape[0]), blocks(wdn, n * (half_model // LANE), half_model // LANE), preferred_element_type=jnp.float32)
            ybuf[u, :, cols] = (hbuf[:, cols].astype(jnp.float32) + down + packs[0, 5:6, cols]).astype(jnp.bfloat16)

            @pl.when(more)
            def _():
                rcopy(ybuf.at[u, :, cols], xbuf.at[u, :, cols], s_send.at[u], x_recv.at[u], tp=r_next, pp=p_next).start()

            @pl.when(jnp.logical_not(more))
            def _():
                store_unit(u, cols)

        return carry

    lax.fori_loop(0, units, unit_step, 0)

    @pl.when(stores_later)
    def _():
        def last(v, carry):
            store_unit(v)
            return carry

        lax.fori_loop(units - hold, units, last, 0)

    @pl.when(stores)
    def _():
        def last_input(v, carry):
            store_input(v)
            return carry

        lax.fori_loop(units - hold + 1, units, last_input, 0)

    @pl.when(relay)
    def _():
        def rest(v, carry):
            relay_unit(v)
            return carry

        lax.fori_loop(units - lag, units, rest, 0)

    @pl.when(moved)
    def _():
        for k, h in pieces:
            sent(sw(k, h), sw_send.at[k, h])

    @pl.when(home)
    def _():
        sent(sw_pack, pk_send.at[0])
        for k, h in mats:
            sent(rl(k, h), rl_send.at[h, k])
        for d in range(4):
            for k, h in pieces:
                sent(sw(k, h), fwd_send.at[d, k, h])

    @pl.when(late_source)
    def _():
        handed_out()

    def drain(u, carry):
        @pl.when(more)
        def _():
            sent(ybuf.at[u], s_send.at[u])

        @pl.when(stores)
        def _():
            sent(ybuf.at[u], da_send.at[u])

            @pl.when(jnp.logical_not(home))
            def _():
                sent(ybuf.at[u], od_send.at[u])

        @pl.when(relay)
        def _():
            sent(ybuf.at[u], rr_send.at[0, u])
            sent(ybuf.at[u], rr_send.at[1, u])

        @pl.when(odd == 1)
        def _():
            sent(ybuf.at[u], db_send.at[u])
            sent(ybuf.at[u], fb_send.at[u])

            @pl.when(x % 2 == 0)
            def _():
                sent(ybuf.at[u], fc_send.at[u])

            @pl.when(c == 1)
            def _():
                sent(ybuf.at[u], fa_send.at[u])

        return carry

    lax.fori_loop(0, units, drain, 0)

    @pl.when(relay)
    def _():
        wwait(out.at[pl.ds(0, out.shape[0] // 2)], o_recv)

    @pl.when(jnp.logical_not(relay))
    def _():
        wwait(out, o_recv)


def solution(mesh):
    tp_size = mesh.shape['tp']
    in_specs = (P('dp'), P('dp'), P('pp'), P('pp'), P('pp', None, None, 'tp'), P('pp', None, 'tp', None), P('pp', 'tp', None), P('pp'), P('pp'), P('pp'), P('pp', None, 'tp'), P('pp', 'tp'), P('pp', 'tp', None), P('pp'))

    def per_device(x_in, seq_lens, ln1_gain, ln1_shift, w_qkv, b_qkv, w_out, b_out, ln2_gain, ln2_shift, w_up, b_up, w_down, b_down):
        micro_n, batch_n, seq_n, model_n = x_in.shape
        heads_n = b_qkv.shape[2] * tp_size
        quarter = w_qkv.shape[3]
        hid_q = w_up.shape[2]
        bf16, f32 = jnp.bfloat16, jnp.float32
        wqkv_t = jnp.transpose(w_qkv[0], (1, 0, 2))
        vectors = (ln1_gain, ln1_shift, b_out, ln2_gain, ln2_shift, b_down, b_up, b_qkv)
        pack_shape = (len(vectors), model_n)
        units = seq_n // UNIT
        pairs = model_n // LANE
        dma = pltpu.SemaphoreType.DMA
        anywhere = pl.BlockSpec(memory_space=pl.ANY)
        tokens = batch_n * seq_n
        out = pl.pallas_call(
            functools.partial(kernel, heads_n),
            out_shape=jax.ShapeDtypeStruct((micro_n, tokens, model_n), bf16),
            in_specs=[anywhere, pl.BlockSpec(memory_space=pltpu.SMEM)] + [anywhere] * 4 + [pl.BlockSpec(memory_space=pltpu.VMEM)] * len(vectors),
            out_specs=anywhere,
            scratch_shapes=[
                pltpu.VMEM((tp_size, 3 * quarter // LANE, model_n, LANE), bf16),
                pltpu.VMEM((model_n // LANE, tp_size * quarter, LANE), bf16),
                pltpu.VMEM((tp_size, hid_q // LANE, model_n, LANE), bf16),
                pltpu.VMEM((model_n // LANE, tp_size * hid_q, LANE), bf16),
                pltpu.VMEM((tp_size,) + pack_shape, f32),
                pltpu.VMEM(pack_shape, f32),
                pltpu.VMEM((2, 3 * quarter // LANE, model_n // 2, LANE), bf16),
                pltpu.VMEM((2, model_n // LANE, quarter // 2, LANE), bf16),
                pltpu.VMEM((2, hid_q // LANE, model_n // 2, LANE), bf16),
                pltpu.VMEM((2, model_n // LANE, hid_q // 2, LANE), bf16),
                pltpu.VMEM((3 * quarter // LANE, model_n, LANE), bf16),
                pltpu.VMEM((model_n // LANE, quarter, LANE), bf16),
                pltpu.VMEM((hid_q // LANE, model_n, LANE), bf16),
                pltpu.VMEM((model_n // LANE, hid_q, LANE), bf16),
                pltpu.VMEM(pack_shape, f32),
                pltpu.VMEM((units, UNIT, model_n), bf16),
                pltpu.VMEM((units, UNIT, model_n), bf16),
                *[pltpu.VMEM((quarter // LANE, seq_n, LANE), bf16)] * tp_size,
                *[pltpu.VMEM((quarter // LANE, units, LANE, UNIT), bf16)] * tp_size,
                pltpu.VMEM((seq_n, LANE), bf16),
                pltpu.VMEM((pairs, 2, KBLK, LANE), bf16),
                pltpu.VMEM((2, KBLK, KBLK), f32),
                pltpu.VMEM((2, seq_n // KBLK, KBLK, KBLK), f32),
                pltpu.VMEM((model_n // LANE, UNIT, LANE), bf16),
                pltpu.VMEM((model_n // LANE, UNIT, LANE), bf16),
                pltpu.VMEM((UNIT, model_n), bf16),
                pltpu.VMEM((tp_size * hid_q // LANE, UNIT, LANE), bf16),
                dma((5, 2)), dma((5, 2)), dma((4, 5, 2)), dma((4, 5, 2)), dma((2, 4)), dma((2, 4)), dma((2, 5, 2)), dma((1,)), pltpu.SemaphoreType.REGULAR,
                *[dma((units,))] * 9,
                dma((2, units)), dma((2, units)), dma,
            ],
            compiler_params=pltpu.CompilerParams(collective_id=0, has_side_effects=True, vmem_limit_bytes=63 * 1024 * 1024),
            cost_estimate=pl.CostEstimate(flops=30 * 10 ** 9, bytes_accessed=40 * 10 ** 6, transcendentals=10 ** 7),
        )(x_in.reshape(micro_n, tokens, model_n), seq_lens.reshape(micro_n * batch_n), wqkv_t, w_out[0], w_up[0], w_down[0], *vectors)
        return out.reshape((1,) + x_in.shape)

    return jax.shard_map(per_device, mesh=mesh, in_specs=in_specs, out_specs=P('pp', 'dp'), check_vma=False)
```

```python
import functools
import math

import jax
import jax.numpy as jnp
import numpy as np
from jax import lax
from jax.experimental import pallas as pl
from jax.experimental.pallas import tpu as pltpu
from jax.sharding import PartitionSpec as P

MESH = pl.DeviceIdType.MESH
UNIT = 128
LANE = 128
KBLK = 256
NEG = -1e30


def alibi_slopes(heads_n):
    closest = 2 ** int(math.floor(math.log2(heads_n)))
    base_rate = 2.0 ** (-8.0 / closest)
    slope_list = [base_rate ** (head_idx + 1) for head_idx in range(closest)]
    extra_rate = 2.0 ** (-4.0 / closest)
    slope_list = slope_list + [extra_rate ** (2 * head_idx + 1) for head_idx in range(min(closest, heads_n - closest))]
    return np.array(slope_list, dtype=np.float32)


def split_bf16(value):
    parts = []
    rest = np.float32(value)
    for _ in range(3):
        part = rest.astype(jnp.bfloat16).astype(np.float32)
        parts.append(float(part))
        rest = np.float32(rest - part)
    return parts


def layer_norm(x, gain, shift):
    mean = jnp.mean(x, axis=-1, keepdims=True)
    cent = x - mean
    var = jnp.mean(cent * cent, axis=-1, keepdims=True)
    return (cent * lax.rsqrt(var + 1e-5) * gain + shift).astype(jnp.bfloat16)


def gelu(x):
    inner = math.sqrt(2.0 / math.pi) * (x + 0.044715 * (x * x * x))
    return 0.5 * x * (1.0 + jnp.tanh(inner))


def kernel(heads_n, x_hbm, lens, wqkv_in, wout_in, wup_in, wdn_in,
           ln1_gain, ln1_shift, b_out, ln2_gain, ln2_shift, b_down, b_up, b_qkv, out,
           wqkv, wout, wup, wdn, packs, pack_in, rl_qkv, rl_out, rl_up, rl_dn, sw_qkv, sw_out, sw_up, sw_dn, sw_pack,
           xbuf, ybuf, kc0, kc1, kc2, kc3, vt0, vt1, vt2, vt3, kx, qaug, cmask, sbuf, abuf, ctx, hbuf, ubuf,
           sw_send, sw_recv, w_recv, fwd_send, rl_send, rl_recv, dir_send, pk_send, go,
           x0_sem, x_recv, s_send, od_send, da_send, db_send, fa_send, fb_send, fc_send,
           rr_recv, rr_send, o_recv):
    tp_n = 4
    units = xbuf.shape[0]
    model = xbuf.shape[2]
    seq = units * UNIT
    quarter = wqkv.shape[1] // 3 * LANE
    hid_q = wup.shape[1] * LANE
    pairs = model // LANE
    per_q = quarter // LANE

    r = lax.axis_index("tp")
    p = lax.axis_index("pp")
    x = p // 2
    c = p % 2
    odd = (r + (x + 1) // 2 + 1) % 2
    even_col = x + (1 - x % 2) * (2 - 2 * x)
    layer = odd * (2 * x + 1) + (1 - odd) * 2 * even_col
    home = odd == c
    moved = jnp.logical_and(c == 0, x % 2 == 0)
    level = x == 1
    ahead = jnp.logical_or(r % 2 == 0, level)
    rp, rm, ro = (r + 1) % tp_n, (r + 3) % tp_n, (r + 2) % tp_n
    partner = 2 * x + (1 - c)
    sig = 1 - 2 * c
    r_fwd = (r + sig + tp_n) % tp_n
    r_bwd = (r - sig + tp_n) % tp_n
    stage0, stage1 = 2 * x, 2 * x + 1
    x_n = 4

    def micro_of(row, core, lay):
        hops = (lay + 1) // 4
        return 2 * (((row + 8 - (1 - 2 * core) * hops) % tp_n) // 2) + core

    m = micro_of(r, c, layer)

    def rcopy(src, dst, ssem, rsem, **dev):
        return pltpu.make_async_remote_copy(src_ref=src, dst_ref=dst, send_sem=ssem, recv_sem=rsem,
                                            device_id=dev, device_id_type=MESH)

    barrier = pltpu.get_barrier_semaphore()
    for dr in range(tp_n):
        for dc in range(2):
            if dr or dc:
                pl.semaphore_signal(barrier, inc=1, device_id={"tp": (r + dr) % tp_n, "pp": 2 * x + (c + dc) % 2}, device_id_type=MESH)
    for dx in range(1, x_n):
        pl.semaphore_signal(barrier, inc=1, device_id={"pp": 2 * ((x + dx) % x_n) + c}, device_id_type=MESH)

    for i, vec in enumerate((ln1_gain, ln1_shift, b_out, ln2_gain, ln2_shift, b_down, b_up)):
        pack_in[i:i + 1, :] = vec[...].astype(jnp.float32)
    width = b_qkv.shape[3]
    for j in range(3):
        for head in range(quarter // width):
            at = j * quarter + head * width
            pack_in[7:8, at:at + width] = b_qkv[0, j, head:head + 1, :].astype(jnp.float32)
    pl.semaphore_wait(barrier, 10)

    def wsrc(k, h, n):
        if k == 0:
            return wqkv_in.at[n // per_q, pl.ds(h * (model // 2), model // 2), pl.ds(n % per_q * LANE, LANE)]
        ref = (None, wout_in, wup_in, wdn_in)[k]
        half = ref.shape[0] // 2
        return ref.at[pl.ds(h * half, half), pl.ds(n * LANE, LANE)]

    def wdst(k, q, h=0):
        if k == 4:
            return packs.at[q]
        if k == 0 or k == 2:
            return (wqkv, None, wup)[k].at[q, :, pl.ds(h * (model // 2), model // 2), :]
        ref, half = (wout, quarter // 2) if k == 1 else (wdn, hid_q // 2)
        return ref.at[:, pl.ds(pl.multiple_of((2 * q + h) * half, half), half), :]

    def rl(k, h):
        return (rl_qkv, rl_out, rl_up, rl_dn)[k].at[h]

    def sw(k, h):
        if k == 4:
            return sw_pack
        ref = (sw_qkv, sw_out, sw_up, sw_dn)[k]
        half = ref.shape[1] // 2
        return ref.at[:, pl.ds(h * half, half), :]

    def fetch(k, h, dst, move):
        if k == 4:
            todo = [(pack_in, dst)]
        else:
            todo = [(wsrc(k, h, n), dst.at[n]) for n in range(dst.shape[0])]
        for src, to in todo:
            if move:
                rcopy(src, to, sw_send.at[k, h], sw_recv.at[k, h], pp=2 * (2 - x)).start()
            else:
                pltpu.make_async_copy(src, to, sw_recv.at[k, h]).start()

    def wwait(view, sem):
        rcopy(view, view, sem, sem, pp=partner).wait_recv()

    pieces = [(4, 0), (1, 0), (1, 1), (0, 0), (0, 1), (2, 0), (2, 1), (3, 0), (3, 1)]
    mats = pieces[1:]

    @pl.when(jnp.logical_and(moved, odd == 1))
    def _():
        for k, h in pieces:
            fetch(k, h, wdst(k, r, h), True)

    @pl.when(jnp.logical_and(moved, odd == 0))
    def _():
        for k, h in pieces:
            fetch(k, h, sw(k, h), True)

    @pl.when(jnp.logical_and(jnp.logical_not(moved), home))
    def _():
        for k, h in pieces:
            fetch(k, h, wdst(k, r, h), False)

    @pl.when(jnp.logical_not(jnp.logical_or(moved, home)))
    def _():
        for k, h in pieces:
            fetch(k, h, sw(k, h), False)

    @pl.when(layer == 0)
    def _():
        for u in range(units):
            pltpu.make_async_copy(x_hbm.at[m, pl.ds(u * UNIT, UNIT)], xbuf.at[u], x0_sem.at[u]).start()

    kc, vt = (kc0, kc1, kc2, kc3), (vt0, vt1, vt2, vt3)
    for ref in kc + vt:
        ref[...] = jnp.zeros_like(ref)
    length = lens[m]
    key = lax.broadcasted_iota(jnp.int32, (seq, LANE), 0)
    lane = lax.broadcasted_iota(jnp.int32, (seq, LANE), 1)
    high = (key // KBLK) * KBLK
    part = jnp.where(lane % 2 == 0, high, key - high).astype(jnp.float32)
    dead = jnp.where(key >= length, NEG, 0.0)
    kx[...] = jnp.where(lane < 6, part, jnp.where(lane == 6, dead, 0.0)).astype(jnp.bfloat16)
    slopes = alibi_slopes(heads_n)
    row = lax.broadcasted_iota(jnp.int32, (LANE, KBLK), 0)
    second = lax.broadcasted_iota(jnp.int32, (LANE, KBLK), 1) >= LANE
    for pair in range(pairs):
        (h0, m0, l0), (h1, m1, l1) = split_bf16(slopes[2 * pair]), split_bf16(slopes[2 * pair + 1])
        hi, mid, low = jnp.where(second, h1, h0), jnp.where(second, m1, m0), jnp.where(second, l1, l0)
        val = jnp.where(row < 2, hi, jnp.where(row < 4, mid, jnp.where(row < 6, low, jnp.where(row == 6, 1.0, 0.0))))
        for side in range(2):
            qaug[pair, side, LANE:, :] = val[:, side * LANE:(side + 1) * LANE].astype(jnp.bfloat16)
    kpos = lax.broadcasted_iota(jnp.int32, (KBLK, KBLK), 0)
    qpos = lax.broadcasted_iota(jnp.int32, (KBLK, KBLK), 1) % LANE
    cmask[0] = jnp.where(kpos <= qpos, 0.0, NEG)
    cmask[1] = jnp.where(kpos <= qpos + LANE, 0.0, NEG)

    def to_relay(k, h):
        rcopy(wdst(k, r, h), rl(k, h), rl_send.at[h, k], rl_recv.at[h, k], tp=(rp, rm)[h]).start()

    def to_partner(k, q, d, h):
        rcopy(wdst(k, q, h), wdst(k, q, h), fwd_send.at[d, k, h], w_recv.at[d, k, h], pp=partner).start()

    def hand_out(behind=()):
        for i, (k, h) in enumerate(pieces):
            wwait(sw(k, h), sw_recv.at[k, h])
            rcopy(sw(k, h), wdst(k, r, h), dir_send.at[0, k, h], w_recv.at[3, k, h], tp=rp).start()
            rcopy(sw(k, h), wdst(k, r, h), dir_send.at[1, k, h], w_recv.at[1, k, h], tp=rm).start()
            if 3 <= i < len(behind) + 3:
                relay_weights(*behind[i - 3])

    def relay_weights(k, h):
        wwait(rl(k, h), rl_recv.at[h, k])
        rcopy(rl(k, h), wdst(k, (rm, rp)[h], h), rl_send.at[h, k], w_recv.at[2, k, h], tp=(rp, rm)[h]).start()

    def from_partner():
        for d, q in ((0, r), (1, rp), (3, rm), (2, ro)):
            for k, h in pieces:
                wwait(wdst(k, q, h), w_recv.at[d, k, h])

    def sent(view, sem):
        rcopy(view, view, sem, sem, pp=partner).wait_send()

    def handed_out():
        for k, h in pieces:
            for d in range(2):
                sent(sw(k, h), dir_send.at[d, k, h])
        for k, h in mats:
            sent(rl(k, h), rl_send.at[h, k])

    @pl.when(home)
    def _():
        for k, h in pieces:
            wwait(wdst(k, r, h), sw_recv.at[k, h])
            if k == 4:
                rcopy(wdst(k, r), wdst(k, r), pk_send.at[0], w_recv.at[2, k, h], tp=ro).start()
            else:
                @pl.when(ahead)
                def _():
                    to_relay(k, h)
            to_partner(k, r, 0, h)

        @pl.when(jnp.logical_not(ahead))
        def _():
            pl.semaphore_wait(go, 1)
            for k, h in mats:
                to_relay(k, h)

        for k, h in pieces:
            for d, q in ((1, rp), (3, rm)):
                wwait(wdst(k, q, h), w_recv.at[d, k, h])
                to_partner(k, q, d, h)
        for k, h in pieces:
            wwait(wdst(k, ro, h), w_recv.at[2, k, h])
            to_partner(k, ro, 2, h)

    late_source = jnp.logical_not(jnp.logical_or(home, jnp.logical_or(r % 2 == 1, level)))

    @pl.when(jnp.logical_not(jnp.logical_or(home, late_source)))
    def _():
        hand_out(mats)
        for k, h in mats[len(pieces) - 3:]:
            relay_weights(k, h)
        handed_out()

        @pl.when(jnp.logical_not(level))
        def _():
            pl.semaphore_signal(go, inc=1, device_id={"pp": partner}, device_id_type=MESH)

        from_partner()

    @pl.when(late_source)
    def _():
        hand_out()
        from_partner()

    def half_cols(half):
        return slice(half * (model // 2), (half + 1) * (model // 2))

    def out_at(mm, u, half=None):
        rows = pl.ds(pl.multiple_of(u * UNIT, UNIT), UNIT)
        return out.at[mm, rows] if half is None else out.at[mm, rows, half_cols(half)]

    m_a = micro_of(rm, 0, stage1)
    m_b = micro_of(rp, 1, stage1)
    relay = jnp.logical_and(odd == 0, jnp.logical_or(c == 1, x % 2 == 0))
    lag = min(5, units) * (x % 2) + (1 - x % 2) * (min(5, units) + (units - min(5, units)) * (x // 2))
    hold = min(5, units) * (1 - (x + 2) // 3) + (x + 2) // 3

    def relay_unit(v):
        for half in range(2):
            for slot, (mm, to) in enumerate(((m_a, rp), (m_b, rm))):
                part = out_at(mm, v, half)
                wwait(part, rr_recv.at[slot, v, half])
                rcopy(part, part, rr_send.at[slot, v], o_recv, tp=to).start()

    def wide(parts):
        return jnp.concatenate(parts, axis=1)

    def blocks(ref, first, count):
        return wide([ref[first + i] for i in range(count)])

    def put_blocks(ref, first, val):
        for i in range(val.shape[1] // LANE):
            ref[first + i] = val[:, i * LANE:(i + 1) * LANE]

    def attention(nb, diag, tok, u):
        head_row = lax.broadcasted_iota(jnp.int32, (LANE, LANE), 0) < 64

        def project(q):
            for j in range(3):
                weights = wide([wqkv[q, j * per_q + i] for i in range(per_q)])
                o = jnp.dot(blocks(abuf, 0, pairs), weights, preferred_element_type=jnp.float32)
                o = (o + packs[q, 7:8, j * quarter:(j + 1) * quarter]).astype(jnp.bfloat16)
                for i in range(per_q):
                    part = o[:, i * LANE:(i + 1) * LANE]
                    if j == 0:
                        q_t = (part.astype(jnp.float32) * 0.125).T
                        qaug[q * per_q + i, 0, :LANE, :] = jnp.where(head_row, q_t, 0.0).astype(jnp.bfloat16)
                        qaug[q * per_q + i, 1, :LANE, :] = jnp.where(head_row, 0.0, q_t).astype(jnp.bfloat16)
                    elif j == 1:
                        kc[q][i, tok, :] = part
                    else:
                        vt[q][i, u] = part.astype(jnp.float32).T.astype(jnp.bfloat16)

        def scores(pair):
            kq = kc[pair // per_q]
            q_rhs = blocks(qaug.at[pair], 0, 2)
            top = None
            for b in range(nb):
                keys = wide([kq[pair % per_q, b * KBLK:(b + 1) * KBLK, :], kx[b * KBLK:(b + 1) * KBLK, :]])
                s = jnp.dot(keys, q_rhs, preferred_element_type=jnp.float32)
                if b == nb - 1:
                    s = s + diag
                sbuf[pair % 2, b] = s
                peak = jnp.max(s, axis=0, keepdims=True)
                top = peak if top is None else jnp.maximum(top, peak)
            return top

        def weigh(pair, top):
            vq = vt[pair // per_q].at[pair % per_q]
            total = None
            acc = None
            for b in range(nb):
                e = jnp.exp(sbuf[pair % 2, b] - top)
                part_sum = jnp.sum(e, axis=0, keepdims=True)
                total = part_sum if total is None else total + part_sum
                pv = jnp.dot(blocks(vq, b * KBLK // UNIT, KBLK // UNIT), e.astype(jnp.bfloat16), preferred_element_type=jnp.float32)
                acc = pv if acc is None else acc + pv
            acc = acc * (1.0 / total)
            both = jnp.concatenate([acc[:64, :LANE], acc[64:, LANE:]], axis=0)
            ctx[pair] = both.T.astype(jnp.bfloat16)

        project(0)
        top = None
        for pair in range(pairs + 1):
            if pair % per_q == 0 and pair // per_q + 1 < tp_n:
                project(pair // per_q + 1)
            later = scores(pair) if pair < pairs else None
            if pair > 0:
                weigh(pair - 1, top)
            top = later

    more = layer < 2 * x_n - 1
    nxt = (layer + 1) % (2 * x_n)
    half_n = nxt // 2
    x_next = half_n + (1 - nxt % 2) * (1 - half_n % 2) * (2 - 2 * half_n)
    p_next = 2 * x_next + c
    r_next = (r + (1 - odd) * (x % 2) * sig + tp_n) % tp_n

    def store_input(v):
        @pl.when(odd == 1)
        def _():
            @pl.when(c == 0)
            def _():
                pltpu.make_async_copy(xbuf.at[v], out_at(m, v), o_recv).start()

            @pl.when(c == 1)
            def _():
                rcopy(xbuf.at[v], out_at(m, v), fa_send.at[v], o_recv, pp=partner).start()

            @pl.when(x % 2 == 1)
            def _():
                rcopy(xbuf.at[v], out_at(m, v), fb_send.at[v], o_recv, tp=r_fwd, pp=stage0).start()

            @pl.when(x % 2 == 0)
            def _():
                for half in range(2):
                    rcopy(xbuf.at[v, :, half_cols(half)], out_at(m, v, half), fb_send.at[v], rr_recv.at[c, v, half], tp=r_fwd, pp=stage0).start()
                rcopy(xbuf.at[v], out_at(m, v), fc_send.at[v], o_recv, tp=r_bwd, pp=stage0).start()

    def store_half(v, half):
        src, dst = ybuf.at[v, :, half_cols(half)], out_at(m, v, half)

        @pl.when(odd == 1)
        def _():
            rcopy(src, dst, db_send.at[v], rr_recv.at[c, v, half], tp=r_fwd, pp=stage1).start()

        rcopy(src, dst, da_send.at[v], o_recv, tp=r_bwd, pp=2 * x + odd).start()

        @pl.when(home)
        def _():
            pltpu.make_async_copy(src, dst, o_recv).start()

        @pl.when(jnp.logical_not(home))
        def _():
            rcopy(src, dst, od_send.at[v], o_recv, pp=partner).start()

    def store_unit(v):
        store_half(v, 0)
        store_half(v, 1)

    stores = jnp.logical_or(odd == 1, x % 2 == 1)
    stores_later = jnp.logical_and(stores, more)

    def unit_step(u, carry):
        tok = pl.ds(pl.multiple_of(u * UNIT, UNIT), UNIT)

        for group, (step0, step1) in (((0, 1), (2, 0)), ((2,), (4, 1)), ((3,), (6, 2))):
            now = jnp.logical_or(jnp.logical_and(layer == 0, u == min(step0, units - 1)),
                                 jnp.logical_or(jnp.logical_and(layer == 1, u == min(step1, units - 1)), jnp.logical_and(layer > 1, u == 0)))

            @pl.when(jnp.logical_and(late_source, now))
            def _():
                for k in group:
                    for h in range(2):
                        relay_weights(k, h)

        @pl.when(jnp.logical_and(relay, u >= lag))
        def _():
            relay_unit(u - lag)

        @pl.when(layer == 0)
        def _():
            pltpu.make_async_copy(x_hbm.at[m, tok], xbuf.at[u], x0_sem.at[u]).wait()

        @pl.when(layer > 0)
        def _():
            wwait(xbuf.at[u], x_recv.at[u])

        @pl.when(jnp.logical_and(stores, u >= hold - 1))
        def _():
            store_input(u - hold + 1)

        @pl.when(jnp.logical_and(stores_later, u >= hold))
        def _():
            store_unit(u - hold)

        xin = xbuf[u].astype(jnp.float32)
        put_blocks(abuf, 0, layer_norm(xin, packs[0, 0:1, :], packs[0, 1:2, :]))
        for nb in range(1, seq // KBLK + 1):
            @pl.when(u // 2 + 1 == nb)
            def _():
                attention(nb, cmask[u % 2], tok, u)

        for n in range(model // KBLK):
            cols = slice(n * KBLK, (n + 1) * KBLK)
            attn = jnp.dot(blocks(ctx, 0, pairs), blocks(wout, 2 * n, 2), preferred_element_type=jnp.float32)
            hbuf[:, cols] = (xbuf[u, :, cols].astype(jnp.float32) + attn + packs[0, 2:3, cols]).astype(jnp.bfloat16)
        put_blocks(abuf, 0, layer_norm(hbuf[...].astype(jnp.float32), packs[0, 3:4, :], packs[0, 4:5, :]))
        for q in range(tp_n):
            for n in range(hid_q // KBLK):
                up = jnp.dot(blocks(abuf, 0, pairs), blocks(wup.at[q], 2 * n, 2), preferred_element_type=jnp.float32)
                up = up + packs[q, 6:7, n * KBLK:(n + 1) * KBLK]
                put_blocks(ubuf, q * (hid_q // LANE) + 2 * n, gelu(up).astype(jnp.bfloat16))
        half_model = model // 2
        for n in range(2):
            cols = slice(n * half_model, (n + 1) * half_model)
            down = jnp.dot(blocks(ubuf, 0, ubuf.shape[0]), blocks(wdn, n * (half_model // LANE), half_model // LANE), preferred_element_type=jnp.float32)
            ybuf[u, :, cols] = (hbuf[:, cols].astype(jnp.float32) + down + packs[0, 5:6, cols]).astype(jnp.bfloat16)

            @pl.when(more)
            def _():
                rcopy(ybuf.at[u, :, cols], xbuf.at[u, :, cols], s_send.at[u], x_recv.at[u], tp=r_next, pp=p_next).start()

            @pl.when(jnp.logical_not(more))
            def _():
                store_half(u, n)

        return carry

    lax.fori_loop(0, units, unit_step, 0)

    @pl.when(stores_later)
    def _():
        def last(v, carry):
            store_unit(v)
            return carry

        lax.fori_loop(units - hold, units, last, 0)

    @pl.when(stores)
    def _():
        def last_input(v, carry):
            store_input(v)
            return carry

        lax.fori_loop(units - hold + 1, units, last_input, 0)

    @pl.when(relay)
    def _():
        def rest(v, carry):
            relay_unit(v)
            return carry

        lax.fori_loop(units - lag, units, rest, 0)

    @pl.when(moved)
    def _():
        for k, h in pieces:
            sent(sw(k, h), sw_send.at[k, h])

    @pl.when(home)
    def _():
        sent(sw_pack, pk_send.at[0])
        for k, h in mats:
            sent(rl(k, h), rl_send.at[h, k])
        for d in range(4):
            for k, h in pieces:
                sent(sw(k, h), fwd_send.at[d, k, h])

    @pl.when(late_source)
    def _():
        handed_out()

    def drain(u, carry):
        @pl.when(more)
        def _():
            sent(ybuf.at[u], s_send.at[u])

        @pl.when(stores)
        def _():
            sent(ybuf.at[u], da_send.at[u])

            @pl.when(jnp.logical_not(home))
            def _():
                sent(ybuf.at[u], od_send.at[u])

        @pl.when(relay)
        def _():
            sent(ybuf.at[u], rr_send.at[0, u])
            sent(ybuf.at[u], rr_send.at[1, u])

        @pl.when(odd == 1)
        def _():
            sent(ybuf.at[u], db_send.at[u])
            sent(ybuf.at[u], fb_send.at[u])

            @pl.when(x % 2 == 0)
            def _():
                sent(ybuf.at[u], fc_send.at[u])

            @pl.when(c == 1)
            def _():
                sent(ybuf.at[u], fa_send.at[u])

        return carry

    lax.fori_loop(0, units, drain, 0)

    @pl.when(relay)
    def _():
        wwait(out.at[pl.ds(0, out.shape[0] // 2)], o_recv)

    @pl.when(jnp.logical_not(relay))
    def _():
        wwait(out, o_recv)


def solution(mesh):
    tp_size = mesh.shape['tp']
    in_specs = (P('dp'), P('dp'), P('pp'), P('pp'), P('pp', None, None, 'tp'), P('pp', None, 'tp', None), P('pp', 'tp', None), P('pp'), P('pp'), P('pp'), P('pp', None, 'tp'), P('pp', 'tp'), P('pp', 'tp', None), P('pp'))

    def per_device(x_in, seq_lens, ln1_gain, ln1_shift, w_qkv, b_qkv, w_out, b_out, ln2_gain, ln2_shift, w_up, b_up, w_down, b_down):
        micro_n, batch_n, seq_n, model_n = x_in.shape
        heads_n = b_qkv.shape[2] * tp_size
        quarter = w_qkv.shape[3]
        hid_q = w_up.shape[2]
        bf16, f32 = jnp.bfloat16, jnp.float32
        wqkv_t = jnp.transpose(w_qkv[0], (1, 0, 2))
        vectors = (ln1_gain, ln1_shift, b_out, ln2_gain, ln2_shift, b_down, b_up, b_qkv)
        pack_shape = (len(vectors), model_n)
        units = seq_n // UNIT
        pairs = model_n // LANE
        dma = pltpu.SemaphoreType.DMA
        anywhere = pl.BlockSpec(memory_space=pl.ANY)
        tokens = batch_n * seq_n
        out = pl.pallas_call(
            functools.partial(kernel, heads_n),
            out_shape=jax.ShapeDtypeStruct((micro_n, tokens, model_n), bf16),
            in_specs=[anywhere, pl.BlockSpec(memory_space=pltpu.SMEM)] + [anywhere] * 4 + [pl.BlockSpec(memory_space=pltpu.VMEM)] * len(vectors),
            out_specs=anywhere,
            scratch_shapes=[
                pltpu.VMEM((tp_size, 3 * quarter // LANE, model_n, LANE), bf16),
                pltpu.VMEM((model_n // LANE, tp_size * quarter, LANE), bf16),
                pltpu.VMEM((tp_size, hid_q // LANE, model_n, LANE), bf16),
                pltpu.VMEM((model_n // LANE, tp_size * hid_q, LANE), bf16),
                pltpu.VMEM((tp_size,) + pack_shape, f32),
                pltpu.VMEM(pack_shape, f32),
                pltpu.VMEM((2, 3 * quarter // LANE, model_n // 2, LANE), bf16),
                pltpu.VMEM((2, model_n // LANE, quarter // 2, LANE), bf16),
                pltpu.VMEM((2, hid_q // LANE, model_n // 2, LANE), bf16),
                pltpu.VMEM((2, model_n // LANE, hid_q // 2, LANE), bf16),
                pltpu.VMEM((3 * quarter // LANE, model_n, LANE), bf16),
                pltpu.VMEM((model_n // LANE, quarter, LANE), bf16),
                pltpu.VMEM((hid_q // LANE, model_n, LANE), bf16),
                pltpu.VMEM((model_n // LANE, hid_q, LANE), bf16),
                pltpu.VMEM(pack_shape, f32),
                pltpu.VMEM((units, UNIT, model_n), bf16),
                pltpu.VMEM((units, UNIT, model_n), bf16),
                *[pltpu.VMEM((quarter // LANE, seq_n, LANE), bf16)] * tp_size,
                *[pltpu.VMEM((quarter // LANE, units, LANE, UNIT), bf16)] * tp_size,
                pltpu.VMEM((seq_n, LANE), bf16),
                pltpu.VMEM((pairs, 2, KBLK, LANE), bf16),
                pltpu.VMEM((2, KBLK, KBLK), f32),
                pltpu.VMEM((2, seq_n // KBLK, KBLK, KBLK), f32),
                pltpu.VMEM((model_n // LANE, UNIT, LANE), bf16),
                pltpu.VMEM((model_n // LANE, UNIT, LANE), bf16),
                pltpu.VMEM((UNIT, model_n), bf16),
                pltpu.VMEM((tp_size * hid_q // LANE, UNIT, LANE), bf16),
                dma((5, 2)), dma((5, 2)), dma((4, 5, 2)), dma((4, 5, 2)), dma((2, 4)), dma((2, 4)), dma((2, 5, 2)), dma((1,)), pltpu.SemaphoreType.REGULAR,
                *[dma((units,))] * 9,
                dma((2, units, 2)), dma((2, units)), dma,
            ],
            compiler_params=pltpu.CompilerParams(collective_id=0, has_side_effects=True, vmem_limit_bytes=63 * 1024 * 1024),
            cost_estimate=pl.CostEstimate(flops=30 * 10 ** 9, bytes_accessed=40 * 10 ** 6, transcendentals=10 ** 7),
        )(x_in.reshape(micro_n, tokens, model_n), seq_lens.reshape(micro_n * batch_n), wqkv_t, w_out[0], w_up[0], w_down[0], *vectors)
        return out.reshape((1,) + x_in.shape)

    return jax.shard_map(per_device, mesh=mesh, in_specs=in_specs, out_specs=P('pp', 'dp'), check_vma=False)
```

```python
import functools
import math

import jax
import jax.numpy as jnp
import numpy as np
from jax import lax
from jax.experimental import pallas as pl
from jax.experimental.pallas import tpu as pltpu
from jax.sharding import PartitionSpec as P

MESH = pl.DeviceIdType.MESH
UNIT = 128
LANE = 128
KBLK = 256
NEG = -1e30


def alibi_slopes(heads_n):
    closest = 2 ** int(math.floor(math.log2(heads_n)))
    base_rate = 2.0 ** (-8.0 / closest)
    slope_list = [base_rate ** (head_idx + 1) for head_idx in range(closest)]
    extra_rate = 2.0 ** (-4.0 / closest)
    slope_list = slope_list + [extra_rate ** (2 * head_idx + 1) for head_idx in range(min(closest, heads_n - closest))]
    return np.array(slope_list, dtype=np.float32)


def split_bf16(value):
    parts = []
    rest = np.float32(value)
    for _ in range(3):
        part = rest.astype(jnp.bfloat16).astype(np.float32)
        parts.append(float(part))
        rest = np.float32(rest - part)
    return parts


def layer_norm(x, gain, shift):
    mean = jnp.mean(x, axis=-1, keepdims=True)
    cent = x - mean
    var = jnp.mean(cent * cent, axis=-1, keepdims=True)
    return (cent * lax.rsqrt(var + 1e-5) * gain + shift).astype(jnp.bfloat16)


def gelu(x):
    inner = math.sqrt(2.0 / math.pi) * (x + 0.044715 * (x * x * x))
    return 0.5 * x * (1.0 + jnp.tanh(inner))


def kernel(heads_n, x_hbm, lens, wqkv_in, wout_in, wup_in, wdn_in,
           ln1_gain, ln1_shift, b_out, ln2_gain, ln2_shift, b_down, b_up, b_qkv, out,
           wqkv, wout, wup, wdn, packs, pack_in, rl_qkv, rl_out, rl_up, rl_dn, sw_qkv, sw_out, sw_up, sw_dn, sw_pack,
           xbuf, ybuf, kc0, kc1, kc2, kc3, vt0, vt1, vt2, vt3, kx, qaug, cmask, sbuf, abuf, ctx, hbuf, ubuf,
           sw_send, sw_recv, w_recv, fwd_send, rl_send, rl_recv, dir_send, pk_send, go,
           x0_sem, x_recv, s_send, od_send, da_send, db_send, fa_send, fb_send, fc_send,
           rr_recv, rr_send, o_recv):
    tp_n = 4
    units = xbuf.shape[0]
    model = xbuf.shape[2]
    seq = units * UNIT
    quarter = wqkv.shape[1] // 3 * LANE
    hid_q = wup.shape[1] * LANE
    pairs = model // LANE
    per_q = quarter // LANE

    r = lax.axis_index("tp")
    p = lax.axis_index("pp")
    x = p // 2
    c = p % 2
    odd = (r + (x + 1) // 2 + 1) % 2
    even_col = x + (1 - x % 2) * (2 - 2 * x)
    layer = odd * (2 * x + 1) + (1 - odd) * 2 * even_col
    home = odd == c
    moved = jnp.logical_and(c == 0, x % 2 == 0)
    level = x == 1
    ahead = jnp.logical_or(r % 2 == 0, level)
    rp, rm, ro = (r + 1) % tp_n, (r + 3) % tp_n, (r + 2) % tp_n
    partner = 2 * x + (1 - c)
    sig = 1 - 2 * c
    r_fwd = (r + sig + tp_n) % tp_n
    r_bwd = (r - sig + tp_n) % tp_n
    stage0, stage1 = 2 * x, 2 * x + 1
    x_n = 4

    def micro_of(row, core, lay):
        hops = (lay + 1) // 4
        return 2 * (((row + 8 - (1 - 2 * core) * hops) % tp_n) // 2) + core

    m = micro_of(r, c, layer)

    def rcopy(src, dst, ssem, rsem, **dev):
        return pltpu.make_async_remote_copy(src_ref=src, dst_ref=dst, send_sem=ssem, recv_sem=rsem,
                                            device_id=dev, device_id_type=MESH)

    barrier = pltpu.get_barrier_semaphore()
    for dr in range(tp_n):
        for dc in range(2):
            if dr or dc:
                pl.semaphore_signal(barrier, inc=1, device_id={"tp": (r + dr) % tp_n, "pp": 2 * x + (c + dc) % 2}, device_id_type=MESH)
    for dx in range(1, x_n):
        pl.semaphore_signal(barrier, inc=1, device_id={"pp": 2 * ((x + dx) % x_n) + c}, device_id_type=MESH)

    for i, vec in enumerate((ln1_gain, ln1_shift, b_out, ln2_gain, ln2_shift, b_down, b_up)):
        pack_in[i:i + 1, :] = vec[...].astype(jnp.float32)
    width = b_qkv.shape[3]
    for j in range(3):
        for head in range(quarter // width):
            at = j * quarter + head * width
            pack_in[7:8, at:at + width] = b_qkv[0, j, head:head + 1, :].astype(jnp.float32)
    pl.semaphore_wait(barrier, 10)

    def wsrc(k, h, n):
        if k == 0:
            return wqkv_in.at[n // per_q, pl.ds(h * (model // 2), model // 2), pl.ds(n % per_q * LANE, LANE)]
        ref = (None, wout_in, wup_in, wdn_in)[k]
        half = ref.shape[0] // 2
        return ref.at[pl.ds(h * half, half), pl.ds(n * LANE, LANE)]

    def wdst(k, q, h=0):
        if k == 4:
            return packs.at[q]
        if k == 0 or k == 2:
            return (wqkv, None, wup)[k].at[q, :, pl.ds(h * (model // 2), model // 2), :]
        ref, half = (wout, quarter // 2) if k == 1 else (wdn, hid_q // 2)
        return ref.at[:, pl.ds(pl.multiple_of((2 * q + h) * half, half), half), :]

    def rl(k, h):
        return (rl_qkv, rl_out, rl_up, rl_dn)[k].at[h]

    def sw(k, h):
        if k == 4:
            return sw_pack
        ref = (sw_qkv, sw_out, sw_up, sw_dn)[k]
        half = ref.shape[1] // 2
        return ref.at[:, pl.ds(h * half, half), :]

    def fetch(k, h, dst, move):
        if k == 4:
            todo = [(pack_in, dst)]
        else:
            todo = [(wsrc(k, h, n), dst.at[n]) for n in range(dst.shape[0])]
        for src, to in todo:
            if move:
                rcopy(src, to, sw_send.at[k, h], sw_recv.at[k, h], pp=2 * (2 - x)).start()
            else:
                pltpu.make_async_copy(src, to, sw_recv.at[k, h]).start()

    def wwait(view, sem):
        rcopy(view, view, sem, sem, pp=partner).wait_recv()

    pieces = [(4, 0), (1, 0), (1, 1), (0, 0), (0, 1), (2, 0), (2, 1), (3, 0), (3, 1)]
    mats = pieces[1:]

    @pl.when(jnp.logical_and(moved, odd == 1))
    def _():
        for k, h in pieces:
            fetch(k, h, wdst(k, r, h), True)

    @pl.when(jnp.logical_and(moved, odd == 0))
    def _():
        for k, h in pieces:
            fetch(k, h, sw(k, h), True)

    @pl.when(jnp.logical_and(jnp.logical_not(moved), home))
    def _():
        for k, h in pieces:
            fetch(k, h, wdst(k, r, h), False)

    @pl.when(jnp.logical_not(jnp.logical_or(moved, home)))
    def _():
        for k, h in pieces:
            fetch(k, h, sw(k, h), False)

    @pl.when(layer == 0)
    def _():
        for u in range(units):
            pltpu.make_async_copy(x_hbm.at[m, pl.ds(u * UNIT, UNIT)], xbuf.at[u], x0_sem.at[u]).start()

    kc, vt = (kc0, kc1, kc2, kc3), (vt0, vt1, vt2, vt3)
    for ref in kc + vt:
        ref[...] = jnp.zeros_like(ref)
    length = lens[m]
    key = lax.broadcasted_iota(jnp.int32, (seq, LANE), 0)
    lane = lax.broadcasted_iota(jnp.int32, (seq, LANE), 1)
    high = (key // KBLK) * KBLK
    part = jnp.where(lane % 2 == 0, high, key - high).astype(jnp.float32)
    dead = jnp.where(key >= length, NEG, 0.0)
    kx[...] = jnp.where(lane < 6, part, jnp.where(lane == 6, dead, 0.0)).astype(jnp.bfloat16)
    slopes = alibi_slopes(heads_n)
    row = lax.broadcasted_iota(jnp.int32, (LANE, KBLK), 0)
    second = lax.broadcasted_iota(jnp.int32, (LANE, KBLK), 1) >= LANE
    for pair in range(pairs):
        (h0, m0, l0), (h1, m1, l1) = split_bf16(slopes[2 * pair]), split_bf16(slopes[2 * pair + 1])
        hi, mid, low = jnp.where(second, h1, h0), jnp.where(second, m1, m0), jnp.where(second, l1, l0)
        val = jnp.where(row < 2, hi, jnp.where(row < 4, mid, jnp.where(row < 6, low, jnp.where(row == 6, 1.0, 0.0))))
        for side in range(2):
            qaug[pair, side, LANE:, :] = val[:, side * LANE:(side + 1) * LANE].astype(jnp.bfloat16)
    kpos = lax.broadcasted_iota(jnp.int32, (KBLK, KBLK), 0)
    qpos = lax.broadcasted_iota(jnp.int32, (KBLK, KBLK), 1) % LANE
    cmask[0] = jnp.where(kpos <= qpos, 0.0, NEG)
    cmask[1] = jnp.where(kpos <= qpos + LANE, 0.0, NEG)

    def to_relay(k, h):
        rcopy(wdst(k, r, h), rl(k, h), rl_send.at[h, k], rl_recv.at[h, k], tp=(rp, rm)[h]).start()

    def to_partner(k, q, d, h):
        rcopy(wdst(k, q, h), wdst(k, q, h), fwd_send.at[d, k, h], w_recv.at[d, k, h], pp=partner).start()

    def hand_out(behind=()):
        for i, (k, h) in enumerate(pieces):
            wwait(sw(k, h), sw_recv.at[k, h])
            rcopy(sw(k, h), wdst(k, r, h), dir_send.at[0, k, h], w_recv.at[3, k, h], tp=rp).start()
            rcopy(sw(k, h), wdst(k, r, h), dir_send.at[1, k, h], w_recv.at[1, k, h], tp=rm).start()
            if 3 <= i < len(behind) + 3:
                relay_weights(*behind[i - 3])

    def relay_weights(k, h):
        wwait(rl(k, h), rl_recv.at[h, k])
        rcopy(rl(k, h), wdst(k, (rm, rp)[h], h), rl_send.at[h, k], w_recv.at[2, k, h], tp=(rp, rm)[h]).start()

    def from_partner():
        for d, q in ((0, r), (1, rp), (3, rm), (2, ro)):
            for k, h in pieces:
                wwait(wdst(k, q, h), w_recv.at[d, k, h])

    def sent(view, sem):
        rcopy(view, view, sem, sem, pp=partner).wait_send()

    def handed_out():
        for k, h in pieces:
            for d in range(2):
                sent(sw(k, h), dir_send.at[d, k, h])
        for k, h in mats:
            sent(rl(k, h), rl_send.at[h, k])

    @pl.when(home)
    def _():
        for k, h in pieces:
            wwait(wdst(k, r, h), sw_recv.at[k, h])
            if k == 4:
                rcopy(wdst(k, r), wdst(k, r), pk_send.at[0], w_recv.at[2, k, h], tp=ro).start()
            else:
                @pl.when(ahead)
                def _():
                    to_relay(k, h)
            to_partner(k, r, 0, h)

        @pl.when(jnp.logical_not(ahead))
        def _():
            pl.semaphore_wait(go, 1)
            for k, h in mats:
                to_relay(k, h)

        for i, (k, h) in enumerate(pieces + mats[:2]):
            if i < len(pieces):
                for d, q in ((1, rp), (3, rm)):
                    wwait(wdst(k, q, h), w_recv.at[d, k, h])
                    to_partner(k, q, d, h)
            if i >= 2:
                k, h = pieces[i - 2]
                wwait(wdst(k, ro, h), w_recv.at[2, k, h])
                to_partner(k, ro, 2, h)

    late_source = jnp.logical_not(jnp.logical_or(home, jnp.logical_or(r % 2 == 1, level)))

    @pl.when(jnp.logical_not(jnp.logical_or(home, late_source)))
    def _():
        hand_out(mats)
        for k, h in mats[len(pieces) - 3:]:
            relay_weights(k, h)
        handed_out()

        @pl.when(jnp.logical_not(level))
        def _():
            pl.semaphore_signal(go, inc=1, device_id={"pp": partner}, device_id_type=MESH)

        from_partner()

    @pl.when(late_source)
    def _():
        hand_out()
        from_partner()

    def half_cols(half):
        return slice(half * (model // 2), (half + 1) * (model // 2))

    def out_at(mm, u, half=None):
        rows = pl.ds(pl.multiple_of(u * UNIT, UNIT), UNIT)
        return out.at[mm, rows] if half is None else out.at[mm, rows, half_cols(half)]

    m_a = micro_of(rm, 0, stage1)
    m_b = micro_of(rp, 1, stage1)
    relay = jnp.logical_and(odd == 0, jnp.logical_or(c == 1, x % 2 == 0))
    lag = min(5, units) * (x % 2) + (1 - x % 2) * (min(5, units) + (units - min(5, units)) * (x // 2))
    hold = min(5, units) * (1 - (x + 2) // 3) + (x + 2) // 3

    def relay_unit(v):
        for half in range(2):
            for slot, (mm, to) in enumerate(((m_a, rp), (m_b, rm))):
                part = out_at(mm, v, half)
                wwait(part, rr_recv.at[slot, v, half])
                rcopy(part, part, rr_send.at[slot, v], o_recv, tp=to).start()

    def wide(parts):
        return jnp.concatenate(parts, axis=1)

    def blocks(ref, first, count):
        return wide([ref[first + i] for i in range(count)])

    def put_blocks(ref, first, val):
        for i in range(val.shape[1] // LANE):
            ref[first + i] = val[:, i * LANE:(i + 1) * LANE]

    def attention(nb, diag, tok, u):
        head_row = lax.broadcasted_iota(jnp.int32, (LANE, LANE), 0) < 64

        def project(q):
            for j in range(3):
                weights = wide([wqkv[q, j * per_q + i] for i in range(per_q)])
                o = jnp.dot(blocks(abuf, 0, pairs), weights, preferred_element_type=jnp.float32)
                o = (o + packs[q, 7:8, j * quarter:(j + 1) * quarter]).astype(jnp.bfloat16)
                for i in range(per_q):
                    part = o[:, i * LANE:(i + 1) * LANE]
                    if j == 0:
                        q_t = (part.astype(jnp.float32) * 0.125).T
                        qaug[q * per_q + i, 0, :LANE, :] = jnp.where(head_row, q_t, 0.0).astype(jnp.bfloat16)
                        qaug[q * per_q + i, 1, :LANE, :] = jnp.where(head_row, 0.0, q_t).astype(jnp.bfloat16)
                    elif j == 1:
                        kc[q][i, tok, :] = part
                    else:
                        vt[q][i, u] = part.astype(jnp.float32).T.astype(jnp.bfloat16)

        def scores(pair):
            kq = kc[pair // per_q]
            q_rhs = blocks(qaug.at[pair], 0, 2)
            top = None
            for b in range(nb):
                keys = wide([kq[pair % per_q, b * KBLK:(b + 1) * KBLK, :], kx[b * KBLK:(b + 1) * KBLK, :]])
                s = jnp.dot(keys, q_rhs, preferred_element_type=jnp.float32)
                if b == nb - 1:
                    s = s + diag
                sbuf[pair % 2, b] = s
                peak = jnp.max(s, axis=0, keepdims=True)
                top = peak if top is None else jnp.maximum(top, peak)
            return top

        def weigh(pair, top):
            vq = vt[pair // per_q].at[pair % per_q]
            total = None
            acc = None
            for b in range(nb):
                e = jnp.exp(sbuf[pair % 2, b] - top)
                part_sum = jnp.sum(e, axis=0, keepdims=True)
                total = part_sum if total is None else total + part_sum
                pv = jnp.dot(blocks(vq, b * KBLK // UNIT, KBLK // UNIT), e.astype(jnp.bfloat16), preferred_element_type=jnp.float32)
                acc = pv if acc is None else acc + pv
            acc = acc * (1.0 / total)
            both = jnp.concatenate([acc[:64, :LANE], acc[64:, LANE:]], axis=0)
            ctx[pair] = both.T.astype(jnp.bfloat16)

        project(0)
        top = None
        for pair in range(pairs + 1):
            if pair % per_q == 0 and pair // per_q + 1 < tp_n:
                project(pair // per_q + 1)
            later = scores(pair) if pair < pairs else None
            if pair > 0:
                weigh(pair - 1, top)
            top = later

    more = layer < 2 * x_n - 1
    nxt = (layer + 1) % (2 * x_n)
    half_n = nxt // 2
    x_next = half_n + (1 - nxt % 2) * (1 - half_n % 2) * (2 - 2 * half_n)
    p_next = 2 * x_next + c
    r_next = (r + (1 - odd) * (x % 2) * sig + tp_n) % tp_n

    def store_input(v):
        @pl.when(odd == 1)
        def _():
            @pl.when(c == 0)
            def _():
                pltpu.make_async_copy(xbuf.at[v], out_at(m, v), o_recv).start()

            @pl.when(c == 1)
            def _():
                rcopy(xbuf.at[v], out_at(m, v), fa_send.at[v], o_recv, pp=partner).start()

            @pl.when(x % 2 == 1)
            def _():
                rcopy(xbuf.at[v], out_at(m, v), fb_send.at[v], o_recv, tp=r_fwd, pp=stage0).start()

            @pl.when(x % 2 == 0)
            def _():
                for half in range(2):
                    rcopy(xbuf.at[v, :, half_cols(half)], out_at(m, v, half), fb_send.at[v], rr_recv.at[c, v, half], tp=r_fwd, pp=stage0).start()
                rcopy(xbuf.at[v], out_at(m, v), fc_send.at[v], o_recv, tp=r_bwd, pp=stage0).start()

    def store_half(v, half):
        src, dst = ybuf.at[v, :, half_cols(half)], out_at(m, v, half)

        @pl.when(odd == 1)
        def _():
            rcopy(src, dst, db_send.at[v], rr_recv.at[c, v, half], tp=r_fwd, pp=stage1).start()

        rcopy(src, dst, da_send.at[v], o_recv, tp=r_bwd, pp=2 * x + odd).start()

        @pl.when(home)
        def _():
            pltpu.make_async_copy(src, dst, o_recv).start()

        @pl.when(jnp.logical_not(home))
        def _():
            rcopy(src, dst, od_send.at[v], o_recv, pp=partner).start()

    def store_unit(v):
        store_half(v, 0)
        store_half(v, 1)

    stores = jnp.logical_or(odd == 1, x % 2 == 1)
    stores_later = jnp.logical_and(stores, more)

    def unit_step(u, carry):
        tok = pl.ds(pl.multiple_of(u * UNIT, UNIT), UNIT)

        for group, (step0, step1) in (((0, 1), (3, 0)), ((2,), (5, 1)), ((3,), (7, 2))):
            now = jnp.logical_or(jnp.logical_and(layer == 0, u == min(step0, units - 1)),
                                 jnp.logical_or(jnp.logical_and(layer == 1, u == min(step1, units - 1)), jnp.logical_and(layer > 1, u == 0)))

            @pl.when(jnp.logical_and(late_source, now))
            def _():
                for k in group:
                    for h in range(2):
                        relay_weights(k, h)

        @pl.when(jnp.logical_and(relay, u >= lag))
        def _():
            relay_unit(u - lag)

        @pl.when(layer == 0)
        def _():
            pltpu.make_async_copy(x_hbm.at[m, tok], xbuf.at[u], x0_sem.at[u]).wait()

        @pl.when(layer > 0)
        def _():
            wwait(xbuf.at[u], x_recv.at[u])

        @pl.when(jnp.logical_and(stores, u >= hold - 1))
        def _():
            store_input(u - hold + 1)

        @pl.when(jnp.logical_and(stores_later, u >= hold))
        def _():
            store_unit(u - hold)

        xin = xbuf[u].astype(jnp.float32)
        put_blocks(abuf, 0, layer_norm(xin, packs[0, 0:1, :], packs[0, 1:2, :]))
        for nb in range(1, seq // KBLK + 1):
            @pl.when(u // 2 + 1 == nb)
            def _():
                attention(nb, cmask[u % 2], tok, u)

        for n in range(model // KBLK):
            cols = slice(n * KBLK, (n + 1) * KBLK)
            attn = jnp.dot(blocks(ctx, 0, pairs), blocks(wout, 2 * n, 2), preferred_element_type=jnp.float32)
            hbuf[:, cols] = (xbuf[u, :, cols].astype(jnp.float32) + attn + packs[0, 2:3, cols]).astype(jnp.bfloat16)
        put_blocks(abuf, 0, layer_norm(hbuf[...].astype(jnp.float32), packs[0, 3:4, :], packs[0, 4:5, :]))
        for q in range(tp_n):
            for n in range(hid_q // KBLK):
                up = jnp.dot(blocks(abuf, 0, pairs), blocks(wup.at[q], 2 * n, 2), preferred_element_type=jnp.float32)
                up = up + packs[q, 6:7, n * KBLK:(n + 1) * KBLK]
                put_blocks(ubuf, q * (hid_q // LANE) + 2 * n, gelu(up).astype(jnp.bfloat16))
        half_model = model // 2
        for n in range(2):
            cols = slice(n * half_model, (n + 1) * half_model)
            down = jnp.dot(blocks(ubuf, 0, ubuf.shape[0]), blocks(wdn, n * (half_model // LANE), half_model // LANE), preferred_element_type=jnp.float32)
            ybuf[u, :, cols] = (hbuf[:, cols].astype(jnp.float32) + down + packs[0, 5:6, cols]).astype(jnp.bfloat16)

            @pl.when(more)
            def _():
                rcopy(ybuf.at[u, :, cols], xbuf.at[u, :, cols], s_send.at[u], x_recv.at[u], tp=r_next, pp=p_next).start()

            @pl.when(jnp.logical_not(more))
            def _():
                store_half(u, n)

        return carry

    lax.fori_loop(0, units, unit_step, 0)

    @pl.when(stores_later)
    def _():
        def last(v, carry):
            store_unit(v)
            return carry

        lax.fori_loop(units - hold, units, last, 0)

    @pl.when(stores)
    def _():
        def last_input(v, carry):
            store_input(v)
            return carry

        lax.fori_loop(units - hold + 1, units, last_input, 0)

    @pl.when(relay)
    def _():
        def rest(v, carry):
            relay_unit(v)
            return carry

        lax.fori_loop(units - lag, units, rest, 0)

    @pl.when(moved)
    def _():
        for k, h in pieces:
            sent(sw(k, h), sw_send.at[k, h])

    @pl.when(home)
    def _():
        sent(sw_pack, pk_send.at[0])
        for k, h in mats:
            sent(rl(k, h), rl_send.at[h, k])
        for d in range(4):
            for k, h in pieces:
                sent(sw(k, h), fwd_send.at[d, k, h])

    @pl.when(late_source)
    def _():
        handed_out()

    def drain(u, carry):
        @pl.when(more)
        def _():
            sent(ybuf.at[u], s_send.at[u])

        @pl.when(stores)
        def _():
            sent(ybuf.at[u], da_send.at[u])

            @pl.when(jnp.logical_not(home))
            def _():
                sent(ybuf.at[u], od_send.at[u])

        @pl.when(relay)
        def _():
            sent(ybuf.at[u], rr_send.at[0, u])
            sent(ybuf.at[u], rr_send.at[1, u])

        @pl.when(odd == 1)
        def _():
            sent(ybuf.at[u], db_send.at[u])
            sent(ybuf.at[u], fb_send.at[u])

            @pl.when(x % 2 == 0)
            def _():
                sent(ybuf.at[u], fc_send.at[u])

            @pl.when(c == 1)
            def _():
                sent(ybuf.at[u], fa_send.at[u])

        return carry

    lax.fori_loop(0, units, drain, 0)

    @pl.when(relay)
    def _():
        wwait(out.at[pl.ds(0, out.shape[0] // 2)], o_recv)

    @pl.when(jnp.logical_not(relay))
    def _():
        wwait(out, o_recv)


def solution(mesh):
    tp_size = mesh.shape['tp']
    in_specs = (P('dp'), P('dp'), P('pp'), P('pp'), P('pp', None, None, 'tp'), P('pp', None, 'tp', None), P('pp', 'tp', None), P('pp'), P('pp'), P('pp'), P('pp', None, 'tp'), P('pp', 'tp'), P('pp', 'tp', None), P('pp'))

    def per_device(x_in, seq_lens, ln1_gain, ln1_shift, w_qkv, b_qkv, w_out, b_out, ln2_gain, ln2_shift, w_up, b_up, w_down, b_down):
        micro_n, batch_n, seq_n, model_n = x_in.shape
        heads_n = b_qkv.shape[2] * tp_size
        quarter = w_qkv.shape[3]
        hid_q = w_up.shape[2]
        bf16, f32 = jnp.bfloat16, jnp.float32
        wqkv_t = jnp.transpose(w_qkv[0], (1, 0, 2))
        vectors = (ln1_gain, ln1_shift, b_out, ln2_gain, ln2_shift, b_down, b_up, b_qkv)
        pack_shape = (len(vectors), model_n)
        units = seq_n // UNIT
        pairs = model_n // LANE
        dma = pltpu.SemaphoreType.DMA
        anywhere = pl.BlockSpec(memory_space=pl.ANY)
        tokens = batch_n * seq_n
        out = pl.pallas_call(
            functools.partial(kernel, heads_n),
            out_shape=jax.ShapeDtypeStruct((micro_n, tokens, model_n), bf16),
            in_specs=[anywhere, pl.BlockSpec(memory_space=pltpu.SMEM)] + [anywhere] * 4 + [pl.BlockSpec(memory_space=pltpu.VMEM)] * len(vectors),
            out_specs=anywhere,
            scratch_shapes=[
                pltpu.VMEM((tp_size, 3 * quarter // LANE, model_n, LANE), bf16),
                pltpu.VMEM((model_n // LANE, tp_size * quarter, LANE), bf16),
                pltpu.VMEM((tp_size, hid_q // LANE, model_n, LANE), bf16),
                pltpu.VMEM((model_n // LANE, tp_size * hid_q, LANE), bf16),
                pltpu.VMEM((tp_size,) + pack_shape, f32),
                pltpu.VMEM(pack_shape, f32),
                pltpu.VMEM((2, 3 * quarter // LANE, model_n // 2, LANE), bf16),
                pltpu.VMEM((2, model_n // LANE, quarter // 2, LANE), bf16),
                pltpu.VMEM((2, hid_q // LANE, model_n // 2, LANE), bf16),
                pltpu.VMEM((2, model_n // LANE, hid_q // 2, LANE), bf16),
                pltpu.VMEM((3 * quarter // LANE, model_n, LANE), bf16),
                pltpu.VMEM((model_n // LANE, quarter, LANE), bf16),
                pltpu.VMEM((hid_q // LANE, model_n, LANE), bf16),
                pltpu.VMEM((model_n // LANE, hid_q, LANE), bf16),
                pltpu.VMEM(pack_shape, f32),
                pltpu.VMEM((units, UNIT, model_n), bf16),
                pltpu.VMEM((units, UNIT, model_n), bf16),
                *[pltpu.VMEM((quarter // LANE, seq_n, LANE), bf16)] * tp_size,
                *[pltpu.VMEM((quarter // LANE, units, LANE, UNIT), bf16)] * tp_size,
                pltpu.VMEM((seq_n, LANE), bf16),
                pltpu.VMEM((pairs, 2, KBLK, LANE), bf16),
                pltpu.VMEM((2, KBLK, KBLK), f32),
                pltpu.VMEM((2, seq_n // KBLK, KBLK, KBLK), f32),
                pltpu.VMEM((model_n // LANE, UNIT, LANE), bf16),
                pltpu.VMEM((model_n // LANE, UNIT, LANE), bf16),
                pltpu.VMEM((UNIT, model_n), bf16),
                pltpu.VMEM((tp_size * hid_q // LANE, UNIT, LANE), bf16),
                dma((5, 2)), dma((5, 2)), dma((4, 5, 2)), dma((4, 5, 2)), dma((2, 4)), dma((2, 4)), dma((2, 5, 2)), dma((1,)), pltpu.SemaphoreType.REGULAR,
                *[dma((units,))] * 9,
                dma((2, units, 2)), dma((2, units)), dma,
            ],
            compiler_params=pltpu.CompilerParams(collective_id=0, has_side_effects=True, vmem_limit_bytes=63 * 1024 * 1024),
            cost_estimate=pl.CostEstimate(flops=30 * 10 ** 9, bytes_accessed=40 * 10 ** 6, transcendentals=10 ** 7),
        )(x_in.reshape(micro_n, tokens, model_n), seq_lens.reshape(micro_n * batch_n), wqkv_t, w_out[0], w_up[0], w_down[0], *vectors)
        return out.reshape((1,) + x_in.shape)

    return jax.shard_map(per_device, mesh=mesh, in_specs=in_specs, out_specs=P('pp', 'dp'), check_vma=False)
```

```python
import functools
import math

import jax
import jax.numpy as jnp
import numpy as np
from jax import lax
from jax.experimental import pallas as pl
from jax.experimental.pallas import tpu as pltpu
from jax.sharding import PartitionSpec as P

MESH = pl.DeviceIdType.MESH
UNIT = 128
LANE = 128
KBLK = 256
NEG = -1e30


def alibi_slopes(heads_n):
    closest = 2 ** int(math.floor(math.log2(heads_n)))
    base_rate = 2.0 ** (-8.0 / closest)
    slope_list = [base_rate ** (head_idx + 1) for head_idx in range(closest)]
    extra_rate = 2.0 ** (-4.0 / closest)
    slope_list = slope_list + [extra_rate ** (2 * head_idx + 1) for head_idx in range(min(closest, heads_n - closest))]
    return np.array(slope_list, dtype=np.float32)


def split_bf16(value):
    parts = []
    rest = np.float32(value)
    for _ in range(3):
        part = rest.astype(jnp.bfloat16).astype(np.float32)
        parts.append(float(part))
        rest = np.float32(rest - part)
    return parts


def layer_norm(x, gain, shift):
    mean = jnp.mean(x, axis=-1, keepdims=True)
    cent = x - mean
    var = jnp.mean(cent * cent, axis=-1, keepdims=True)
    return (cent * lax.rsqrt(var + 1e-5) * gain + shift).astype(jnp.bfloat16)


def gelu(x):
    inner = math.sqrt(2.0 / math.pi) * (x + 0.044715 * (x * x * x))
    return 0.5 * x * (1.0 + jnp.tanh(inner))


def kernel(heads_n, x_hbm, lens, wqkv_in, wout_in, wup_in, wdn_in,
           ln1_gain, ln1_shift, b_out, ln2_gain, ln2_shift, b_down, b_up, b_qkv, out,
           wqkv, wout, wup, wdn, packs, pack_in, rl_qkv, rl_out, rl_up, rl_dn, sw_qkv, sw_out, sw_up, sw_dn, sw_pack,
           xbuf, ybuf, kc0, kc1, kc2, kc3, vt0, vt1, vt2, vt3, kx, qaug, cmask, sbuf, abuf, ctx, hbuf, ubuf,
           sw_send, sw_recv, w_recv, fwd_send, rl_send, rl_recv, dir_send, pk_send, go,
           x0_sem, x_recv, s_send, od_send, da_send, db_send, fa_send, fb_send, fc_send,
           rr_recv, rr_send, o_recv):
    tp_n = 4
    units = xbuf.shape[0]
    model = xbuf.shape[2]
    seq = units * UNIT
    quarter = wqkv.shape[1] // 3 * LANE
    hid_q = wup.shape[1] * LANE
    pairs = model // LANE
    per_q = quarter // LANE

    r = lax.axis_index("tp")
    p = lax.axis_index("pp")
    x = p // 2
    c = p % 2
    odd = (r + (x + 1) // 2 + 1) % 2
    even_col = x + (1 - x % 2) * (2 - 2 * x)
    layer = odd * (2 * x + 1) + (1 - odd) * 2 * even_col
    home = odd == c
    moved = jnp.logical_and(c == 0, x % 2 == 0)
    level = x == 1
    ahead = jnp.logical_or(r % 2 == 0, level)
    rp, rm, ro = (r + 1) % tp_n, (r + 3) % tp_n, (r + 2) % tp_n
    partner = 2 * x + (1 - c)
    sig = 1 - 2 * c
    r_fwd = (r + sig + tp_n) % tp_n
    r_bwd = (r - sig + tp_n) % tp_n
    stage0, stage1 = 2 * x, 2 * x + 1
    x_n = 4

    def micro_of(row, core, lay):
        hops = (lay + 1) // 4
        return 2 * (((row + 8 - (1 - 2 * core) * hops) % tp_n) // 2) + core

    m = micro_of(r, c, layer)

    def rcopy(src, dst, ssem, rsem, **dev):
        return pltpu.make_async_remote_copy(src_ref=src, dst_ref=dst, send_sem=ssem, recv_sem=rsem,
                                            device_id=dev, device_id_type=MESH)

    barrier = pltpu.get_barrier_semaphore()
    for dr in range(tp_n):
        for dc in range(2):
            if dr or dc:
                pl.semaphore_signal(barrier, inc=1, device_id={"tp": (r + dr) % tp_n, "pp": 2 * x + (c + dc) % 2}, device_id_type=MESH)
    for dx in range(1, x_n):
        pl.semaphore_signal(barrier, inc=1, device_id={"pp": 2 * ((x + dx) % x_n) + c}, device_id_type=MESH)

    for i, vec in enumerate((ln1_gain, ln1_shift, b_out, ln2_gain, ln2_shift, b_down, b_up)):
        pack_in[i:i + 1, :] = vec[...].astype(jnp.float32)
    width = b_qkv.shape[3]
    for j in range(3):
        for head in range(quarter // width):
            at = j * quarter + head * width
            pack_in[7:8, at:at + width] = b_qkv[0, j, head:head + 1, :].astype(jnp.float32)
    pl.semaphore_wait(barrier, 10)

    def wsrc(k, h, n):
        if k == 0:
            return wqkv_in.at[n // per_q, pl.ds(h * (model // 2), model // 2), pl.ds(n % per_q * LANE, LANE)]
        ref = (None, wout_in, wup_in, wdn_in)[k]
        half = ref.shape[0] // 2
        return ref.at[pl.ds(h * half, half), pl.ds(n * LANE, LANE)]

    def wdst(k, q, h=0):
        if k == 4:
            return packs.at[q]
        if k == 0 or k == 2:
            return (wqkv, None, wup)[k].at[q, :, pl.ds(h * (model // 2), model // 2), :]
        ref, half = (wout, quarter // 2) if k == 1 else (wdn, hid_q // 2)
        return ref.at[:, pl.ds(pl.multiple_of((2 * q + h) * half, half), half), :]

    def rl(k, h):
        return (rl_qkv, rl_out, rl_up, rl_dn)[k].at[h]

    def sw(k, h):
        if k == 4:
            return sw_pack
        ref = (sw_qkv, sw_out, sw_up, sw_dn)[k]
        half = ref.shape[1] // 2
        return ref.at[:, pl.ds(h * half, half), :]

    def fetch(k, h, dst, move):
        if k == 4:
            todo = [(pack_in, dst)]
        else:
            todo = [(wsrc(k, h, n), dst.at[n]) for n in range(dst.shape[0])]
        for src, to in todo:
            if move:
                rcopy(src, to, sw_send.at[k, h], sw_recv.at[k, h], pp=2 * (2 - x)).start()
            else:
                pltpu.make_async_copy(src, to, sw_recv.at[k, h]).start()

    def wwait(view, sem):
        rcopy(view, view, sem, sem, pp=partner).wait_recv()

    pieces = [(4, 0), (1, 0), (1, 1), (0, 0), (0, 1), (2, 0), (2, 1), (3, 0), (3, 1)]
    mats = pieces[1:]

    @pl.when(jnp.logical_and(moved, odd == 1))
    def _():
        for k, h in pieces:
            fetch(k, h, wdst(k, r, h), True)

    @pl.when(jnp.logical_and(moved, odd == 0))
    def _():
        for k, h in pieces:
            fetch(k, h, sw(k, h), True)

    @pl.when(jnp.logical_and(jnp.logical_not(moved), home))
    def _():
        for k, h in pieces:
            fetch(k, h, wdst(k, r, h), False)

    @pl.when(jnp.logical_not(jnp.logical_or(moved, home)))
    def _():
        for k, h in pieces:
            fetch(k, h, sw(k, h), False)

    @pl.when(layer == 0)
    def _():
        for u in range(units):
            pltpu.make_async_copy(x_hbm.at[m, pl.ds(u * UNIT, UNIT)], xbuf.at[u], x0_sem.at[u]).start()

    kc, vt = (kc0, kc1, kc2, kc3), (vt0, vt1, vt2, vt3)
    for ref in kc + vt:
        ref[...] = jnp.zeros_like(ref)
    length = lens[m]
    key = lax.broadcasted_iota(jnp.int32, (seq, LANE), 0)
    lane = lax.broadcasted_iota(jnp.int32, (seq, LANE), 1)
    high = (key // KBLK) * KBLK
    part = jnp.where(lane % 2 == 0, high, key - high).astype(jnp.float32)
    dead = jnp.where(key >= length, NEG, 0.0)
    kx[...] = jnp.where(lane < 6, part, jnp.where(lane == 6, dead, 0.0)).astype(jnp.bfloat16)
    slopes = alibi_slopes(heads_n)
    row = lax.broadcasted_iota(jnp.int32, (LANE, KBLK), 0)
    second = lax.broadcasted_iota(jnp.int32, (LANE, KBLK), 1) >= LANE
    for pair in range(pairs):
        (h0, m0, l0), (h1, m1, l1) = split_bf16(slopes[2 * pair]), split_bf16(slopes[2 * pair + 1])
        hi, mid, low = jnp.where(second, h1, h0), jnp.where(second, m1, m0), jnp.where(second, l1, l0)
        val = jnp.where(row < 2, hi, jnp.where(row < 4, mid, jnp.where(row < 6, low, jnp.where(row == 6, 1.0, 0.0))))
        for side in range(2):
            qaug[pair, side, LANE:, :] = val[:, side * LANE:(side + 1) * LANE].astype(jnp.bfloat16)
    kpos = lax.broadcasted_iota(jnp.int32, (KBLK, KBLK), 0)
    qpos = lax.broadcasted_iota(jnp.int32, (KBLK, KBLK), 1) % LANE
    cmask[0] = jnp.where(kpos <= qpos, 0.0, NEG)
    cmask[1] = jnp.where(kpos <= qpos + LANE, 0.0, NEG)

    def to_relay(k, h):
        rcopy(wdst(k, r, h), rl(k, h), rl_send.at[h, k], rl_recv.at[h, k], tp=(rp, rm)[h]).start()

    def to_partner(k, q, d, h):
        rcopy(wdst(k, q, h), wdst(k, q, h), fwd_send.at[d, k, h], w_recv.at[d, k, h], pp=partner).start()

    def hand_out(behind=()):
        for i, (k, h) in enumerate(pieces):
            wwait(sw(k, h), sw_recv.at[k, h])
            rcopy(sw(k, h), wdst(k, r, h), dir_send.at[0, k, h], w_recv.at[3, k, h], tp=rp).start()
            rcopy(sw(k, h), wdst(k, r, h), dir_send.at[1, k, h], w_recv.at[1, k, h], tp=rm).start()
            if 3 <= i < len(behind) + 3:
                relay_weights(*behind[i - 3])

    def relay_weights(k, h):
        wwait(rl(k, h), rl_recv.at[h, k])
        rcopy(rl(k, h), wdst(k, (rm, rp)[h], h), rl_send.at[h, k], w_recv.at[2, k, h], tp=(rp, rm)[h]).start()

    def from_partner():
        for d, q in ((0, r), (1, rp), (3, rm), (2, ro)):
            for k, h in pieces:
                wwait(wdst(k, q, h), w_recv.at[d, k, h])

    def sent(view, sem):
        rcopy(view, view, sem, sem, pp=partner).wait_send()

    def handed_out():
        for k, h in pieces:
            for d in range(2):
                sent(sw(k, h), dir_send.at[d, k, h])
        for k, h in mats:
            sent(rl(k, h), rl_send.at[h, k])

    @pl.when(home)
    def _():
        for k, h in pieces:
            wwait(wdst(k, r, h), sw_recv.at[k, h])
            if k == 4:
                rcopy(wdst(k, r), wdst(k, r), pk_send.at[0], w_recv.at[2, k, h], tp=ro).start()
            else:
                @pl.when(ahead)
                def _():
                    to_relay(k, h)
            to_partner(k, r, 0, h)

        @pl.when(jnp.logical_not(ahead))
        def _():
            pl.semaphore_wait(go, 1)
            for k, h in mats:
                to_relay(k, h)

        for i, (k, h) in enumerate(pieces + mats[:2]):
            if i < len(pieces):
                for d, q in ((1, rp), (3, rm)):
                    wwait(wdst(k, q, h), w_recv.at[d, k, h])
                    to_partner(k, q, d, h)
            if i >= 2:
                k, h = pieces[i - 2]
                wwait(wdst(k, ro, h), w_recv.at[2, k, h])
                to_partner(k, ro, 2, h)

    late_source = jnp.logical_not(jnp.logical_or(home, jnp.logical_or(r % 2 == 1, level)))

    @pl.when(jnp.logical_not(jnp.logical_or(home, late_source)))
    def _():
        hand_out(mats)
        for k, h in mats[len(pieces) - 3:]:
            relay_weights(k, h)
        handed_out()

        @pl.when(jnp.logical_not(level))
        def _():
            pl.semaphore_signal(go, inc=1, device_id={"pp": partner}, device_id_type=MESH)

        from_partner()

    @pl.when(late_source)
    def _():
        hand_out()
        from_partner()

    def half_cols(half):
        return slice(half * (model // 2), (half + 1) * (model // 2))

    def out_at(mm, u, half=None):
        rows = pl.ds(pl.multiple_of(u * UNIT, UNIT), UNIT)
        return out.at[mm, rows] if half is None else out.at[mm, rows, half_cols(half)]

    m_a = micro_of(rm, 0, stage1)
    m_b = micro_of(rp, 1, stage1)
    relay = jnp.logical_and(odd == 0, jnp.logical_or(c == 1, x % 2 == 0))
    lag = min(5, units) * (x % 2) + (1 - x % 2) * (min(5, units) + (units - min(5, units)) * (x // 2))
    hold = min(5, units) * (1 - (x + 2) // 3) + (x + 2) // 3

    def relay_unit(v):
        for half in range(2):
            for slot, (mm, to) in enumerate(((m_a, rp), (m_b, rm))):
                part = out_at(mm, v, half)
                wwait(part, rr_recv.at[slot, v, half])
                rcopy(part, part, rr_send.at[slot, v], o_recv, tp=to).start()

    def wide(parts):
        return jnp.concatenate(parts, axis=1)

    def blocks(ref, first, count):
        return wide([ref[first + i] for i in range(count)])

    def put_blocks(ref, first, val):
        for i in range(val.shape[1] // LANE):
            ref[first + i] = val[:, i * LANE:(i + 1) * LANE]

    def attention(nb, diag, tok, u):
        head_row = lax.broadcasted_iota(jnp.int32, (LANE, LANE), 0) < 64

        def project(q):
            for j in range(3):
                weights = wide([wqkv[q, j * per_q + i] for i in range(per_q)])
                o = jnp.dot(blocks(abuf, 0, pairs), weights, preferred_element_type=jnp.float32)
                o = (o + packs[q, 7:8, j * quarter:(j + 1) * quarter]).astype(jnp.bfloat16)
                for i in range(per_q):
                    part = o[:, i * LANE:(i + 1) * LANE]
                    if j == 0:
                        q_t = (part.astype(jnp.float32) * 0.125).T
                        qaug[q * per_q + i, 0, :LANE, :] = jnp.where(head_row, q_t, 0.0).astype(jnp.bfloat16)
                        qaug[q * per_q + i, 1, :LANE, :] = jnp.where(head_row, 0.0, q_t).astype(jnp.bfloat16)
                    elif j == 1:
                        kc[q][i, tok, :] = part
                    else:
                        vt[q][i, u] = part.astype(jnp.float32).T.astype(jnp.bfloat16)

        def scores(pair):
            kq = kc[pair // per_q]
            q_rhs = blocks(qaug.at[pair], 0, 2)
            top = None
            for b in range(nb):
                keys = wide([kq[pair % per_q, b * KBLK:(b + 1) * KBLK, :], kx[b * KBLK:(b + 1) * KBLK, :]])
                s = jnp.dot(keys, q_rhs, preferred_element_type=jnp.float32)
                if b == nb - 1:
                    s = s + diag
                sbuf[pair % 2, b] = s
                peak = jnp.max(s, axis=0, keepdims=True)
                top = peak if top is None else jnp.maximum(top, peak)
            return top

        def weigh(pair, top):
            vq = vt[pair // per_q].at[pair % per_q]
            total = None
            acc = None
            for b in range(nb):
                e = jnp.exp(sbuf[pair % 2, b] - top)
                part_sum = jnp.sum(e, axis=0, keepdims=True)
                total = part_sum if total is None else total + part_sum
                pv = jnp.dot(blocks(vq, b * KBLK // UNIT, KBLK // UNIT), e.astype(jnp.bfloat16), preferred_element_type=jnp.float32)
                acc = pv if acc is None else acc + pv
            acc = acc * (1.0 / total)
            both = jnp.concatenate([acc[:64, :LANE], acc[64:, LANE:]], axis=0)
            ctx[pair] = both.T.astype(jnp.bfloat16)

        project(0)
        top = None
        for pair in range(pairs + 1):
            if pair % per_q == 0 and pair // per_q + 1 < tp_n:
                project(pair // per_q + 1)
            later = scores(pair) if pair < pairs else None
            if pair > 0:
                weigh(pair - 1, top)
            top = later

    more = layer < 2 * x_n - 1
    nxt = (layer + 1) % (2 * x_n)
    half_n = nxt // 2
    x_next = half_n + (1 - nxt % 2) * (1 - half_n % 2) * (2 - 2 * half_n)
    p_next = 2 * x_next + c
    r_next = (r + (1 - odd) * (x % 2) * sig + tp_n) % tp_n

    def store_input(v):
        @pl.when(odd == 1)
        def _():
            @pl.when(c == 0)
            def _():
                pltpu.make_async_copy(xbuf.at[v], out_at(m, v), o_recv).start()

            @pl.when(c == 1)
            def _():
                rcopy(xbuf.at[v], out_at(m, v), fa_send.at[v], o_recv, pp=partner).start()

            @pl.when(x % 2 == 1)
            def _():
                rcopy(xbuf.at[v], out_at(m, v), fb_send.at[v], o_recv, tp=r_fwd, pp=stage0).start()

            @pl.when(x % 2 == 0)
            def _():
                for half in range(2):
                    rcopy(xbuf.at[v, :, half_cols(half)], out_at(m, v, half), fb_send.at[v], rr_recv.at[c, v, half], tp=r_fwd, pp=stage0).start()
                rcopy(xbuf.at[v], out_at(m, v), fc_send.at[v], o_recv, tp=r_bwd, pp=stage0).start()

    def store_half(v, half):
        src, dst = ybuf.at[v, :, half_cols(half)], out_at(m, v, half)

        @pl.when(odd == 1)
        def _():
            rcopy(src, dst, db_send.at[v], rr_recv.at[c, v, half], tp=r_fwd, pp=stage1).start()

        rcopy(src, dst, da_send.at[v], o_recv, tp=r_bwd, pp=2 * x + odd).start()

        @pl.when(home)
        def _():
            pltpu.make_async_copy(src, dst, o_recv).start()

        @pl.when(jnp.logical_not(home))
        def _():
            rcopy(src, dst, od_send.at[v], o_recv, pp=partner).start()

    def store_unit(v):
        store_half(v, 0)
        store_half(v, 1)

    stores = jnp.logical_or(odd == 1, x % 2 == 1)
    stores_later = jnp.logical_and(stores, more)

    def unit_step(u, carry):
        tok = pl.ds(pl.multiple_of(u * UNIT, UNIT), UNIT)

        for group, (step0, step1) in (((0, 1), (2, 0)), ((2,), (3, 1)), ((3,), (5, 2))):
            now = jnp.logical_or(jnp.logical_and(layer == 0, u == min(step0, units - 1)),
                                 jnp.logical_or(jnp.logical_and(layer == 1, u == min(step1, units - 1)), jnp.logical_and(layer > 1, u == 0)))

            @pl.when(jnp.logical_and(late_source, now))
            def _():
                for k in group:
                    for h in range(2):
                        relay_weights(k, h)

        @pl.when(jnp.logical_and(relay, u >= lag))
        def _():
            relay_unit(u - lag)

        @pl.when(layer == 0)
        def _():
            pltpu.make_async_copy(x_hbm.at[m, tok], xbuf.at[u], x0_sem.at[u]).wait()

        @pl.when(layer > 0)
        def _():
            wwait(xbuf.at[u], x_recv.at[u])

        @pl.when(jnp.logical_and(stores, u >= hold - 1))
        def _():
            store_input(u - hold + 1)

        @pl.when(jnp.logical_and(stores_later, u >= hold))
        def _():
            store_unit(u - hold)

        xin = xbuf[u].astype(jnp.float32)
        put_blocks(abuf, 0, layer_norm(xin, packs[0, 0:1, :], packs[0, 1:2, :]))
        for nb in range(1, seq // KBLK + 1):
            @pl.when(u // 2 + 1 == nb)
            def _():
                attention(nb, cmask[u % 2], tok, u)

        for n in range(model // KBLK):
            cols = slice(n * KBLK, (n + 1) * KBLK)
            attn = jnp.dot(blocks(ctx, 0, pairs), blocks(wout, 2 * n, 2), preferred_element_type=jnp.float32)
            hbuf[:, cols] = (xbuf[u, :, cols].astype(jnp.float32) + attn + packs[0, 2:3, cols]).astype(jnp.bfloat16)
        put_blocks(abuf, 0, layer_norm(hbuf[...].astype(jnp.float32), packs[0, 3:4, :], packs[0, 4:5, :]))
        for q in range(tp_n):
            for n in range(hid_q // KBLK):
                up = jnp.dot(blocks(abuf, 0, pairs), blocks(wup.at[q], 2 * n, 2), preferred_element_type=jnp.float32)
                up = up + packs[q, 6:7, n * KBLK:(n + 1) * KBLK]
                put_blocks(ubuf, q * (hid_q // LANE) + 2 * n, gelu(up).astype(jnp.bfloat16))
        half_model = model // 2
        for n in range(2):
            cols = slice(n * half_model, (n + 1) * half_model)
            down = jnp.dot(blocks(ubuf, 0, ubuf.shape[0]), blocks(wdn, n * (half_model // LANE), half_model // LANE), preferred_element_type=jnp.float32)
            ybuf[u, :, cols] = (hbuf[:, cols].astype(jnp.float32) + down + packs[0, 5:6, cols]).astype(jnp.bfloat16)

            @pl.when(more)
            def _():
                rcopy(ybuf.at[u, :, cols], xbuf.at[u, :, cols], s_send.at[u], x_recv.at[u], tp=r_next, pp=p_next).start()

            @pl.when(jnp.logical_not(more))
            def _():
                store_half(u, n)

        return carry

    lax.fori_loop(0, units, unit_step, 0)

    @pl.when(stores_later)
    def _():
        def last(v, carry):
            store_unit(v)
            return carry

        lax.fori_loop(units - hold, units, last, 0)

    @pl.when(stores)
    def _():
        def last_input(v, carry):
            store_input(v)
            return carry

        lax.fori_loop(units - hold + 1, units, last_input, 0)

    @pl.when(relay)
    def _():
        def rest(v, carry):
            relay_unit(v)
            return carry

        lax.fori_loop(units - lag, units, rest, 0)

    @pl.when(moved)
    def _():
        for k, h in pieces:
            sent(sw(k, h), sw_send.at[k, h])

    @pl.when(home)
    def _():
        sent(sw_pack, pk_send.at[0])
        for k, h in mats:
            sent(rl(k, h), rl_send.at[h, k])
        for d in range(4):
            for k, h in pieces:
                sent(sw(k, h), fwd_send.at[d, k, h])

    @pl.when(late_source)
    def _():
        handed_out()

    def drain(u, carry):
        @pl.when(more)
        def _():
            sent(ybuf.at[u], s_send.at[u])

        @pl.when(stores)
        def _():
            sent(ybuf.at[u], da_send.at[u])

            @pl.when(jnp.logical_not(home))
            def _():
                sent(ybuf.at[u], od_send.at[u])

        @pl.when(relay)
        def _():
            sent(ybuf.at[u], rr_send.at[0, u])
            sent(ybuf.at[u], rr_send.at[1, u])

        @pl.when(odd == 1)
        def _():
            sent(ybuf.at[u], db_send.at[u])
            sent(ybuf.at[u], fb_send.at[u])

            @pl.when(x % 2 == 0)
            def _():
                sent(ybuf.at[u], fc_send.at[u])

            @pl.when(c == 1)
            def _():
                sent(ybuf.at[u], fa_send.at[u])

        return carry

    lax.fori_loop(0, units, drain, 0)

    @pl.when(relay)
    def _():
        wwait(out.at[pl.ds(0, out.shape[0] // 2)], o_recv)

    @pl.when(jnp.logical_not(relay))
    def _():
        wwait(out, o_recv)


def solution(mesh):
    tp_size = mesh.shape['tp']
    in_specs = (P('dp'), P('dp'), P('pp'), P('pp'), P('pp', None, None, 'tp'), P('pp', None, 'tp', None), P('pp', 'tp', None), P('pp'), P('pp'), P('pp'), P('pp', None, 'tp'), P('pp', 'tp'), P('pp', 'tp', None), P('pp'))

    def per_device(x_in, seq_lens, ln1_gain, ln1_shift, w_qkv, b_qkv, w_out, b_out, ln2_gain, ln2_shift, w_up, b_up, w_down, b_down):
        micro_n, batch_n, seq_n, model_n = x_in.shape
        heads_n = b_qkv.shape[2] * tp_size
        quarter = w_qkv.shape[3]
        hid_q = w_up.shape[2]
        bf16, f32 = jnp.bfloat16, jnp.float32
        wqkv_t = jnp.transpose(w_qkv[0], (1, 0, 2))
        vectors = (ln1_gain, ln1_shift, b_out, ln2_gain, ln2_shift, b_down, b_up, b_qkv)
        pack_shape = (len(vectors), model_n)
        units = seq_n // UNIT
        pairs = model_n // LANE
        dma = pltpu.SemaphoreType.DMA
        anywhere = pl.BlockSpec(memory_space=pl.ANY)
        tokens = batch_n * seq_n
        out = pl.pallas_call(
            functools.partial(kernel, heads_n),
            out_shape=jax.ShapeDtypeStruct((micro_n, tokens, model_n), bf16),
            in_specs=[anywhere, pl.BlockSpec(memory_space=pltpu.SMEM)] + [anywhere] * 4 + [pl.BlockSpec(memory_space=pltpu.VMEM)] * len(vectors),
            out_specs=anywhere,
            scratch_shapes=[
                pltpu.VMEM((tp_size, 3 * quarter // LANE, model_n, LANE), bf16),
                pltpu.VMEM((model_n // LANE, tp_size * quarter, LANE), bf16),
                pltpu.VMEM((tp_size, hid_q // LANE, model_n, LANE), bf16),
                pltpu.VMEM((model_n // LANE, tp_size * hid_q, LANE), bf16),
                pltpu.VMEM((tp_size,) + pack_shape, f32),
                pltpu.VMEM(pack_shape, f32),
                pltpu.VMEM((2, 3 * quarter // LANE, model_n // 2, LANE), bf16),
                pltpu.VMEM((2, model_n // LANE, quarter // 2, LANE), bf16),
                pltpu.VMEM((2, hid_q // LANE, model_n // 2, LANE), bf16),
                pltpu.VMEM((2, model_n // LANE, hid_q // 2, LANE), bf16),
                pltpu.VMEM((3 * quarter // LANE, model_n, LANE), bf16),
                pltpu.VMEM((model_n // LANE, quarter, LANE), bf16),
                pltpu.VMEM((hid_q // LANE, model_n, LANE), bf16),
                pltpu.VMEM((model_n // LANE, hid_q, LANE), bf16),
                pltpu.VMEM(pack_shape, f32),
                pltpu.VMEM((units, UNIT, model_n), bf16),
                pltpu.VMEM((units, UNIT, model_n), bf16),
                *[pltpu.VMEM((quarter // LANE, seq_n, LANE), bf16)] * tp_size,
                *[pltpu.VMEM((quarter // LANE, units, LANE, UNIT), bf16)] * tp_size,
                pltpu.VMEM((seq_n, LANE), bf16),
                pltpu.VMEM((pairs, 2, KBLK, LANE), bf16),
                pltpu.VMEM((2, KBLK, KBLK), f32),
                pltpu.VMEM((2, seq_n // KBLK, KBLK, KBLK), f32),
                pltpu.VMEM((model_n // LANE, UNIT, LANE), bf16),
                pltpu.VMEM((model_n // LANE, UNIT, LANE), bf16),
                pltpu.VMEM((UNIT, model_n), bf16),
                pltpu.VMEM((tp_size * hid_q // LANE, UNIT, LANE), bf16),
                dma((5, 2)), dma((5, 2)), dma((4, 5, 2)), dma((4, 5, 2)), dma((2, 4)), dma((2, 4)), dma((2, 5, 2)), dma((1,)), pltpu.SemaphoreType.REGULAR,
                *[dma((units,))] * 9,
                dma((2, units, 2)), dma((2, units)), dma,
            ],
            compiler_params=pltpu.CompilerParams(collective_id=0, has_side_effects=True, vmem_limit_bytes=63 * 1024 * 1024),
            cost_estimate=pl.CostEstimate(flops=30 * 10 ** 9, bytes_accessed=40 * 10 ** 6, transcendentals=10 ** 7),
        )(x_in.reshape(micro_n, tokens, model_n), seq_lens.reshape(micro_n * batch_n), wqkv_t, w_out[0], w_up[0], w_down[0], *vectors)
        return out.reshape((1,) + x_in.shape)

    return jax.shard_map(per_device, mesh=mesh, in_specs=in_specs, out_specs=P('pp', 'dp'), check_vma=False)
```

```python
import functools
import math

import jax
import jax.numpy as jnp
import numpy as np
from jax import lax
from jax.experimental import pallas as pl
from jax.experimental.pallas import tpu as pltpu
from jax.sharding import PartitionSpec as P

MESH = pl.DeviceIdType.MESH
UNIT = 128
LANE = 128
KBLK = 256
NEG = -1e30


def alibi_slopes(heads_n):
    closest = 2 ** int(math.floor(math.log2(heads_n)))
    base_rate = 2.0 ** (-8.0 / closest)
    slope_list = [base_rate ** (head_idx + 1) for head_idx in range(closest)]
    extra_rate = 2.0 ** (-4.0 / closest)
    slope_list = slope_list + [extra_rate ** (2 * head_idx + 1) for head_idx in range(min(closest, heads_n - closest))]
    return np.array(slope_list, dtype=np.float32)


def split_bf16(value):
    parts = []
    rest = np.float32(value)
    for _ in range(3):
        part = rest.astype(jnp.bfloat16).astype(np.float32)
        parts.append(float(part))
        rest = np.float32(rest - part)
    return parts


def layer_norm(x, gain, shift):
    mean = jnp.mean(x, axis=-1, keepdims=True)
    cent = x - mean
    var = jnp.mean(cent * cent, axis=-1, keepdims=True)
    return (cent * lax.rsqrt(var + 1e-5) * gain + shift).astype(jnp.bfloat16)


def gelu(x):
    inner = math.sqrt(2.0 / math.pi) * (x + 0.044715 * (x * x * x))
    return 0.5 * x * (1.0 + jnp.tanh(inner))


def kernel(heads_n, x_hbm, lens, wqkv_in, wout_in, wup_in, wdn_in,
           ln1_gain, ln1_shift, b_out, ln2_gain, ln2_shift, b_down, b_up, b_qkv, out,
           wqkv, wout, wup, wdn, packs, pack_in, rl_qkv, rl_out, rl_up, rl_dn, sw_qkv, sw_out, sw_up, sw_dn, sw_pack,
           xbuf, ybuf, kc0, kc1, kc2, kc3, vt0, vt1, vt2, vt3, kx, qaug, cmask, sbuf, abuf, ctx, hbuf, ubuf,
           sw_send, sw_recv, w_recv, fwd_send, rl_send, rl_recv, dir_send, pk_send, go,
           x0_sem, x_recv, s_send, od_send, da_send, db_send, fa_send, fb_send, fc_send,
           rr_recv, rr_send, o_recv):
    tp_n = 4
    units = xbuf.shape[0]
    model = xbuf.shape[2]
    seq = units * UNIT
    quarter = wqkv.shape[1] // 3 * LANE
    hid_q = wup.shape[1] * LANE
    pairs = model // LANE
    per_q = quarter // LANE

    r = lax.axis_index("tp")
    p = lax.axis_index("pp")
    x = p // 2
    c = p % 2
    odd = (r + (x + 1) // 2 + 1) % 2
    even_col = x + (1 - x % 2) * (2 - 2 * x)
    layer = odd * (2 * x + 1) + (1 - odd) * 2 * even_col
    home = odd == c
    moved = jnp.logical_and(c == 0, x % 2 == 0)
    level = x == 1
    ahead = jnp.logical_or(r % 2 == 0, level)
    rp, rm, ro = (r + 1) % tp_n, (r + 3) % tp_n, (r + 2) % tp_n
    partner = 2 * x + (1 - c)
    sig = 1 - 2 * c
    r_fwd = (r + sig + tp_n) % tp_n
    r_bwd = (r - sig + tp_n) % tp_n
    stage0, stage1 = 2 * x, 2 * x + 1
    x_n = 4

    def micro_of(row, core, lay):
        hops = (lay + 1) // 4
        return 2 * (((row + 8 - (1 - 2 * core) * hops) % tp_n) // 2) + core

    m = micro_of(r, c, layer)

    def rcopy(src, dst, ssem, rsem, **dev):
        return pltpu.make_async_remote_copy(src_ref=src, dst_ref=dst, send_sem=ssem, recv_sem=rsem,
                                            device_id=dev, device_id_type=MESH)

    barrier = pltpu.get_barrier_semaphore()
    for dr in range(tp_n):
        for dc in range(2):
            if dr or dc:
                pl.semaphore_signal(barrier, inc=1, device_id={"tp": (r + dr) % tp_n, "pp": 2 * x + (c + dc) % 2}, device_id_type=MESH)
    for dx in range(1, x_n):
        pl.semaphore_signal(barrier, inc=1, device_id={"pp": 2 * ((x + dx) % x_n) + c}, device_id_type=MESH)

    for i, vec in enumerate((ln1_gain, ln1_shift, b_out, ln2_gain, ln2_shift, b_down, b_up)):
        pack_in[i:i + 1, :] = vec[...].astype(jnp.float32)
    width = b_qkv.shape[3]
    for j in range(3):
        for head in range(quarter // width):
            at = j * quarter + head * width
            pack_in[7:8, at:at + width] = b_qkv[0, j, head:head + 1, :].astype(jnp.float32)

    def wsrc(k, h, n):
        if k == 0:
            return wqkv_in.at[n // per_q, pl.ds(h * (model // 2), model // 2), pl.ds(n % per_q * LANE, LANE)]
        ref = (None, wout_in, wup_in, wdn_in)[k]
        half = ref.shape[0] // 2
        return ref.at[pl.ds(h * half, half), pl.ds(n * LANE, LANE)]

    def wdst(k, q, h=0):
        if k == 4:
            return packs.at[q]
        if k == 0 or k == 2:
            return (wqkv, None, wup)[k].at[q, :, pl.ds(h * (model // 2), model // 2), :]
        ref, half = (wout, quarter // 2) if k == 1 else (wdn, hid_q // 2)
        return ref.at[:, pl.ds(pl.multiple_of((2 * q + h) * half, half), half), :]

    def rl(k, h):
        return (rl_qkv, rl_out, rl_up, rl_dn)[k].at[h]

    def sw(k, h):
        if k == 4:
            return sw_pack
        ref = (sw_qkv, sw_out, sw_up, sw_dn)[k]
        half = ref.shape[1] // 2
        return ref.at[:, pl.ds(h * half, half), :]

    def fetch(k, h, dst, move):
        if k == 4:
            todo = [(pack_in, dst)]
        else:
            todo = [(wsrc(k, h, n), dst.at[n]) for n in range(dst.shape[0])]
        for src, to in todo:
            if move:
                rcopy(src, to, sw_send.at[k, h], sw_recv.at[k, h], pp=2 * (2 - x)).start()
            else:
                pltpu.make_async_copy(src, to, sw_recv.at[k, h]).start()

    def wwait(view, sem):
        rcopy(view, view, sem, sem, pp=partner).wait_recv()

    pieces = [(4, 0), (1, 0), (1, 1), (0, 0), (0, 1), (2, 0), (2, 1), (3, 0), (3, 1)]
    mats = pieces[1:]

    @pl.when(jnp.logical_and(jnp.logical_not(moved), home))
    def _():
        for k, h in pieces:
            fetch(k, h, wdst(k, r, h), False)

    @pl.when(jnp.logical_not(jnp.logical_or(moved, home)))
    def _():
        for k, h in pieces:
            fetch(k, h, sw(k, h), False)

    pl.semaphore_wait(barrier, 10)

    @pl.when(jnp.logical_and(moved, odd == 1))
    def _():
        for k, h in pieces:
            fetch(k, h, wdst(k, r, h), True)

    @pl.when(jnp.logical_and(moved, odd == 0))
    def _():
        for k, h in pieces:
            fetch(k, h, sw(k, h), True)

    @pl.when(layer == 0)
    def _():
        for u in range(units):
            pltpu.make_async_copy(x_hbm.at[m, pl.ds(u * UNIT, UNIT)], xbuf.at[u], x0_sem.at[u]).start()

    kc, vt = (kc0, kc1, kc2, kc3), (vt0, vt1, vt2, vt3)
    for ref in kc + vt:
        ref[...] = jnp.zeros_like(ref)
    length = lens[m]
    key = lax.broadcasted_iota(jnp.int32, (seq, LANE), 0)
    lane = lax.broadcasted_iota(jnp.int32, (seq, LANE), 1)
    high = (key // KBLK) * KBLK
    part = jnp.where(lane % 2 == 0, high, key - high).astype(jnp.float32)
    dead = jnp.where(key >= length, NEG, 0.0)
    kx[...] = jnp.where(lane < 6, part, jnp.where(lane == 6, dead, 0.0)).astype(jnp.bfloat16)
    slopes = alibi_slopes(heads_n)
    row = lax.broadcasted_iota(jnp.int32, (LANE, KBLK), 0)
    second = lax.broadcasted_iota(jnp.int32, (LANE, KBLK), 1) >= LANE
    for pair in range(pairs):
        (h0, m0, l0), (h1, m1, l1) = split_bf16(slopes[2 * pair]), split_bf16(slopes[2 * pair + 1])
        hi, mid, low = jnp.where(second, h1, h0), jnp.where(second, m1, m0), jnp.where(second, l1, l0)
        val = jnp.where(row < 2, hi, jnp.where(row < 4, mid, jnp.where(row < 6, low, jnp.where(row == 6, 1.0, 0.0))))
        for side in range(2):
            qaug[pair, side, LANE:, :] = val[:, side * LANE:(side + 1) * LANE].astype(jnp.bfloat16)
    kpos = lax.broadcasted_iota(jnp.int32, (KBLK, KBLK), 0)
    qpos = lax.broadcasted_iota(jnp.int32, (KBLK, KBLK), 1) % LANE
    cmask[0] = jnp.where(kpos <= qpos, 0.0, NEG)
    cmask[1] = jnp.where(kpos <= qpos + LANE, 0.0, NEG)

    def to_relay(k, h):
        rcopy(wdst(k, r, h), rl(k, h), rl_send.at[h, k], rl_recv.at[h, k], tp=(rp, rm)[h]).start()

    def to_partner(k, q, d, h):
        rcopy(wdst(k, q, h), wdst(k, q, h), fwd_send.at[d, k, h], w_recv.at[d, k, h], pp=partner).start()

    def hand_out(behind=()):
        for i, (k, h) in enumerate(pieces):
            wwait(sw(k, h), sw_recv.at[k, h])
            rcopy(sw(k, h), wdst(k, r, h), dir_send.at[0, k, h], w_recv.at[3, k, h], tp=rp).start()
            rcopy(sw(k, h), wdst(k, r, h), dir_send.at[1, k, h], w_recv.at[1, k, h], tp=rm).start()
            if 3 <= i < len(behind) + 3:
                relay_weights(*behind[i - 3])

    def relay_weights(k, h):
        wwait(rl(k, h), rl_recv.at[h, k])
        rcopy(rl(k, h), wdst(k, (rm, rp)[h], h), rl_send.at[h, k], w_recv.at[2, k, h], tp=(rp, rm)[h]).start()

    def from_partner():
        for d, q in ((0, r), (1, rp), (3, rm), (2, ro)):
            for k, h in pieces:
                wwait(wdst(k, q, h), w_recv.at[d, k, h])

    def sent(view, sem):
        rcopy(view, view, sem, sem, pp=partner).wait_send()

    def handed_out():
        for k, h in pieces:
            for d in range(2):
                sent(sw(k, h), dir_send.at[d, k, h])
        for k, h in mats:
            sent(rl(k, h), rl_send.at[h, k])

    @pl.when(home)
    def _():
        for k, h in pieces:
            wwait(wdst(k, r, h), sw_recv.at[k, h])
            if k == 4:
                rcopy(wdst(k, r), wdst(k, r), pk_send.at[0], w_recv.at[2, k, h], tp=ro).start()
            else:
                @pl.when(ahead)
                def _():
                    to_relay(k, h)
            to_partner(k, r, 0, h)

        @pl.when(jnp.logical_not(ahead))
        def _():
            pl.semaphore_wait(go, 1)
            for k, h in mats:
                to_relay(k, h)

        for i, (k, h) in enumerate(pieces + mats[:2]):
            if i < len(pieces):
                for d, q in ((1, rp), (3, rm)):
                    wwait(wdst(k, q, h), w_recv.at[d, k, h])
                    to_partner(k, q, d, h)
            if i >= 2:
                k, h = pieces[i - 2]
                wwait(wdst(k, ro, h), w_recv.at[2, k, h])
                to_partner(k, ro, 2, h)

    late_source = jnp.logical_not(jnp.logical_or(home, jnp.logical_or(r % 2 == 1, level)))

    @pl.when(jnp.logical_not(jnp.logical_or(home, late_source)))
    def _():
        hand_out(mats)
        for k, h in mats[len(pieces) - 3:]:
            relay_weights(k, h)
        handed_out()

        @pl.when(jnp.logical_not(level))
        def _():
            pl.semaphore_signal(go, inc=1, device_id={"pp": partner}, device_id_type=MESH)

        from_partner()

    @pl.when(late_source)
    def _():
        hand_out()
        from_partner()

    def half_cols(half):
        return slice(half * (model // 2), (half + 1) * (model // 2))

    def out_at(mm, u, half=None):
        rows = pl.ds(pl.multiple_of(u * UNIT, UNIT), UNIT)
        return out.at[mm, rows] if half is None else out.at[mm, rows, half_cols(half)]

    m_a = micro_of(rm, 0, stage1)
    m_b = micro_of(rp, 1, stage1)
    relay = jnp.logical_and(odd == 0, jnp.logical_or(c == 1, x % 2 == 0))
    lag = min(5, units) * (x % 2) + (1 - x % 2) * (min(5, units) + (units - min(5, units)) * (x // 2))
    hold = min(5, units) * (1 - (x + 2) // 3) + (x + 2) // 3

    def relay_unit(v):
        for half in range(2):
            for slot, (mm, to) in enumerate(((m_a, rp), (m_b, rm))):
                part = out_at(mm, v, half)
                wwait(part, rr_recv.at[slot, v, half])
                rcopy(part, part, rr_send.at[slot, v], o_recv, tp=to).start()

    def wide(parts):
        return jnp.concatenate(parts, axis=1)

    def blocks(ref, first, count):
        return wide([ref[first + i] for i in range(count)])

    def put_blocks(ref, first, val):
        for i in range(val.shape[1] // LANE):
            ref[first + i] = val[:, i * LANE:(i + 1) * LANE]

    def attention(nb, diag, tok, u):
        head_row = lax.broadcasted_iota(jnp.int32, (LANE, LANE), 0) < 64

        def project(q):
            for j in range(3):
                weights = wide([wqkv[q, j * per_q + i] for i in range(per_q)])
                o = jnp.dot(blocks(abuf, 0, pairs), weights, preferred_element_type=jnp.float32)
                o = (o + packs[q, 7:8, j * quarter:(j + 1) * quarter]).astype(jnp.bfloat16)
                for i in range(per_q):
                    part = o[:, i * LANE:(i + 1) * LANE]
                    if j == 0:
                        q_t = (part.astype(jnp.float32) * 0.125).T
                        qaug[q * per_q + i, 0, :LANE, :] = jnp.where(head_row, q_t, 0.0).astype(jnp.bfloat16)
                        qaug[q * per_q + i, 1, :LANE, :] = jnp.where(head_row, 0.0, q_t).astype(jnp.bfloat16)
                    elif j == 1:
                        kc[q][i, tok, :] = part
                    else:
                        vt[q][i, u] = part.astype(jnp.float32).T.astype(jnp.bfloat16)

        def scores(pair):
            kq = kc[pair // per_q]
            q_rhs = blocks(qaug.at[pair], 0, 2)
            top = None
            for b in range(nb):
                keys = wide([kq[pair % per_q, b * KBLK:(b + 1) * KBLK, :], kx[b * KBLK:(b + 1) * KBLK, :]])
                s = jnp.dot(keys, q_rhs, preferred_element_type=jnp.float32)
                if b == nb - 1:
                    s = s + diag
                sbuf[pair % 2, b] = s
                peak = jnp.max(s, axis=0, keepdims=True)
                top = peak if top is None else jnp.maximum(top, peak)
            return top

        def weigh(pair, top):
            vq = vt[pair // per_q].at[pair % per_q]
            total = None
            acc = None
            for b in range(nb):
                e = jnp.exp(sbuf[pair % 2, b] - top)
                part_sum = jnp.sum(e, axis=0, keepdims=True)
                total = part_sum if total is None else total + part_sum
                pv = jnp.dot(blocks(vq, b * KBLK // UNIT, KBLK // UNIT), e.astype(jnp.bfloat16), preferred_element_type=jnp.float32)
                acc = pv if acc is None else acc + pv
            acc = acc * (1.0 / total)
            both = jnp.concatenate([acc[:64, :LANE], acc[64:, LANE:]], axis=0)
            ctx[pair] = both.T.astype(jnp.bfloat16)

        project(0)
        top = None
        for pair in range(pairs + 1):
            if pair % per_q == 0 and pair // per_q + 1 < tp_n:
                project(pair // per_q + 1)
            later = scores(pair) if pair < pairs else None
            if pair > 0:
                weigh(pair - 1, top)
            top = later

    more = layer < 2 * x_n - 1
    nxt = (layer + 1) % (2 * x_n)
    half_n = nxt // 2
    x_next = half_n + (1 - nxt % 2) * (1 - half_n % 2) * (2 - 2 * half_n)
    p_next = 2 * x_next + c
    r_next = (r + (1 - odd) * (x % 2) * sig + tp_n) % tp_n

    def store_input(v):
        @pl.when(odd == 1)
        def _():
            @pl.when(c == 0)
            def _():
                pltpu.make_async_copy(xbuf.at[v], out_at(m, v), o_recv).start()

            @pl.when(c == 1)
            def _():
                rcopy(xbuf.at[v], out_at(m, v), fa_send.at[v], o_recv, pp=partner).start()

            @pl.when(x % 2 == 1)
            def _():
                rcopy(xbuf.at[v], out_at(m, v), fb_send.at[v], o_recv, tp=r_fwd, pp=stage0).start()

            @pl.when(x % 2 == 0)
            def _():
                for half in range(2):
                    rcopy(xbuf.at[v, :, half_cols(half)], out_at(m, v, half), fb_send.at[v], rr_recv.at[c, v, half], tp=r_fwd, pp=stage0).start()
                rcopy(xbuf.at[v], out_at(m, v), fc_send.at[v], o_recv, tp=r_bwd, pp=stage0).start()

    def store_half(v, half):
        src, dst = ybuf.at[v, :, half_cols(half)], out_at(m, v, half)

        @pl.when(odd == 1)
        def _():
            rcopy(src, dst, db_send.at[v], rr_recv.at[c, v, half], tp=r_fwd, pp=stage1).start()

        rcopy(src, dst, da_send.at[v], o_recv, tp=r_bwd, pp=2 * x + odd).start()

        @pl.when(home)
        def _():
            pltpu.make_async_copy(src, dst, o_recv).start()

        @pl.when(jnp.logical_not(home))
        def _():
            rcopy(src, dst, od_send.at[v], o_recv, pp=partner).start()

    def store_unit(v):
        store_half(v, 0)
        store_half(v, 1)

    stores = jnp.logical_or(odd == 1, x % 2 == 1)
    stores_later = jnp.logical_and(stores, more)

    def unit_step(u, carry):
        tok = pl.ds(pl.multiple_of(u * UNIT, UNIT), UNIT)

        for group, (step0, step1) in (((0, 1), (2, 0)), ((2,), (3, 1)), ((3,), (5, 2))):
            now = jnp.logical_or(jnp.logical_and(layer == 0, u == min(step0, units - 1)),
                                 jnp.logical_or(jnp.logical_and(layer == 1, u == min(step1, units - 1)), jnp.logical_and(layer > 1, u == 0)))

            @pl.when(jnp.logical_and(late_source, now))
            def _():
                for k in group:
                    for h in range(2):
                        relay_weights(k, h)

        @pl.when(jnp.logical_and(relay, u >= lag))
        def _():
            relay_unit(u - lag)

        @pl.when(layer == 0)
        def _():
            pltpu.make_async_copy(x_hbm.at[m, tok], xbuf.at[u], x0_sem.at[u]).wait()

        @pl.when(layer > 0)
        def _():
            wwait(xbuf.at[u], x_recv.at[u])

        @pl.when(jnp.logical_and(stores, u >= hold - 1))
        def _():
            store_input(u - hold + 1)

        @pl.when(jnp.logical_and(stores_later, u >= hold))
        def _():
            store_unit(u - hold)

        xin = xbuf[u].astype(jnp.float32)
        put_blocks(abuf, 0, layer_norm(xin, packs[0, 0:1, :], packs[0, 1:2, :]))
        for nb in range(1, seq // KBLK + 1):
            @pl.when(u // 2 + 1 == nb)
            def _():
                attention(nb, cmask[u % 2], tok, u)

        for n in range(model // KBLK):
            cols = slice(n * KBLK, (n + 1) * KBLK)
            attn = jnp.dot(blocks(ctx, 0, pairs), blocks(wout, 2 * n, 2), preferred_element_type=jnp.float32)
            hbuf[:, cols] = (xbuf[u, :, cols].astype(jnp.float32) + attn + packs[0, 2:3, cols]).astype(jnp.bfloat16)
        put_blocks(abuf, 0, layer_norm(hbuf[...].astype(jnp.float32), packs[0, 3:4, :], packs[0, 4:5, :]))
        for q in range(tp_n):
            for n in range(hid_q // KBLK):
                up = jnp.dot(blocks(abuf, 0, pairs), blocks(wup.at[q], 2 * n, 2), preferred_element_type=jnp.float32)
                up = up + packs[q, 6:7, n * KBLK:(n + 1) * KBLK]
                put_blocks(ubuf, q * (hid_q // LANE) + 2 * n, gelu(up).astype(jnp.bfloat16))
        half_model = model // 2
        for n in range(2):
            cols = slice(n * half_model, (n + 1) * half_model)
            down = jnp.dot(blocks(ubuf, 0, ubuf.shape[0]), blocks(wdn, n * (half_model // LANE), half_model // LANE), preferred_element_type=jnp.float32)
            ybuf[u, :, cols] = (hbuf[:, cols].astype(jnp.float32) + down + packs[0, 5:6, cols]).astype(jnp.bfloat16)

            @pl.when(more)
            def _():
                rcopy(ybuf.at[u, :, cols], xbuf.at[u, :, cols], s_send.at[u], x_recv.at[u], tp=r_next, pp=p_next).start()

            @pl.when(jnp.logical_not(more))
            def _():
                store_half(u, n)

        return carry

    lax.fori_loop(0, units, unit_step, 0)

    @pl.when(stores_later)
    def _():
        def last(v, carry):
            store_unit(v)
            return carry

        lax.fori_loop(units - hold, units, last, 0)

    @pl.when(stores)
    def _():
        def last_input(v, carry):
            store_input(v)
            return carry

        lax.fori_loop(units - hold + 1, units, last_input, 0)

    @pl.when(relay)
    def _():
        def rest(v, carry):
            relay_unit(v)
            return carry

        lax.fori_loop(units - lag, units, rest, 0)

    @pl.when(moved)
    def _():
        for k, h in pieces:
            sent(sw(k, h), sw_send.at[k, h])

    @pl.when(home)
    def _():
        sent(sw_pack, pk_send.at[0])
        for k, h in mats:
            sent(rl(k, h), rl_send.at[h, k])
        for d in range(4):
            for k, h in pieces:
                sent(sw(k, h), fwd_send.at[d, k, h])

    @pl.when(late_source)
    def _():
        handed_out()

    def drain(u, carry):
        @pl.when(more)
        def _():
            sent(ybuf.at[u], s_send.at[u])

        @pl.when(stores)
        def _():
            sent(ybuf.at[u], da_send.at[u])

            @pl.when(jnp.logical_not(home))
            def _():
                sent(ybuf.at[u], od_send.at[u])

        @pl.when(relay)
        def _():
            sent(ybuf.at[u], rr_send.at[0, u])
            sent(ybuf.at[u], rr_send.at[1, u])

        @pl.when(odd == 1)
        def _():
            sent(ybuf.at[u], db_send.at[u])
            sent(ybuf.at[u], fb_send.at[u])

            @pl.when(x % 2 == 0)
            def _():
                sent(ybuf.at[u], fc_send.at[u])

            @pl.when(c == 1)
            def _():
                sent(ybuf.at[u], fa_send.at[u])

        return carry

    lax.fori_loop(0, units, drain, 0)

    @pl.when(relay)
    def _():
        wwait(out.at[pl.ds(0, out.shape[0] // 2)], o_recv)

    @pl.when(jnp.logical_not(relay))
    def _():
        wwait(out, o_recv)


def solution(mesh):
    tp_size = mesh.shape['tp']
    in_specs = (P('dp'), P('dp'), P('pp'), P('pp'), P('pp', None, None, 'tp'), P('pp', None, 'tp', None), P('pp', 'tp', None), P('pp'), P('pp'), P('pp'), P('pp', None, 'tp'), P('pp', 'tp'), P('pp', 'tp', None), P('pp'))

    def per_device(x_in, seq_lens, ln1_gain, ln1_shift, w_qkv, b_qkv, w_out, b_out, ln2_gain, ln2_shift, w_up, b_up, w_down, b_down):
        micro_n, batch_n, seq_n, model_n = x_in.shape
        heads_n = b_qkv.shape[2] * tp_size
        quarter = w_qkv.shape[3]
        hid_q = w_up.shape[2]
        bf16, f32 = jnp.bfloat16, jnp.float32
        wqkv_t = jnp.transpose(w_qkv[0], (1, 0, 2))
        vectors = (ln1_gain, ln1_shift, b_out, ln2_gain, ln2_shift, b_down, b_up, b_qkv)
        pack_shape = (len(vectors), model_n)
        units = seq_n // UNIT
        pairs = model_n // LANE
        dma = pltpu.SemaphoreType.DMA
        anywhere = pl.BlockSpec(memory_space=pl.ANY)
        tokens = batch_n * seq_n
        out = pl.pallas_call(
            functools.partial(kernel, heads_n),
            out_shape=jax.ShapeDtypeStruct((micro_n, tokens, model_n), bf16),
            in_specs=[anywhere, pl.BlockSpec(memory_space=pltpu.SMEM)] + [anywhere] * 4 + [pl.BlockSpec(memory_space=pltpu.VMEM)] * len(vectors),
            out_specs=anywhere,
            scratch_shapes=[
                pltpu.VMEM((tp_size, 3 * quarter // LANE, model_n, LANE), bf16),
                pltpu.VMEM((model_n // LANE, tp_size * quarter, LANE), bf16),
                pltpu.VMEM((tp_size, hid_q // LANE, model_n, LANE), bf16),
                pltpu.VMEM((model_n // LANE, tp_size * hid_q, LANE), bf16),
                pltpu.VMEM((tp_size,) + pack_shape, f32),
                pltpu.VMEM(pack_shape, f32),
                pltpu.VMEM((2, 3 * quarter // LANE, model_n // 2, LANE), bf16),
                pltpu.VMEM((2, model_n // LANE, quarter // 2, LANE), bf16),
                pltpu.VMEM((2, hid_q // LANE, model_n // 2, LANE), bf16),
                pltpu.VMEM((2, model_n // LANE, hid_q // 2, LANE), bf16),
                pltpu.VMEM((3 * quarter // LANE, model_n, LANE), bf16),
                pltpu.VMEM((model_n // LANE, quarter, LANE), bf16),
                pltpu.VMEM((hid_q // LANE, model_n, LANE), bf16),
                pltpu.VMEM((model_n // LANE, hid_q, LANE), bf16),
                pltpu.VMEM(pack_shape, f32),
                pltpu.VMEM((units, UNIT, model_n), bf16),
                pltpu.VMEM((units, UNIT, model_n), bf16),
                *[pltpu.VMEM((quarter // LANE, seq_n, LANE), bf16)] * tp_size,
                *[pltpu.VMEM((quarter // LANE, units, LANE, UNIT), bf16)] * tp_size,
                pltpu.VMEM((seq_n, LANE), bf16),
                pltpu.VMEM((pairs, 2, KBLK, LANE), bf16),
                pltpu.VMEM((2, KBLK, KBLK), f32),
                pltpu.VMEM((2, seq_n // KBLK, KBLK, KBLK), f32),
                pltpu.VMEM((model_n // LANE, UNIT, LANE), bf16),
                pltpu.VMEM((model_n // LANE, UNIT, LANE), bf16),
                pltpu.VMEM((UNIT, model_n), bf16),
                pltpu.VMEM((tp_size * hid_q // LANE, UNIT, LANE), bf16),
                dma((5, 2)), dma((5, 2)), dma((4, 5, 2)), dma((4, 5, 2)), dma((2, 4)), dma((2, 4)), dma((2, 5, 2)), dma((1,)), pltpu.SemaphoreType.REGULAR,
                *[dma((units,))] * 9,
                dma((2, units, 2)), dma((2, units)), dma,
            ],
            compiler_params=pltpu.CompilerParams(collective_id=0, has_side_effects=True, vmem_limit_bytes=63 * 1024 * 1024),
            cost_estimate=pl.CostEstimate(flops=30 * 10 ** 9, bytes_accessed=40 * 10 ** 6, transcendentals=10 ** 7),
        )(x_in.reshape(micro_n, tokens, model_n), seq_lens.reshape(micro_n * batch_n), wqkv_t, w_out[0], w_up[0], w_down[0], *vectors)
        return out.reshape((1,) + x_in.shape)

    return jax.shard_map(per_device, mesh=mesh, in_specs=in_specs, out_specs=P('pp', 'dp'), check_vma=False)
```
